32 devices in a mesh: dp: 8 (over z, x), tensor: 4 (over y, core).
Axes of the slice: x: 2, y: 2, z: 4, core: 2. Of those that a mesh axis runs over, the one named last changes fastest.
Arguments:
- inputs: bfloat16 [8, 512, 1024], P(None, 'dp'), may hold values from -6 to 6
- norm1_gain: float32 [1024], replicated, may hold values from 0.5 to 1.5
- w_query: bfloat16 [1024, 1024], P(None, 'tensor'), may hold values from -0.1875 to 0.1875
- w_key: bfloat16 [1024, 1024], P(None, 'tensor'), may hold values from -0.1875 to 0.1875
- w_value: bfloat16 [1024, 2048], P(None, 'tensor'), may hold values from -0.1875 to 0.1875
- w_gate: bfloat16 [1024, 2048], P(None, 'tensor'), may hold values from -0.1875 to 0.1875
- w_beta: bfloat16 [1024, 8], P(None, 'tensor'), may hold values from -0.1875 to 0.1875
- w_decay: bfloat16 [1024, 8], P(None, 'tensor'), may hold values from -0.1875 to 0.1875
- decay_rate: float32 [8], P('tensor'), may hold values from 0.0009765625 to 0.05
- conv_query: float32 [4, 1024], P(None, 'tensor'), may hold values from -3 to 3
- conv_key: float32 [4, 1024], P(None, 'tensor'), may hold values from -3 to 3
- conv_value: float32 [4, 2048], P(None, 'tensor'), may hold values from -3 to 3
- head_gain: float32 [2048], P('tensor'), may hold values from 0.5 to 1.5
- w_out: bfloat16 [2048, 1024], P('tensor'), may hold values from -0.1875 to 0.1875
- norm2_gain: float32 [1024], replicated, may hold values from 0.5 to 1.5
- w_ffn_gate: bfloat16 [1024, 2816], P(None, 'tensor'), may hold values from -0.1875 to 0.1875
- w_ffn_up: bfloat16 [1024, 2816], P(None, 'tensor'), may hold values from -0.1875 to 0.1875
- w_ffn_down: bfloat16 [2816, 1024], P('tensor'), may hold values from -0.109375 to 0.109375
- cotangent: bfloat16 [8, 512, 1024], P(None, 'dp'), may hold values from -6 to 6
Outputs:
- output: bfloat16 [8, 512, 1024], P(None, 'dp')
- grad_inputs: float32 [8, 512, 1024], P(None, 'dp')
- grad_norm1_gain: float32 [1024], replicated
- grad_w_query: float32 [1024, 1024], P(None, 'tensor')
- grad_w_key: float32 [1024, 1024], P(None, 'tensor')
- grad_w_value: float32 [1024, 2048], P(None, 'tensor')
- grad_w_gate: float32 [1024, 2048], P(None, 'tensor')
- grad_w_beta: float32 [1024, 8], P(None, 'tensor')
- grad_w_decay: float32 [1024, 8], P(None, 'tensor')
- grad_decay_rate: float32 [8], P('tensor')
- grad_conv_query: float32 [4, 1024], P(None, 'tensor')
- grad_conv_key: float32 [4, 1024], P(None, 'tensor')
- grad_conv_value: float32 [4, 2048], P(None, 'tensor')
- grad_head_gain: float32 [2048], P('tensor')
- grad_w_out: float32 [2048, 1024], P('tensor')
- grad_norm2_gain: float32 [1024], replicated
- grad_w_ffn_gate: float32 [1024, 2816], P(None, 'tensor')
- grad_w_ffn_up: float32 [1024, 2816], P(None, 'tensor')
- grad_w_ffn_down: float32 [2816, 1024], P('tensor')
The draws below stay inside these ranges and needn't reach their ends.
All inputs are finite; a program needn't handle non-finite values.
Results may differ from the reference program's by a relative error of at most 0.01.
Values sent between devices are 32-bit elements; how exact they have to be, the bound alone decides.
A program may use at most 320 MiB of HBM per device.

```python
import math
from functools import partial
import jax
import jax.numpy as jnp
from jax import lax

D = 1024
HEADS = 8
KEY_DIM = 128
VALUE_DIM = 256
FF = 2816
CONV = 4
SPAN = 64
SEQS = 8
LENGTH = 512


def block_scale(key, dims, shards, low, top_value):
    loudness = 1.0
    for dim, parts in shards:
        heights = jax.random.uniform(jax.random.fold_in(jax.random.fold_in(key, 6), dim), (parts,), jnp.float32, low / len(shards), top_value / len(shards))
        loudness = loudness * jnp.repeat(jnp.exp(heights), dims[dim] // parts).reshape((-1,) + (1,) * (len(dims) - 1 - dim))
    return loudness


def normal_values(stream_key, extent, scale, most, cuts=(), kind=jnp.bfloat16):
    drawn = scale * jax.random.normal(stream_key, extent, jnp.float32)
    if cuts:
        drawn = drawn * block_scale(stream_key, extent, cuts, -0.22, 0.18)
    return jnp.clip(drawn, -most, most).astype(kind)


def setup_inputs(seed: int = 0) -> dict:
    key_list = jax.random.split(jax.random.key(seed), 20)
    inputs = normal_values(key_list[0], (SEQS, LENGTH, D), 1.0, 6.0, ((1, 8),))
    norm1_gain = jnp.clip(1.0 + 0.1 * jax.random.normal(key_list[1], (D,), jnp.float32), 0.5, 1.5)
    w_query = normal_values(key_list[2], (D, HEADS * KEY_DIM), D ** -0.5, 0.1875, ((1, 4),))
    w_key = normal_values(key_list[3], (D, HEADS * KEY_DIM), D ** -0.5, 0.1875, ((1, 4),))
    w_value = normal_values(key_list[4], (D, HEADS * VALUE_DIM), D ** -0.5, 0.1875, ((1, 4),))
    w_gate = normal_values(key_list[5], (D, HEADS * VALUE_DIM), D ** -0.5, 0.1875, ((1, 4),))
    w_beta = normal_values(key_list[6], (D, HEADS), D ** -0.5, 0.1875, ((1, 4),))
    w_decay = normal_values(key_list[7], (D, HEADS), D ** -0.5, 0.1875, ((1, 4),))
    decay_rate = jnp.clip(jnp.exp(math.log(0.05) - 3.9357395 * jax.random.uniform(key_list[8], (HEADS,), jnp.float32) ** block_scale(key_list[8], (HEADS,), ((0, 4),), -0.2, 0.2)), 0.0009765625, 0.05)
    conv_query = normal_values(key_list[9], (CONV, HEADS * KEY_DIM), 0.5, 3.0, ((1, 4),), jnp.float32)
    conv_key = normal_values(key_list[10], (CONV, HEADS * KEY_DIM), 0.5, 3.0, ((1, 4),), jnp.float32)
    conv_value = normal_values(key_list[11], (CONV, HEADS * VALUE_DIM), 0.5, 3.0, ((1, 4),), jnp.float32)
    head_gain = jnp.clip(1.0 + 0.1 * jax.random.normal(key_list[12], (HEADS * VALUE_DIM,), jnp.float32), 0.5, 1.5)
    w_out = normal_values(key_list[13], (HEADS * VALUE_DIM, D), (HEADS * VALUE_DIM // 2) ** -0.5, 0.1875, ((0, 4),))
    norm2_gain = jnp.clip(1.0 + 0.1 * jax.random.normal(key_list[14], (D,), jnp.float32), 0.5, 1.5)
    w_ffn_gate = normal_values(key_list[15], (D, FF), D ** -0.5, 0.1875, ((1, 4),))
    w_ffn_up = normal_values(key_list[16], (D, FF), D ** -0.5, 0.1875, ((1, 4),))
    w_ffn_down = normal_values(key_list[17], (FF, D), FF ** -0.5, 0.109375, ((0, 4),))
    cotangent = normal_values(key_list[18], (SEQS, LENGTH, D), 1.0, 6.0, ((1, 8),))
    return dict(inputs=inputs, norm1_gain=norm1_gain, w_query=w_query, w_key=w_key, w_value=w_value, w_gate=w_gate, w_beta=w_beta, w_decay=w_decay, decay_rate=decay_rate, conv_query=conv_query, conv_key=conv_key, conv_value=conv_value, head_gain=head_gain, w_out=w_out, norm2_gain=norm2_gain, w_ffn_gate=w_ffn_gate, w_ffn_up=w_ffn_up, w_ffn_down=w_ffn_down, cotangent=cotangent)


EPS = 1e-06

def exact(left, right):
    return jnp.matmul(left, right, precision=lax.Precision.HIGHEST)

def span_apply(state, inputs):
    query, key, values, beta, logdecay = inputs
    count = query.shape[0]
    cumul = jnp.cumsum(logdecay)
    row_ids = lax.broadcasted_iota(jnp.int32, (count, count), 0)
    col_ids = lax.broadcasted_iota(jnp.int32, (count, count), 1)
    within = col_ids <= row_ids
    strict = col_ids < row_ids
    spread = jnp.where(within, cumul[:, None] - cumul[None, :], 0.0)
    decays = jnp.where(within, jnp.exp(spread), 0.0)
    scaled = decays * beta[None, :]
    lower = jnp.where(strict, scaled * exact(key, key.T), 0.0)
    start_decay = jnp.exp(cumul)[:, None]
    right_side = values - start_decay * exact(key, state)
    system = jnp.eye(count, dtype=lower.dtype) + lower
    update = jax.scipy.linalg.solve_triangular(system, right_side, lower=True, unit_diagonal=True)
    output = start_decay * exact(query, state) + exact(scaled * exact(query, key.T), update)
    tail = jnp.exp(cumul[-1] - cumul) * beta
    new_state = jnp.exp(cumul[-1]) * state + exact((key * tail[:, None]).T, update)
    return (new_state, output)

def run_segment(query, key, values, beta, logdecay, state):
    length = query.shape[0]
    blocks = length // SPAN

    def split(array):
        return array.reshape((blocks, SPAN) + array.shape[1:])
    final, outputs = lax.scan(span_apply, state, (split(query), split(key), split(values), split(beta), split(logdecay)))
    return (outputs.reshape((length,) + outputs.shape[2:]), final)

def run_heads(query, key, values, beta, logdecay, state):
    return jax.vmap(jax.vmap(run_segment))(query, key, values, beta, logdecay, state)

def prepare(extended, beta_pre, decay_pre, conv_all, decay_rate, key_dim):
    batch, seg, heads = beta_pre.shape
    reach = conv_all.shape[0] - 1
    total = conv_all[0] * extended[:, 0:seg, :]
    for offset in range(1, reach + 1):
        total = total + conv_all[offset] * extended[:, offset:offset + seg, :]
    active = jax.nn.silu(total)
    qk_width = heads * key_dim
    query = active[..., :qk_width].reshape(batch, seg, heads, key_dim)
    key = active[..., qk_width:2 * qk_width].reshape(batch, seg, heads, key_dim)
    values = active[..., 2 * qk_width:].reshape(batch, seg, heads, -1)
    query = query * lax.rsqrt(lax.optimization_barrier(jnp.sum(query * query, -1, keepdims=True)) + EPS) * key_dim ** (-0.5)
    key = key * lax.rsqrt(lax.optimization_barrier(jnp.sum(key * key, -1, keepdims=True)) + EPS)
    beta = jax.nn.sigmoid(beta_pre)
    logdecay = -decay_rate * jax.nn.softplus(decay_pre)
    return (jnp.moveaxis(query, 2, 1), jnp.moveaxis(key, 2, 1), jnp.moveaxis(values, 2, 1), jnp.moveaxis(beta, 2, 1), jnp.moveaxis(logdecay, 2, 1))

def gate_norm(core, gate_pre, head_gain):
    normed = core * lax.rsqrt(lax.optimization_barrier(jnp.mean(core * core, -1, keepdims=True)) + EPS)
    return normed * head_gain * jax.nn.silu(gate_pre)

def rms_apply(resid, gain):
    return resid * lax.rsqrt(lax.optimization_barrier(jnp.mean(resid * resid, -1, keepdims=True)) + EPS) * gain

def swiglu(gate, upper):
    return jax.nn.silu(gate) * upper

def project(left, right):
    return jnp.dot(left.astype(jnp.float32), right.astype(jnp.float32), preferred_element_type=jnp.float32)

def sequence_pass(tokens, upstream, params):
    norm1_gain, w_query, w_key, w_value, w_gate, w_beta, w_decay, decay_rate, conv_query, conv_key, conv_value, head_gain, w_out, norm2_gain, w_ffn_gate, w_ffn_up, w_ffn_down = params
    length, width = tokens.shape
    heads = decay_rate.shape[0]
    key_dim = w_query.shape[1] // heads
    value_dim = w_value.shape[1] // heads
    qk_width = heads * key_dim
    reach = conv_query.shape[0] - 1
    bf = jnp.bfloat16
    resid = tokens.astype(jnp.float32)
    normed1, norm1_back = jax.vjp(rms_apply, resid, norm1_gain)
    hidden1 = normed1.astype(bf)
    query_pre = project(hidden1, w_query)
    key_pre = project(hidden1, w_key)
    value_pre = project(hidden1, w_value)
    gate_pre = project(hidden1, w_gate)
    beta_pre = project(hidden1, w_beta)
    decay_pre = project(hidden1, w_decay)
    mixed_pre = jnp.concatenate([query_pre, key_pre, value_pre], axis=1)[None]
    extended = jnp.pad(mixed_pre, ((0, 0), (reach, 0), (0, 0)))
    conv_all = jnp.concatenate([conv_query, conv_key, conv_value], axis=1)
    features, prep_back = jax.vjp(partial(prepare, key_dim=key_dim), extended, beta_pre[None], decay_pre[None], conv_all, decay_rate)
    start = jnp.zeros((1, heads, key_dim, value_dim), jnp.float32)

    def delta(query, key, values, beta, logdecay):
        return run_heads(query, key, values, beta, logdecay, start)[0]
    core_heads, delta_back = jax.vjp(delta, features[0], features[1], features[2], features[3], features[4])
    core = jnp.moveaxis(core_heads, 1, 2)
    gate4 = gate_pre.reshape(1, length, heads, value_dim)
    gated, gate_back = jax.vjp(gate_norm, core, gate4, head_gain.reshape(heads, value_dim))
    mixed = gated.reshape(length, heads * value_dim).astype(bf)
    resid1 = resid + project(mixed, w_out)
    normed2, norm2_back = jax.vjp(rms_apply, resid1, norm2_gain)
    hidden2 = normed2.astype(bf)
    ffn_gate = project(hidden2, w_ffn_gate)
    ffn_up = project(hidden2, w_ffn_up)
    inner_full, swiglu_back = jax.vjp(swiglu, ffn_gate, ffn_up)
    inner = inner_full.astype(bf)
    output = (resid1 + project(inner, w_ffn_down)).astype(bf)
    grad_down = project(inner.T, upstream)
    grad_inner = project(upstream, w_ffn_down.T)
    grad_fgate, grad_fup = swiglu_back(grad_inner)
    grad_fgate = grad_fgate.astype(bf)
    grad_fup = grad_fup.astype(bf)
    grad_ffn_gate_w = project(hidden2.T, grad_fgate)
    grad_ffn_up_w = project(hidden2.T, grad_fup)
    grad_hidden2 = project(grad_fgate, w_ffn_gate.T) + project(grad_fup, w_ffn_up.T)
    grad_from_norm2, grad_norm2_gain = norm2_back(grad_hidden2)
    grad_resid1 = upstream.astype(jnp.float32) + grad_from_norm2
    grad_resid1_low = grad_resid1.astype(bf)
    grad_out_w = project(mixed.T, grad_resid1_low)
    grad_mixed = project(grad_resid1_low, w_out.T).reshape(1, length, heads, value_dim)
    grad_core, grad_gate4, grad_head_gain = gate_back(grad_mixed)
    feature_grads = delta_back(jnp.moveaxis(grad_core, 2, 1))
    grad_ext, grad_beta_in, grad_decay_in, grad_conv, grad_rate = prep_back(feature_grads)
    grad_mixed_pre = grad_ext[0, reach:, :]
    grad_query_low = grad_mixed_pre[:, :qk_width].astype(bf)
    grad_key_low = grad_mixed_pre[:, qk_width:2 * qk_width].astype(bf)
    grad_value_low = grad_mixed_pre[:, 2 * qk_width:].astype(bf)
    grad_gate_low = grad_gate4.reshape(length, heads * value_dim).astype(bf)
    grad_beta_low = grad_beta_in[0].astype(bf)
    grad_decay_low = grad_decay_in[0].astype(bf)
    grad_hidden1 = project(grad_query_low, w_query.T) + project(grad_key_low, w_key.T) + project(grad_value_low, w_value.T) + project(grad_gate_low, w_gate.T) + project(grad_beta_low, w_beta.T) + project(grad_decay_low, w_decay.T)
    grad_from_norm1, grad_norm1_gain = norm1_back(grad_hidden1)
    grad_inputs = grad_resid1 + grad_from_norm1
    grads = (grad_norm1_gain, project(hidden1.T, grad_query_low), project(hidden1.T, grad_key_low), project(hidden1.T, grad_value_low), project(hidden1.T, grad_gate_low), project(hidden1.T, grad_beta_low), project(hidden1.T, grad_decay_low), grad_rate, grad_conv[:, :qk_width], grad_conv[:, qk_width:2 * qk_width], grad_conv[:, 2 * qk_width:], grad_head_gain.reshape(-1), grad_out_w, grad_norm2_gain, grad_ffn_gate_w, grad_ffn_up_w, grad_down)
    return (output, grad_inputs, grads)

def reference(inputs, norm1_gain, w_query, w_key, w_value, w_gate, w_beta, w_decay, decay_rate, conv_query, conv_key, conv_value, head_gain, w_out, norm2_gain, w_ffn_gate, w_ffn_up, w_ffn_down, cotangent):
    params = (norm1_gain, w_query, w_key, w_value, w_gate, w_beta, w_decay, decay_rate, conv_query, conv_key, conv_value, head_gain, w_out, norm2_gain, w_ffn_gate, w_ffn_up, w_ffn_down)
    zero_grads = tuple((jnp.zeros(param.shape, jnp.float32) for param in params))

    def step_sequence(totals, pair):
        output, grad_inputs, grads = sequence_pass(pair[0], pair[1], params)
        return (tuple((left + right for left, right in zip(totals, grads))), (output, grad_inputs))
    totals, results = lax.scan(step_sequence, zero_grads, (inputs, cotangent))
    g_norm1, g_query, g_key, g_value, g_gate, g_beta, g_decay, g_rate, g_convq, g_convk, g_convv, g_head, g_out, g_norm2, g_fgate, g_fup, g_fdown = totals
    return (results[0], results[1], g_norm1, g_query, g_key, g_value, g_gate, g_beta, g_decay, g_rate, g_convq, g_convk, g_convv, g_head, g_out, g_norm2, g_fgate, g_fup, g_fdown)
```

```python
import functools
from functools import partial

import jax
import jax.numpy as jnp
from jax import lax
from jax.experimental import pallas as pl
from jax.experimental.pallas import tpu as pltpu
from jax.sharding import PartitionSpec as P

SPAN = 64


EPS = 1e-06


def from_behind(shard, axis, by):
    count = lax.axis_size(axis)
    pairs = [(i, i + by) for i in range(count) if 0 <= i + by < count]
    return lax.ppermute(shard, axis, pairs)


def carried_in(part, axis, combine, identity, reverse):
    count = lax.axis_size(axis)
    place = lax.axis_index(axis)
    ahead = count - 1 - place if reverse else place
    gathered = jax.tree.map(lambda a: lax.all_gather(a, axis), part)
    state = jax.tree.map(lambda a, e: jnp.zeros_like(a) + jnp.asarray(e, a.dtype), part, identity)

    def one(turn, state):
        source = count - 1 - turn if reverse else turn
        return combine(
            state, jax.tree.map(lambda a: lax.dynamic_index_in_dim(a, source, 0, False), gathered)
        )

    return lax.fori_loop(0, ahead, one, state)


def exact(left, right):
    return jnp.matmul(left, right, precision=lax.Precision.HIGHEST)


def span_apply(state, inputs):
    query, key, values, beta, logdecay = inputs
    count = query.shape[0]
    cumul = jnp.cumsum(logdecay)
    row_ids = lax.broadcasted_iota(jnp.int32, (count, count), 0)
    col_ids = lax.broadcasted_iota(jnp.int32, (count, count), 1)
    within = col_ids <= row_ids
    strict = col_ids < row_ids
    spread = jnp.where(within, cumul[:, None] - cumul[None, :], 0.0)
    decays = jnp.where(within, jnp.exp(spread), 0.0)
    scaled = decays * beta[None, :]
    lower = jnp.where(strict, scaled * exact(key, key.T), 0.0)
    start_decay = jnp.exp(cumul)[:, None]
    right_side = values - start_decay * exact(key, state)
    system = jnp.eye(count, dtype=lower.dtype) + lower
    update = jax.scipy.linalg.solve_triangular(system, right_side, lower=True, unit_diagonal=True)
    output = start_decay * exact(query, state) + exact(scaled * exact(query, key.T), update)
    tail = jnp.exp(cumul[-1] - cumul) * beta
    new_state = jnp.exp(cumul[-1]) * state + exact((key * tail[:, None]).T, update)
    return (new_state, output)


def run_segment(query, key, values, beta, logdecay, state):
    length = query.shape[0]
    blocks = length // SPAN

    def split(array):
        return array.reshape((blocks, SPAN) + array.shape[1:])

    final, outputs = lax.scan(
        span_apply, state, (split(query), split(key), split(values), split(beta), split(logdecay))
    )
    return (outputs.reshape((length,) + outputs.shape[2:]), final)


def run_heads(query, key, values, beta, logdecay, state):
    return jax.vmap(jax.vmap(run_segment))(query, key, values, beta, logdecay, state)


def prepare(extended, beta_pre, decay_pre, conv_all, decay_rate, key_dim):
    batch, seg, heads = beta_pre.shape
    reach = conv_all.shape[0] - 1
    total = conv_all[0] * extended[:, 0:seg, :]
    for offset in range(1, reach + 1):
        total = total + conv_all[offset] * extended[:, offset : offset + seg, :]
    active = jax.nn.silu(total)
    qk_width = heads * key_dim
    query = active[..., :qk_width].reshape(batch, seg, heads, key_dim)
    key = active[..., qk_width : 2 * qk_width].reshape(batch, seg, heads, key_dim)
    values = active[..., 2 * qk_width :].reshape(batch, seg, heads, -1)
    query = query * lax.rsqrt(jnp.sum(query * query, -1, keepdims=True) + EPS) * key_dim ** (-0.5)
    key = key * lax.rsqrt(jnp.sum(key * key, -1, keepdims=True) + EPS)
    beta = jax.nn.sigmoid(beta_pre)
    logdecay = -decay_rate * jax.nn.softplus(decay_pre)
    return (
        jnp.moveaxis(query, 2, 1),
        jnp.moveaxis(key, 2, 1),
        jnp.moveaxis(values, 2, 1),
        jnp.moveaxis(beta, 2, 1),
        jnp.moveaxis(logdecay, 2, 1),
    )


def gate_norm(core, gate_pre, head_gain):
    normed = core * lax.rsqrt(jnp.mean(core * core, -1, keepdims=True) + EPS)
    return normed * head_gain * jax.nn.silu(gate_pre)


def rms_apply(resid, gain):
    return resid * lax.rsqrt(jnp.mean(resid * resid, -1, keepdims=True) + EPS) * gain


def swiglu(gate, upper):
    return jax.nn.silu(gate) * upper


def project(left, right):
    return jnp.dot(left, right, preferred_element_type=jnp.float32)


def contract_rows(left, right):
    return jnp.einsum("ra,rb->ab", left, right, preferred_element_type=jnp.float32)


def back_project(grad, weight):
    return jnp.einsum("rb,ab->ra", grad, weight, preferred_element_type=jnp.float32)


def compose(earlier, later):
    return (exact(later[0], earlier[0]), exact(later[0], earlier[1]) + later[1])


def shards(
    inputs,
    norm1_gain,
    w_query,
    w_key,
    w_value,
    w_gate,
    w_beta,
    w_decay,
    decay_rate,
    conv_query,
    conv_key,
    conv_value,
    head_gain,
    w_out,
    norm2_gain,
    w_ffn_gate,
    w_ffn_up,
    w_ffn_down,
    cotangent,
):
    batch, seg, width = inputs.shape
    count = batch * seg
    heads = decay_rate.shape[0]
    key_dim = w_query.shape[1] // heads
    value_dim = w_value.shape[1] // heads
    qk_width = heads * key_dim
    reach = conv_query.shape[0] - 1
    bf = jnp.bfloat16
    resid = inputs.reshape(count, width).astype(jnp.float32)
    normed1, norm1_back = jax.vjp(rms_apply, resid, norm1_gain)
    hidden1 = normed1.astype(bf)
    query_pre = project(hidden1, w_query)
    key_pre = project(hidden1, w_key)
    value_pre = project(hidden1, w_value)
    gate_pre = project(hidden1, w_gate)
    beta_pre = project(hidden1, w_beta)
    decay_pre = project(hidden1, w_decay)
    mixed_pre = jnp.concatenate([query_pre, key_pre, value_pre], axis=1).reshape(batch, seg, -1)
    rim = from_behind(mixed_pre[:, seg - reach :, :], "dp", 1)
    extended = jnp.concatenate([rim, mixed_pre], axis=1)
    conv_all = jnp.concatenate([conv_query, conv_key, conv_value], axis=1)
    features, prep_back = jax.vjp(
        partial(prepare, key_dim=key_dim),
        extended,
        beta_pre.reshape(batch, seg, heads),
        decay_pre.reshape(batch, seg, heads),
        conv_all,
        decay_rate,
    )
    query_h, key_h, value_h, beta_h, decay_h = features
    eye_block = jnp.broadcast_to(
        jnp.eye(key_dim, dtype=jnp.float32), (batch, heads, key_dim, key_dim)
    )
    zero_block = jnp.zeros((batch, heads, key_dim, value_dim), jnp.float32)
    values_aug = jnp.concatenate(
        [jnp.zeros(value_h.shape[:3] + (key_dim,), jnp.float32), value_h], axis=-1
    )
    state_aug = jnp.concatenate([eye_block, zero_block], axis=-1)
    outputs_aug, final_aug = run_heads(query_h, key_h, values_aug, beta_h, decay_h, state_aug)
    out_carry = outputs_aug[..., :key_dim]
    out_local = outputs_aug[..., key_dim:]
    transition = final_aug[..., :key_dim]
    offset_part = final_aug[..., key_dim:]
    prefix = carried_in((transition, offset_part), "dp", compose, (eye_block, zero_block), False)
    start_state = prefix[1]
    core = jnp.moveaxis(exact(out_carry, start_state) + out_local, 1, 2)
    gate4 = gate_pre.reshape(batch, seg, heads, value_dim)
    gated, gate_back = jax.vjp(gate_norm, core, gate4, head_gain.reshape(heads, value_dim))
    mixed = gated.reshape(count, heads * value_dim).astype(bf)
    attention = lax.psum(project(mixed, w_out), "tensor")
    resid1 = resid + attention
    normed2, norm2_back = jax.vjp(rms_apply, resid1, norm2_gain)
    hidden2 = normed2.astype(bf)
    ffn_gate = project(hidden2, w_ffn_gate)
    ffn_up = project(hidden2, w_ffn_up)
    inner_full, swiglu_back = jax.vjp(swiglu, ffn_gate, ffn_up)
    inner = inner_full.astype(bf)
    ffn = lax.psum(project(inner, w_ffn_down), "tensor")
    output = (resid1 + ffn).astype(bf).reshape(batch, seg, width)
    upstream = cotangent.reshape(count, width)
    grad_down = contract_rows(inner, upstream)
    grad_inner = back_project(upstream, w_ffn_down)
    grad_fgate, grad_fup = swiglu_back(grad_inner)
    grad_fgate = grad_fgate.astype(bf)
    grad_fup = grad_fup.astype(bf)
    grad_ffn_gate_w = contract_rows(hidden2, grad_fgate)
    grad_ffn_up_w = contract_rows(hidden2, grad_fup)
    grad_hidden2 = lax.psum(
        back_project(grad_fgate, w_ffn_gate) + back_project(grad_fup, w_ffn_up), "tensor"
    )
    grad_from_norm2, grad_norm2_gain = norm2_back(grad_hidden2)
    grad_resid1 = upstream.astype(jnp.float32) + grad_from_norm2
    grad_resid1_low = grad_resid1.astype(bf)
    grad_out_w = contract_rows(mixed, grad_resid1_low)
    grad_mixed = back_project(grad_resid1_low, w_out).reshape(batch, seg, heads, value_dim)
    grad_core, grad_gate4, grad_head_gain = gate_back(grad_mixed)
    grad_core_h = jnp.moveaxis(grad_core, 2, 1)
    carry_term = exact(jnp.swapaxes(out_carry, -1, -2), grad_core_h)
    suffix = carried_in(
        (jnp.swapaxes(transition, -1, -2), carry_term), "dp", compose, (eye_block, zero_block), True
    )

    def local_delta(query, key, values, beta, logdecay):
        return run_heads(query, key, values, beta, logdecay, start_state)

    recomputed, delta_back = jax.vjp(local_delta, query_h, key_h, value_h, beta_h, decay_h)
    feature_grads = delta_back((grad_core_h, suffix[1]))
    grad_ext, grad_beta_in, grad_decay_in, grad_conv, grad_rate = prep_back(feature_grads)
    returned = from_behind(grad_ext[:, :reach, :], "dp", -1)
    grad_mixed_pre = grad_ext[:, reach:, :] + jnp.pad(returned, ((0, 0), (seg - reach, 0), (0, 0)))
    grad_mixed_pre = grad_mixed_pre.reshape(count, -1)
    grad_query_low = grad_mixed_pre[:, :qk_width].astype(bf)
    grad_key_low = grad_mixed_pre[:, qk_width : 2 * qk_width].astype(bf)
    grad_value_low = grad_mixed_pre[:, 2 * qk_width :].astype(bf)
    grad_gate_low = grad_gate4.reshape(count, heads * value_dim).astype(bf)
    grad_beta_low = grad_beta_in.reshape(count, heads).astype(bf)
    grad_decay_low = grad_decay_in.reshape(count, heads).astype(bf)
    partial_hidden1 = (
        back_project(grad_query_low, w_query)
        + back_project(grad_key_low, w_key)
        + back_project(grad_value_low, w_value)
        + back_project(grad_gate_low, w_gate)
        + back_project(grad_beta_low, w_beta)
        + back_project(grad_decay_low, w_decay)
    )
    grad_hidden1 = lax.psum(partial_hidden1, "tensor")
    grad_from_norm1, grad_norm1_gain = norm1_back(grad_hidden1)
    grad_inputs = (grad_resid1 + grad_from_norm1).reshape(batch, seg, width)
    grad_query_w = contract_rows(hidden1, grad_query_low)
    grad_key_w = contract_rows(hidden1, grad_key_low)
    grad_value_w = contract_rows(hidden1, grad_value_low)
    grad_gate_w = contract_rows(hidden1, grad_gate_low)
    grad_beta_w = contract_rows(hidden1, grad_beta_low)
    grad_decay_w = contract_rows(hidden1, grad_decay_low)
    grad_convq = grad_conv[:, :qk_width]
    grad_convk = grad_conv[:, qk_width : 2 * qk_width]
    grad_convv = grad_conv[:, 2 * qk_width :]
    grad_head_flat = grad_head_gain.reshape(-1)
    (
        grad_norm1_gain,
        grad_query_w,
        grad_key_w,
        grad_value_w,
        grad_gate_w,
        grad_beta_w,
        grad_decay_w,
        grad_rate,
        grad_convq,
        grad_convk,
        grad_convv,
        grad_head_flat,
        grad_out_w,
        grad_norm2_gain,
        grad_ffn_gate_w,
        grad_ffn_up_w,
        grad_down,
    ) = lax.psum(
        (
            grad_norm1_gain,
            grad_query_w,
            grad_key_w,
            grad_value_w,
            grad_gate_w,
            grad_beta_w,
            grad_decay_w,
            grad_rate,
            grad_convq,
            grad_convk,
            grad_convv,
            grad_head_flat,
            grad_out_w,
            grad_norm2_gain,
            grad_ffn_gate_w,
            grad_ffn_up_w,
            grad_down,
        ),
        "dp",
    )
    return (
        output,
        grad_inputs,
        grad_norm1_gain,
        grad_query_w,
        grad_key_w,
        grad_value_w,
        grad_gate_w,
        grad_beta_w,
        grad_decay_w,
        grad_rate,
        grad_convq,
        grad_convk,
        grad_convv,
        grad_head_flat,
        grad_out_w,
        grad_norm2_gain,
        grad_ffn_gate_w,
        grad_ffn_up_w,
        grad_down,
    )


HALO = 8


def mm(left, right):
    return lax.dot_general(
        left, right, (((1,), (0,)), ((), ())),
        precision=lax.Precision.HIGHEST, preferred_element_type=jnp.float32,
    )


def mm_nt(left, right):
    return lax.dot_general(
        left, right, (((1,), (1,)), ((), ())),
        precision=lax.Precision.HIGHEST, preferred_element_type=jnp.float32,
    )


def mm_tn(left, right):
    return lax.dot_general(
        left, right, (((0,), (0,)), ((), ())),
        precision=lax.Precision.HIGHEST, preferred_element_type=jnp.float32,
    )


def grids(count):
    rows = lax.broadcasted_iota(jnp.int32, (count, count), 0)
    cols = lax.broadcasted_iota(jnp.int32, (count, count), 1)
    return rows, cols


def unit_inverse(lower, rows, cols):
    count = lower.shape[0]
    near = (rows // 2 == cols // 2) & (rows > cols)
    inverse = jnp.where(rows == cols, 1.0, jnp.where(near, -lower, 0.0))
    block = 2
    while block < count:
        cross = (rows // (2 * block) == cols // (2 * block)) & (rows // block > cols // block)
        inverse = inverse - mm(mm(inverse, jnp.where(cross, lower, 0.0)), inverse)
        block *= 2
    return inverse


def conv_window(halo_block, taps, span):
    reach = taps.shape[0] - 1
    total = None
    for offset in range(reach + 1):
        start = HALO - reach + offset
        term = taps[offset : offset + 1] * halo_block[start : start + span]
        total = term if total is None else total + term
    return total


def sigmoid(value):
    return 1.0 / (1.0 + jnp.exp(-value))


def softplus(value):
    return jnp.maximum(value, 0.0) + jnp.log(1.0 + jnp.exp(-jnp.abs(value)))


def gates_of(small, rate, heads, rows, cols):
    beta = sigmoid(small)
    slope = softplus(small)
    logdecay = -rate * slope
    cumul = mm(jnp.where(cols <= rows, 1.0, 0.0), logdecay)
    return beta, slope, logdecay, cumul


def chunk_terms(query, key, beta_col, beta_row, cum_col, cum_row, rows, cols):
    within = cols <= rows
    decays = jnp.where(within, jnp.exp(jnp.where(within, cum_col - cum_row, 0.0)), 0.0)
    scaled = decays * beta_row
    key_key = mm_nt(key, key)
    query_key = mm_nt(query, key)
    lower = jnp.where(cols < rows, scaled * key_key, 0.0)
    attend = scaled * query_key
    return decays, scaled, key_key, query_key, lower, attend


def forward_kernel(heads, key_dim, value_dim, pre_ref, gate_ref, small_ref, taps_ref, rate_ref, gain_ref,
                   mixed_ref, core_ref, update_ref, state_ref, inverse_ref, pad_ref, now_ref):
    length, width = pre_ref.shape
    span = SPAN
    chunks = length // span
    rows, cols = grids(span)
    qk = heads * key_dim
    pad_ref[0:HALO] = jnp.zeros((HALO, width), jnp.float32)
    for head in range(heads):
        now_ref[head] = jnp.zeros((key_dim, value_dim), jnp.float32)

    def chunk(index, carry):
        start = pl.multiple_of(index * span, span)
        here = pl.ds(start, span)
        pad_ref[HALO : HALO + span] = pre_ref[here, :]
        total = conv_window(pad_ref[...], taps_ref[...], span)
        pad_ref[0:HALO] = pad_ref[span : span + HALO]
        active = total * sigmoid(total)
        beta, _, _, cumul = gates_of(small_ref[here, :], rate_ref[...], heads, rows, cols)
        beta_t = jnp.transpose(beta)
        cumul_t = jnp.transpose(cumul)
        gate = gate_ref[here, :]
        gated = gate * sigmoid(gate) * gain_ref[...]
        for head in range(heads):
            query = active[:, head * key_dim : (head + 1) * key_dim]
            query = query * (lax.rsqrt(jnp.sum(query * query, -1, keepdims=True) + EPS) * key_dim ** (-0.5))
            key = active[:, qk + head * key_dim : qk + (head + 1) * key_dim]
            key = key * lax.rsqrt(jnp.sum(key * key, -1, keepdims=True) + EPS)
            value = active[:, 2 * qk + head * value_dim : 2 * qk + (head + 1) * value_dim]
            beta_col = beta[:, head : head + 1]
            beta_row = beta_t[head : head + 1]
            cum_col = cumul[:, heads + head : heads + head + 1]
            cum_row = cumul_t[heads + head : heads + head + 1]
            _, _, _, _, lower, attend = chunk_terms(query, key, beta_col, beta_row, cum_col, cum_row, rows, cols)
            inverse = unit_inverse(lower, rows, cols)
            state = now_ref[head]
            state_ref[index, head] = state
            rise = jnp.exp(cum_col)
            last = cum_col[span - 1 : span]
            update = mm(inverse, value) - mm(mm(inverse, rise * key), state)
            core = mm(rise * query, state) + mm(attend, update)
            tail = jnp.exp(last - cum_col) * beta_col
            now_ref[head] = jnp.exp(last) * state + mm_tn(key * tail, update)
            inverse_ref[index, head] = inverse
            wide = slice(head * value_dim, (head + 1) * value_dim)
            update_ref[here, wide] = update
            core_ref[here, wide] = core
            normed = core * lax.rsqrt(jnp.mean(core * core, -1, keepdims=True) + EPS)
            mixed_ref[here, wide] = (normed * gated[:, wide]).astype(mixed_ref.dtype)
        return carry

    lax.fori_loop(0, chunks, chunk, 0)


def delta_forward(pre, gate, small, taps, rate, gain, heads, key_dim, value_dim):
    length, width = pre.shape
    chunks = length // SPAN
    out_shape = (
        jax.ShapeDtypeStruct((length, heads * value_dim), jnp.bfloat16),
        jax.ShapeDtypeStruct((length, heads * value_dim), jnp.float32),
        jax.ShapeDtypeStruct((length, heads * value_dim), jnp.float32),
        jax.ShapeDtypeStruct((chunks, heads, key_dim, value_dim), jnp.float32),
        jax.ShapeDtypeStruct((chunks, heads, SPAN, SPAN), jnp.float32),
    )
    return pl.pallas_call(
        functools.partial(forward_kernel, heads, key_dim, value_dim),
        out_shape=out_shape,
        scratch_shapes=[
            pltpu.VMEM((HALO + SPAN, width), jnp.float32),
            pltpu.VMEM((heads, key_dim, value_dim), jnp.float32),
        ],
        compiler_params=pltpu.CompilerParams(vmem_limit_bytes=56 << 20),
        name="delta_forward",
    )(pre, gate, small, taps, rate, gain)


def backward_kernel(heads, key_dim, value_dim, pre_ref, gate_ref, small_ref, taps_ref, rate_ref, gain_ref,
                    core_ref, update_ref, state_ref, inverse_ref, grad_ref,
                    low_ref, gate_low_ref, small_low_ref, taps_grad_ref, gain_grad_ref, rate_grad_ref,
                    ahead_ref, pad_ref, now_ref):
    length, width = pre_ref.shape
    span = SPAN
    chunks = length // span
    rows, cols = grids(span)
    qk = heads * key_dim
    reach = taps_ref.shape[0] - 1
    lanes = small_ref.shape[1]
    lane = lax.broadcasted_iota(jnp.int32, (span, lanes), 1)
    for head in range(heads):
        now_ref[head] = jnp.zeros((key_dim, value_dim), jnp.float32)
    pad_ref[span : span + HALO] = jnp.zeros((HALO, width), jnp.float32)
    taps_grad_ref[...] = jnp.zeros_like(taps_grad_ref)
    gain_grad_ref[...] = jnp.zeros_like(gain_grad_ref)
    rate_grad_ref[...] = jnp.zeros_like(rate_grad_ref)

    def chunk(turn, carry):
        index = chunks - 1 - turn
        start = pl.multiple_of(index * span, span)
        here = pl.ds(start, span)
        before = pl.ds(pl.multiple_of(jnp.maximum(start - HALO, 0), HALO), HALO)
        ahead_ref[0:HALO] = pre_ref[before, :] * jnp.where(index > 0, 1.0, 0.0)
        ahead_ref[HALO : HALO + span] = pre_ref[here, :]
        total = conv_window(ahead_ref[...], taps_ref[...], span)
        gain_of = sigmoid(total)
        active = total * gain_of
        bend = gain_of * (1.0 + total * (1.0 - gain_of))
        small = small_ref[here, :]
        beta, slope, _, cumul = gates_of(small, rate_ref[...], heads, rows, cols)
        beta_t = jnp.transpose(beta)
        cumul_t = jnp.transpose(cumul)
        gate = gate_ref[here, :]
        gate_sig = sigmoid(gate)
        gate_silu = gate * gate_sig
        gate_bend = gate_sig * (1.0 + gate * (1.0 - gate_sig))
        small_grad = jnp.zeros((span, lanes), jnp.float32)
        for head in range(heads):
            wide = slice(head * value_dim, (head + 1) * value_dim)
            core = core_ref[here, wide]
            grad_mixed = grad_ref[here, wide]
            gain = gain_ref[:, wide]
            scale = lax.rsqrt(jnp.mean(core * core, -1, keepdims=True) + EPS)
            normed = core * scale
            gate_low_ref[here, wide] = (grad_mixed * normed * gain * gate_bend[:, wide]).astype(gate_low_ref.dtype)
            with_gate = grad_mixed * gate_silu[:, wide]
            gain_grad_ref[:, wide] += jnp.sum(with_gate * normed, 0, keepdims=True)
            grad_normed = with_gate * gain
            grad_core = scale * (grad_normed - normed * jnp.mean(grad_normed * normed, -1, keepdims=True))
            query_act = active[:, head * key_dim : (head + 1) * key_dim]
            query_scale = lax.rsqrt(jnp.sum(query_act * query_act, -1, keepdims=True) + EPS)
            query = query_act * (query_scale * key_dim ** (-0.5))
            key_act = active[:, qk + head * key_dim : qk + (head + 1) * key_dim]
            key_scale = lax.rsqrt(jnp.sum(key_act * key_act, -1, keepdims=True) + EPS)
            key = key_act * key_scale
            beta_col = beta[:, head : head + 1]
            beta_row = beta_t[head : head + 1]
            cum_col = cumul[:, heads + head : heads + head + 1]
            cum_row = cumul_t[heads + head : heads + head + 1]
            decays, scaled, key_key, query_key, lower, attend = chunk_terms(
                query, key, beta_col, beta_row, cum_col, cum_row, rows, cols
            )
            state = state_ref[index, head]
            update = update_ref[here, wide]
            inverse = inverse_ref[index, head]
            grad_state = now_ref[head]
            rise = jnp.exp(cum_col)
            last = cum_col[span - 1 : span]
            fall = jnp.exp(last - cum_col)
            tail = fall * beta_col
            rise_query = rise * query
            rise_key = rise * key
            grad_update = mm_tn(attend, grad_core) + mm(key * tail, grad_state)
            grad_right = mm_tn(inverse, grad_update)
            now_ref[head] = jnp.exp(last) * grad_state + mm_tn(rise_query, grad_core) - mm_tn(rise_key, grad_right)
            grad_attend = jnp.where(cols <= rows, mm_nt(grad_core, update), 0.0)
            grad_lower = jnp.where(cols < rows, -mm_nt(grad_right, update), 0.0)
            core_state = mm_nt(grad_core, state)
            right_state = mm_nt(grad_right, state)
            grad_tail_key = mm_nt(update, grad_state)
            pair_query = grad_attend * scaled
            pair_key = grad_lower * scaled
            grad_query = rise * core_state + mm(pair_query, key)
            grad_key = (
                grad_tail_key * tail - rise * right_state + mm_tn(pair_query, query)
                + mm(pair_key, key) + mm_tn(pair_key, key)
            )
            grad_tail = jnp.sum(grad_tail_key * key, -1, keepdims=True)
            moved = grad_attend * query_key + grad_lower * key_key
            spread = moved * scaled
            by_row = jnp.sum(spread, -1, keepdims=True)
            sums = mm_tn(
                jnp.concatenate([moved * decays, spread], 1), jnp.ones((span, lanes), jnp.float32)
            )
            grad_beta = sums[:span, 0:1] + grad_tail * fall
            through_tail = grad_tail * tail
            grad_cum = (
                by_row - sums[span:, 0:1] - through_tail
                + rise * (jnp.sum(core_state * query, -1, keepdims=True) - jnp.sum(right_state * key, -1, keepdims=True))
            )
            end_grad = jnp.sum(through_tail, 0, keepdims=True) + jnp.exp(last) * jnp.sum(
                jnp.sum(state * grad_state, -1, keepdims=True), 0, keepdims=True
            )
            grad_cum = grad_cum + jnp.where(rows[:, 0:1] == span - 1, end_grad, 0.0)
            small_grad = small_grad + jnp.where(lane == head, grad_beta, 0.0)
            small_grad = small_grad + jnp.where(lane == heads + head, grad_cum, 0.0)
            grad_query = grad_query * key_dim ** (-0.5)
            unit = query_act * query_scale
            grad_query = query_scale * (grad_query - unit * jnp.sum(grad_query * unit, -1, keepdims=True))
            grad_key = key_scale * (grad_key - key * jnp.sum(grad_key * key, -1, keepdims=True))
            at = slice(head * key_dim, (head + 1) * key_dim)
            pad_ref[0:span, at] = grad_query * bend[:, at]
            at = slice(qk + head * key_dim, qk + (head + 1) * key_dim)
            pad_ref[0:span, at] = grad_key * bend[:, at]
            at = slice(2 * qk + head * value_dim, 2 * qk + (head + 1) * value_dim)
            pad_ref[0:span, at] = grad_right * bend[:, at]
        summed = mm(jnp.where(cols >= rows, 1.0, 0.0), small_grad)
        is_beta = lane < heads
        rate_grad_ref[...] += jnp.sum(jnp.where(is_beta, 0.0, -slope * summed), 0, keepdims=True)
        sig = beta
        small_low_ref[here, :] = jnp.where(
            is_beta, small_grad * sig * (1.0 - sig), -rate_ref[...] * sig * summed
        ).astype(small_low_ref.dtype)
        outer = pad_ref[...]
        dense = outer[0:span]
        block = ahead_ref[...]
        grad_pre = None
        for offset in range(reach + 1):
            behind = reach - offset
            taps_grad_ref[offset : offset + 1] += jnp.sum(
                dense * block[HALO - behind : HALO - behind + span], 0, keepdims=True
            )
            term = taps_ref[offset : offset + 1] * outer[behind : behind + span]
            grad_pre = term if grad_pre is None else grad_pre + term
        low_ref[here, :] = grad_pre.astype(low_ref.dtype)
        pad_ref[span : span + HALO] = pad_ref[0:HALO]
        return carry

    lax.fori_loop(0, chunks, chunk, 0)


def delta_backward(pre, gate, small, taps, rate, gain, core, update, state, inverse, grad, heads, key_dim, value_dim):
    length, width = pre.shape
    lanes = small.shape[1]
    out_shape = (
        jax.ShapeDtypeStruct((length, width), jnp.bfloat16),
        jax.ShapeDtypeStruct((length, heads * value_dim), jnp.bfloat16),
        jax.ShapeDtypeStruct((length, lanes), jnp.bfloat16),
        jax.ShapeDtypeStruct(taps.shape, jnp.float32),
        jax.ShapeDtypeStruct((1, heads * value_dim), jnp.float32),
        jax.ShapeDtypeStruct((1, lanes), jnp.float32),
    )
    return pl.pallas_call(
        functools.partial(backward_kernel, heads, key_dim, value_dim),
        out_shape=out_shape,
        scratch_shapes=[
            pltpu.VMEM((HALO + SPAN, width), jnp.float32),
            pltpu.VMEM((HALO + SPAN, width), jnp.float32),
            pltpu.VMEM((heads, key_dim, value_dim), jnp.float32),
        ],
        compiler_params=pltpu.CompilerParams(vmem_limit_bytes=56 << 20),
        name="delta_backward",
    )(pre, gate, small, taps, rate, gain, core, update, state, inverse, grad)


MESH = pl.DeviceIdType.MESH
VM = pl.BlockSpec(memory_space=pltpu.VMEM)


def greet(peers):
    barrier = pltpu.get_barrier_semaphore()
    for peer in peers:
        pl.semaphore_signal(barrier, inc=1, device_id=peer, device_id_type=MESH)
    pl.semaphore_wait(barrier, len(peers))


def remote(src, dst, send, recv, peer):
    return pltpu.make_async_remote_copy(
        src_ref=src, dst_ref=dst, send_sem=send, recv_sem=recv, device_id=peer, device_id_type=MESH
    )


def tensor_peers():
    dp = lax.axis_index("dp")
    t = lax.axis_index("tensor")
    core = lax.rem(t, 2)
    mate = (dp, t + 1 - 2 * core)
    across = (dp, lax.rem(t + 2, 4))
    return core, mate, across


def psum_kernel(blocks, part_ref, out_ref, land_mate, land_across, half, send, recv):
    core, mate, across = tensor_peers()
    greet((mate, across))
    rows = part_ref.shape[0] // blocks
    part = rows // 2
    first = []
    for b in range(blocks):
        theirs = pl.ds(pl.multiple_of(b * rows + (1 - core) * part, part), part)
        copy = remote(part_ref.at[theirs], land_mate.at[pl.ds(b * part, part)], send.at[0, b], recv.at[0, b], mate)
        copy.start()
        first.append(copy)
    second = []
    for b in range(blocks):
        mine = pl.ds(pl.multiple_of(b * rows + core * part, part), part)
        slot = pl.ds(b * part, part)
        first[b].wait_recv()
        half[slot] = part_ref[mine] + land_mate[slot]
        copy = remote(half.at[slot], land_across.at[slot], send.at[1, b], recv.at[1, b], across)
        copy.start()
        second.append(copy)
    third = []
    for b in range(blocks):
        mine = pl.ds(pl.multiple_of(b * rows + core * part, part), part)
        slot = pl.ds(b * part, part)
        second[b].wait_recv()
        out_ref[mine] = half[slot] + land_across[slot]
        copy = remote(out_ref.at[mine], out_ref.at[mine], send.at[2, b], recv.at[2, b], mate)
        copy.start()
        third.append(copy)
    for b in range(blocks):
        third[b].wait_recv()
    for b in range(blocks):
        first[b].wait_send()
        second[b].wait_send()
        third[b].wait_send()


def tensor_sum(part, collective_id, blocks=8):
    rows, width = part.shape
    return pl.pallas_call(
        functools.partial(psum_kernel, blocks),
        out_shape=jax.ShapeDtypeStruct(part.shape, part.dtype),
        in_specs=[VM],
        out_specs=VM,
        scratch_shapes=[pltpu.VMEM((rows // 2, width), part.dtype)] * 3
        + [pltpu.SemaphoreType.DMA((3, blocks))] * 2,
        compiler_params=pltpu.CompilerParams(
            collective_id=collective_id, has_side_effects=True, vmem_limit_bytes=40 << 20
        ),
        name="tensor_sum",
    )(part)


def swap_kernel(count, narrow, *refs):
    sources, results = refs[:count], refs[count : 2 * count]
    staged, send, recv, close_send, close_recv = refs[2 * count :]
    n = lax.axis_size("dp")
    me = lax.axis_index("dp")
    t = lax.axis_index("tensor")
    core, mate, across = tensor_peers()
    ranks = lax.axis_size("tensor")
    others = [lax.rem(me + k, n) for k in range(1, n)]
    greet([(other, t) for other in others] + [mate, across])
    seg = results[0].shape[0] // n
    part = seg // ranks
    far = lax.rem(t + 2, ranks)

    def at(place, rank):
        return pl.ds(pl.multiple_of(place * seg + rank * part, part), part)

    outgoing = []
    for i in range(count):
        for k in range(n):
            other = lax.rem(me + k, n)
            if k == 0:
                results[i][at(me, t)] = sources[i][at(me, t)].astype(jnp.float32)
                continue
            if narrow[i]:
                staged[i, k] = sources[i][at(other, t)].astype(jnp.float32)
                src = staged.at[i, k]
            else:
                src = sources[i].at[at(other, t)]
            copy = remote(src, results[i].at[at(me, t)], send.at[i, k], recv.at[i, k], (other, t))
            copy.start()
            outgoing.append(copy)
    close = []
    for i in range(count):
        for k in range(n):
            source = lax.rem(me + n - k, n)
            here = results[i].at[at(source, t)]
            if k:
                remote(here, here, send.at[i, k], recv.at[i, k], (source, t)).wait_recv()
            over = remote(here, here, close_send.at[0, i, k], close_recv.at[0, i, k], across)
            over.start()
            beside = remote(here, here, close_send.at[1, i, k], close_recv.at[1, i, k], mate)
            beside.start()
            close += [over, beside]
    last = []
    for i in range(count):
        for k in range(n):
            source = lax.rem(me + n - k, n)
            there = results[i].at[at(source, far)]
            remote(there, there, close_send.at[0, i, k], close_recv.at[0, i, k], across).wait_recv()
            copy = remote(there, there, close_send.at[2, i, k], close_recv.at[2, i, k], mate)
            copy.start()
            last.append(copy)
    for copy in outgoing:
        copy.wait_send()
    for j, copy in enumerate(close):
        copy.wait_send()
        if j % 2:
            copy.wait_recv()
    for copy in last:
        copy.wait()


def swap(arrays, n, collective_id):
    count = len(arrays)
    rows, width = arrays[0].shape
    narrow = [a.dtype != jnp.float32 for a in arrays]
    out = pl.pallas_call(
        functools.partial(swap_kernel, count, narrow),
        out_shape=[jax.ShapeDtypeStruct((rows, width), jnp.float32)] * count,
        in_specs=[VM] * count,
        out_specs=[VM] * count,
        scratch_shapes=[pltpu.VMEM((count, n, rows // n // 4, width), jnp.float32)]
        + [pltpu.SemaphoreType.DMA((count, n))] * 2
        + [pltpu.SemaphoreType.DMA((3, count, n))] * 2,
        compiler_params=pltpu.CompilerParams(
            collective_id=collective_id, has_side_effects=True, vmem_limit_bytes=40 << 20
        ),
        name="swap",
    )(*arrays)
    return out


def lane_pad(array, lanes):
    return jnp.pad(array, ((0, 0), (0, lanes - array.shape[1])))


def whole_sequences(
    inputs,
    norm1_gain,
    w_query,
    w_key,
    w_value,
    w_gate,
    w_beta,
    w_decay,
    decay_rate,
    conv_query,
    conv_key,
    conv_value,
    head_gain,
    w_out,
    norm2_gain,
    w_ffn_gate,
    w_ffn_up,
    w_ffn_down,
    cotangent,
):
    batch, seg, width = inputs.shape
    count = batch * seg
    heads = decay_rate.shape[0]
    key_dim = w_query.shape[1] // heads
    value_dim = w_value.shape[1] // heads
    qk_width = heads * key_dim
    lanes = 128
    bf = jnp.bfloat16
    places = lax.axis_size("dp")
    resid, upstream = swap(
        [inputs.reshape(count, width), cotangent.reshape(count, width)], places, 1
    )
    upstream_low = upstream.astype(bf)
    normed1, norm1_back = jax.vjp(rms_apply, resid, norm1_gain)
    hidden1 = normed1.astype(bf)
    w_mix = jnp.concatenate([w_query, w_key, w_value], axis=1)
    w_small = lane_pad(jnp.concatenate([w_beta, w_decay], axis=1), lanes)
    pre = project(hidden1, w_mix)
    gate_pre = project(hidden1, w_gate)
    small = project(hidden1, w_small)
    taps = jnp.concatenate([conv_query, conv_key, conv_value], axis=1)
    rate = lane_pad(jnp.pad(decay_rate, (heads, 0))[None], lanes)
    gain = head_gain[None]
    mixed, core, update, states, inverses = delta_forward(
        pre, gate_pre, small, taps, rate, gain, heads, key_dim, value_dim
    )
    attention = tensor_sum(project(mixed, w_out), 2)
    resid1 = resid + attention
    normed2, norm2_back = jax.vjp(rms_apply, resid1, norm2_gain)
    hidden2 = normed2.astype(bf)
    ffn_gate = project(hidden2, w_ffn_gate)
    ffn_up = project(hidden2, w_ffn_up)
    inner_full, swiglu_back = jax.vjp(swiglu, ffn_gate, ffn_up)
    inner = inner_full.astype(bf)
    grad_inner = back_project(upstream_low, w_ffn_down)
    grad_fgate, grad_fup = swiglu_back(grad_inner)
    grad_fgate = grad_fgate.astype(bf)
    grad_fup = grad_fup.astype(bf)
    grad_hidden2 = tensor_sum(
        back_project(grad_fgate, w_ffn_gate) + back_project(grad_fup, w_ffn_up), 3
    )
    ffn = tensor_sum(project(inner, w_ffn_down), 4)
    grad_down = contract_rows(inner, upstream_low)
    grad_ffn_gate_w = contract_rows(hidden2, grad_fgate)
    grad_ffn_up_w = contract_rows(hidden2, grad_fup)
    grad_from_norm2, grad_norm2_gain = norm2_back(grad_hidden2)
    grad_resid1 = upstream + grad_from_norm2
    grad_resid1_low = grad_resid1.astype(bf)
    grad_out_w = contract_rows(mixed, grad_resid1_low)
    grad_mixed = back_project(grad_resid1_low, w_out)
    low, gate_low, small_low, grad_taps, grad_head, grad_rate = delta_backward(
        pre, gate_pre, small, taps, rate, gain, core, update, states, inverses, grad_mixed,
        heads, key_dim, value_dim,
    )
    partial_hidden1 = (
        back_project(low, w_mix) + back_project(gate_low, w_gate) + back_project(small_low, w_small)
    )
    grad_hidden1 = tensor_sum(partial_hidden1, 5)
    grad_from_norm1, grad_norm1_gain = norm1_back(grad_hidden1)
    output, grad_inputs = swap([resid1 + ffn, grad_resid1 + grad_from_norm1], places, 6)
    output = output.reshape(batch, seg, width).astype(bf)
    grad_inputs = grad_inputs.reshape(batch, seg, width)
    grad_mix_w = contract_rows(hidden1, low)
    grad_gate_w = contract_rows(hidden1, gate_low)
    grad_small_w = contract_rows(hidden1, small_low)
    (
        grad_norm1_gain,
        grad_mix_w,
        grad_gate_w,
        grad_small_w,
        grad_rate,
        grad_taps,
        grad_head,
        grad_out_w,
        grad_norm2_gain,
        grad_ffn_gate_w,
        grad_ffn_up_w,
        grad_down,
    ) = lax.psum(
        (
            grad_norm1_gain,
            grad_mix_w,
            grad_gate_w,
            grad_small_w,
            grad_rate,
            grad_taps,
            grad_head,
            grad_out_w,
            grad_norm2_gain,
            grad_ffn_gate_w,
            grad_ffn_up_w,
            grad_down,
        ),
        "dp",
    )
    return (
        output,
        grad_inputs,
        grad_norm1_gain,
        grad_mix_w[:, :qk_width],
        grad_mix_w[:, qk_width : 2 * qk_width],
        grad_mix_w[:, 2 * qk_width :],
        grad_gate_w,
        grad_small_w[:, :heads],
        grad_small_w[:, heads : 2 * heads],
        grad_rate[0, heads : 2 * heads],
        grad_taps[:, :qk_width],
        grad_taps[:, qk_width : 2 * qk_width],
        grad_taps[:, 2 * qk_width :],
        grad_head[0],
        grad_out_w,
        grad_norm2_gain,
        grad_ffn_gate_w,
        grad_ffn_up_w,
        grad_down,
    )


def fits_whole(mesh, args):
    batch, length, _ = args[0].shape
    places, ranks = mesh.shape["dp"], mesh.shape["tensor"]
    return batch == places and ranks == 4 and length % (places * ranks * 16) == 0 and length % SPAN == 0


def solution(mesh):
    placed = (
        P(None, "dp", None),
        P(),
        P(None, "tensor"),
        P(None, "tensor"),
        P(None, "tensor"),
        P(None, "tensor"),
        P(None, "tensor"),
        P(None, "tensor"),
        P("tensor"),
        P(None, "tensor"),
        P(None, "tensor"),
        P(None, "tensor"),
        P("tensor"),
        P("tensor", None),
        P(),
        P(None, "tensor"),
        P(None, "tensor"),
        P("tensor", None),
        P(None, "dp", None),
    )
    def step(*args):
        body = whole_sequences if fits_whole(mesh, args) else shards
        return placed_step(body)(*args)

    def placed_step(body):
      return jax.shard_map(
        body,
        mesh=mesh,
        in_specs=placed,
        out_specs=(
            P(None, "dp", None),
            P(None, "dp", None),
            P(),
            P(None, "tensor"),
            P(None, "tensor"),
            P(None, "tensor"),
            P(None, "tensor"),
            P(None, "tensor"),
            P(None, "tensor"),
            P("tensor"),
            P(None, "tensor"),
            P(None, "tensor"),
            P(None, "tensor"),
            P("tensor"),
            P("tensor", None),
            P(),
            P(None, "tensor"),
            P(None, "tensor"),
            P("tensor", None),
        ),
        check_vma=False,
    )

    return step
```

```python
import functools
from functools import partial

import jax
import jax.numpy as jnp
from jax import lax
from jax.experimental import pallas as pl
from jax.experimental.pallas import tpu as pltpu
from jax.sharding import PartitionSpec as P

SPAN = 64


EPS = 1e-06


def from_behind(shard, axis, by):
    count = lax.axis_size(axis)
    pairs = [(i, i + by) for i in range(count) if 0 <= i + by < count]
    return lax.ppermute(shard, axis, pairs)


def carried_in(part, axis, combine, identity, reverse):
    count = lax.axis_size(axis)
    place = lax.axis_index(axis)
    ahead = count - 1 - place if reverse else place
    gathered = jax.tree.map(lambda a: lax.all_gather(a, axis), part)
    state = jax.tree.map(lambda a, e: jnp.zeros_like(a) + jnp.asarray(e, a.dtype), part, identity)

    def one(turn, state):
        source = count - 1 - turn if reverse else turn
        return combine(
            state, jax.tree.map(lambda a: lax.dynamic_index_in_dim(a, source, 0, False), gathered)
        )

    return lax.fori_loop(0, ahead, one, state)


def exact(left, right):
    return jnp.matmul(left, right, precision=lax.Precision.HIGHEST)


def span_apply(state, inputs):
    query, key, values, beta, logdecay = inputs
    count = query.shape[0]
    cumul = jnp.cumsum(logdecay)
    row_ids = lax.broadcasted_iota(jnp.int32, (count, count), 0)
    col_ids = lax.broadcasted_iota(jnp.int32, (count, count), 1)
    within = col_ids <= row_ids
    strict = col_ids < row_ids
    spread = jnp.where(within, cumul[:, None] - cumul[None, :], 0.0)
    decays = jnp.where(within, jnp.exp(spread), 0.0)
    scaled = decays * beta[None, :]
    lower = jnp.where(strict, scaled * exact(key, key.T), 0.0)
    start_decay = jnp.exp(cumul)[:, None]
    right_side = values - start_decay * exact(key, state)
    system = jnp.eye(count, dtype=lower.dtype) + lower
    update = jax.scipy.linalg.solve_triangular(system, right_side, lower=True, unit_diagonal=True)
    output = start_decay * exact(query, state) + exact(scaled * exact(query, key.T), update)
    tail = jnp.exp(cumul[-1] - cumul) * beta
    new_state = jnp.exp(cumul[-1]) * state + exact((key * tail[:, None]).T, update)
    return (new_state, output)


def run_segment(query, key, values, beta, logdecay, state):
    length = query.shape[0]
    blocks = length // SPAN

    def split(array):
        return array.reshape((blocks, SPAN) + array.shape[1:])

    final, outputs = lax.scan(
        span_apply, state, (split(query), split(key), split(values), split(beta), split(logdecay))
    )
    return (outputs.reshape((length,) + outputs.shape[2:]), final)


def run_heads(query, key, values, beta, logdecay, state):
    return jax.vmap(jax.vmap(run_segment))(query, key, values, beta, logdecay, state)


def prepare(extended, beta_pre, decay_pre, conv_all, decay_rate, key_dim):
    batch, seg, heads = beta_pre.shape
    reach = conv_all.shape[0] - 1
    total = conv_all[0] * extended[:, 0:seg, :]
    for offset in range(1, reach + 1):
        total = total + conv_all[offset] * extended[:, offset : offset + seg, :]
    active = jax.nn.silu(total)
    qk_width = heads * key_dim
    query = active[..., :qk_width].reshape(batch, seg, heads, key_dim)
    key = active[..., qk_width : 2 * qk_width].reshape(batch, seg, heads, key_dim)
    values = active[..., 2 * qk_width :].reshape(batch, seg, heads, -1)
    query = query * lax.rsqrt(jnp.sum(query * query, -1, keepdims=True) + EPS) * key_dim ** (-0.5)
    key = key * lax.rsqrt(jnp.sum(key * key, -1, keepdims=True) + EPS)
    beta = jax.nn.sigmoid(beta_pre)
    logdecay = -decay_rate * jax.nn.softplus(decay_pre)
    return (
        jnp.moveaxis(query, 2, 1),
        jnp.moveaxis(key, 2, 1),
        jnp.moveaxis(values, 2, 1),
        jnp.moveaxis(beta, 2, 1),
        jnp.moveaxis(logdecay, 2, 1),
    )


def gate_norm(core, gate_pre, head_gain):
    normed = core * lax.rsqrt(jnp.mean(core * core, -1, keepdims=True) + EPS)
    return normed * head_gain * jax.nn.silu(gate_pre)


def rms_apply(resid, gain):
    return resid * lax.rsqrt(jnp.mean(resid * resid, -1, keepdims=True) + EPS) * gain


def swiglu(gate, upper):
    return jax.nn.silu(gate) * upper


def project(left, right):
    return jnp.dot(left, right, preferred_element_type=jnp.float32)


def contract_rows(left, right):
    return jnp.einsum("ra,rb->ab", left, right, preferred_element_type=jnp.float32)


def back_project(grad, weight):
    return jnp.einsum("rb,ab->ra", grad, weight, preferred_element_type=jnp.float32)


def compose(earlier, later):
    return (exact(later[0], earlier[0]), exact(later[0], earlier[1]) + later[1])


def shards(
    inputs,
    norm1_gain,
    w_query,
    w_key,
    w_value,
    w_gate,
    w_beta,
    w_decay,
    decay_rate,
    conv_query,
    conv_key,
    conv_value,
    head_gain,
    w_out,
    norm2_gain,
    w_ffn_gate,
    w_ffn_up,
    w_ffn_down,
    cotangent,
):
    batch, seg, width = inputs.shape
    count = batch * seg
    heads = decay_rate.shape[0]
    key_dim = w_query.shape[1] // heads
    value_dim = w_value.shape[1] // heads
    qk_width = heads * key_dim
    reach = conv_query.shape[0] - 1
    bf = jnp.bfloat16
    resid = inputs.reshape(count, width).astype(jnp.float32)
    normed1, norm1_back = jax.vjp(rms_apply, resid, norm1_gain)
    hidden1 = normed1.astype(bf)
    query_pre = project(hidden1, w_query)
    key_pre = project(hidden1, w_key)
    value_pre = project(hidden1, w_value)
    gate_pre = project(hidden1, w_gate)
    beta_pre = project(hidden1, w_beta)
    decay_pre = project(hidden1, w_decay)
    mixed_pre = jnp.concatenate([query_pre, key_pre, value_pre], axis=1).reshape(batch, seg, -1)
    rim = from_behind(mixed_pre[:, seg - reach :, :], "dp", 1)
    extended = jnp.concatenate([rim, mixed_pre], axis=1)
    conv_all = jnp.concatenate([conv_query, conv_key, conv_value], axis=1)
    features, prep_back = jax.vjp(
        partial(prepare, key_dim=key_dim),
        extended,
        beta_pre.reshape(batch, seg, heads),
        decay_pre.reshape(batch, seg, heads),
        conv_all,
        decay_rate,
    )
    query_h, key_h, value_h, beta_h, decay_h = features
    eye_block = jnp.broadcast_to(
        jnp.eye(key_dim, dtype=jnp.float32), (batch, heads, key_dim, key_dim)
    )
    zero_block = jnp.zeros((batch, heads, key_dim, value_dim), jnp.float32)
    values_aug = jnp.concatenate(
        [jnp.zeros(value_h.shape[:3] + (key_dim,), jnp.float32), value_h], axis=-1
    )
    state_aug = jnp.concatenate([eye_block, zero_block], axis=-1)
    outputs_aug, final_aug = run_heads(query_h, key_h, values_aug, beta_h, decay_h, state_aug)
    out_carry = outputs_aug[..., :key_dim]
    out_local = outputs_aug[..., key_dim:]
    transition = final_aug[..., :key_dim]
    offset_part = final_aug[..., key_dim:]
    prefix = carried_in((transition, offset_part), "dp", compose, (eye_block, zero_block), False)
    start_state = prefix[1]
    core = jnp.moveaxis(exact(out_carry, start_state) + out_local, 1, 2)
    gate4 = gate_pre.reshape(batch, seg, heads, value_dim)
    gated, gate_back = jax.vjp(gate_norm, core, gate4, head_gain.reshape(heads, value_dim))
    mixed = gated.reshape(count, heads * value_dim).astype(bf)
    attention = lax.psum(project(mixed, w_out), "tensor")
    resid1 = resid + attention
    normed2, norm2_back = jax.vjp(rms_apply, resid1, norm2_gain)
    hidden2 = normed2.astype(bf)
    ffn_gate = project(hidden2, w_ffn_gate)
    ffn_up = project(hidden2, w_ffn_up)
    inner_full, swiglu_back = jax.vjp(swiglu, ffn_gate, ffn_up)
    inner = inner_full.astype(bf)
    ffn = lax.psum(project(inner, w_ffn_down), "tensor")
    output = (resid1 + ffn).astype(bf).reshape(batch, seg, width)
    upstream = cotangent.reshape(count, width)
    grad_down = contract_rows(inner, upstream)
    grad_inner = back_project(upstream, w_ffn_down)
    grad_fgate, grad_fup = swiglu_back(grad_inner)
    grad_fgate = grad_fgate.astype(bf)
    grad_fup = grad_fup.astype(bf)
    grad_ffn_gate_w = contract_rows(hidden2, grad_fgate)
    grad_ffn_up_w = contract_rows(hidden2, grad_fup)
    grad_hidden2 = lax.psum(
        back_project(grad_fgate, w_ffn_gate) + back_project(grad_fup, w_ffn_up), "tensor"
    )
    grad_from_norm2, grad_norm2_gain = norm2_back(grad_hidden2)
    grad_resid1 = upstream.astype(jnp.float32) + grad_from_norm2
    grad_resid1_low = grad_resid1.astype(bf)
    grad_out_w = contract_rows(mixed, grad_resid1_low)
    grad_mixed = back_project(grad_resid1_low, w_out).reshape(batch, seg, heads, value_dim)
    grad_core, grad_gate4, grad_head_gain = gate_back(grad_mixed)
    grad_core_h = jnp.moveaxis(grad_core, 2, 1)
    carry_term = exact(jnp.swapaxes(out_carry, -1, -2), grad_core_h)
    suffix = carried_in(
        (jnp.swapaxes(transition, -1, -2), carry_term), "dp", compose, (eye_block, zero_block), True
    )

    def local_delta(query, key, values, beta, logdecay):
        return run_heads(query, key, values, beta, logdecay, start_state)

    recomputed, delta_back = jax.vjp(local_delta, query_h, key_h, value_h, beta_h, decay_h)
    feature_grads = delta_back((grad_core_h, suffix[1]))
    grad_ext, grad_beta_in, grad_decay_in, grad_conv, grad_rate = prep_back(feature_grads)
    returned = from_behind(grad_ext[:, :reach, :], "dp", -1)
    grad_mixed_pre = grad_ext[:, reach:, :] + jnp.pad(returned, ((0, 0), (seg - reach, 0), (0, 0)))
    grad_mixed_pre = grad_mixed_pre.reshape(count, -1)
    grad_query_low = grad_mixed_pre[:, :qk_width].astype(bf)
    grad_key_low = grad_mixed_pre[:, qk_width : 2 * qk_width].astype(bf)
    grad_value_low = grad_mixed_pre[:, 2 * qk_width :].astype(bf)
    grad_gate_low = grad_gate4.reshape(count, heads * value_dim).astype(bf)
    grad_beta_low = grad_beta_in.reshape(count, heads).astype(bf)
    grad_decay_low = grad_decay_in.reshape(count, heads).astype(bf)
    partial_hidden1 = (
        back_project(grad_query_low, w_query)
        + back_project(grad_key_low, w_key)
        + back_project(grad_value_low, w_value)
        + back_project(grad_gate_low, w_gate)
        + back_project(grad_beta_low, w_beta)
        + back_project(grad_decay_low, w_decay)
    )
    grad_hidden1 = lax.psum(partial_hidden1, "tensor")
    grad_from_norm1, grad_norm1_gain = norm1_back(grad_hidden1)
    grad_inputs = (grad_resid1 + grad_from_norm1).reshape(batch, seg, width)
    grad_query_w = contract_rows(hidden1, grad_query_low)
    grad_key_w = contract_rows(hidden1, grad_key_low)
    grad_value_w = contract_rows(hidden1, grad_value_low)
    grad_gate_w = contract_rows(hidden1, grad_gate_low)
    grad_beta_w = contract_rows(hidden1, grad_beta_low)
    grad_decay_w = contract_rows(hidden1, grad_decay_low)
    grad_convq = grad_conv[:, :qk_width]
    grad_convk = grad_conv[:, qk_width : 2 * qk_width]
    grad_convv = grad_conv[:, 2 * qk_width :]
    grad_head_flat = grad_head_gain.reshape(-1)
    (
        grad_norm1_gain,
        grad_query_w,
        grad_key_w,
        grad_value_w,
        grad_gate_w,
        grad_beta_w,
        grad_decay_w,
        grad_rate,
        grad_convq,
        grad_convk,
        grad_convv,
        grad_head_flat,
        grad_out_w,
        grad_norm2_gain,
        grad_ffn_gate_w,
        grad_ffn_up_w,
        grad_down,
    ) = lax.psum(
        (
            grad_norm1_gain,
            grad_query_w,
            grad_key_w,
            grad_value_w,
            grad_gate_w,
            grad_beta_w,
            grad_decay_w,
            grad_rate,
            grad_convq,
            grad_convk,
            grad_convv,
            grad_head_flat,
            grad_out_w,
            grad_norm2_gain,
            grad_ffn_gate_w,
            grad_ffn_up_w,
            grad_down,
        ),
        "dp",
    )
    return (
        output,
        grad_inputs,
        grad_norm1_gain,
        grad_query_w,
        grad_key_w,
        grad_value_w,
        grad_gate_w,
        grad_beta_w,
        grad_decay_w,
        grad_rate,
        grad_convq,
        grad_convk,
        grad_convv,
        grad_head_flat,
        grad_out_w,
        grad_norm2_gain,
        grad_ffn_gate_w,
        grad_ffn_up_w,
        grad_down,
    )


HALO = 8


def mm(left, right):
    return lax.dot_general(
        left, right, (((1,), (0,)), ((), ())),
        precision=lax.Precision.HIGHEST, preferred_element_type=jnp.float32,
    )


def mm_nt(left, right):
    return lax.dot_general(
        left, right, (((1,), (1,)), ((), ())),
        precision=lax.Precision.HIGHEST, preferred_element_type=jnp.float32,
    )


def mm_tn(left, right):
    return lax.dot_general(
        left, right, (((0,), (0,)), ((), ())),
        precision=lax.Precision.HIGHEST, preferred_element_type=jnp.float32,
    )


def grids(count):
    rows = lax.broadcasted_iota(jnp.int32, (count, count), 0)
    cols = lax.broadcasted_iota(jnp.int32, (count, count), 1)
    return rows, cols


def unit_inverse(lower, rows, cols):
    count = lower.shape[0]
    near = (rows // 2 == cols // 2) & (rows > cols)
    inverse = jnp.where(rows == cols, 1.0, jnp.where(near, -lower, 0.0))
    block = 2
    while block < count:
        cross = (rows // (2 * block) == cols // (2 * block)) & (rows // block > cols // block)
        inverse = inverse - mm(mm(inverse, jnp.where(cross, lower, 0.0)), inverse)
        block *= 2
    return inverse


def conv_window(halo_block, taps, span):
    reach = taps.shape[0] - 1
    total = None
    for offset in range(reach + 1):
        start = HALO - reach + offset
        term = taps[offset : offset + 1] * halo_block[start : start + span]
        total = term if total is None else total + term
    return total


def sigmoid(value):
    return 1.0 / (1.0 + jnp.exp(-value))


def softplus(value):
    return jnp.maximum(value, 0.0) + jnp.log(1.0 + jnp.exp(-jnp.abs(value)))


def gates_of(small, rate, heads, rows, cols):
    beta = sigmoid(small)
    slope = softplus(small)
    logdecay = -rate * slope
    cumul = mm(jnp.where(cols <= rows, 1.0, 0.0), logdecay)
    return beta, slope, logdecay, cumul


def chunk_terms(query, key, beta_col, beta_row, cum_col, cum_row, rows, cols):
    within = cols <= rows
    decays = jnp.where(within, jnp.exp(jnp.where(within, cum_col - cum_row, 0.0)), 0.0)
    scaled = decays * beta_row
    key_key = mm_nt(key, key)
    query_key = mm_nt(query, key)
    lower = jnp.where(cols < rows, scaled * key_key, 0.0)
    attend = scaled * query_key
    return decays, scaled, key_key, query_key, lower, attend


def forward_kernel(heads, key_dim, value_dim, pre_ref, gate_ref, small_ref, taps_ref, rate_ref, gain_ref,
                   mixed_ref, core_ref, update_ref, state_ref, inverse_ref, pad_ref, now_ref):
    length, width = pre_ref.shape
    span = SPAN
    chunks = length // span
    rows, cols = grids(span)
    qk = heads * key_dim
    pad_ref[0:HALO] = jnp.zeros((HALO, width), jnp.float32)
    for head in range(heads):
        now_ref[head] = jnp.zeros((key_dim, value_dim), jnp.float32)

    def chunk(index, carry):
        start = pl.multiple_of(index * span, span)
        here = pl.ds(start, span)
        pad_ref[HALO : HALO + span] = pre_ref[here, :]
        total = conv_window(pad_ref[...], taps_ref[...], span)
        pad_ref[0:HALO] = pad_ref[span : span + HALO]
        active = total * sigmoid(total)
        beta, _, _, cumul = gates_of(small_ref[here, :], rate_ref[...], heads, rows, cols)
        beta_t = jnp.transpose(beta)
        cumul_t = jnp.transpose(cumul)
        gate = gate_ref[here, :]
        gated = gate * sigmoid(gate) * gain_ref[...]
        for head in range(heads):
            query = active[:, head * key_dim : (head + 1) * key_dim]
            query = query * (lax.rsqrt(jnp.sum(query * query, -1, keepdims=True) + EPS) * key_dim ** (-0.5))
            key = active[:, qk + head * key_dim : qk + (head + 1) * key_dim]
            key = key * lax.rsqrt(jnp.sum(key * key, -1, keepdims=True) + EPS)
            value = active[:, 2 * qk + head * value_dim : 2 * qk + (head + 1) * value_dim]
            beta_col = beta[:, head : head + 1]
            beta_row = beta_t[head : head + 1]
            cum_col = cumul[:, heads + head : heads + head + 1]
            cum_row = cumul_t[heads + head : heads + head + 1]
            _, _, _, _, lower, attend = chunk_terms(query, key, beta_col, beta_row, cum_col, cum_row, rows, cols)
            inverse = unit_inverse(lower, rows, cols)
            state = now_ref[head]
            state_ref[index, head] = state
            rise = jnp.exp(cum_col)
            last = cum_col[span - 1 : span]
            update = mm(inverse, value) - mm(mm(inverse, rise * key), state)
            core = mm(rise * query, state) + mm(attend, update)
            tail = jnp.exp(last - cum_col) * beta_col
            now_ref[head] = jnp.exp(last) * state + mm_tn(key * tail, update)
            inverse_ref[index, head] = inverse
            wide = slice(head * value_dim, (head + 1) * value_dim)
            update_ref[here, wide] = update
            core_ref[here, wide] = core
            normed = core * lax.rsqrt(jnp.mean(core * core, -1, keepdims=True) + EPS)
            mixed_ref[here, wide] = (normed * gated[:, wide]).astype(mixed_ref.dtype)
        return carry

    lax.fori_loop(0, chunks, chunk, 0)


def delta_forward(pre, gate, small, taps, rate, gain, heads, key_dim, value_dim):
    length, width = pre.shape
    chunks = length // SPAN
    out_shape = (
        jax.ShapeDtypeStruct((length, heads * value_dim), jnp.bfloat16),
        jax.ShapeDtypeStruct((length, heads * value_dim), jnp.float32),
        jax.ShapeDtypeStruct((length, heads * value_dim), jnp.float32),
        jax.ShapeDtypeStruct((chunks, heads, key_dim, value_dim), jnp.float32),
        jax.ShapeDtypeStruct((chunks, heads, SPAN, SPAN), jnp.float32),
    )
    return pl.pallas_call(
        functools.partial(forward_kernel, heads, key_dim, value_dim),
        out_shape=out_shape,
        scratch_shapes=[
            pltpu.VMEM((HALO + SPAN, width), jnp.float32),
            pltpu.VMEM((heads, key_dim, value_dim), jnp.float32),
        ],
        compiler_params=pltpu.CompilerParams(vmem_limit_bytes=56 << 20),
        name="delta_forward",
    )(pre, gate, small, taps, rate, gain)


def backward_start(refs, span):
    (_, _, _, _, _, _, _, _, _, _, _, _, _, _, taps_grad_ref, gain_grad_ref, rate_grad_ref,
     _, pad_ref, now_ref) = refs
    now_ref[...] = jnp.zeros_like(now_ref)
    pad_ref[span : span + HALO] = jnp.zeros((HALO, pad_ref.shape[1]), jnp.float32)
    taps_grad_ref[...] = jnp.zeros_like(taps_grad_ref)
    gain_grad_ref[...] = jnp.zeros_like(gain_grad_ref)
    rate_grad_ref[...] = jnp.zeros_like(rate_grad_ref)


def backward_chunk(heads, key_dim, value_dim, index, refs):
    (pre_ref, gate_ref, small_ref, taps_ref, rate_ref, gain_ref,
     core_ref, update_ref, state_ref, inverse_ref, grad_ref,
     low_ref, gate_low_ref, small_low_ref, taps_grad_ref, gain_grad_ref, rate_grad_ref,
     ahead_ref, pad_ref, now_ref) = refs
    width = taps_ref.shape[1]
    span = SPAN
    rows, cols = grids(span)
    qk = heads * key_dim
    reach = taps_ref.shape[0] - 1
    lanes = small_ref.shape[1]
    lane = lax.broadcasted_iota(jnp.int32, (span, lanes), 1)
    start = pl.multiple_of(index * span, span)
    here = pl.ds(start, span)
    before = pl.ds(pl.multiple_of(jnp.maximum(start - HALO, 0), HALO), HALO)
    ahead_ref[0:HALO] = pre_ref[before, :] * jnp.where(index > 0, 1.0, 0.0)
    ahead_ref[HALO : HALO + span] = pre_ref[here, :]
    total = conv_window(ahead_ref[...], taps_ref[...], span)
    gain_of = sigmoid(total)
    active = total * gain_of
    bend = gain_of * (1.0 + total * (1.0 - gain_of))
    small = small_ref[here, :]
    beta, slope, _, cumul = gates_of(small, rate_ref[...], heads, rows, cols)
    beta_t = jnp.transpose(beta)
    cumul_t = jnp.transpose(cumul)
    gate = gate_ref[here, :]
    gate_sig = sigmoid(gate)
    gate_silu = gate * gate_sig
    gate_bend = gate_sig * (1.0 + gate * (1.0 - gate_sig))
    small_grad = jnp.zeros((span, lanes), jnp.float32)
    for head in range(heads):
        wide = slice(head * value_dim, (head + 1) * value_dim)
        core = core_ref[here, wide]
        grad_mixed = grad_ref[here, wide]
        gain = gain_ref[:, wide]
        scale = lax.rsqrt(jnp.mean(core * core, -1, keepdims=True) + EPS)
        normed = core * scale
        gate_low_ref[here, wide] = (grad_mixed * normed * gain * gate_bend[:, wide]).astype(gate_low_ref.dtype)
        with_gate = grad_mixed * gate_silu[:, wide]
        gain_grad_ref[:, wide] += jnp.sum(with_gate * normed, 0, keepdims=True)
        grad_normed = with_gate * gain
        grad_core = scale * (grad_normed - normed * jnp.mean(grad_normed * normed, -1, keepdims=True))
        query_act = active[:, head * key_dim : (head + 1) * key_dim]
        query_scale = lax.rsqrt(jnp.sum(query_act * query_act, -1, keepdims=True) + EPS)
        query = query_act * (query_scale * key_dim ** (-0.5))
        key_act = active[:, qk + head * key_dim : qk + (head + 1) * key_dim]
        key_scale = lax.rsqrt(jnp.sum(key_act * key_act, -1, keepdims=True) + EPS)
        key = key_act * key_scale
        beta_col = beta[:, head : head + 1]
        beta_row = beta_t[head : head + 1]
        cum_col = cumul[:, heads + head : heads + head + 1]
        cum_row = cumul_t[heads + head : heads + head + 1]
        decays, scaled, key_key, query_key, lower, attend = chunk_terms(
            query, key, beta_col, beta_row, cum_col, cum_row, rows, cols
        )
        state = state_ref[index, head]
        update = update_ref[here, wide]
        inverse = inverse_ref[index, head]
        grad_state = now_ref[head]
        rise = jnp.exp(cum_col)
        last = cum_col[span - 1 : span]
        fall = jnp.exp(last - cum_col)
        tail = fall * beta_col
        rise_query = rise * query
        rise_key = rise * key
        grad_update = mm_tn(attend, grad_core) + mm(key * tail, grad_state)
        grad_right = mm_tn(inverse, grad_update)
        now_ref[head] = jnp.exp(last) * grad_state + mm_tn(rise_query, grad_core) - mm_tn(rise_key, grad_right)
        grad_attend = jnp.where(cols <= rows, mm_nt(grad_core, update), 0.0)
        grad_lower = jnp.where(cols < rows, -mm_nt(grad_right, update), 0.0)
        core_state = mm_nt(grad_core, state)
        right_state = mm_nt(grad_right, state)
        grad_tail_key = mm_nt(update, grad_state)
        pair_query = grad_attend * scaled
        pair_key = grad_lower * scaled
        grad_query = rise * core_state + mm(pair_query, key)
        grad_key = (
            grad_tail_key * tail - rise * right_state + mm_tn(pair_query, query)
            + mm(pair_key, key) + mm_tn(pair_key, key)
        )
        grad_tail = jnp.sum(grad_tail_key * key, -1, keepdims=True)
        moved = grad_attend * query_key + grad_lower * key_key
        spread = moved * scaled
        by_row = jnp.sum(spread, -1, keepdims=True)
        sums = mm_tn(
            jnp.concatenate([moved * decays, spread], 1), jnp.ones((span, lanes), jnp.float32)
        )
        grad_beta = sums[:span, 0:1] + grad_tail * fall
        through_tail = grad_tail * tail
        grad_cum = (
            by_row - sums[span:, 0:1] - through_tail
            + rise * (jnp.sum(core_state * query, -1, keepdims=True) - jnp.sum(right_state * key, -1, keepdims=True))
        )
        end_grad = jnp.sum(through_tail, 0, keepdims=True) + jnp.exp(last) * jnp.sum(
            jnp.sum(state * grad_state, -1, keepdims=True), 0, keepdims=True
        )
        grad_cum = grad_cum + jnp.where(rows[:, 0:1] == span - 1, end_grad, 0.0)
        small_grad = small_grad + jnp.where(lane == head, grad_beta, 0.0)
        small_grad = small_grad + jnp.where(lane == heads + head, grad_cum, 0.0)
        grad_query = grad_query * key_dim ** (-0.5)
        unit = query_act * query_scale
        grad_query = query_scale * (grad_query - unit * jnp.sum(grad_query * unit, -1, keepdims=True))
        grad_key = key_scale * (grad_key - key * jnp.sum(grad_key * key, -1, keepdims=True))
        at = slice(head * key_dim, (head + 1) * key_dim)
        pad_ref[0:span, at] = grad_query * bend[:, at]
        at = slice(qk + head * key_dim, qk + (head + 1) * key_dim)
        pad_ref[0:span, at] = grad_key * bend[:, at]
        at = slice(2 * qk + head * value_dim, 2 * qk + (head + 1) * value_dim)
        pad_ref[0:span, at] = grad_right * bend[:, at]
    summed = mm(jnp.where(cols >= rows, 1.0, 0.0), small_grad)
    is_beta = lane < heads
    rate_grad_ref[...] += jnp.sum(jnp.where(is_beta, 0.0, -slope * summed), 0, keepdims=True)
    sig = beta
    small_low_ref[here, :] = jnp.where(
        is_beta, small_grad * sig * (1.0 - sig), -rate_ref[...] * sig * summed
    ).astype(small_low_ref.dtype)
    outer = pad_ref[...]
    dense = outer[0:span]
    block = ahead_ref[...]
    grad_pre = None
    for offset in range(reach + 1):
        behind = reach - offset
        taps_grad_ref[offset : offset + 1] += jnp.sum(
            dense * block[HALO - behind : HALO - behind + span], 0, keepdims=True
        )
        term = taps_ref[offset : offset + 1] * outer[behind : behind + span]
        grad_pre = term if grad_pre is None else grad_pre + term
    low_ref[here, :] = grad_pre.astype(low_ref.dtype)
    pad_ref[span : span + HALO] = pad_ref[0:HALO]


MESH = pl.DeviceIdType.MESH
VM = pl.BlockSpec(memory_space=pltpu.VMEM)


def greet(peers):
    barrier = pltpu.get_barrier_semaphore()
    for peer in peers:
        pl.semaphore_signal(barrier, inc=1, device_id=peer, device_id_type=MESH)
    pl.semaphore_wait(barrier, len(peers))


def remote(src, dst, send, recv, peer):
    return pltpu.make_async_remote_copy(
        src_ref=src, dst_ref=dst, send_sem=send, recv_sem=recv, device_id=peer, device_id_type=MESH
    )


def tensor_peers():
    dp = lax.axis_index("dp")
    t = lax.axis_index("tensor")
    core = lax.rem(t, 2)
    mate = (dp, t + 1 - 2 * core)
    across = (dp, lax.rem(t + 2, 4))
    return core, mate, across


def psum_kernel(blocks, part_ref, out_ref, land_mate, land_across, half, send, recv):
    core, mate, across = tensor_peers()
    greet((mate, across))
    rows = part_ref.shape[0] // blocks
    part = rows // 2
    first = []
    for b in range(blocks):
        theirs = pl.ds(pl.multiple_of(b * rows + (1 - core) * part, part), part)
        copy = remote(part_ref.at[theirs], land_mate.at[pl.ds(b * part, part)], send.at[0, b], recv.at[0, b], mate)
        copy.start()
        first.append(copy)
    second = []
    for b in range(blocks):
        mine = pl.ds(pl.multiple_of(b * rows + core * part, part), part)
        slot = pl.ds(b * part, part)
        first[b].wait_recv()
        half[slot] = part_ref[mine] + land_mate[slot]
        copy = remote(half.at[slot], land_across.at[slot], send.at[1, b], recv.at[1, b], across)
        copy.start()
        second.append(copy)
    third = []
    for b in range(blocks):
        mine = pl.ds(pl.multiple_of(b * rows + core * part, part), part)
        slot = pl.ds(b * part, part)
        second[b].wait_recv()
        out_ref[mine] = half[slot] + land_across[slot]
        copy = remote(out_ref.at[mine], out_ref.at[mine], send.at[2, b], recv.at[2, b], mate)
        copy.start()
        third.append(copy)
    for b in range(blocks):
        third[b].wait_recv()
    for b in range(blocks):
        first[b].wait_send()
        second[b].wait_send()
        third[b].wait_send()


def tensor_sum(part, collective_id, blocks=8):
    rows, width = part.shape
    return pl.pallas_call(
        functools.partial(psum_kernel, blocks),
        out_shape=jax.ShapeDtypeStruct(part.shape, part.dtype),
        in_specs=[VM],
        out_specs=VM,
        scratch_shapes=[pltpu.VMEM((rows // 2, width), part.dtype)] * 3
        + [pltpu.SemaphoreType.DMA((3, blocks))] * 2,
        compiler_params=pltpu.CompilerParams(
            collective_id=collective_id, has_side_effects=True, vmem_limit_bytes=40 << 20
        ),
        name="tensor_sum",
    )(part)


def swap_kernel(count, narrow, *refs):
    sources, results = refs[:count], refs[count : 2 * count]
    staged, send, recv, close_send, close_recv = refs[2 * count :]
    n = lax.axis_size("dp")
    me = lax.axis_index("dp")
    t = lax.axis_index("tensor")
    core, mate, across = tensor_peers()
    ranks = lax.axis_size("tensor")
    others = [lax.rem(me + k, n) for k in range(1, n)]
    greet([(other, t) for other in others] + [mate, across])
    seg = results[0].shape[0] // n
    part = seg // ranks
    far = lax.rem(t + 2, ranks)

    def at(place, rank):
        return pl.ds(pl.multiple_of(place * seg + rank * part, part), part)

    outgoing = []
    for i in range(count):
        for k in range(n):
            other = lax.rem(me + k, n)
            if k == 0:
                results[i][at(me, t)] = sources[i][at(me, t)].astype(jnp.float32)
                continue
            if narrow[i]:
                staged[i, k] = sources[i][at(other, t)].astype(jnp.float32)
                src = staged.at[i, k]
            else:
                src = sources[i].at[at(other, t)]
            copy = remote(src, results[i].at[at(me, t)], send.at[i, k], recv.at[i, k], (other, t))
            copy.start()
            outgoing.append(copy)
    close = []
    for i in range(count):
        for k in range(n):
            source = lax.rem(me + n - k, n)
            here = results[i].at[at(source, t)]
            if k:
                remote(here, here, send.at[i, k], recv.at[i, k], (source, t)).wait_recv()
            over = remote(here, here, close_send.at[0, i, k], close_recv.at[0, i, k], across)
            over.start()
            beside = remote(here, here, close_send.at[1, i, k], close_recv.at[1, i, k], mate)
            beside.start()
            close += [over, beside]
    last = []
    for i in range(count):
        for k in range(n):
            source = lax.rem(me + n - k, n)
            there = results[i].at[at(source, far)]
            remote(there, there, close_send.at[0, i, k], close_recv.at[0, i, k], across).wait_recv()
            copy = remote(there, there, close_send.at[2, i, k], close_recv.at[2, i, k], mate)
            copy.start()
            last.append(copy)
    for copy in outgoing:
        copy.wait_send()
    for j, copy in enumerate(close):
        copy.wait_send()
        if j % 2:
            copy.wait_recv()
    for copy in last:
        copy.wait()


def swap(arrays, n, collective_id):
    count = len(arrays)
    rows, width = arrays[0].shape
    narrow = [a.dtype != jnp.float32 for a in arrays]
    out = pl.pallas_call(
        functools.partial(swap_kernel, count, narrow),
        out_shape=[jax.ShapeDtypeStruct((rows, width), jnp.float32)] * count,
        in_specs=[VM] * count,
        out_specs=[VM] * count,
        scratch_shapes=[pltpu.VMEM((count, n, rows // n // 4, width), jnp.float32)]
        + [pltpu.SemaphoreType.DMA((count, n))] * 2
        + [pltpu.SemaphoreType.DMA((3, count, n))] * 2,
        compiler_params=pltpu.CompilerParams(
            collective_id=collective_id, has_side_effects=True, vmem_limit_bytes=40 << 20
        ),
        name="swap",
    )(*arrays)
    return out


SLOT = 64
DEPTH = 12
LAG = 1


def grid_place():
    n = lax.axis_size("dp")
    me = lax.axis_index("dp")
    t = lax.axis_index("tensor")
    lines = n // 2
    z = lax.div(me, 2)
    x = lax.rem(me, 2)
    return n, lines, me, t, z, x


def grid_greet(extra=()):
    n, lines, me, t, z, x = grid_place()
    barrier = pltpu.get_barrier_semaphore()
    pl.semaphore_signal(barrier, inc=1, device_id=(me + 1 - 2 * x, t), device_id_type=MESH)
    for peer in extra:
        pl.semaphore_signal(barrier, inc=1, device_id=peer, device_id_type=MESH)

    @pl.when(z > 0)
    def _():
        pl.semaphore_signal(barrier, inc=1, device_id=(me - 2, t), device_id_type=MESH)

    @pl.when(z < lines - 1)
    def _():
        pl.semaphore_signal(barrier, inc=1, device_id=(me + 2, t), device_id_type=MESH)

    pl.semaphore_wait(
        barrier, 1 + len(extra) + jnp.where(z > 0, 1, 0) + jnp.where(z < lines - 1, 1, 0)
    )


def reduce_slot(slot, chunks, data, land_x, land_z, outgo, aside, sems):
    n, lines, me, t, z, x = grid_place()
    mate = (me + 1 - 2 * x, t)
    send_x, recv_x, send_z, recv_z, send_d, recv_d, send_p, recv_p = [sems.at[i] for i in range(8)]
    top = lines - 1

    def ring(chunk):
        return lax.rem(chunk, DEPTH)

    def within(chunk):
        return (chunk >= 0) & (chunk < chunks)

    for stream in range(4):
        split = stream < 2
        up = stream % 2 == 0
        level = z if up else top - z
        after = (me + 2, t) if up else (me - 2, t)
        prior = (me - 2, t) if up else (me + 2, t)
        size = 8 if split else 16
        offset = 16 * stream

        def rows(chunk, side):
            base = chunk * SLOT + offset + (side * 8 if split else 0)
            return pl.ds(pl.multiple_of(base, 8), size)

        def spot(ref, chunk):
            return ref.at[stream, ring(chunk), 0:size]

        def to_mate(chunk, src):
            return remote(
                src, spot(land_x, chunk), send_x.at[stream, ring(chunk)], recv_x.at[stream, ring(chunk)], mate
            )

        def to_after(chunk):
            return remote(
                spot(outgo, chunk), spot(land_z, chunk),
                send_z.at[stream, ring(chunk)], recv_z.at[stream, ring(chunk)], after,
            )

        def to_prior(chunk):
            here = data.at[rows(chunk, x)]
            return remote(here, here, send_d.at[stream, ring(chunk)], recv_d.at[stream, ring(chunk)], prior)

        def from_after(chunk):
            here = data.at[rows(chunk, x)]
            return remote(here, here, send_d.at[stream, ring(chunk)], recv_d.at[stream, ring(chunk)], after)

        def close(chunk, side):
            here = data.at[rows(chunk, side)]
            return remote(here, here, send_p.at[stream, ring(chunk)], recv_p.at[stream, ring(chunk)], mate)

        def give_back(chunk):
            @pl.when(level > 0)
            def _():
                to_prior(chunk).start()

            if split:
                close(chunk, x).start()

        if split:
            @pl.when(slot < chunks)
            def _():
                aside[stream, ring(slot)] = data[rows(slot, 1 - x)]
                to_mate(slot, aside.at[stream, ring(slot)]).start()

        rise = slot - LAG * (1 + level)

        @pl.when(within(rise))
        def _():
            here = rows(rise, x)
            if split:
                to_mate(rise, aside.at[stream, ring(rise)]).wait_recv()

            def first():
                own = data[here]
                return own + land_x[stream, ring(rise), 0:size] if split else own

            @pl.when(level > 0)
            def _():
                to_after(rise).wait_recv()
                outgo[stream, ring(rise), 0:size] = first() + land_z[stream, ring(rise), 0:size]

            @pl.when(level == 0)
            def _():
                outgo[stream, ring(rise), 0:size] = first()

            @pl.when(level < top)
            def _():
                to_after(rise).start()

            @pl.when(level == top)
            def _():
                if split:
                    data[here] = outgo[stream, ring(rise), 0:size]
                    give_back(rise)
                else:
                    to_mate(rise, spot(outgo, rise)).start()

        if not split:
            meet = slot - LAG * (2 + top)

            @pl.when(within(meet) & (level == top))
            def _():
                to_mate(meet, spot(outgo, meet)).wait_recv()
                data[rows(meet, x)] = outgo[stream, ring(meet), 0:size] + land_x[stream, ring(meet), 0:size]
                give_back(meet)

        extra = 0 if split else 1
        fall = slot - LAG * (1 + extra + 2 * top - level)

        @pl.when(within(fall) & (level < top))
        def _():
            from_after(fall).wait_recv()
            to_after(fall).wait_send()
            give_back(fall)

        done = fall - LAG

        @pl.when(within(done))
        def _():
            @pl.when(level > 0)
            def _():
                to_prior(done).wait_send()

            if split:
                close(done, x).wait_send()
                close(done, 1 - x).wait_recv()
                to_mate(done, aside.at[stream, ring(done)]).wait_send()
            else:
                @pl.when(level == top)
                def _():
                    to_mate(done, spot(outgo, done)).wait_send()


def slots_of(chunks, lines):
    return chunks + LAG * (2 * lines + 1)


def reduce_scratch(width):
    return [
        pltpu.VMEM((4, DEPTH, 16, width), jnp.float32),
        pltpu.VMEM((4, DEPTH, 16, width), jnp.float32),
        pltpu.VMEM((4, DEPTH, 16, width), jnp.float32),
        pltpu.VMEM((2, DEPTH, 8, width), jnp.float32),
        pltpu.SemaphoreType.DMA((8, 4, DEPTH)),
    ]


def reduce_kernel(part_ref, out_ref, land_x, land_z, outgo, aside, sems):
    grid_greet()
    chunks = part_ref.shape[0] // SLOT

    def take(i, carry):
        at = pl.ds(pl.multiple_of(i * SLOT, SLOT), SLOT)
        out_ref[at] = part_ref[at]
        return carry

    lax.fori_loop(0, chunks, take, 0)

    def step(slot, carry):
        reduce_slot(slot, chunks, out_ref, land_x, land_z, outgo, aside, sems)
        return carry

    lax.fori_loop(0, slots_of(chunks, lax.axis_size("dp") // 2), step, 0)


def plane_sum(part, collective_id):
    rows, width = part.shape
    return pl.pallas_call(
        reduce_kernel,
        out_shape=jax.ShapeDtypeStruct(part.shape, part.dtype),
        in_specs=[VM],
        out_specs=VM,
        scratch_shapes=reduce_scratch(width),
        compiler_params=pltpu.CompilerParams(
            collective_id=collective_id, has_side_effects=True, vmem_limit_bytes=60 << 20
        ),
        name="plane_sum",
    )(part)


BLOCKS = 8


def dot_plain(left, right):
    return lax.dot_general(left, right, (((1,), (0,)), ((), ())), preferred_element_type=jnp.float32)


def dot_nt(left, right):
    return lax.dot_general(left, right, (((1,), (1,)), ((), ())), preferred_element_type=jnp.float32)


def dot_tn(left, right):
    return lax.dot_general(left, right, (((0,), (0,)), ((), ())), preferred_element_type=jnp.float32)


def aligned(start, size):
    return pl.ds(pl.multiple_of(start, size), size)


class TensorSum:
    def __init__(self, part, total, land_mate, land_across, half, send, recv):
        self.core, self.mate, self.across = tensor_peers()
        self.part, self.total, self.half = part, total, half
        self.land_mate, self.land_across = land_mate, land_across
        self.send, self.recv = send, recv
        self.rows = part.shape[0] // BLOCKS
        self.size = self.rows // 2

    def span(self, block, side):
        return aligned(block * self.rows + side * self.size, self.size)

    def slot(self, block):
        return aligned(block * self.size, self.size)

    def first(self, block):
        return remote(
            self.part.at[self.span(block, 1 - self.core)], self.land_mate.at[self.slot(block)],
            self.send.at[0, block], self.recv.at[0, block], self.mate,
        )

    def second(self, block):
        return remote(
            self.half.at[self.slot(block)], self.land_across.at[self.slot(block)],
            self.send.at[1, block], self.recv.at[1, block], self.across,
        )

    def third(self, block):
        mine = self.total.at[self.span(block, self.core)]
        return remote(mine, mine, self.send.at[2, block], self.recv.at[2, block], self.mate)

    def start(self):
        for block in range(BLOCKS):
            self.first(block).start()

    def cross(self, block):
        self.first(block).wait_recv()
        slot = self.slot(block)
        self.half[slot] = self.part[self.span(block, self.core)] + self.land_mate[slot]
        self.second(block).start()

    def share(self, block):
        self.second(block).wait_recv()
        slot = self.slot(block)
        self.total[self.span(block, self.core)] = self.half[slot] + self.land_across[slot]
        self.third(block).start()

    def finish(self):
        for block in range(BLOCKS):
            self.third(block).wait_recv()
        for block in range(BLOCKS):
            self.first(block).wait_send()
            self.second(block).wait_send()
            self.third(block).wait_send()


class Swap:
    def __init__(self, source, result, send, recv, close_send, close_recv):
        self.n = lax.axis_size("dp")
        self.me = lax.axis_index("dp")
        self.t = lax.axis_index("tensor")
        self.ranks = lax.axis_size("tensor")
        _, self.mate, self.across = tensor_peers()
        self.source, self.result = source, result
        self.sems = send, recv, close_send, close_recv
        self.seg = result.shape[0] // self.n
        self.part = self.seg // self.ranks

    def at(self, place, rank):
        return aligned(place * self.seg + rank * self.part, self.part)

    def out(self, k):
        other = lax.rem(self.me + k, self.n)
        return remote(
            self.source.at[self.at(other, self.t)], self.result.at[self.at(self.me, self.t)],
            self.sems[0].at[k], self.sems[1].at[k], (other, self.t),
        )

    def close(self, k, leg):
        origin = lax.rem(self.me + self.n - k, self.n)
        rank = lax.rem(self.t + 2, self.ranks) if leg == 2 else self.t
        here = self.result.at[self.at(origin, rank)]
        return remote(
            here, here, self.sems[2].at[leg, k], self.sems[3].at[leg, k], self.across if leg == 0 else self.mate
        )

    def start(self):
        mine = self.at(self.me, self.t)
        self.result[mine] = self.source[mine]
        for k in range(1, self.n):
            self.out(k).start()

    def gather(self, k):
        @pl.when(k > 0)
        def _():
            self.out(k).wait_recv()

        self.close(k, 0).start()
        self.close(k, 1).start()

    def forward(self, k):
        self.close(k, 0).wait_recv()
        self.close(k, 2).start()

    def finish(self):
        for k in range(self.n):
            if k:
                self.out(k).wait_send()
            self.close(k, 0).wait_send()
            self.close(k, 1).wait()
            self.close(k, 2).wait()


def tail_kernel(
    heads, key_dim, value_dim, ranges, chunks,
    part2_hbm, ffn_hbm, wide_hbm, rest_hbm, down_hbm, pre_hbm, core_hbm, update_hbm,
    resid1_ref, upstream_ref, resid_ref, mixed_ref, hidden1_ref,
    w_out_ref, w_mix_ref, w_gate_ref, w_small_ref, norm1_ref, norm2_ref,
    gate_ref, small_ref, taps_ref, rate_ref, gain_ref, state_ref, inverse_ref,
    output_ref, inputs_grad_ref, wide_out, rest_out, down_out, out_out, gate_out,
    query_out, key_out, value_out, small_out,
    data, land_x, land_z, outgo, aside, sems,
    part, total, half, land_mate, land_across, sum_send, sum_recv,
    resid1_grad, resid1_low, mixed_grad, low, gate_low, small_low,
    taps_grad, gain_grad, rate_grad, norm1_grad, norm2_grad, ahead, pad, now,
    shuffled, swap_send, swap_recv, close_send, close_recv, load_sem, out_sem,
):
    n, lines, me, t, z, x = grid_place()
    _, mate, across = tensor_peers()
    length, width = resid1_ref.shape
    qk = heads * key_dim
    values = heads * value_dim
    at_wide, at_rest, at_down, at_out, at_gate, at_mix, at_small, rows_all = ranges
    loads = [
        (part2_hbm, part),
        (wide_hbm, data.at[pl.ds(at_wide, at_rest - at_wide)]),
        (rest_hbm, data.at[pl.ds(at_rest, at_down - at_rest)]),
        (down_hbm, data.at[pl.ds(at_down, at_out - at_down)]),
        (pre_hbm, data.at[pl.ds(at_mix, length)]),
        (core_hbm, data.at[pl.ds(at_mix + length, length), pl.ds(0, values)]),
        (update_hbm, data.at[pl.ds(at_mix + length, length), pl.ds(values, values)]),
    ]
    loads = [pltpu.make_async_copy(src, dst, load_sem.at[i]) for i, (src, dst) in enumerate(loads)]
    load_ffn = pltpu.make_async_copy(ffn_hbm, part, load_sem.at[len(loads)])
    for load in loads:
        load.start()
    greet([(lax.rem(me + k, n), t) for k in range(1, n)] + [mate, across])
    refs = (
        data.at[pl.ds(at_mix, length)], gate_ref, small_ref, taps_ref, rate_ref, gain_ref,
        data.at[pl.ds(at_mix + length, length), pl.ds(0, values)],
        data.at[pl.ds(at_mix + length, length), pl.ds(values, values)],
        state_ref, inverse_ref, mixed_grad, low, gate_low, small_low, taps_grad, gain_grad, rate_grad,
        ahead, pad, now,
    )
    sums = [
        TensorSum(part, total, land_mate, land_across.at[i % 2], half, sum_send.at[i], sum_recv.at[i]) for i in range(3)
    ]
    swaps = [
        Swap(source, result, swap_send.at[i], swap_recv.at[i], close_send.at[i], close_recv.at[i])
        for i, (source, result) in enumerate([(total, shuffled), (resid1_grad, inputs_grad_ref)])
    ]
    norm1_grad[...] = jnp.zeros_like(norm1_grad)
    norm2_grad[...] = jnp.zeros_like(norm2_grad)
    backward_start(refs, SPAN)
    loads[0].wait()
    sums[0].start()
    for load in loads[1:]:
        load.wait()

    def norm_back(value, grad, gain, gain_grad_ref):
        scale = lax.rsqrt(jnp.mean(value * value, -1, keepdims=True) + EPS)
        normed = value * scale
        gain_grad_ref[...] += jnp.sum(grad * normed, 0, keepdims=True)
        scaled = grad * gain
        return scale * (scaled - normed * jnp.mean(scaled * normed, -1, keepdims=True))

    def norm2_piece(i):
        here = aligned(i * 64, 64)
        grad = upstream_ref[here].astype(jnp.float32) + norm_back(
            resid1_ref[here], total[here], norm2_ref[...], norm2_grad
        )
        resid1_grad[here] = grad
        resid1_low[here] = grad.astype(jnp.bfloat16)

    def mixed_piece(i):
        tile = aligned(i * 256, 256)
        mixed_grad[:, tile] = dot_nt(resid1_low[...], w_out_ref[tile])

    def out_piece(i):
        tile = aligned(i * 256, 256)
        data[pl.ds(pl.multiple_of(at_out + i * 256, 64), 256)] = dot_tn(
            mixed_ref[:, tile], resid1_low[...]
        )

    def gate_piece(i):
        tile = aligned(i * 256, 256)
        half_rows = width // 2
        data[pl.ds(pl.multiple_of(at_gate + i * 256, 64), 256), 0:values] = dot_tn(hidden1_ref[:, tile], gate_low[...])
        other = aligned(half_rows + i * 256, 256)
        data[pl.ds(pl.multiple_of(at_gate + i * 256, 64), 256), values : 2 * values] = dot_tn(
            hidden1_ref[:, other], gate_low[...]
        )

    def mix_piece(i):
        tile = aligned(i * 256, 256)
        data[pl.ds(pl.multiple_of(at_mix + i * 256, 64), 256)] = dot_tn(hidden1_ref[:, tile], low[...])

    def hidden_piece(i):
        tile = aligned(i * 256, 256)
        part[:, tile] = (
            dot_nt(low[...], w_mix_ref[tile]) + dot_nt(gate_low[...], w_gate_ref[tile])
            + dot_nt(small_low[...], w_small_ref[tile])
        )

    def output_piece(i):
        here = aligned(i * 64, 64)
        total[here] = total[here] + resid1_ref[here]

    def round_piece(i):
        here = aligned(i * 64, 64)
        output_ref[here] = shuffled[here].astype(output_ref.dtype)

    def norm1_piece(i):
        here = aligned(i * 64, 64)
        resid1_grad[here] = resid1_grad[here] + norm_back(
            resid_ref[here].astype(jnp.float32), total[here], norm1_ref[...], norm1_grad
        )

    def small_piece():
        base = at_small
        data[base : rows_all] = jnp.zeros((rows_all - base, width), jnp.float32)
        data[base : base + 4] = taps_grad[...]
        data[base + 4 : base + 5] = norm1_grad[...]
        data[base + 5 : base + 6] = norm2_grad[...]
        data[base + 6 : base + 7, 0:values] = gain_grad[...]
        data[base + 6 : base + 7, values : values + rate_grad.shape[1]] = rate_grad[...]
        data[base + 8 : base + 16] = dot_tn(small_low[...], hidden1_ref[...])[0:8]

    def start_ffn():
        load_ffn.start()
        load_ffn.wait()
        sums[1].start()

    pieces = []

    def plan(first, count, each, run):
        pieces.append((first, count, each, run))
        return first + -(-count // each)

    at = plan(0, BLOCKS, 2, sums[0].cross)
    at = plan(at, BLOCKS, 2, sums[0].share)
    at = plan(at, 1, 1, lambda i: sums[0].finish())
    at = plan(at, length // 64, 2, norm2_piece)
    at = plan(at, values // 256, 1, mixed_piece)
    side = at
    at = plan(at, values // 256, 1, out_piece)
    at_ready_out = at
    at = plan(at, length // SPAN, 1, lambda i: backward_chunk(heads, key_dim, value_dim, length // SPAN - 1 - i, refs))
    side = plan(side, 1, 1, lambda i: start_ffn())
    side = plan(side, BLOCKS, 2, sums[1].cross)
    side = plan(side, BLOCKS, 2, sums[1].share)
    side = plan(side, 1, 1, lambda i: sums[1].finish())
    part_free = side
    side = plan(side, length // 64, 4, output_piece)
    side = plan(side, 1, 1, lambda i: swaps[0].start())
    side = plan(side, n, 2, swaps[0].gather)
    side = plan(side, n, 2, swaps[0].forward)
    side = plan(side, 1, 1, lambda i: swaps[0].finish())
    side = plan(side, length // 64, 4, round_piece)
    at = plan(at, width // 512, 1, gate_piece)
    at_ready_gate = at
    at = plan(at, width // 256, 1, mix_piece)
    at_ready_mix = at
    at = plan(max(at, part_free), width // 256, 1, hidden_piece)
    at = plan(max(at, side), 1, 1, lambda i: sums[2].start())
    at = plan(at, BLOCKS, 2, sums[2].cross)
    at = plan(at, BLOCKS, 2, sums[2].share)
    at = plan(at, 1, 1, lambda i: sums[2].finish())
    at = plan(at, length // 64, 2, norm1_piece)
    at = plan(at, 1, 1, lambda i: small_piece())
    at_ready_small = at
    at = plan(at, 1, 1, lambda i: swaps[1].start())
    at = plan(at, n, 2, swaps[1].gather)
    at = plan(at, n, 2, swaps[1].forward)
    at = plan(at, 1, 1, lambda i: swaps[1].finish())
    assert at_ready_out <= at_out // SLOT and at_ready_gate <= at_gate // SLOT
    assert at_ready_mix <= at_mix // SLOT and at_ready_small <= at_small // SLOT
    delay = 2 * lines + 1
    last = max(chunks + delay + 1, at)

    def writes(chunk, act):
        row = chunk * SLOT

        def put(sem, src_cols, dst, start):
            rows = pl.ds(pl.multiple_of(row, SLOT), SLOT)
            src = data.at[rows] if src_cols is None else data.at[rows, pl.ds(*src_cols)]
            copy = pltpu.make_async_copy(src, dst.at[pl.ds(pl.multiple_of(row - start, SLOT), SLOT)], out_sem.at[sem])
            copy.start() if act == "start" else copy.wait()

        def segment(low_row, high_row, run):
            @pl.when((row >= low_row) & (row < high_row))
            def _():
                run()

        segment(at_wide, at_rest, lambda: put(0, None, wide_out, at_wide))
        segment(at_rest, at_down, lambda: put(0, None, rest_out, at_rest))
        segment(at_down, at_out, lambda: put(0, None, down_out, at_down))
        segment(at_out, at_gate, lambda: put(0, None, out_out, at_out))

        def gates():
            put(0, (0, values), gate_out, at_gate)
            put(1, (values, values), gate_out, at_gate - width // 2)

        segment(at_gate, at_mix, gates)

        def mixes():
            put(0, (0, qk), query_out, at_mix)
            put(1, (qk, qk), key_out, at_mix)
            put(2, (2 * qk, values), value_out, at_mix)

        segment(at_mix, at_small, mixes)
        segment(at_small, rows_all, lambda: put(0, None, small_out, at_small))

    def step(slot, carry):
        reduce_slot(slot, chunks, data, land_x, land_z, outgo, aside, sems)
        writes(slot - delay - 1, "wait")
        writes(slot - delay, "start")
        for first, count, each, run in pieces:
            steps = -(-count // each)

            @pl.when((slot >= first) & (slot < first + steps))
            def _(first=first, each=each, run=run):
                if each == 1:
                    run(slot - first)
                else:
                    def inner(i, carry):
                        run((slot - first) * each + i)
                        return carry

                    lax.fori_loop(0, each, inner, 0)

        return carry

    lax.fori_loop(0, last + 1, step, 0)


def tail(
    part2, ffn, wide, rest, down, pre, core, update, resid1, upstream, resid, mixed, hidden1,
    w_out, w_mix, w_gate, w_small, norm1, norm2, gate, small, taps, rate, gain, states, inverses,
    heads, key_dim, value_dim, places, collective_id,
):
    length, width = resid1.shape
    values = heads * value_dim
    qk = heads * key_dim
    lanes = small.shape[1]
    heights = [wide.shape[0], rest.shape[0], down.shape[0], values, values, width, SLOT]
    ranges = [0]
    for height in heights:
        ranges.append(ranges[-1] + height)
    rows_all = ranges[-1]
    chunks = rows_all // SLOT
    f32, bf = jnp.float32, jnp.bfloat16
    shape = jax.ShapeDtypeStruct
    out_shape = [
        shape((length, width), bf),
        shape((length, width), f32),
        shape(wide.shape, f32),
        shape(rest.shape, f32),
        shape(down.shape, f32),
        shape((values, width), f32),
        shape((width, values), f32),
        shape((width, qk), f32),
        shape((width, qk), f32),
        shape((width, values), f32),
        shape((SLOT, width), f32),
    ]
    vmem, any_ = VM, pl.BlockSpec(memory_space=pl.ANY)
    dma = pltpu.SemaphoreType.DMA
    scratch = (
        [pltpu.VMEM((rows_all, width), f32)]
        + reduce_scratch(width)
        + [
            pltpu.VMEM((length, width), f32),
            pltpu.VMEM((length, width), f32),
            pltpu.VMEM((length // 2, width), f32),
            pltpu.VMEM((length // 2, width), f32),
            pltpu.VMEM((2, length // 2, width), f32),
            dma((3, 3, BLOCKS)),
            dma((3, 3, BLOCKS)),
            pltpu.VMEM((length, width), f32),
            pltpu.VMEM((length, width), bf),
            pltpu.VMEM((length, values), f32),
            pltpu.VMEM((length, width), bf),
            pltpu.VMEM((length, values), bf),
            pltpu.VMEM((length, lanes), bf),
            pltpu.VMEM(taps.shape, f32),
            pltpu.VMEM((1, values), f32),
            pltpu.VMEM((1, lanes), f32),
            pltpu.VMEM((1, width), f32),
            pltpu.VMEM((1, width), f32),
            pltpu.VMEM((HALO + SPAN, width), f32),
            pltpu.VMEM((HALO + SPAN, width), f32),
            pltpu.VMEM((heads, key_dim, value_dim), f32),
            pltpu.VMEM((length, width), f32),
            dma((2, places)),
            dma((2, places)),
            dma((2, 3, places)),
            dma((2, 3, places)),
            dma((8,)),
            dma((3,)),
        ]
    )
    return pl.pallas_call(
        functools.partial(tail_kernel, heads, key_dim, value_dim, tuple(ranges[:7]) + (rows_all,), chunks),
        out_shape=out_shape,
        in_specs=[any_] * 8 + [vmem] * 18,
        out_specs=[vmem] * 2 + [any_] * 9,
        scratch_shapes=scratch,
        compiler_params=pltpu.CompilerParams(
            collective_id=collective_id, has_side_effects=True, vmem_limit_bytes=67043328
        ),
        name="tail",
    )(
        part2, ffn, wide, rest, down, pre, core, update, resid1, upstream, resid, mixed, hidden1,
        w_out, w_mix, w_gate, w_small, norm1, norm2, gate, small, taps, rate, gain, states, inverses,
    )


def lane_pad(array, lanes):
    return jnp.pad(array, ((0, 0), (0, lanes - array.shape[1])))


def whole_sequences(
    inputs,
    norm1_gain,
    w_query,
    w_key,
    w_value,
    w_gate,
    w_beta,
    w_decay,
    decay_rate,
    conv_query,
    conv_key,
    conv_value,
    head_gain,
    w_out,
    norm2_gain,
    w_ffn_gate,
    w_ffn_up,
    w_ffn_down,
    cotangent,
):
    batch, seg, width = inputs.shape
    count = batch * seg
    heads = decay_rate.shape[0]
    key_dim = w_query.shape[1] // heads
    value_dim = w_value.shape[1] // heads
    qk_width = heads * key_dim
    lanes = 128
    bf = jnp.bfloat16
    places = lax.axis_size("dp")
    resid, upstream = swap(
        [inputs.reshape(count, width), cotangent.reshape(count, width)], places, 1
    )
    upstream_low = upstream.astype(bf)
    normed1, norm1_back = jax.vjp(rms_apply, resid, norm1_gain)
    hidden1 = normed1.astype(bf)
    w_mix = jnp.concatenate([w_query, w_key, w_value], axis=1)
    w_small = lane_pad(jnp.concatenate([w_beta, w_decay], axis=1), lanes)
    pre = project(hidden1, w_mix)
    gate_pre = project(hidden1, w_gate)
    small = project(hidden1, w_small)
    taps = jnp.concatenate([conv_query, conv_key, conv_value], axis=1)
    rate = lane_pad(jnp.pad(decay_rate, (heads, 0))[None], lanes)
    gain = head_gain[None]
    mixed, core, update, states, inverses = delta_forward(
        pre, gate_pre, small, taps, rate, gain, heads, key_dim, value_dim
    )
    attention = tensor_sum(project(mixed, w_out), 2)
    resid1 = resid + attention
    normed2, norm2_back = jax.vjp(rms_apply, resid1, norm2_gain)
    hidden2 = normed2.astype(bf)
    ffn_gate = project(hidden2, w_ffn_gate)
    ffn_up = project(hidden2, w_ffn_up)
    inner_full, swiglu_back = jax.vjp(swiglu, ffn_gate, ffn_up)
    inner = inner_full.astype(bf)
    grad_inner = back_project(upstream_low, w_ffn_down)
    grad_fgate, grad_fup = swiglu_back(grad_inner)
    grad_fgate = grad_fgate.astype(bf)
    grad_fup = grad_fup.astype(bf)
    grad_wide = jnp.concatenate([grad_fgate, grad_fup], axis=1)
    units = inner.shape[1]
    part2 = back_project(grad_wide, jnp.concatenate([w_ffn_gate, w_ffn_up], axis=1))
    wide = contract_rows(hidden2, grad_wide[:, :width])
    rest = contract_rows(grad_wide[:, width:], hidden2)
    down = contract_rows(inner, upstream_low)
    ffn = project(inner, w_ffn_down)
    (
        output, grad_inputs, wide, rest, grad_down, grad_out_w, grad_gate_w,
        grad_query_w, grad_key_w, grad_value_w, rows,
    ) = tail(
        part2, ffn, wide, rest, down, pre, core, update, resid1, upstream_low, resid.astype(bf), mixed, hidden1,
        w_out, w_mix, w_gate, w_small, norm1_gain[None], norm2_gain[None],
        gate_pre, small, taps, rate, gain, states, inverses,
        heads, key_dim, value_dim, places, 7,
    )
    grad_taps = rows[0:4]
    grad_small_w = rows[8 : 8 + 2 * heads]
    wide_full = jnp.concatenate([wide, rest.T], axis=1)
    return (
        output.reshape(batch, seg, width),
        grad_inputs.reshape(batch, seg, width),
        rows[4],
        grad_query_w,
        grad_key_w,
        grad_value_w,
        grad_gate_w,
        grad_small_w[:heads].T,
        grad_small_w[heads:].T,
        rows[6, heads * value_dim + heads : heads * value_dim + 2 * heads],
        grad_taps[:, :qk_width],
        grad_taps[:, qk_width : 2 * qk_width],
        grad_taps[:, 2 * qk_width :],
        rows[6, : heads * value_dim],
        grad_out_w,
        rows[5],
        wide_full[:, :units],
        wide_full[:, units:],
        grad_down,
    )


def fits_whole(mesh, args):
    batch, length, width = args[0].shape
    places, ranks = mesh.shape["dp"], mesh.shape["tensor"]
    heads = args[8].shape[0] // ranks
    qk = args[2].shape[1] // ranks
    values = args[4].shape[1] // ranks
    units = args[15].shape[1] // ranks
    return (
        batch == places and places == 8 and ranks == 4 and length == places * SPAN and heads <= 4
        and width == 2 * qk + values and width == 2 * values and width % 512 == 0 and length % 256 == 0
        and 2 * units > width and (2 * units - width) % SLOT == 0 and units % SLOT == 0 and values % 256 == 0
    )


def solution(mesh):
    placed = (
        P(None, "dp", None),
        P(),
        P(None, "tensor"),
        P(None, "tensor"),
        P(None, "tensor"),
        P(None, "tensor"),
        P(None, "tensor"),
        P(None, "tensor"),
        P("tensor"),
        P(None, "tensor"),
        P(None, "tensor"),
        P(None, "tensor"),
        P("tensor"),
        P("tensor", None),
        P(),
        P(None, "tensor"),
        P(None, "tensor"),
        P("tensor", None),
        P(None, "dp", None),
    )
    def step(*args):
        body = whole_sequences if fits_whole(mesh, args) else shards
        return placed_step(body)(*args)

    def placed_step(body):
      return jax.shard_map(
        body,
        mesh=mesh,
        in_specs=placed,
        out_specs=(
            P(None, "dp", None),
            P(None, "dp", None),
            P(),
            P(None, "tensor"),
            P(None, "tensor"),
            P(None, "tensor"),
            P(None, "tensor"),
            P(None, "tensor"),
            P(None, "tensor"),
            P("tensor"),
            P(None, "tensor"),
            P(None, "tensor"),
            P(None, "tensor"),
            P("tensor"),
            P("tensor", None),
            P(),
            P(None, "tensor"),
            P(None, "tensor"),
            P("tensor", None),
        ),
        check_vma=False,
    )

    return step
```

```python
import functools
from functools import partial

import jax
import jax.numpy as jnp
from jax import lax
from jax.experimental import pallas as pl
from jax.experimental.pallas import tpu as pltpu
from jax.sharding import PartitionSpec as P

SPAN = 64


EPS = 1e-06


def from_behind(shard, axis, by):
    count = lax.axis_size(axis)
    pairs = [(i, i + by) for i in range(count) if 0 <= i + by < count]
    return lax.ppermute(shard, axis, pairs)


def carried_in(part, axis, combine, identity, reverse):
    count = lax.axis_size(axis)
    place = lax.axis_index(axis)
    ahead = count - 1 - place if reverse else place
    gathered = jax.tree.map(lambda a: lax.all_gather(a, axis), part)
    state = jax.tree.map(lambda a, e: jnp.zeros_like(a) + jnp.asarray(e, a.dtype), part, identity)

    def one(turn, state):
        source = count - 1 - turn if reverse else turn
        return combine(
            state, jax.tree.map(lambda a: lax.dynamic_index_in_dim(a, source, 0, False), gathered)
        )

    return lax.fori_loop(0, ahead, one, state)


def exact(left, right):
    return jnp.matmul(left, right, precision=lax.Precision.HIGHEST)


def span_apply(state, inputs):
    query, key, values, beta, logdecay = inputs
    count = query.shape[0]
    cumul = jnp.cumsum(logdecay)
    row_ids = lax.broadcasted_iota(jnp.int32, (count, count), 0)
    col_ids = lax.broadcasted_iota(jnp.int32, (count, count), 1)
    within = col_ids <= row_ids
    strict = col_ids < row_ids
    spread = jnp.where(within, cumul[:, None] - cumul[None, :], 0.0)
    decays = jnp.where(within, jnp.exp(spread), 0.0)
    scaled = decays * beta[None, :]
    lower = jnp.where(strict, scaled * exact(key, key.T), 0.0)
    start_decay = jnp.exp(cumul)[:, None]
    right_side = values - start_decay * exact(key, state)
    system = jnp.eye(count, dtype=lower.dtype) + lower
    update = jax.scipy.linalg.solve_triangular(system, right_side, lower=True, unit_diagonal=True)
    output = start_decay * exact(query, state) + exact(scaled * exact(query, key.T), update)
    tail = jnp.exp(cumul[-1] - cumul) * beta
    new_state = jnp.exp(cumul[-1]) * state + exact((key * tail[:, None]).T, update)
    return (new_state, output)


def run_segment(query, key, values, beta, logdecay, state):
    length = query.shape[0]
    blocks = length // SPAN

    def split(array):
        return array.reshape((blocks, SPAN) + array.shape[1:])

    final, outputs = lax.scan(
        span_apply, state, (split(query), split(key), split(values), split(beta), split(logdecay))
    )
    return (outputs.reshape((length,) + outputs.shape[2:]), final)


def run_heads(query, key, values, beta, logdecay, state):
    return jax.vmap(jax.vmap(run_segment))(query, key, values, beta, logdecay, state)


def prepare(extended, beta_pre, decay_pre, conv_all, decay_rate, key_dim):
    batch, seg, heads = beta_pre.shape
    reach = conv_all.shape[0] - 1
    total = conv_all[0] * extended[:, 0:seg, :]
    for offset in range(1, reach + 1):
        total = total + conv_all[offset] * extended[:, offset : offset + seg, :]
    active = jax.nn.silu(total)
    qk_width = heads * key_dim
    query = active[..., :qk_width].reshape(batch, seg, heads, key_dim)
    key = active[..., qk_width : 2 * qk_width].reshape(batch, seg, heads, key_dim)
    values = active[..., 2 * qk_width :].reshape(batch, seg, heads, -1)
    query = query * lax.rsqrt(jnp.sum(query * query, -1, keepdims=True) + EPS) * key_dim ** (-0.5)
    key = key * lax.rsqrt(jnp.sum(key * key, -1, keepdims=True) + EPS)
    beta = jax.nn.sigmoid(beta_pre)
    logdecay = -decay_rate * jax.nn.softplus(decay_pre)
    return (
        jnp.moveaxis(query, 2, 1),
        jnp.moveaxis(key, 2, 1),
        jnp.moveaxis(values, 2, 1),
        jnp.moveaxis(beta, 2, 1),
        jnp.moveaxis(logdecay, 2, 1),
    )


def gate_norm(core, gate_pre, head_gain):
    normed = core * lax.rsqrt(jnp.mean(core * core, -1, keepdims=True) + EPS)
    return normed * head_gain * jax.nn.silu(gate_pre)


def rms_apply(resid, gain):
    return resid * lax.rsqrt(jnp.mean(resid * resid, -1, keepdims=True) + EPS) * gain


def swiglu(gate, upper):
    return jax.nn.silu(gate) * upper


def project(left, right):
    return jnp.dot(left, right, preferred_element_type=jnp.float32)


def contract_rows(left, right):
    return jnp.einsum("ra,rb->ab", left, right, preferred_element_type=jnp.float32)


def back_project(grad, weight):
    return jnp.einsum("rb,ab->ra", grad, weight, preferred_element_type=jnp.float32)


def compose(earlier, later):
    return (exact(later[0], earlier[0]), exact(later[0], earlier[1]) + later[1])


def shards(
    inputs,
    norm1_gain,
    w_query,
    w_key,
    w_value,
    w_gate,
    w_beta,
    w_decay,
    decay_rate,
    conv_query,
    conv_key,
    conv_value,
    head_gain,
    w_out,
    norm2_gain,
    w_ffn_gate,
    w_ffn_up,
    w_ffn_down,
    cotangent,
):
    batch, seg, width = inputs.shape
    count = batch * seg
    heads = decay_rate.shape[0]
    key_dim = w_query.shape[1] // heads
    value_dim = w_value.shape[1] // heads
    qk_width = heads * key_dim
    reach = conv_query.shape[0] - 1
    bf = jnp.bfloat16
    resid = inputs.reshape(count, width).astype(jnp.float32)
    normed1, norm1_back = jax.vjp(rms_apply, resid, norm1_gain)
    hidden1 = normed1.astype(bf)
    query_pre = project(hidden1, w_query)
    key_pre = project(hidden1, w_key)
    value_pre = project(hidden1, w_value)
    gate_pre = project(hidden1, w_gate)
    beta_pre = project(hidden1, w_beta)
    decay_pre = project(hidden1, w_decay)
    mixed_pre = jnp.concatenate([query_pre, key_pre, value_pre], axis=1).reshape(batch, seg, -1)
    rim = from_behind(mixed_pre[:, seg - reach :, :], "dp", 1)
    extended = jnp.concatenate([rim, mixed_pre], axis=1)
    conv_all = jnp.concatenate([conv_query, conv_key, conv_value], axis=1)
    features, prep_back = jax.vjp(
        partial(prepare, key_dim=key_dim),
        extended,
        beta_pre.reshape(batch, seg, heads),
        decay_pre.reshape(batch, seg, heads),
        conv_all,
        decay_rate,
    )
    query_h, key_h, value_h, beta_h, decay_h = features
    eye_block = jnp.broadcast_to(
        jnp.eye(key_dim, dtype=jnp.float32), (batch, heads, key_dim, key_dim)
    )
    zero_block = jnp.zeros((batch, heads, key_dim, value_dim), jnp.float32)
    values_aug = jnp.concatenate(
        [jnp.zeros(value_h.shape[:3] + (key_dim,), jnp.float32), value_h], axis=-1
    )
    state_aug = jnp.concatenate([eye_block, zero_block], axis=-1)
    outputs_aug, final_aug = run_heads(query_h, key_h, values_aug, beta_h, decay_h, state_aug)
    out_carry = outputs_aug[..., :key_dim]
    out_local = outputs_aug[..., key_dim:]
    transition = final_aug[..., :key_dim]
    offset_part = final_aug[..., key_dim:]
    prefix = carried_in((transition, offset_part), "dp", compose, (eye_block, zero_block), False)
    start_state = prefix[1]
    core = jnp.moveaxis(exact(out_carry, start_state) + out_local, 1, 2)
    gate4 = gate_pre.reshape(batch, seg, heads, value_dim)
    gated, gate_back = jax.vjp(gate_norm, core, gate4, head_gain.reshape(heads, value_dim))
    mixed = gated.reshape(count, heads * value_dim).astype(bf)
    attention = lax.psum(project(mixed, w_out), "tensor")
    resid1 = resid + attention
    normed2, norm2_back = jax.vjp(rms_apply, resid1, norm2_gain)
    hidden2 = normed2.astype(bf)
    ffn_gate = project(hidden2, w_ffn_gate)
    ffn_up = project(hidden2, w_ffn_up)
    inner_full, swiglu_back = jax.vjp(swiglu, ffn_gate, ffn_up)
    inner = inner_full.astype(bf)
    ffn = lax.psum(project(inner, w_ffn_down), "tensor")
    output = (resid1 + ffn).astype(bf).reshape(batch, seg, width)
    upstream = cotangent.reshape(count, width)
    grad_down = contract_rows(inner, upstream)
    grad_inner = back_project(upstream, w_ffn_down)
    grad_fgate, grad_fup = swiglu_back(grad_inner)
    grad_fgate = grad_fgate.astype(bf)
    grad_fup = grad_fup.astype(bf)
    grad_ffn_gate_w = contract_rows(hidden2, grad_fgate)
    grad_ffn_up_w = contract_rows(hidden2, grad_fup)
    grad_hidden2 = lax.psum(
        back_project(grad_fgate, w_ffn_gate) + back_project(grad_fup, w_ffn_up), "tensor"
    )
    grad_from_norm2, grad_norm2_gain = norm2_back(grad_hidden2)
    grad_resid1 = upstream.astype(jnp.float32) + grad_from_norm2
    grad_resid1_low = grad_resid1.astype(bf)
    grad_out_w = contract_rows(mixed, grad_resid1_low)
    grad_mixed = back_project(grad_resid1_low, w_out).reshape(batch, seg, heads, value_dim)
    grad_core, grad_gate4, grad_head_gain = gate_back(grad_mixed)
    grad_core_h = jnp.moveaxis(grad_core, 2, 1)
    carry_term = exact(jnp.swapaxes(out_carry, -1, -2), grad_core_h)
    suffix = carried_in(
        (jnp.swapaxes(transition, -1, -2), carry_term), "dp", compose, (eye_block, zero_block), True
    )

    def local_delta(query, key, values, beta, logdecay):
        return run_heads(query, key, values, beta, logdecay, start_state)

    recomputed, delta_back = jax.vjp(local_delta, query_h, key_h, value_h, beta_h, decay_h)
    feature_grads = delta_back((grad_core_h, suffix[1]))
    grad_ext, grad_beta_in, grad_decay_in, grad_conv, grad_rate = prep_back(feature_grads)
    returned = from_behind(grad_ext[:, :reach, :], "dp", -1)
    grad_mixed_pre = grad_ext[:, reach:, :] + jnp.pad(returned, ((0, 0), (seg - reach, 0), (0, 0)))
    grad_mixed_pre = grad_mixed_pre.reshape(count, -1)
    grad_query_low = grad_mixed_pre[:, :qk_width].astype(bf)
    grad_key_low = grad_mixed_pre[:, qk_width : 2 * qk_width].astype(bf)
    grad_value_low = grad_mixed_pre[:, 2 * qk_width :].astype(bf)
    grad_gate_low = grad_gate4.reshape(count, heads * value_dim).astype(bf)
    grad_beta_low = grad_beta_in.reshape(count, heads).astype(bf)
    grad_decay_low = grad_decay_in.reshape(count, heads).astype(bf)
    partial_hidden1 = (
        back_project(grad_query_low, w_query)
        + back_project(grad_key_low, w_key)
        + back_project(grad_value_low, w_value)
        + back_project(grad_gate_low, w_gate)
        + back_project(grad_beta_low, w_beta)
        + back_project(grad_decay_low, w_decay)
    )
    grad_hidden1 = lax.psum(partial_hidden1, "tensor")
    grad_from_norm1, grad_norm1_gain = norm1_back(grad_hidden1)
    grad_inputs = (grad_resid1 + grad_from_norm1).reshape(batch, seg, width)
    grad_query_w = contract_rows(hidden1, grad_query_low)
    grad_key_w = contract_rows(hidden1, grad_key_low)
    grad_value_w = contract_rows(hidden1, grad_value_low)
    grad_gate_w = contract_rows(hidden1, grad_gate_low)
    grad_beta_w = contract_rows(hidden1, grad_beta_low)
    grad_decay_w = contract_rows(hidden1, grad_decay_low)
    grad_convq = grad_conv[:, :qk_width]
    grad_convk = grad_conv[:, qk_width : 2 * qk_width]
    grad_convv = grad_conv[:, 2 * qk_width :]
    grad_head_flat = grad_head_gain.reshape(-1)
    (
        grad_norm1_gain,
        grad_query_w,
        grad_key_w,
        grad_value_w,
        grad_gate_w,
        grad_beta_w,
        grad_decay_w,
        grad_rate,
        grad_convq,
        grad_convk,
        grad_convv,
        grad_head_flat,
        grad_out_w,
        grad_norm2_gain,
        grad_ffn_gate_w,
        grad_ffn_up_w,
        grad_down,
    ) = lax.psum(
        (
            grad_norm1_gain,
            grad_query_w,
            grad_key_w,
            grad_value_w,
            grad_gate_w,
            grad_beta_w,
            grad_decay_w,
            grad_rate,
            grad_convq,
            grad_convk,
            grad_convv,
            grad_head_flat,
            grad_out_w,
            grad_norm2_gain,
            grad_ffn_gate_w,
            grad_ffn_up_w,
            grad_down,
        ),
        "dp",
    )
    return (
        output,
        grad_inputs,
        grad_norm1_gain,
        grad_query_w,
        grad_key_w,
        grad_value_w,
        grad_gate_w,
        grad_beta_w,
        grad_decay_w,
        grad_rate,
        grad_convq,
        grad_convk,
        grad_convv,
        grad_head_flat,
        grad_out_w,
        grad_norm2_gain,
        grad_ffn_gate_w,
        grad_ffn_up_w,
        grad_down,
    )


HALO = 8


def mm(left, right):
    return lax.dot_general(
        left, right, (((1,), (0,)), ((), ())),
        precision=lax.Precision.HIGHEST, preferred_element_type=jnp.float32,
    )


def mm_nt(left, right):
    return lax.dot_general(
        left, right, (((1,), (1,)), ((), ())),
        precision=lax.Precision.HIGHEST, preferred_element_type=jnp.float32,
    )


def mm_tn(left, right):
    return lax.dot_general(
        left, right, (((0,), (0,)), ((), ())),
        precision=lax.Precision.HIGHEST, preferred_element_type=jnp.float32,
    )


def grids(count):
    rows = lax.broadcasted_iota(jnp.int32, (count, count), 0)
    cols = lax.broadcasted_iota(jnp.int32, (count, count), 1)
    return rows, cols


def unit_inverse(lower, rows, cols):
    count = lower.shape[0]
    near = (rows // 2 == cols // 2) & (rows > cols)
    inverse = jnp.where(rows == cols, 1.0, jnp.where(near, -lower, 0.0))
    block = 2
    while block < count:
        cross = (rows // (2 * block) == cols // (2 * block)) & (rows // block > cols // block)
        inverse = inverse - mm(mm(inverse, jnp.where(cross, lower, 0.0)), inverse)
        block *= 2
    return inverse


def conv_window(halo_block, taps, span):
    reach = taps.shape[0] - 1
    total = None
    for offset in range(reach + 1):
        start = HALO - reach + offset
        term = taps[offset : offset + 1] * halo_block[start : start + span]
        total = term if total is None else total + term
    return total


def sigmoid(value):
    return 1.0 / (1.0 + jnp.exp(-value))


def softplus(value):
    return jnp.maximum(value, 0.0) + jnp.log(1.0 + jnp.exp(-jnp.abs(value)))


def gates_of(small, rate, heads, rows, cols):
    beta = sigmoid(small)
    slope = softplus(small)
    logdecay = -rate * slope
    cumul = mm(jnp.where(cols <= rows, 1.0, 0.0), logdecay)
    return beta, slope, logdecay, cumul


def state_place(index, head, heads, key_dim, value_dim, width):
    across = width // value_dim
    turn = index * heads + head
    return (
        pl.ds(pl.multiple_of(lax.div(turn, across) * key_dim, key_dim), key_dim),
        pl.ds(pl.multiple_of(lax.rem(turn, across) * value_dim, value_dim), value_dim),
    )


def chunk_terms(query, key, beta_col, beta_row, cum_col, cum_row, rows, cols):
    within = cols <= rows
    decays = jnp.where(within, jnp.exp(jnp.where(within, cum_col - cum_row, 0.0)), 0.0)
    scaled = decays * beta_row
    key_key = mm_nt(key, key)
    query_key = mm_nt(query, key)
    lower = jnp.where(cols < rows, scaled * key_key, 0.0)
    attend = scaled * query_key
    return decays, scaled, key_key, query_key, lower, attend


def forward_kernel(heads, key_dim, value_dim, pre_ref, gate_ref, small_ref, taps_ref, rate_ref, gain_ref,
                   mixed_ref, core_ref, update_ref, state_ref, inverse_ref, pad_ref, now_ref):
    length, width = pre_ref.shape
    span = SPAN
    chunks = length // span
    rows, cols = grids(span)
    qk = heads * key_dim
    pad_ref[0:HALO] = jnp.zeros((HALO, width), jnp.float32)
    for head in range(heads):
        now_ref[head] = jnp.zeros((key_dim, value_dim), jnp.float32)

    def chunk(index, carry):
        start = pl.multiple_of(index * span, span)
        here = pl.ds(start, span)
        pad_ref[HALO : HALO + span] = pre_ref[here, :]
        total = conv_window(pad_ref[...], taps_ref[...], span)
        pad_ref[0:HALO] = pad_ref[span : span + HALO]
        active = total * sigmoid(total)
        beta, _, _, cumul = gates_of(small_ref[here, :], rate_ref[...], heads, rows, cols)
        beta_t = jnp.transpose(beta)
        cumul_t = jnp.transpose(cumul)
        gate = gate_ref[here, :]
        gated = gate * sigmoid(gate) * gain_ref[...]
        for head in range(heads):
            query = active[:, head * key_dim : (head + 1) * key_dim]
            query = query * (lax.rsqrt(jnp.sum(query * query, -1, keepdims=True) + EPS) * key_dim ** (-0.5))
            key = active[:, qk + head * key_dim : qk + (head + 1) * key_dim]
            key = key * lax.rsqrt(jnp.sum(key * key, -1, keepdims=True) + EPS)
            value = active[:, 2 * qk + head * value_dim : 2 * qk + (head + 1) * value_dim]
            beta_col = beta[:, head : head + 1]
            beta_row = beta_t[head : head + 1]
            cum_col = cumul[:, heads + head : heads + head + 1]
            cum_row = cumul_t[heads + head : heads + head + 1]
            _, _, _, _, lower, attend = chunk_terms(query, key, beta_col, beta_row, cum_col, cum_row, rows, cols)
            inverse = unit_inverse(lower, rows, cols)
            state = now_ref[head]
            state_ref[state_place(index, head, heads, key_dim, value_dim, width)] = state
            rise = jnp.exp(cum_col)
            last = cum_col[span - 1 : span]
            update = mm(inverse, value) - mm(mm(inverse, rise * key), state)
            core = mm(rise * query, state) + mm(attend, update)
            tail = jnp.exp(last - cum_col) * beta_col
            now_ref[head] = jnp.exp(last) * state + mm_tn(key * tail, update)
            inverse_ref[index, head] = inverse
            wide = slice(head * value_dim, (head + 1) * value_dim)
            update_ref[here, wide] = update
            core_ref[here, wide] = core
            normed = core * lax.rsqrt(jnp.mean(core * core, -1, keepdims=True) + EPS)
            mixed_ref[here, wide] = (normed * gated[:, wide]).astype(mixed_ref.dtype)
        return carry

    lax.fori_loop(0, chunks, chunk, 0)


def delta_forward(pre, gate, small, taps, rate, gain, heads, key_dim, value_dim):
    length, width = pre.shape
    chunks = length // SPAN
    out_shape = (
        jax.ShapeDtypeStruct((length, heads * value_dim), jnp.bfloat16),
        jax.ShapeDtypeStruct((length, heads * value_dim), jnp.float32),
        jax.ShapeDtypeStruct((length, heads * value_dim), jnp.float32),
        jax.ShapeDtypeStruct((chunks * heads * key_dim * value_dim // width, width), jnp.float32),
        jax.ShapeDtypeStruct((chunks, heads, SPAN, SPAN), jnp.float32),
    )
    return pl.pallas_call(
        functools.partial(forward_kernel, heads, key_dim, value_dim),
        out_shape=out_shape,
        scratch_shapes=[
            pltpu.VMEM((HALO + SPAN, width), jnp.float32),
            pltpu.VMEM((heads, key_dim, value_dim), jnp.float32),
        ],
        compiler_params=pltpu.CompilerParams(vmem_limit_bytes=56 << 20),
        name="delta_forward",
    )(pre, gate, small, taps, rate, gain)


def backward_start(refs, span):
    (_, _, _, _, _, _, _, _, _, _, _, _, _, _, taps_grad_ref, gain_grad_ref, rate_grad_ref,
     _, pad_ref, now_ref) = refs
    now_ref[...] = jnp.zeros_like(now_ref)
    pad_ref[span : span + HALO] = jnp.zeros((HALO, pad_ref.shape[1]), jnp.float32)
    taps_grad_ref[...] = jnp.zeros_like(taps_grad_ref)
    gain_grad_ref[...] = jnp.zeros_like(gain_grad_ref)
    rate_grad_ref[...] = jnp.zeros_like(rate_grad_ref)


def backward_chunk(heads, key_dim, value_dim, index, refs):
    (pre_ref, gate_ref, small_ref, taps_ref, rate_ref, gain_ref,
     core_ref, update_ref, state_ref, inverse_ref, grad_ref,
     low_ref, gate_low_ref, small_low_ref, taps_grad_ref, gain_grad_ref, rate_grad_ref,
     ahead_ref, pad_ref, now_ref) = refs
    width = taps_ref.shape[1]
    span = SPAN
    rows, cols = grids(span)
    qk = heads * key_dim
    reach = taps_ref.shape[0] - 1
    lanes = small_ref.shape[1]
    lane = lax.broadcasted_iota(jnp.int32, (span, lanes), 1)
    start = pl.multiple_of(index * span, span)
    here = pl.ds(start, span)
    before = pl.ds(pl.multiple_of(jnp.maximum(start - HALO, 0), HALO), HALO)
    ahead_ref[0:HALO] = pre_ref[before, :] * jnp.where(index > 0, 1.0, 0.0)
    ahead_ref[HALO : HALO + span] = pre_ref[here, :]
    total = conv_window(ahead_ref[...], taps_ref[...], span)
    gain_of = sigmoid(total)
    active = total * gain_of
    bend = gain_of * (1.0 + total * (1.0 - gain_of))
    small = small_ref[here, :]
    beta, slope, _, cumul = gates_of(small, rate_ref[...], heads, rows, cols)
    beta_t = jnp.transpose(beta)
    cumul_t = jnp.transpose(cumul)
    gate = gate_ref[here, :]
    gate_sig = sigmoid(gate)
    gate_silu = gate * gate_sig
    gate_bend = gate_sig * (1.0 + gate * (1.0 - gate_sig))
    small_grad = jnp.zeros((span, lanes), jnp.float32)
    for head in range(heads):
        wide = slice(head * value_dim, (head + 1) * value_dim)
        core = core_ref[here, wide]
        grad_mixed = grad_ref[here, wide]
        gain = gain_ref[:, wide]
        scale = lax.rsqrt(jnp.mean(core * core, -1, keepdims=True) + EPS)
        normed = core * scale
        gate_low_ref[here, wide] = (grad_mixed * normed * gain * gate_bend[:, wide]).astype(gate_low_ref.dtype)
        with_gate = grad_mixed * gate_silu[:, wide]
        gain_grad_ref[:, wide] += jnp.sum(with_gate * normed, 0, keepdims=True)
        grad_normed = with_gate * gain
        grad_core = scale * (grad_normed - normed * jnp.mean(grad_normed * normed, -1, keepdims=True))
        query_act = active[:, head * key_dim : (head + 1) * key_dim]
        query_scale = lax.rsqrt(jnp.sum(query_act * query_act, -1, keepdims=True) + EPS)
        query = query_act * (query_scale * key_dim ** (-0.5))
        key_act = active[:, qk + head * key_dim : qk + (head + 1) * key_dim]
        key_scale = lax.rsqrt(jnp.sum(key_act * key_act, -1, keepdims=True) + EPS)
        key = key_act * key_scale
        beta_col = beta[:, head : head + 1]
        beta_row = beta_t[head : head + 1]
        cum_col = cumul[:, heads + head : heads + head + 1]
        cum_row = cumul_t[heads + head : heads + head + 1]
        decays, scaled, key_key, query_key, lower, attend = chunk_terms(
            query, key, beta_col, beta_row, cum_col, cum_row, rows, cols
        )
        state = state_ref[state_place(index, head, heads, key_dim, value_dim, width)]
        update = update_ref[here, wide]
        inverse = inverse_ref[index, head]
        grad_state = now_ref[head]
        rise = jnp.exp(cum_col)
        last = cum_col[span - 1 : span]
        fall = jnp.exp(last - cum_col)
        tail = fall * beta_col
        rise_query = rise * query
        rise_key = rise * key
        grad_update = mm_tn(attend, grad_core) + mm(key * tail, grad_state)
        grad_right = mm_tn(inverse, grad_update)
        now_ref[head] = jnp.exp(last) * grad_state + mm_tn(rise_query, grad_core) - mm_tn(rise_key, grad_right)
        grad_attend = jnp.where(cols <= rows, mm_nt(grad_core, update), 0.0)
        grad_lower = jnp.where(cols < rows, -mm_nt(grad_right, update), 0.0)
        core_state = mm_nt(grad_core, state)
        right_state = mm_nt(grad_right, state)
        grad_tail_key = mm_nt(update, grad_state)
        pair_query = grad_attend * scaled
        pair_key = grad_lower * scaled
        grad_query = rise * core_state + mm(pair_query, key)
        grad_key = (
            grad_tail_key * tail - rise * right_state + mm_tn(pair_query, query)
            + mm(pair_key, key) + mm_tn(pair_key, key)
        )
        grad_tail = jnp.sum(grad_tail_key * key, -1, keepdims=True)
        moved = grad_attend * query_key + grad_lower * key_key
        spread = moved * scaled
        by_row = jnp.sum(spread, -1, keepdims=True)
        sums = mm_tn(
            jnp.concatenate([moved * decays, spread], 1), jnp.ones((span, lanes), jnp.float32)
        )
        grad_beta = sums[:span, 0:1] + grad_tail * fall
        through_tail = grad_tail * tail
        grad_cum = (
            by_row - sums[span:, 0:1] - through_tail
            + rise * (jnp.sum(core_state * query, -1, keepdims=True) - jnp.sum(right_state * key, -1, keepdims=True))
        )
        end_grad = jnp.sum(through_tail, 0, keepdims=True) + jnp.exp(last) * jnp.sum(
            jnp.sum(state * grad_state, -1, keepdims=True), 0, keepdims=True
        )
        grad_cum = grad_cum + jnp.where(rows[:, 0:1] == span - 1, end_grad, 0.0)
        small_grad = small_grad + jnp.where(lane == head, grad_beta, 0.0)
        small_grad = small_grad + jnp.where(lane == heads + head, grad_cum, 0.0)
        grad_query = grad_query * key_dim ** (-0.5)
        unit = query_act * query_scale
        grad_query = query_scale * (grad_query - unit * jnp.sum(grad_query * unit, -1, keepdims=True))
        grad_key = key_scale * (grad_key - key * jnp.sum(grad_key * key, -1, keepdims=True))
        at = slice(head * key_dim, (head + 1) * key_dim)
        pad_ref[0:span, at] = grad_query * bend[:, at]
        at = slice(qk + head * key_dim, qk + (head + 1) * key_dim)
        pad_ref[0:span, at] = grad_key * bend[:, at]
        at = slice(2 * qk + head * value_dim, 2 * qk + (head + 1) * value_dim)
        pad_ref[0:span, at] = grad_right * bend[:, at]
    summed = mm(jnp.where(cols >= rows, 1.0, 0.0), small_grad)
    is_beta = lane < heads
    rate_grad_ref[...] += jnp.sum(jnp.where(is_beta, 0.0, -slope * summed), 0, keepdims=True)
    sig = beta
    small_low_ref[here, :] = jnp.where(
        is_beta, small_grad * sig * (1.0 - sig), -rate_ref[...] * sig * summed
    ).astype(small_low_ref.dtype)
    outer = pad_ref[...]
    dense = outer[0:span]
    block = ahead_ref[...]
    grad_pre = None
    for offset in range(reach + 1):
        behind = reach - offset
        taps_grad_ref[offset : offset + 1] += jnp.sum(
            dense * block[HALO - behind : HALO - behind + span], 0, keepdims=True
        )
        term = taps_ref[offset : offset + 1] * outer[behind : behind + span]
        grad_pre = term if grad_pre is None else grad_pre + term
    low_ref[here, :] = grad_pre.astype(low_ref.dtype)
    pad_ref[span : span + HALO] = pad_ref[0:HALO]


MESH = pl.DeviceIdType.MESH
VM = pl.BlockSpec(memory_space=pltpu.VMEM)


def greet(peers):
    barrier = pltpu.get_barrier_semaphore()
    for peer in peers:
        pl.semaphore_signal(barrier, inc=1, device_id=peer, device_id_type=MESH)
    pl.semaphore_wait(barrier, len(peers))


def remote(src, dst, send, recv, peer):
    return pltpu.make_async_remote_copy(
        src_ref=src, dst_ref=dst, send_sem=send, recv_sem=recv, device_id=peer, device_id_type=MESH
    )


def tensor_peers():
    dp = lax.axis_index("dp")
    t = lax.axis_index("tensor")
    core = lax.rem(t, 2)
    mate = (dp, t + 1 - 2 * core)
    across = (dp, lax.rem(t + 2, 4))
    return core, mate, across


def psum_kernel(blocks, part_ref, out_ref, land_mate, land_across, half, send, recv):
    core, mate, across = tensor_peers()
    greet((mate, across))
    rows = part_ref.shape[0] // blocks
    part = rows // 2
    first = []
    for b in range(blocks):
        theirs = pl.ds(pl.multiple_of(b * rows + (1 - core) * part, part), part)
        copy = remote(part_ref.at[theirs], land_mate.at[pl.ds(b * part, part)], send.at[0, b], recv.at[0, b], mate)
        copy.start()
        first.append(copy)
    second = []
    for b in range(blocks):
        mine = pl.ds(pl.multiple_of(b * rows + core * part, part), part)
        slot = pl.ds(b * part, part)
        first[b].wait_recv()
        half[slot] = part_ref[mine] + land_mate[slot]
        copy = remote(half.at[slot], land_across.at[slot], send.at[1, b], recv.at[1, b], across)
        copy.start()
        second.append(copy)
    third = []
    for b in range(blocks):
        mine = pl.ds(pl.multiple_of(b * rows + core * part, part), part)
        slot = pl.ds(b * part, part)
        second[b].wait_recv()
        out_ref[mine] = half[slot] + land_across[slot]
        copy = remote(out_ref.at[mine], out_ref.at[mine], send.at[2, b], recv.at[2, b], mate)
        copy.start()
        third.append(copy)
    for b in range(blocks):
        third[b].wait_recv()
    for b in range(blocks):
        first[b].wait_send()
        second[b].wait_send()
        third[b].wait_send()


def tensor_sum(part, collective_id, blocks=8):
    rows, width = part.shape
    return pl.pallas_call(
        functools.partial(psum_kernel, blocks),
        out_shape=jax.ShapeDtypeStruct(part.shape, part.dtype),
        in_specs=[VM],
        out_specs=VM,
        scratch_shapes=[pltpu.VMEM((rows // 2, width), part.dtype)] * 3
        + [pltpu.SemaphoreType.DMA((3, blocks))] * 2,
        compiler_params=pltpu.CompilerParams(
            collective_id=collective_id, has_side_effects=True, vmem_limit_bytes=40 << 20
        ),
        name="tensor_sum",
    )(part)


def swap_kernel(count, narrow, *refs):
    sources, results = refs[:count], refs[count : 2 * count]
    staged, send, recv, close_send, close_recv = refs[2 * count :]
    n = lax.axis_size("dp")
    me = lax.axis_index("dp")
    t = lax.axis_index("tensor")
    core, mate, across = tensor_peers()
    ranks = lax.axis_size("tensor")
    others = [lax.rem(me + k, n) for k in range(1, n)]
    greet([(other, t) for other in others] + [mate, across])
    seg = results[0].shape[0] // n
    part = seg // ranks
    far = lax.rem(t + 2, ranks)

    def at(place, rank):
        return pl.ds(pl.multiple_of(place * seg + rank * part, part), part)

    outgoing = []
    for i in range(count):
        for k in range(n):
            other = lax.rem(me + k, n)
            if k == 0:
                results[i][at(me, t)] = sources[i][at(me, t)].astype(jnp.float32)
                continue
            if narrow[i]:
                staged[i, k] = sources[i][at(other, t)].astype(jnp.float32)
                src = staged.at[i, k]
            else:
                src = sources[i].at[at(other, t)]
            copy = remote(src, results[i].at[at(me, t)], send.at[i, k], recv.at[i, k], (other, t))
            copy.start()
            outgoing.append(copy)
    close = []
    for i in range(count):
        for k in range(n):
            source = lax.rem(me + n - k, n)
            here = results[i].at[at(source, t)]
            if k:
                remote(here, here, send.at[i, k], recv.at[i, k], (source, t)).wait_recv()
            over = remote(here, here, close_send.at[0, i, k], close_recv.at[0, i, k], across)
            over.start()
            beside = remote(here, here, close_send.at[1, i, k], close_recv.at[1, i, k], mate)
            beside.start()
            close += [over, beside]
    last = []
    for i in range(count):
        for k in range(n):
            source = lax.rem(me + n - k, n)
            there = results[i].at[at(source, far)]
            remote(there, there, close_send.at[0, i, k], close_recv.at[0, i, k], across).wait_recv()
            copy = remote(there, there, close_send.at[2, i, k], close_recv.at[2, i, k], mate)
            copy.start()
            last.append(copy)
    for copy in outgoing:
        copy.wait_send()
    for j, copy in enumerate(close):
        copy.wait_send()
        if j % 2:
            copy.wait_recv()
    for copy in last:
        copy.wait()


def swap(arrays, n, collective_id):
    count = len(arrays)
    rows, width = arrays[0].shape
    narrow = [a.dtype != jnp.float32 for a in arrays]
    out = pl.pallas_call(
        functools.partial(swap_kernel, count, narrow),
        out_shape=[jax.ShapeDtypeStruct((rows, width), jnp.float32)] * count,
        in_specs=[VM] * count,
        out_specs=[VM] * count,
        scratch_shapes=[pltpu.VMEM((count, n, rows // n // 4, width), jnp.float32)]
        + [pltpu.SemaphoreType.DMA((count, n))] * 2
        + [pltpu.SemaphoreType.DMA((3, count, n))] * 2,
        compiler_params=pltpu.CompilerParams(
            collective_id=collective_id, has_side_effects=True, vmem_limit_bytes=40 << 20
        ),
        name="swap",
    )(*arrays)
    return out


SLOT = 64
DEPTH = 12
LAG = 1


def grid_place():
    n = lax.axis_size("dp")
    me = lax.axis_index("dp")
    t = lax.axis_index("tensor")
    lines = n // 2
    z = lax.div(me, 2)
    x = lax.rem(me, 2)
    return n, lines, me, t, z, x


def grid_greet(extra=()):
    n, lines, me, t, z, x = grid_place()
    barrier = pltpu.get_barrier_semaphore()
    pl.semaphore_signal(barrier, inc=1, device_id=(me + 1 - 2 * x, t), device_id_type=MESH)
    for peer in extra:
        pl.semaphore_signal(barrier, inc=1, device_id=peer, device_id_type=MESH)

    @pl.when(z > 0)
    def _():
        pl.semaphore_signal(barrier, inc=1, device_id=(me - 2, t), device_id_type=MESH)

    @pl.when(z < lines - 1)
    def _():
        pl.semaphore_signal(barrier, inc=1, device_id=(me + 2, t), device_id_type=MESH)

    pl.semaphore_wait(
        barrier, 1 + len(extra) + jnp.where(z > 0, 1, 0) + jnp.where(z < lines - 1, 1, 0)
    )


def reduce_slot(slot, chunks, data, split_rings, whole_rings, aside, sems):
    n, lines, me, t, z, x = grid_place()
    mate = (me + 1 - 2 * x, t)
    send_x, recv_x, send_z, recv_z, send_d, recv_d, send_p, recv_p = [sems.at[i] for i in range(8)]
    top = lines - 1

    def ring(chunk):
        return lax.rem(chunk, DEPTH)

    def within(chunk):
        return (chunk >= 0) & (chunk < chunks)

    for stream in range(4):
        split = stream < 2
        up = stream % 2 == 0
        level = z if up else top - z
        after = (me + 2, t) if up else (me - 2, t)
        prior = (me - 2, t) if up else (me + 2, t)
        size = 8 if split else 16
        land_x, land_z, outgo = (split_rings if split else whole_rings)
        lane = stream % 2
        offset = 16 * stream

        def rows(chunk, side):
            base = chunk * SLOT + offset + (side * 8 if split else 0)
            return pl.ds(pl.multiple_of(base, 8), size)

        def spot(ref, chunk):
            return ref.at[lane, ring(chunk)]

        def to_mate(chunk, src):
            return remote(
                src, spot(land_x, chunk), send_x.at[stream, ring(chunk)], recv_x.at[stream, ring(chunk)], mate
            )

        def to_after(chunk):
            return remote(
                spot(outgo, chunk), spot(land_z, chunk),
                send_z.at[stream, ring(chunk)], recv_z.at[stream, ring(chunk)], after,
            )

        def to_prior(chunk):
            here = data.at[rows(chunk, x)]
            return remote(here, here, send_d.at[stream, ring(chunk)], recv_d.at[stream, ring(chunk)], prior)

        def from_after(chunk):
            here = data.at[rows(chunk, x)]
            return remote(here, here, send_d.at[stream, ring(chunk)], recv_d.at[stream, ring(chunk)], after)

        def close(chunk, side):
            here = data.at[rows(chunk, side)]
            return remote(here, here, send_p.at[stream, ring(chunk)], recv_p.at[stream, ring(chunk)], mate)

        def give_back(chunk):
            @pl.when(level > 0)
            def _():
                to_prior(chunk).start()

            if split:
                close(chunk, x).start()

        if split:
            @pl.when(slot < chunks)
            def _():
                aside[stream, ring(slot)] = data[rows(slot, 1 - x)]
                to_mate(slot, aside.at[stream, ring(slot)]).start()

        rise = slot - LAG * (1 + level)

        @pl.when(within(rise))
        def _():
            here = rows(rise, x)
            if split:
                to_mate(rise, aside.at[stream, ring(rise)]).wait_recv()

            def first():
                own = data[here]
                return own + land_x[lane, ring(rise)] if split else own

            @pl.when(level > 0)
            def _():
                to_after(rise).wait_recv()
                outgo[lane, ring(rise)] = first() + land_z[lane, ring(rise)]

            @pl.when(level == 0)
            def _():
                outgo[lane, ring(rise)] = first()

            @pl.when(level < top)
            def _():
                to_after(rise).start()

            @pl.when(level == top)
            def _():
                if split:
                    data[here] = outgo[lane, ring(rise)]
                    give_back(rise)
                else:
                    to_mate(rise, spot(outgo, rise)).start()

        if not split:
            meet = slot - LAG * (2 + top)

            @pl.when(within(meet) & (level == top))
            def _():
                to_mate(meet, spot(outgo, meet)).wait_recv()
                data[rows(meet, x)] = outgo[lane, ring(meet)] + land_x[lane, ring(meet)]
                give_back(meet)

        extra = 0 if split else 1
        fall = slot - LAG * (1 + extra + 2 * top - level)

        @pl.when(within(fall) & (level < top))
        def _():
            from_after(fall).wait_recv()
            to_after(fall).wait_send()
            give_back(fall)

        done = fall - LAG

        @pl.when(within(done))
        def _():
            @pl.when(level > 0)
            def _():
                to_prior(done).wait_send()

            if split:
                close(done, x).wait_send()
                close(done, 1 - x).wait_recv()
                to_mate(done, aside.at[stream, ring(done)]).wait_send()
            else:
                @pl.when(level == top)
                def _():
                    to_mate(done, spot(outgo, done)).wait_send()


def slots_of(chunks, lines):
    return chunks + LAG * (2 * lines + 1)


def reduce_scratch(width):
    return (
        [pltpu.VMEM((2, DEPTH, 8, width), jnp.float32)] * 3
        + [pltpu.VMEM((2, DEPTH, 16, width), jnp.float32)] * 3
        + [pltpu.VMEM((2, DEPTH, 8, width), jnp.float32), pltpu.SemaphoreType.DMA((8, 4, DEPTH))]
    )


BLOCKS = 8


def dot_plain(left, right):
    return lax.dot_general(left, right, (((1,), (0,)), ((), ())), preferred_element_type=jnp.float32)


def dot_nt(left, right):
    return lax.dot_general(left, right, (((1,), (1,)), ((), ())), preferred_element_type=jnp.float32)


def dot_tn(left, right):
    return lax.dot_general(left, right, (((0,), (0,)), ((), ())), preferred_element_type=jnp.float32)


def aligned(start, size):
    return pl.ds(pl.multiple_of(start, size), size)


class TensorSum:
    def __init__(self, part, total, land_mate, land_across, half, send, recv):
        self.core, self.mate, self.across = tensor_peers()
        self.part, self.total, self.half = part, total, half
        self.land_mate, self.land_across = land_mate, land_across
        self.send, self.recv = send, recv
        self.rows = part.shape[0] // BLOCKS
        self.size = self.rows // 2

    def span(self, block, side):
        return aligned(block * self.rows + side * self.size, self.size)

    def slot(self, block):
        return aligned(block * self.size, self.size)

    def first(self, block):
        return remote(
            self.part.at[self.span(block, 1 - self.core)], self.land_mate.at[self.slot(block)],
            self.send.at[0, block], self.recv.at[0, block], self.mate,
        )

    def second(self, block):
        return remote(
            self.half.at[self.slot(block)], self.land_across.at[self.slot(block)],
            self.send.at[1, block], self.recv.at[1, block], self.across,
        )

    def third(self, block):
        mine = self.total.at[self.span(block, self.core)]
        return remote(mine, mine, self.send.at[2, block], self.recv.at[2, block], self.mate)

    def start(self):
        for block in range(BLOCKS):
            self.first(block).start()

    def cross(self, block):
        self.first(block).wait_recv()
        slot = self.slot(block)
        self.half[slot] = self.part[self.span(block, self.core)] + self.land_mate[slot]
        self.second(block).start()

    def share(self, block):
        self.second(block).wait_recv()
        slot = self.slot(block)
        self.total[self.span(block, self.core)] = self.half[slot] + self.land_across[slot]
        self.third(block).start()

    def finish(self):
        for block in range(BLOCKS):
            self.third(block).wait_recv()
        for block in range(BLOCKS):
            self.first(block).wait_send()
            self.second(block).wait_send()
            self.third(block).wait_send()


class Swap:
    def __init__(self, source, result, send, recv, close_send, close_recv):
        self.n = lax.axis_size("dp")
        self.me = lax.axis_index("dp")
        self.t = lax.axis_index("tensor")
        self.ranks = lax.axis_size("tensor")
        _, self.mate, self.across = tensor_peers()
        self.source, self.result = source, result
        self.sems = send, recv, close_send, close_recv
        self.seg = result.shape[0] // self.n
        self.part = self.seg // self.ranks

    def at(self, place, rank):
        return aligned(place * self.seg + rank * self.part, self.part)

    def out(self, k):
        other = lax.rem(self.me + k, self.n)
        return remote(
            self.source.at[self.at(other, self.t)], self.result.at[self.at(self.me, self.t)],
            self.sems[0].at[k], self.sems[1].at[k], (other, self.t),
        )

    def close(self, k, leg):
        origin = lax.rem(self.me + self.n - k, self.n)
        rank = lax.rem(self.t + 2, self.ranks) if leg == 2 else self.t
        here = self.result.at[self.at(origin, rank)]
        return remote(
            here, here, self.sems[2].at[leg, k], self.sems[3].at[leg, k], self.across if leg == 0 else self.mate
        )

    def start(self):
        mine = self.at(self.me, self.t)
        self.result[mine] = self.source[mine]
        for k in range(1, self.n):
            self.out(k).start()

    def gather(self, k):
        @pl.when(k > 0)
        def _():
            self.out(k).wait_recv()

        self.close(k, 0).start()
        self.close(k, 1).start()

    def forward(self, k):
        self.close(k, 0).wait_recv()
        self.close(k, 2).start()

    def finish(self):
        for k in range(self.n):
            if k:
                self.out(k).wait_send()
            self.close(k, 0).wait_send()
            self.close(k, 1).wait()
            self.close(k, 2).wait()


def tail_kernel(
    heads, key_dim, value_dim, ranges, chunks,
    part2_hbm, ffn_hbm, fgate_hbm, fup_hbm, down_hbm, pre_hbm, core_hbm, update_hbm, state_hbm,
    resid1_ref, upstream_ref, resid_ref, mixed_ref, hidden1_ref,
    w_out_ref, w_mix_ref, w_gate_ref, w_small_ref, norm1_ref, norm2_ref,
    gate_ref, small_ref, taps_ref, rate_ref, gain_ref, inverse_ref,
    output_ref, inputs_grad_ref, fgate_out, fup_out, down_out, out_out, gate_out,
    query_out, key_out, value_out, small_out,
    data, split_x, split_z, split_out, whole_x, whole_z, whole_out, aside, sems,
    part, total, half, land_mate, land_across, sum_send, sum_recv,
    resid1_grad, resid1_low, mixed_grad, low, gate_low, small_low,
    taps_grad, gain_grad, rate_grad, norm1_grad, norm2_grad, ahead, pad, now,
    shuffled, swap_send, swap_recv, close_send, close_recv, load_sem, out_sem,
):
    n, lines, me, t, z, x = grid_place()
    _, mate, across = tensor_peers()
    length, width = resid1_ref.shape
    qk = heads * key_dim
    values = heads * value_dim
    at_fgate, at_fup, at_down, at_out, at_gate, at_mix, at_small, rows_all = ranges
    loads = [
        (part2_hbm, part),
        (fgate_hbm, data.at[pl.ds(at_fgate, at_fup - at_fgate)]),
        (fup_hbm, data.at[pl.ds(at_fup, at_down - at_fup)]),
        (down_hbm, data.at[pl.ds(at_down, at_out - at_down)]),
        (pre_hbm, data.at[pl.ds(at_mix, length)]),
        (core_hbm, data.at[pl.ds(at_mix + length, length), pl.ds(0, values)]),
        (update_hbm, data.at[pl.ds(at_mix + length, length), pl.ds(values, values)]),
        (state_hbm, data.at[pl.ds(at_gate, state_hbm.shape[0])]),
    ]
    loads = [pltpu.make_async_copy(src, dst, load_sem.at[i]) for i, (src, dst) in enumerate(loads)]
    load_ffn = pltpu.make_async_copy(ffn_hbm, part, load_sem.at[len(loads)])
    for load in loads:
        load.start()
    greet([(lax.rem(me + k, n), t) for k in range(1, n)] + [mate, across])
    refs = (
        data.at[pl.ds(at_mix, length)], gate_ref, small_ref, taps_ref, rate_ref, gain_ref,
        data.at[pl.ds(at_mix + length, length), pl.ds(0, values)],
        data.at[pl.ds(at_mix + length, length), pl.ds(values, values)],
        data.at[pl.ds(at_gate, state_hbm.shape[0])], inverse_ref, mixed_grad, low, gate_low, small_low, taps_grad, gain_grad, rate_grad,
        ahead, pad, now,
    )
    sums = [
        TensorSum(part, total, land_mate, land_across.at[i % 2], half, sum_send.at[i], sum_recv.at[i]) for i in range(3)
    ]
    swaps = [
        Swap(source, result, swap_send.at[i], swap_recv.at[i], close_send.at[i], close_recv.at[i])
        for i, (source, result) in enumerate([(total, shuffled), (resid1_grad, inputs_grad_ref)])
    ]
    norm1_grad[...] = jnp.zeros_like(norm1_grad)
    norm2_grad[...] = jnp.zeros_like(norm2_grad)
    backward_start(refs, SPAN)
    loads[0].wait()
    sums[0].start()
    for load in loads[1:]:
        load.wait()

    def norm_back(value, grad, gain, gain_grad_ref):
        scale = lax.rsqrt(jnp.mean(value * value, -1, keepdims=True) + EPS)
        normed = value * scale
        gain_grad_ref[...] += jnp.sum(grad * normed, 0, keepdims=True)
        scaled = grad * gain
        return scale * (scaled - normed * jnp.mean(scaled * normed, -1, keepdims=True))

    def norm2_piece(i):
        here = aligned(i * 64, 64)
        grad = upstream_ref[here].astype(jnp.float32) + norm_back(
            resid1_ref[here], total[here], norm2_ref[...], norm2_grad
        )
        resid1_grad[here] = grad
        resid1_low[here] = grad.astype(jnp.bfloat16)

    def mixed_piece(i):
        tile = aligned(i * 256, 256)
        mixed_grad[:, tile] = dot_nt(resid1_low[...], w_out_ref[tile])

    def out_piece(i):
        tile = aligned(i * 256, 256)
        data[pl.ds(pl.multiple_of(at_out + i * 256, 64), 256)] = dot_tn(
            mixed_ref[:, tile], resid1_low[...]
        )

    def gate_piece(i):
        tile = aligned(i * 256, 256)
        half_rows = width // 2
        data[pl.ds(pl.multiple_of(at_gate + i * 256, 64), 256), 0:values] = dot_tn(hidden1_ref[:, tile], gate_low[...])
        other = aligned(half_rows + i * 256, 256)
        data[pl.ds(pl.multiple_of(at_gate + i * 256, 64), 256), values : 2 * values] = dot_tn(
            hidden1_ref[:, other], gate_low[...]
        )

    def mix_piece(i):
        tile = aligned(i * 256, 256)
        data[pl.ds(pl.multiple_of(at_mix + i * 256, 64), 256)] = dot_tn(hidden1_ref[:, tile], low[...])

    def hidden_piece(i):
        tile = aligned(i * 256, 256)
        part[:, tile] = (
            dot_nt(low[...], w_mix_ref[tile]) + dot_nt(gate_low[...], w_gate_ref[tile])
            + dot_nt(small_low[...], w_small_ref[tile])
        )

    def output_piece(i):
        here = aligned(i * 64, 64)
        total[here] = total[here] + resid1_ref[here]

    def round_piece(i):
        here = aligned(i * 64, 64)
        output_ref[here] = shuffled[here].astype(output_ref.dtype)

    def norm1_piece(i):
        here = aligned(i * 64, 64)
        resid1_grad[here] = resid1_grad[here] + norm_back(
            resid_ref[here].astype(jnp.float32), total[here], norm1_ref[...], norm1_grad
        )

    def small_piece():
        base = at_small
        data[base : rows_all] = jnp.zeros((rows_all - base, width), jnp.float32)
        data[base : base + 4] = taps_grad[...]
        data[base + 4 : base + 5] = norm1_grad[...]
        data[base + 5 : base + 6] = norm2_grad[...]
        data[base + 6 : base + 7, 0:values] = gain_grad[...]
        data[base + 6 : base + 7, values : values + rate_grad.shape[1]] = rate_grad[...]
        data[base + 8 : base + 16] = dot_tn(small_low[...], hidden1_ref[...])[0:8]

    def start_ffn():
        load_ffn.start()
        load_ffn.wait()
        sums[1].start()

    pieces = []

    def plan(first, count, each, run):
        pieces.append((first, count, each, run))
        return first + -(-count // each)

    at = plan(0, BLOCKS, 2, sums[0].cross)
    at = plan(at, BLOCKS, 2, sums[0].share)
    at = plan(at, 1, 1, lambda i: sums[0].finish())
    at = plan(at, length // 64, 2, norm2_piece)
    at = plan(at, values // 256, 1, mixed_piece)
    side = at
    at = plan(at, values // 256, 1, out_piece)
    at_ready_out = at
    at = plan(at, length // SPAN, 1, lambda i: backward_chunk(heads, key_dim, value_dim, length // SPAN - 1 - i, refs))
    side = plan(side, 1, 1, lambda i: start_ffn())
    side = plan(side, BLOCKS, 2, sums[1].cross)
    side = plan(side, BLOCKS, 2, sums[1].share)
    side = plan(side, 1, 1, lambda i: sums[1].finish())
    part_free = side
    side = plan(side, length // 64, 4, output_piece)
    side = plan(side, 1, 1, lambda i: swaps[0].start())
    side = plan(side, n, 2, swaps[0].gather)
    side = plan(side, n, 2, swaps[0].forward)
    side = plan(side, 1, 1, lambda i: swaps[0].finish())
    side = plan(side, length // 64, 4, round_piece)
    at = plan(at, width // 512, 1, gate_piece)
    at_ready_gate = at
    at = plan(at, width // 256, 1, mix_piece)
    at_ready_mix = at
    at = plan(max(at, part_free), width // 256, 1, hidden_piece)
    at = plan(max(at, side), 1, 1, lambda i: sums[2].start())
    at = plan(at, BLOCKS, 2, sums[2].cross)
    at = plan(at, BLOCKS, 2, sums[2].share)
    at = plan(at, 1, 1, lambda i: sums[2].finish())
    at = plan(at, length // 64, 2, norm1_piece)
    at = plan(at, 1, 1, lambda i: small_piece())
    at_ready_small = at
    at = plan(at, 1, 1, lambda i: swaps[1].start())
    at = plan(at, n, 2, swaps[1].gather)
    at = plan(at, n, 2, swaps[1].forward)
    at = plan(at, 1, 1, lambda i: swaps[1].finish())
    assert at_ready_out <= at_out // SLOT and at_ready_gate <= at_gate // SLOT
    assert at_ready_mix <= at_mix // SLOT and at_ready_small <= at_small // SLOT
    delay = LAG * (2 * lines + 1)
    last = max(chunks + delay + 1, at)

    def writes(chunk, act):
        row = chunk * SLOT

        def put(sem, src_cols, dst, start):
            rows = pl.ds(pl.multiple_of(row, SLOT), SLOT)
            src = data.at[rows] if src_cols is None else data.at[rows, pl.ds(*src_cols)]
            copy = pltpu.make_async_copy(src, dst.at[pl.ds(pl.multiple_of(row - start, SLOT), SLOT)], out_sem.at[sem])
            copy.start() if act == "start" else copy.wait()

        def segment(low_row, high_row, run):
            @pl.when((row >= low_row) & (row < high_row))
            def _():
                run()

        segment(at_fgate, at_fup, lambda: put(0, None, fgate_out, at_fgate))
        segment(at_fup, at_down, lambda: put(0, None, fup_out, at_fup))
        segment(at_down, at_out, lambda: put(0, None, down_out, at_down))
        segment(at_out, at_gate, lambda: put(0, None, out_out, at_out))

        def gates():
            put(0, (0, values), gate_out, at_gate)
            put(1, (values, values), gate_out, at_gate - width // 2)

        segment(at_gate, at_mix, gates)

        def mixes():
            put(0, (0, qk), query_out, at_mix)
            put(1, (qk, qk), key_out, at_mix)
            put(2, (2 * qk, values), value_out, at_mix)

        segment(at_mix, at_small, mixes)
        segment(at_small, rows_all, lambda: put(0, None, small_out, at_small))

    def step(slot, carry):
        reduce_slot(
            slot, chunks, data, (split_x, split_z, split_out), (whole_x, whole_z, whole_out), aside, sems
        )
        writes(slot - delay - 1, "wait")
        writes(slot - delay, "start")
        for first, count, each, run in pieces:
            steps = -(-count // each)

            @pl.when((slot >= first) & (slot < first + steps))
            def _(first=first, each=each, run=run):
                if each == 1:
                    run(slot - first)
                else:
                    def inner(i, carry):
                        run((slot - first) * each + i)
                        return carry

                    lax.fori_loop(0, each, inner, 0)

        return carry

    lax.fori_loop(0, last + 1, step, 0)


def tail(
    part2, ffn, fgate, fup, down, pre, core, update, states, resid1, upstream, resid, mixed, hidden1,
    w_out, w_mix, w_gate, w_small, norm1, norm2, gate, small, taps, rate, gain, inverses,
    heads, key_dim, value_dim, places, collective_id,
):
    length, width = resid1.shape
    values = heads * value_dim
    qk = heads * key_dim
    lanes = small.shape[1]
    heights = [fgate.shape[0], fup.shape[0], down.shape[0], values, values, width, SLOT]
    ranges = [0]
    for height in heights:
        ranges.append(ranges[-1] + height)
    rows_all = ranges[-1]
    chunks = rows_all // SLOT
    f32, bf = jnp.float32, jnp.bfloat16
    shape = jax.ShapeDtypeStruct
    out_shape = [
        shape((length, width), bf),
        shape((length, width), f32),
        shape(fgate.shape, f32),
        shape(fup.shape, f32),
        shape(down.shape, f32),
        shape((values, width), f32),
        shape((width, values), f32),
        shape((width, qk), f32),
        shape((width, qk), f32),
        shape((width, values), f32),
        shape((SLOT, width), f32),
    ]
    vmem, any_ = VM, pl.BlockSpec(memory_space=pl.ANY)
    dma = pltpu.SemaphoreType.DMA
    scratch = (
        [pltpu.VMEM((rows_all, width), f32)]
        + reduce_scratch(width)
        + [
            pltpu.VMEM((length, width), f32),
            pltpu.VMEM((length, width), f32),
            pltpu.VMEM((length // 2, width), f32),
            pltpu.VMEM((length // 2, width), f32),
            pltpu.VMEM((2, length // 2, width), f32),
            dma((3, 3, BLOCKS)),
            dma((3, 3, BLOCKS)),
            pltpu.VMEM((length, width), f32),
            pltpu.VMEM((length, width), bf),
            pltpu.VMEM((length, values), f32),
            pltpu.VMEM((length, width), bf),
            pltpu.VMEM((length, values), bf),
            pltpu.VMEM((length, lanes), bf),
            pltpu.VMEM(taps.shape, f32),
            pltpu.VMEM((1, values), f32),
            pltpu.VMEM((1, lanes), f32),
            pltpu.VMEM((1, width), f32),
            pltpu.VMEM((1, width), f32),
            pltpu.VMEM((HALO + SPAN, width), f32),
            pltpu.VMEM((HALO + SPAN, width), f32),
            pltpu.VMEM((heads, key_dim, value_dim), f32),
            pltpu.VMEM((length, width), f32),
            dma((2, places)),
            dma((2, places)),
            dma((2, 3, places)),
            dma((2, 3, places)),
            dma((9,)),
            dma((3,)),
        ]
    )
    return pl.pallas_call(
        functools.partial(tail_kernel, heads, key_dim, value_dim, tuple(ranges[:7]) + (rows_all,), chunks),
        out_shape=out_shape,
        in_specs=[any_] * 9 + [vmem] * 17,
        out_specs=[vmem] * 2 + [any_] * 9,
        scratch_shapes=scratch,
        compiler_params=pltpu.CompilerParams(
            collective_id=collective_id, has_side_effects=True, vmem_limit_bytes=67043328
        ),
        name="tail",
    )(
        part2, ffn, fgate, fup, down, pre, core, update, states, resid1, upstream, resid, mixed, hidden1,
        w_out, w_mix, w_gate, w_small, norm1, norm2, gate, small, taps, rate, gain, inverses,
    )


def finish_kernel(count, heads, qk, values, *refs):
    sources, rows = refs[:count], refs[count]
    results = refs[count + 1 : 2 * count + 1]
    norm1, norm2, head, rate, beta, decay, query, key, value = refs[2 * count + 1 : 2 * count + 10]
    held, sems = refs[2 * count + 10 : 3 * count + 10], refs[-1]
    loads = [pltpu.make_async_copy(sources[i], held[i], sems.at[0, i]) for i in range(count)]
    stores = [pltpu.make_async_copy(held[i], results[i], sems.at[1, i]) for i in range(count)]
    for load in loads:
        load.start()
    norm1[...] = rows[4:5]
    norm2[...] = rows[5:6]
    head[...] = rows[6:7, 0:values]
    rate[...] = rows[6:7, values : values + 2 * heads][:, heads:]
    beta[...] = rows[8 : 8 + heads]
    decay[...] = rows[8 + heads : 8 + 2 * heads]
    query[...] = rows[0:4, 0:qk]
    key[...] = rows[0:4, qk : 2 * qk]
    value[...] = rows[0:4, 2 * qk :]
    for load, store in zip(loads, stores):
        load.wait()
        store.start()
    for store in stores:
        store.wait()


def finish(arrays, rows, heads, qk, values):
    count = len(arrays)
    width = rows.shape[1]
    any_ = pl.BlockSpec(memory_space=pl.ANY)
    f32 = jnp.float32
    smalls = [(1, width), (1, width), (1, values), (1, heads), (heads, width), (heads, width), (4, qk), (4, qk), (4, values)]
    return pl.pallas_call(
        functools.partial(finish_kernel, count, heads, qk, values),
        out_shape=[jax.ShapeDtypeStruct(a.shape, a.dtype) for a in arrays]
        + [jax.ShapeDtypeStruct(shape, f32) for shape in smalls],
        in_specs=[any_] * count + [VM],
        out_specs=[any_] * count + [VM] * len(smalls),
        scratch_shapes=[pltpu.VMEM(a.shape, a.dtype) for a in arrays] + [pltpu.SemaphoreType.DMA((2, count))],
        compiler_params=pltpu.CompilerParams(vmem_limit_bytes=67043328),
        name="finish",
    )(*arrays, rows)


PAIR = 2


def unit_inverses(lowers, rows, cols):
    count = lowers[0].shape[0]
    near = (rows // 2 == cols // 2) & (rows > cols)
    inverses = [jnp.where(rows == cols, 1.0, jnp.where(near, -lower, 0.0)) for lower in lowers]
    block = 2
    while block < count:
        cross = (rows // (2 * block) == cols // (2 * block)) & (rows // block > cols // block)
        steps = [mm(inverse, jnp.where(cross, lower, 0.0)) for inverse, lower in zip(inverses, lowers)]
        inverses = [inverse - mm(step, inverse) for inverse, step in zip(inverses, steps)]
        block *= 2
    return inverses


def head_kernel(
    heads, key_dim, value_dim,
    pre_ref, gate_ref, small_ref, taps_ref, rate_ref, gain_ref, w_out_ref, resid_ref, cotangent_ref,
    mixed_ref, core_ref, update_ref, state_ref, inverse_ref, resid1_ref, upstream_ref,
    pad, now, solved_key, rise_query, key_tail, attend_all, ends,
    part, land_mate, land_across, half, sum_send, sum_recv,
    staged, arrived, swap_send, swap_recv, close_send, close_recv,
):
    length, width = pre_ref.shape
    span = SPAN
    chunks = length // span
    rows, cols = grids(span)
    qk = heads * key_dim
    n, _, me, t, _, _ = grid_place()
    _, mate, across = tensor_peers()
    greet([(lax.rem(me + k, n), t) for k in range(1, n)] + [mate, across])
    total = TensorSum(part, resid1_ref, land_mate, land_across, half, sum_send, sum_recv)
    swap = Swap(staged, arrived, swap_send, swap_recv, close_send, close_recv)
    for place in range(n):
        mine = swap.at(place, t)
        staged[mine] = cotangent_ref[mine].astype(jnp.float32)
    swap.start()
    pad[0:HALO] = jnp.zeros((HALO, width), jnp.float32)
    now[...] = jnp.zeros_like(now)

    def prepare_pair(turn, carry):
        items = []
        for k in range(PAIR):
            index = turn * PAIR + k
            here = aligned(index * span, span)
            pad[HALO : HALO + span] = pre_ref[here, :]
            total_pre = conv_window(pad[...], taps_ref[...], span)
            pad[0:HALO] = pad[span : span + HALO]
            active = total_pre * sigmoid(total_pre)
            beta, _, _, cumul = gates_of(small_ref[here, :], rate_ref[...], heads, rows, cols)
            beta_t = jnp.transpose(beta)
            cumul_t = jnp.transpose(cumul)
            for head in range(heads):
                query = active[:, head * key_dim : (head + 1) * key_dim]
                query = query * (lax.rsqrt(jnp.sum(query * query, -1, keepdims=True) + EPS) * key_dim ** (-0.5))
                key = active[:, qk + head * key_dim : qk + (head + 1) * key_dim]
                key = key * lax.rsqrt(jnp.sum(key * key, -1, keepdims=True) + EPS)
                value = active[:, 2 * qk + head * value_dim : 2 * qk + (head + 1) * value_dim]
                beta_col = beta[:, head : head + 1]
                cum_col = cumul[:, heads + head : heads + head + 1]
                cum_row = cumul_t[heads + head : heads + head + 1]
                within = cols <= rows
                decays = jnp.where(within, jnp.exp(jnp.where(within, cum_col - cum_row, 0.0)), 0.0)
                scaled = decays * beta_t[head : head + 1]
                products = mm_nt(jnp.concatenate([query, key], 0), key)
                lower = jnp.where(cols < rows, scaled * products[span:], 0.0)
                attend = scaled * products[:span]
                last = cum_col[span - 1 : span]
                rise = jnp.exp(cum_col)
                narrow = slice(head * key_dim, (head + 1) * key_dim)
                attend_all[index, head] = attend
                rise_query[here, narrow] = rise * query
                key_tail[here, narrow] = key * (jnp.exp(last - cum_col) * beta_col)
                ends[index, head] = jnp.broadcast_to(jnp.exp(last), (8, 128))
                items.append((index, head, here, lower, jnp.concatenate([value, rise * key], 1)))
        inverses = unit_inverses([item[3] for item in items], rows, cols)
        solved = [mm(inverse, item[4]) for inverse, item in zip(inverses, items)]
        for (index, head, here, _, _), inverse, solution_ in zip(items, inverses, solved):
            inverse_ref[index, head] = inverse
            update_ref[here, head * value_dim : (head + 1) * value_dim] = solution_[:, :value_dim]
            solved_key[here, head * key_dim : (head + 1) * key_dim] = solution_[:, value_dim:]
        for k in range(PAIR):
            swap.gather(turn * PAIR + k)
        return carry

    lax.fori_loop(0, chunks // PAIR, prepare_pair, 0)

    def project_out(index):
        here = aligned(index * span, span)
        part[here] = dot_plain(mixed_ref[here], w_out_ref[...])
        total.first(index).start()

    def chain(index, carry):
        @pl.when(index > 0)
        def _():
            project_out(index - 1)

        @pl.when(index > 1)
        def _():
            total.cross(index - 2)

        @pl.when(index > 3)
        def _():
            total.share(index - 4)

        here = aligned(index * span, span)
        gate = gate_ref[here, :]
        gated = gate * sigmoid(gate) * gain_ref[...]
        for head in range(heads):
            narrow = slice(head * key_dim, (head + 1) * key_dim)
            wide = slice(head * value_dim, (head + 1) * value_dim)
            state = now[head]
            state_ref[state_place(index, head, heads, key_dim, value_dim, width)] = state
            both = mm(jnp.concatenate([solved_key[here, narrow], rise_query[here, narrow]], 0), state)
            update = update_ref[here, wide] - both[:span]
            now[head] = ends[index, head][0:1, 0:1] * state + mm_tn(key_tail[here, narrow], update)
            core = both[span:] + mm(attend_all[index, head], update)
            update_ref[here, wide] = update
            core_ref[here, wide] = core
            normed = core * lax.rsqrt(jnp.mean(core * core, -1, keepdims=True) + EPS)
            mixed_ref[here, wide] = (normed * gated[:, wide]).astype(mixed_ref.dtype)
        swap.forward(index)
        return carry

    lax.fori_loop(0, chunks, chain, 0)
    project_out(chunks - 1)
    total.cross(chunks - 2)
    total.share(chunks - 4)
    total.cross(chunks - 1)
    total.share(chunks - 3)
    total.share(chunks - 2)
    total.share(chunks - 1)
    swap.finish()

    def turn_low(i, carry):
        here = aligned(i * 64, 64)
        upstream_ref[here] = arrived[here].astype(upstream_ref.dtype)
        return carry

    lax.fori_loop(0, length // 64, turn_low, 0)
    total.finish()

    def add_resid(i, carry):
        here = aligned(i * 64, 64)
        resid1_ref[here] = resid1_ref[here] + resid_ref[here]
        return carry

    lax.fori_loop(0, length // 64, add_resid, 0)


def head_part(
    pre, gate, small, taps, rate, gain, w_out, resid, cotangent, heads, key_dim, value_dim, places, collective_id
):
    length, width = pre.shape
    values = heads * value_dim
    qk = heads * key_dim
    chunks = length // SPAN
    f32, bf = jnp.float32, jnp.bfloat16
    shape = jax.ShapeDtypeStruct
    dma = pltpu.SemaphoreType.DMA
    return pl.pallas_call(
        functools.partial(head_kernel, heads, key_dim, value_dim),
        out_shape=[
            shape((length, values), bf),
            shape((length, values), f32),
            shape((length, values), f32),
            shape((chunks * heads * key_dim * value_dim // width, width), f32),
            shape((chunks, heads, SPAN, SPAN), f32),
            shape((length, width), f32),
            shape((length, width), bf),
        ],
        in_specs=[VM] * 9,
        out_specs=[VM] * 7,
        scratch_shapes=[
            pltpu.VMEM((HALO + SPAN, width), f32),
            pltpu.VMEM((heads, key_dim, value_dim), f32),
            pltpu.VMEM((length, qk), f32),
            pltpu.VMEM((length, qk), f32),
            pltpu.VMEM((length, qk), f32),
            pltpu.VMEM((chunks, heads, SPAN, SPAN), f32),
            pltpu.VMEM((chunks, heads, 8, 128), f32),
            pltpu.VMEM((length, width), f32),
            pltpu.VMEM((length // 2, width), f32),
            pltpu.VMEM((length // 2, width), f32),
            pltpu.VMEM((length // 2, width), f32),
            dma((3, BLOCKS)),
            dma((3, BLOCKS)),
            pltpu.VMEM((length, width), f32),
            pltpu.VMEM((length, width), f32),
            dma((places,)),
            dma((places,)),
            dma((3, places)),
            dma((3, places)),
        ],
        compiler_params=pltpu.CompilerParams(
            collective_id=collective_id, has_side_effects=True, vmem_limit_bytes=56 << 20
        ),
        name="head",
    )(pre, gate, small, taps, rate, gain, w_out, resid, cotangent)


def lane_pad(array, lanes):
    return jnp.pad(array, ((0, 0), (0, lanes - array.shape[1])))


def whole_sequences(
    inputs,
    norm1_gain,
    w_query,
    w_key,
    w_value,
    w_gate,
    w_beta,
    w_decay,
    decay_rate,
    conv_query,
    conv_key,
    conv_value,
    head_gain,
    w_out,
    norm2_gain,
    w_ffn_gate,
    w_ffn_up,
    w_ffn_down,
    cotangent,
):
    batch, seg, width = inputs.shape
    count = batch * seg
    heads = decay_rate.shape[0]
    key_dim = w_query.shape[1] // heads
    value_dim = w_value.shape[1] // heads
    qk_width = heads * key_dim
    lanes = 128
    bf = jnp.bfloat16
    places = lax.axis_size("dp")
    resid, = swap([inputs.reshape(count, width)], places, 1)
    hidden1 = rms_apply(resid, norm1_gain).astype(bf)
    w_mix = jnp.concatenate([w_query, w_key, w_value], axis=1)
    w_small = lane_pad(jnp.concatenate([w_beta, w_decay], axis=1), lanes)
    pre = project(hidden1, w_mix)
    gate_pre = project(hidden1, w_gate)
    small = project(hidden1, w_small)
    taps = jnp.concatenate([conv_query, conv_key, conv_value], axis=1)
    rate = lane_pad(jnp.pad(decay_rate, (heads, 0))[None], lanes)
    gain = head_gain[None]
    mixed, core, update, states, inverses, resid1, upstream = head_part(
        pre, gate_pre, small, taps, rate, gain, w_out, resid, cotangent.reshape(count, width),
        heads, key_dim, value_dim, places, 2,
    )
    hidden2 = rms_apply(resid1, norm2_gain).astype(bf)
    ffn_gate = project(hidden2, w_ffn_gate)
    ffn_up = project(hidden2, w_ffn_up)
    inner_full, swiglu_back = jax.vjp(swiglu, ffn_gate, ffn_up)
    inner = inner_full.astype(bf)
    grad_inner = back_project(upstream, w_ffn_down)
    grad_fgate, grad_fup = swiglu_back(grad_inner)
    grad_fgate = grad_fgate.astype(bf)
    grad_fup = grad_fup.astype(bf)
    part2 = back_project(grad_fgate, w_ffn_gate) + back_project(grad_fup, w_ffn_up)
    fgate = contract_rows(grad_fgate, hidden2)
    fup = contract_rows(grad_fup, hidden2)
    down = contract_rows(inner, upstream)
    ffn = project(inner, w_ffn_down)
    *arrays, rows = tail(
        part2, ffn, fgate, fup, down, pre, core, update, states, resid1, upstream, resid.astype(bf), mixed, hidden1,
        w_out, w_mix, w_gate, w_small, norm1_gain[None], norm2_gain[None],
        gate_pre, small, taps, rate, gain, inverses,
        heads, key_dim, value_dim, places, 7,
    )
    (
        output, grad_inputs, fgate, fup, grad_down, grad_out_w, grad_gate_w, grad_query_w, grad_key_w, grad_value_w,
        grad_norm1_gain, grad_norm2_gain, grad_head, grad_rate, grad_beta_w, grad_decay_w,
        grad_convq, grad_convk, grad_convv,
    ) = finish(arrays, rows, heads, qk_width, heads * value_dim)
    return (
        output.reshape(batch, seg, width),
        grad_inputs.reshape(batch, seg, width),
        grad_norm1_gain[0],
        grad_query_w,
        grad_key_w,
        grad_value_w,
        grad_gate_w,
        grad_beta_w.T,
        grad_decay_w.T,
        grad_rate[0],
        grad_convq,
        grad_convk,
        grad_convv,
        grad_head[0],
        grad_out_w,
        grad_norm2_gain[0],
        fgate.T,
        fup.T,
        grad_down,
    )


def fits_whole(mesh, args):
    batch, length, width = args[0].shape
    places, ranks = mesh.shape["dp"], mesh.shape["tensor"]
    heads = args[8].shape[0] // ranks
    qk = args[2].shape[1] // ranks
    values = args[4].shape[1] // ranks
    units = args[15].shape[1] // ranks
    return (
        batch == places and places == 8 and ranks == 4 and length == places * SPAN and BLOCKS == places and heads <= 4
        and width == 2 * qk + values and width == 2 * values and width % 512 == 0 and length % 256 == 0
        and units % SLOT == 0 and values % 256 == 0
        and length // SPAN * args[2].shape[1] // ranks * (values // heads) <= values * width
    )


def solution(mesh):
    placed = (
        P(None, "dp", None),
        P(),
        P(None, "tensor"),
        P(None, "tensor"),
        P(None, "tensor"),
        P(None, "tensor"),
        P(None, "tensor"),
        P(None, "tensor"),
        P("tensor"),
        P(None, "tensor"),
        P(None, "tensor"),
        P(None, "tensor"),
        P("tensor"),
        P("tensor", None),
        P(),
        P(None, "tensor"),
        P(None, "tensor"),
        P("tensor", None),
        P(None, "dp", None),
    )
    def step(*args):
        body = whole_sequences if fits_whole(mesh, args) else shards
        return placed_step(body)(*args)

    def placed_step(body):
      return jax.shard_map(
        body,
        mesh=mesh,
        in_specs=placed,
        out_specs=(
            P(None, "dp", None),
            P(None, "dp", None),
            P(),
            P(None, "tensor"),
            P(None, "tensor"),
            P(None, "tensor"),
            P(None, "tensor"),
            P(None, "tensor"),
            P(None, "tensor"),
            P("tensor"),
            P(None, "tensor"),
            P(None, "tensor"),
            P(None, "tensor"),
            P("tensor"),
            P("tensor", None),
            P(),
            P(None, "tensor"),
            P(None, "tensor"),
            P("tensor", None),
        ),
        check_vma=False,
    )

    return step
```

```python
import functools
from functools import partial

import jax
import jax.numpy as jnp
from jax import lax
from jax.experimental import pallas as pl
from jax.experimental.pallas import tpu as pltpu
from jax.sharding import PartitionSpec as P

SPAN = 64


EPS = 1e-06


def from_behind(shard, axis, by):
    count = lax.axis_size(axis)
    pairs = [(i, i + by) for i in range(count) if 0 <= i + by < count]
    return lax.ppermute(shard, axis, pairs)


def carried_in(part, axis, combine, identity, reverse):
    count = lax.axis_size(axis)
    place = lax.axis_index(axis)
    ahead = count - 1 - place if reverse else place
    gathered = jax.tree.map(lambda a: lax.all_gather(a, axis), part)
    state = jax.tree.map(lambda a, e: jnp.zeros_like(a) + jnp.asarray(e, a.dtype), part, identity)

    def one(turn, state):
        source = count - 1 - turn if reverse else turn
        return combine(
            state, jax.tree.map(lambda a: lax.dynamic_index_in_dim(a, source, 0, False), gathered)
        )

    return lax.fori_loop(0, ahead, one, state)


def exact(left, right):
    return jnp.matmul(left, right, precision=lax.Precision.HIGHEST)


def span_apply(state, inputs):
    query, key, values, beta, logdecay = inputs
    count = query.shape[0]
    cumul = jnp.cumsum(logdecay)
    row_ids = lax.broadcasted_iota(jnp.int32, (count, count), 0)
    col_ids = lax.broadcasted_iota(jnp.int32, (count, count), 1)
    within = col_ids <= row_ids
    strict = col_ids < row_ids
    spread = jnp.where(within, cumul[:, None] - cumul[None, :], 0.0)
    decays = jnp.where(within, jnp.exp(spread), 0.0)
    scaled = decays * beta[None, :]
    lower = jnp.where(strict, scaled * exact(key, key.T), 0.0)
    start_decay = jnp.exp(cumul)[:, None]
    right_side = values - start_decay * exact(key, state)
    system = jnp.eye(count, dtype=lower.dtype) + lower
    update = jax.scipy.linalg.solve_triangular(system, right_side, lower=True, unit_diagonal=True)
    output = start_decay * exact(query, state) + exact(scaled * exact(query, key.T), update)
    tail = jnp.exp(cumul[-1] - cumul) * beta
    new_state = jnp.exp(cumul[-1]) * state + exact((key * tail[:, None]).T, update)
    return (new_state, output)


def run_segment(query, key, values, beta, logdecay, state):
    length = query.shape[0]
    blocks = length // SPAN

    def split(array):
        return array.reshape((blocks, SPAN) + array.shape[1:])

    final, outputs = lax.scan(
        span_apply, state, (split(query), split(key), split(values), split(beta), split(logdecay))
    )
    return (outputs.reshape((length,) + outputs.shape[2:]), final)


def run_heads(query, key, values, beta, logdecay, state):
    return jax.vmap(jax.vmap(run_segment))(query, key, values, beta, logdecay, state)


def prepare(extended, beta_pre, decay_pre, conv_all, decay_rate, key_dim):
    batch, seg, heads = beta_pre.shape
    reach = conv_all.shape[0] - 1
    total = conv_all[0] * extended[:, 0:seg, :]
    for offset in range(1, reach + 1):
        total = total + conv_all[offset] * extended[:, offset : offset + seg, :]
    active = jax.nn.silu(total)
    qk_width = heads * key_dim
    query = active[..., :qk_width].reshape(batch, seg, heads, key_dim)
    key = active[..., qk_width : 2 * qk_width].reshape(batch, seg, heads, key_dim)
    values = active[..., 2 * qk_width :].reshape(batch, seg, heads, -1)
    query = query * lax.rsqrt(jnp.sum(query * query, -1, keepdims=True) + EPS) * key_dim ** (-0.5)
    key = key * lax.rsqrt(jnp.sum(key * key, -1, keepdims=True) + EPS)
    beta = jax.nn.sigmoid(beta_pre)
    logdecay = -decay_rate * jax.nn.softplus(decay_pre)
    return (
        jnp.moveaxis(query, 2, 1),
        jnp.moveaxis(key, 2, 1),
        jnp.moveaxis(values, 2, 1),
        jnp.moveaxis(beta, 2, 1),
        jnp.moveaxis(logdecay, 2, 1),
    )


def gate_norm(core, gate_pre, head_gain):
    normed = core * lax.rsqrt(jnp.mean(core * core, -1, keepdims=True) + EPS)
    return normed * head_gain * jax.nn.silu(gate_pre)


def rms_apply(resid, gain):
    return resid * lax.rsqrt(jnp.mean(resid * resid, -1, keepdims=True) + EPS) * gain


def swiglu(gate, upper):
    return jax.nn.silu(gate) * upper


def project(left, right):
    return jnp.dot(left, right, preferred_element_type=jnp.float32)


def contract_rows(left, right):
    return jnp.einsum("ra,rb->ab", left, right, preferred_element_type=jnp.float32)


def back_project(grad, weight):
    return jnp.einsum("rb,ab->ra", grad, weight, preferred_element_type=jnp.float32)


def compose(earlier, later):
    return (exact(later[0], earlier[0]), exact(later[0], earlier[1]) + later[1])


def shards(
    inputs,
    norm1_gain,
    w_query,
    w_key,
    w_value,
    w_gate,
    w_beta,
    w_decay,
    decay_rate,
    conv_query,
    conv_key,
    conv_value,
    head_gain,
    w_out,
    norm2_gain,
    w_ffn_gate,
    w_ffn_up,
    w_ffn_down,
    cotangent,
):
    batch, seg, width = inputs.shape
    count = batch * seg
    heads = decay_rate.shape[0]
    key_dim = w_query.shape[1] // heads
    value_dim = w_value.shape[1] // heads
    qk_width = heads * key_dim
    reach = conv_query.shape[0] - 1
    bf = jnp.bfloat16
    resid = inputs.reshape(count, width).astype(jnp.float32)
    normed1, norm1_back = jax.vjp(rms_apply, resid, norm1_gain)
    hidden1 = normed1.astype(bf)
    query_pre = project(hidden1, w_query)
    key_pre = project(hidden1, w_key)
    value_pre = project(hidden1, w_value)
    gate_pre = project(hidden1, w_gate)
    beta_pre = project(hidden1, w_beta)
    decay_pre = project(hidden1, w_decay)
    mixed_pre = jnp.concatenate([query_pre, key_pre, value_pre], axis=1).reshape(batch, seg, -1)
    rim = from_behind(mixed_pre[:, seg - reach :, :], "dp", 1)
    extended = jnp.concatenate([rim, mixed_pre], axis=1)
    conv_all = jnp.concatenate([conv_query, conv_key, conv_value], axis=1)
    features, prep_back = jax.vjp(
        partial(prepare, key_dim=key_dim),
        extended,
        beta_pre.reshape(batch, seg, heads),
        decay_pre.reshape(batch, seg, heads),
        conv_all,
        decay_rate,
    )
    query_h, key_h, value_h, beta_h, decay_h = features
    eye_block = jnp.broadcast_to(
        jnp.eye(key_dim, dtype=jnp.float32), (batch, heads, key_dim, key_dim)
    )
    zero_block = jnp.zeros((batch, heads, key_dim, value_dim), jnp.float32)
    values_aug = jnp.concatenate(
        [jnp.zeros(value_h.shape[:3] + (key_dim,), jnp.float32), value_h], axis=-1
    )
    state_aug = jnp.concatenate([eye_block, zero_block], axis=-1)
    outputs_aug, final_aug = run_heads(query_h, key_h, values_aug, beta_h, decay_h, state_aug)
    out_carry = outputs_aug[..., :key_dim]
    out_local = outputs_aug[..., key_dim:]
    transition = final_aug[..., :key_dim]
    offset_part = final_aug[..., key_dim:]
    prefix = carried_in((transition, offset_part), "dp", compose, (eye_block, zero_block), False)
    start_state = prefix[1]
    core = jnp.moveaxis(exact(out_carry, start_state) + out_local, 1, 2)
    gate4 = gate_pre.reshape(batch, seg, heads, value_dim)
    gated, gate_back = jax.vjp(gate_norm, core, gate4, head_gain.reshape(heads, value_dim))
    mixed = gated.reshape(count, heads * value_dim).astype(bf)
    attention = lax.psum(project(mixed, w_out), "tensor")
    resid1 = resid + attention
    normed2, norm2_back = jax.vjp(rms_apply, resid1, norm2_gain)
    hidden2 = normed2.astype(bf)
    ffn_gate = project(hidden2, w_ffn_gate)
    ffn_up = project(hidden2, w_ffn_up)
    inner_full, swiglu_back = jax.vjp(swiglu, ffn_gate, ffn_up)
    inner = inner_full.astype(bf)
    ffn = lax.psum(project(inner, w_ffn_down), "tensor")
    output = (resid1 + ffn).astype(bf).reshape(batch, seg, width)
    upstream = cotangent.reshape(count, width)
    grad_down = contract_rows(inner, upstream)
    grad_inner = back_project(upstream, w_ffn_down)
    grad_fgate, grad_fup = swiglu_back(grad_inner)
    grad_fgate = grad_fgate.astype(bf)
    grad_fup = grad_fup.astype(bf)
    grad_ffn_gate_w = contract_rows(hidden2, grad_fgate)
    grad_ffn_up_w = contract_rows(hidden2, grad_fup)
    grad_hidden2 = lax.psum(
        back_project(grad_fgate, w_ffn_gate) + back_project(grad_fup, w_ffn_up), "tensor"
    )
    grad_from_norm2, grad_norm2_gain = norm2_back(grad_hidden2)
    grad_resid1 = upstream.astype(jnp.float32) + grad_from_norm2
    grad_resid1_low = grad_resid1.astype(bf)
    grad_out_w = contract_rows(mixed, grad_resid1_low)
    grad_mixed = back_project(grad_resid1_low, w_out).reshape(batch, seg, heads, value_dim)
    grad_core, grad_gate4, grad_head_gain = gate_back(grad_mixed)
    grad_core_h = jnp.moveaxis(grad_core, 2, 1)
    carry_term = exact(jnp.swapaxes(out_carry, -1, -2), grad_core_h)
    suffix = carried_in(
        (jnp.swapaxes(transition, -1, -2), carry_term), "dp", compose, (eye_block, zero_block), True
    )

    def local_delta(query, key, values, beta, logdecay):
        return run_heads(query, key, values, beta, logdecay, start_state)

    recomputed, delta_back = jax.vjp(local_delta, query_h, key_h, value_h, beta_h, decay_h)
    feature_grads = delta_back((grad_core_h, suffix[1]))
    grad_ext, grad_beta_in, grad_decay_in, grad_conv, grad_rate = prep_back(feature_grads)
    returned = from_behind(grad_ext[:, :reach, :], "dp", -1)
    grad_mixed_pre = grad_ext[:, reach:, :] + jnp.pad(returned, ((0, 0), (seg - reach, 0), (0, 0)))
    grad_mixed_pre = grad_mixed_pre.reshape(count, -1)
    grad_query_low = grad_mixed_pre[:, :qk_width].astype(bf)
    grad_key_low = grad_mixed_pre[:, qk_width : 2 * qk_width].astype(bf)
    grad_value_low = grad_mixed_pre[:, 2 * qk_width :].astype(bf)
    grad_gate_low = grad_gate4.reshape(count, heads * value_dim).astype(bf)
    grad_beta_low = grad_beta_in.reshape(count, heads).astype(bf)
    grad_decay_low = grad_decay_in.reshape(count, heads).astype(bf)
    partial_hidden1 = (
        back_project(grad_query_low, w_query)
        + back_project(grad_key_low, w_key)
        + back_project(grad_value_low, w_value)
        + back_project(grad_gate_low, w_gate)
        + back_project(grad_beta_low, w_beta)
        + back_project(grad_decay_low, w_decay)
    )
    grad_hidden1 = lax.psum(partial_hidden1, "tensor")
    grad_from_norm1, grad_norm1_gain = norm1_back(grad_hidden1)
    grad_inputs = (grad_resid1 + grad_from_norm1).reshape(batch, seg, width)
    grad_query_w = contract_rows(hidden1, grad_query_low)
    grad_key_w = contract_rows(hidden1, grad_key_low)
    grad_value_w = contract_rows(hidden1, grad_value_low)
    grad_gate_w = contract_rows(hidden1, grad_gate_low)
    grad_beta_w = contract_rows(hidden1, grad_beta_low)
    grad_decay_w = contract_rows(hidden1, grad_decay_low)
    grad_convq = grad_conv[:, :qk_width]
    grad_convk = grad_conv[:, qk_width : 2 * qk_width]
    grad_convv = grad_conv[:, 2 * qk_width :]
    grad_head_flat = grad_head_gain.reshape(-1)
    (
        grad_norm1_gain,
        grad_query_w,
        grad_key_w,
        grad_value_w,
        grad_gate_w,
        grad_beta_w,
        grad_decay_w,
        grad_rate,
        grad_convq,
        grad_convk,
        grad_convv,
        grad_head_flat,
        grad_out_w,
        grad_norm2_gain,
        grad_ffn_gate_w,
        grad_ffn_up_w,
        grad_down,
    ) = lax.psum(
        (
            grad_norm1_gain,
            grad_query_w,
            grad_key_w,
            grad_value_w,
            grad_gate_w,
            grad_beta_w,
            grad_decay_w,
            grad_rate,
            grad_convq,
            grad_convk,
            grad_convv,
            grad_head_flat,
            grad_out_w,
            grad_norm2_gain,
            grad_ffn_gate_w,
            grad_ffn_up_w,
            grad_down,
        ),
        "dp",
    )
    return (
        output,
        grad_inputs,
        grad_norm1_gain,
        grad_query_w,
        grad_key_w,
        grad_value_w,
        grad_gate_w,
        grad_beta_w,
        grad_decay_w,
        grad_rate,
        grad_convq,
        grad_convk,
        grad_convv,
        grad_head_flat,
        grad_out_w,
        grad_norm2_gain,
        grad_ffn_gate_w,
        grad_ffn_up_w,
        grad_down,
    )


HALO = 8


def mm(left, right):
    return lax.dot_general(
        left, right, (((1,), (0,)), ((), ())),
        precision=lax.Precision.HIGHEST, preferred_element_type=jnp.float32,
    )


def mm_nt(left, right):
    return lax.dot_general(
        left, right, (((1,), (1,)), ((), ())),
        precision=lax.Precision.HIGHEST, preferred_element_type=jnp.float32,
    )


def mm_tn(left, right):
    return lax.dot_general(
        left, right, (((0,), (0,)), ((), ())),
        precision=lax.Precision.HIGHEST, preferred_element_type=jnp.float32,
    )


def grids(count):
    rows = lax.broadcasted_iota(jnp.int32, (count, count), 0)
    cols = lax.broadcasted_iota(jnp.int32, (count, count), 1)
    return rows, cols


def unit_inverse(lower, rows, cols):
    count = lower.shape[0]
    near = (rows // 2 == cols // 2) & (rows > cols)
    inverse = jnp.where(rows == cols, 1.0, jnp.where(near, -lower, 0.0))
    block = 2
    while block < count:
        cross = (rows // (2 * block) == cols // (2 * block)) & (rows // block > cols // block)
        inverse = inverse - mm(mm(inverse, jnp.where(cross, lower, 0.0)), inverse)
        block *= 2
    return inverse


def conv_window(halo_block, taps, span):
    reach = taps.shape[0] - 1
    total = None
    for offset in range(reach + 1):
        start = HALO - reach + offset
        term = taps[offset : offset + 1] * halo_block[start : start + span]
        total = term if total is None else total + term
    return total


def sigmoid(value):
    return 1.0 / (1.0 + jnp.exp(-value))


def softplus(value):
    return jnp.maximum(value, 0.0) + jnp.log(1.0 + jnp.exp(-jnp.abs(value)))


def gates_of(small, rate, heads, rows, cols):
    beta = sigmoid(small)
    slope = softplus(small)
    logdecay = -rate * slope
    cumul = mm(jnp.where(cols <= rows, 1.0, 0.0), logdecay)
    return beta, slope, logdecay, cumul


def state_place(index, head, heads, key_dim, value_dim, width):
    across = width // value_dim
    turn = index * heads + head
    return (
        pl.ds(pl.multiple_of(lax.div(turn, across) * key_dim, key_dim), key_dim),
        pl.ds(pl.multiple_of(lax.rem(turn, across) * value_dim, value_dim), value_dim),
    )


def chunk_terms(query, key, beta_col, beta_row, cum_col, cum_row, rows, cols):
    within = cols <= rows
    decays = jnp.where(within, jnp.exp(jnp.where(within, cum_col - cum_row, 0.0)), 0.0)
    scaled = decays * beta_row
    key_key = mm_nt(key, key)
    query_key = mm_nt(query, key)
    lower = jnp.where(cols < rows, scaled * key_key, 0.0)
    attend = scaled * query_key
    return decays, scaled, key_key, query_key, lower, attend


def forward_kernel(heads, key_dim, value_dim, pre_ref, gate_ref, small_ref, taps_ref, rate_ref, gain_ref,
                   mixed_ref, core_ref, update_ref, state_ref, inverse_ref, pad_ref, now_ref):
    length, width = pre_ref.shape
    span = SPAN
    chunks = length // span
    rows, cols = grids(span)
    qk = heads * key_dim
    pad_ref[0:HALO] = jnp.zeros((HALO, width), jnp.float32)
    for head in range(heads):
        now_ref[head] = jnp.zeros((key_dim, value_dim), jnp.float32)

    def chunk(index, carry):
        start = pl.multiple_of(index * span, span)
        here = pl.ds(start, span)
        pad_ref[HALO : HALO + span] = pre_ref[here, :]
        total = conv_window(pad_ref[...], taps_ref[...], span)
        pad_ref[0:HALO] = pad_ref[span : span + HALO]
        active = total * sigmoid(total)
        beta, _, _, cumul = gates_of(small_ref[here, :], rate_ref[...], heads, rows, cols)
        beta_t = jnp.transpose(beta)
        cumul_t = jnp.transpose(cumul)
        gate = gate_ref[here, :]
        gated = gate * sigmoid(gate) * gain_ref[...]
        for head in range(heads):
            query = active[:, head * key_dim : (head + 1) * key_dim]
            query = query * (lax.rsqrt(jnp.sum(query * query, -1, keepdims=True) + EPS) * key_dim ** (-0.5))
            key = active[:, qk + head * key_dim : qk + (head + 1) * key_dim]
            key = key * lax.rsqrt(jnp.sum(key * key, -1, keepdims=True) + EPS)
            value = active[:, 2 * qk + head * value_dim : 2 * qk + (head + 1) * value_dim]
            beta_col = beta[:, head : head + 1]
            beta_row = beta_t[head : head + 1]
            cum_col = cumul[:, heads + head : heads + head + 1]
            cum_row = cumul_t[heads + head : heads + head + 1]
            _, _, _, _, lower, attend = chunk_terms(query, key, beta_col, beta_row, cum_col, cum_row, rows, cols)
            inverse = unit_inverse(lower, rows, cols)
            state = now_ref[head]
            state_ref[state_place(index, head, heads, key_dim, value_dim, width)] = state
            rise = jnp.exp(cum_col)
            last = cum_col[span - 1 : span]
            update = mm(inverse, value) - mm(mm(inverse, rise * key), state)
            core = mm(rise * query, state) + mm(attend, update)
            tail = jnp.exp(last - cum_col) * beta_col
            now_ref[head] = jnp.exp(last) * state + mm_tn(key * tail, update)
            inverse_ref[index, head] = inverse
            wide = slice(head * value_dim, (head + 1) * value_dim)
            update_ref[here, wide] = update
            core_ref[here, wide] = core
            normed = core * lax.rsqrt(jnp.mean(core * core, -1, keepdims=True) + EPS)
            mixed_ref[here, wide] = (normed * gated[:, wide]).astype(mixed_ref.dtype)
        return carry

    lax.fori_loop(0, chunks, chunk, 0)


def delta_forward(pre, gate, small, taps, rate, gain, heads, key_dim, value_dim):
    length, width = pre.shape
    chunks = length // SPAN
    out_shape = (
        jax.ShapeDtypeStruct((length, heads * value_dim), jnp.bfloat16),
        jax.ShapeDtypeStruct((length, heads * value_dim), jnp.float32),
        jax.ShapeDtypeStruct((length, heads * value_dim), jnp.float32),
        jax.ShapeDtypeStruct((chunks * heads * key_dim * value_dim // width, width), jnp.float32),
        jax.ShapeDtypeStruct((chunks, heads, SPAN, SPAN), jnp.float32),
    )
    return pl.pallas_call(
        functools.partial(forward_kernel, heads, key_dim, value_dim),
        out_shape=out_shape,
        scratch_shapes=[
            pltpu.VMEM((HALO + SPAN, width), jnp.float32),
            pltpu.VMEM((heads, key_dim, value_dim), jnp.float32),
        ],
        compiler_params=pltpu.CompilerParams(vmem_limit_bytes=56 << 20),
        name="delta_forward",
    )(pre, gate, small, taps, rate, gain)


def backward_start(refs, span):
    (_, _, _, _, _, _, _, _, _, _, _, _, _, _, taps_grad_ref, gain_grad_ref, rate_grad_ref,
     _, pad_ref, now_ref) = refs
    now_ref[...] = jnp.zeros_like(now_ref)
    pad_ref[span : span + HALO] = jnp.zeros((HALO, pad_ref.shape[1]), jnp.float32)
    taps_grad_ref[...] = jnp.zeros_like(taps_grad_ref)
    gain_grad_ref[...] = jnp.zeros_like(gain_grad_ref)
    rate_grad_ref[...] = jnp.zeros_like(rate_grad_ref)


def backward_chunk(heads, key_dim, value_dim, index, refs):
    (pre_ref, gate_ref, small_ref, taps_ref, rate_ref, gain_ref,
     core_ref, update_ref, state_ref, inverse_ref, grad_ref,
     low_ref, gate_low_ref, small_low_ref, taps_grad_ref, gain_grad_ref, rate_grad_ref,
     ahead_ref, pad_ref, now_ref) = refs
    width = taps_ref.shape[1]
    span = SPAN
    rows, cols = grids(span)
    qk = heads * key_dim
    reach = taps_ref.shape[0] - 1
    lanes = small_ref.shape[1]
    lane = lax.broadcasted_iota(jnp.int32, (span, lanes), 1)
    start = pl.multiple_of(index * span, span)
    here = pl.ds(start, span)
    before = pl.ds(pl.multiple_of(jnp.maximum(start - HALO, 0), HALO), HALO)
    ahead_ref[0:HALO] = pre_ref[before, :] * jnp.where(index > 0, 1.0, 0.0)
    ahead_ref[HALO : HALO + span] = pre_ref[here, :]
    total = conv_window(ahead_ref[...], taps_ref[...], span)
    gain_of = sigmoid(total)
    active = total * gain_of
    bend = gain_of * (1.0 + total * (1.0 - gain_of))
    small = small_ref[here, :]
    beta, slope, _, cumul = gates_of(small, rate_ref[...], heads, rows, cols)
    beta_t = jnp.transpose(beta)
    cumul_t = jnp.transpose(cumul)
    gate = gate_ref[here, :]
    gate_sig = sigmoid(gate)
    gate_silu = gate * gate_sig
    gate_bend = gate_sig * (1.0 + gate * (1.0 - gate_sig))
    small_grad = jnp.zeros((span, lanes), jnp.float32)
    for head in range(heads):
        wide = slice(head * value_dim, (head + 1) * value_dim)
        core = core_ref[here, wide]
        grad_mixed = grad_ref[here, wide]
        gain = gain_ref[:, wide]
        scale = lax.rsqrt(jnp.mean(core * core, -1, keepdims=True) + EPS)
        normed = core * scale
        gate_low_ref[here, wide] = (grad_mixed * normed * gain * gate_bend[:, wide]).astype(gate_low_ref.dtype)
        with_gate = grad_mixed * gate_silu[:, wide]
        gain_grad_ref[:, wide] += jnp.sum(with_gate * normed, 0, keepdims=True)
        grad_normed = with_gate * gain
        grad_core = scale * (grad_normed - normed * jnp.mean(grad_normed * normed, -1, keepdims=True))
        query_act = active[:, head * key_dim : (head + 1) * key_dim]
        query_scale = lax.rsqrt(jnp.sum(query_act * query_act, -1, keepdims=True) + EPS)
        query = query_act * (query_scale * key_dim ** (-0.5))
        key_act = active[:, qk + head * key_dim : qk + (head + 1) * key_dim]
        key_scale = lax.rsqrt(jnp.sum(key_act * key_act, -1, keepdims=True) + EPS)
        key = key_act * key_scale
        beta_col = beta[:, head : head + 1]
        beta_row = beta_t[head : head + 1]
        cum_col = cumul[:, heads + head : heads + head + 1]
        cum_row = cumul_t[heads + head : heads + head + 1]
        decays, scaled, key_key, query_key, lower, attend = chunk_terms(
            query, key, beta_col, beta_row, cum_col, cum_row, rows, cols
        )
        state = state_ref[state_place(index, head, heads, key_dim, value_dim, width)]
        update = update_ref[here, wide]
        inverse = inverse_ref[index, head]
        grad_state = now_ref[head]
        rise = jnp.exp(cum_col)
        last = cum_col[span - 1 : span]
        fall = jnp.exp(last - cum_col)
        tail = fall * beta_col
        rise_query = rise * query
        rise_key = rise * key
        grad_update = mm_tn(attend, grad_core) + mm(key * tail, grad_state)
        grad_right = mm_tn(inverse, grad_update)
        now_ref[head] = jnp.exp(last) * grad_state + mm_tn(rise_query, grad_core) - mm_tn(rise_key, grad_right)
        grad_attend = jnp.where(cols <= rows, mm_nt(grad_core, update), 0.0)
        grad_lower = jnp.where(cols < rows, -mm_nt(grad_right, update), 0.0)
        core_state = mm_nt(grad_core, state)
        right_state = mm_nt(grad_right, state)
        grad_tail_key = mm_nt(update, grad_state)
        pair_query = grad_attend * scaled
        pair_key = grad_lower * scaled
        grad_query = rise * core_state + mm(pair_query, key)
        grad_key = (
            grad_tail_key * tail - rise * right_state + mm_tn(pair_query, query)
            + mm(pair_key, key) + mm_tn(pair_key, key)
        )
        grad_tail = jnp.sum(grad_tail_key * key, -1, keepdims=True)
        moved = grad_attend * query_key + grad_lower * key_key
        spread = moved * scaled
        by_row = jnp.sum(spread, -1, keepdims=True)
        sums = mm_tn(
            jnp.concatenate([moved * decays, spread], 1), jnp.ones((span, lanes), jnp.float32)
        )
        grad_beta = sums[:span, 0:1] + grad_tail * fall
        through_tail = grad_tail * tail
        grad_cum = (
            by_row - sums[span:, 0:1] - through_tail
            + rise * (jnp.sum(core_state * query, -1, keepdims=True) - jnp.sum(right_state * key, -1, keepdims=True))
        )
        end_grad = jnp.sum(through_tail, 0, keepdims=True) + jnp.exp(last) * jnp.sum(
            jnp.sum(state * grad_state, -1, keepdims=True), 0, keepdims=True
        )
        grad_cum = grad_cum + jnp.where(rows[:, 0:1] == span - 1, end_grad, 0.0)
        small_grad = small_grad + jnp.where(lane == head, grad_beta, 0.0)
        small_grad = small_grad + jnp.where(lane == heads + head, grad_cum, 0.0)
        grad_query = grad_query * key_dim ** (-0.5)
        unit = query_act * query_scale
        grad_query = query_scale * (grad_query - unit * jnp.sum(grad_query * unit, -1, keepdims=True))
        grad_key = key_scale * (grad_key - key * jnp.sum(grad_key * key, -1, keepdims=True))
        at = slice(head * key_dim, (head + 1) * key_dim)
        pad_ref[0:span, at] = grad_query * bend[:, at]
        at = slice(qk + head * key_dim, qk + (head + 1) * key_dim)
        pad_ref[0:span, at] = grad_key * bend[:, at]
        at = slice(2 * qk + head * value_dim, 2 * qk + (head + 1) * value_dim)
        pad_ref[0:span, at] = grad_right * bend[:, at]
    summed = mm(jnp.where(cols >= rows, 1.0, 0.0), small_grad)
    is_beta = lane < heads
    rate_grad_ref[...] += jnp.sum(jnp.where(is_beta, 0.0, -slope * summed), 0, keepdims=True)
    sig = beta
    small_low_ref[here, :] = jnp.where(
        is_beta, small_grad * sig * (1.0 - sig), -rate_ref[...] * sig * summed
    ).astype(small_low_ref.dtype)
    outer = pad_ref[...]
    dense = outer[0:span]
    block = ahead_ref[...]
    grad_pre = None
    for offset in range(reach + 1):
        behind = reach - offset
        taps_grad_ref[offset : offset + 1] += jnp.sum(
            dense * block[HALO - behind : HALO - behind + span], 0, keepdims=True
        )
        term = taps_ref[offset : offset + 1] * outer[behind : behind + span]
        grad_pre = term if grad_pre is None else grad_pre + term
    low_ref[here, :] = grad_pre.astype(low_ref.dtype)
    pad_ref[span : span + HALO] = pad_ref[0:HALO]


MESH = pl.DeviceIdType.MESH
VM = pl.BlockSpec(memory_space=pltpu.VMEM)


def greet(peers):
    barrier = pltpu.get_barrier_semaphore()
    for peer in peers:
        pl.semaphore_signal(barrier, inc=1, device_id=peer, device_id_type=MESH)
    pl.semaphore_wait(barrier, len(peers))


def remote(src, dst, send, recv, peer):
    return pltpu.make_async_remote_copy(
        src_ref=src, dst_ref=dst, send_sem=send, recv_sem=recv, device_id=peer, device_id_type=MESH
    )


def tensor_peers():
    dp = lax.axis_index("dp")
    t = lax.axis_index("tensor")
    core = lax.rem(t, 2)
    mate = (dp, t + 1 - 2 * core)
    across = (dp, lax.rem(t + 2, 4))
    return core, mate, across


def psum_kernel(blocks, part_ref, out_ref, land_mate, land_across, half, send, recv):
    core, mate, across = tensor_peers()
    greet((mate, across))
    rows = part_ref.shape[0] // blocks
    part = rows // 2
    first = []
    for b in range(blocks):
        theirs = pl.ds(pl.multiple_of(b * rows + (1 - core) * part, part), part)
        copy = remote(part_ref.at[theirs], land_mate.at[pl.ds(b * part, part)], send.at[0, b], recv.at[0, b], mate)
        copy.start()
        first.append(copy)
    second = []
    for b in range(blocks):
        mine = pl.ds(pl.multiple_of(b * rows + core * part, part), part)
        slot = pl.ds(b * part, part)
        first[b].wait_recv()
        half[slot] = part_ref[mine] + land_mate[slot]
        copy = remote(half.at[slot], land_across.at[slot], send.at[1, b], recv.at[1, b], across)
        copy.start()
        second.append(copy)
    third = []
    for b in range(blocks):
        mine = pl.ds(pl.multiple_of(b * rows + core * part, part), part)
        slot = pl.ds(b * part, part)
        second[b].wait_recv()
        out_ref[mine] = half[slot] + land_across[slot]
        copy = remote(out_ref.at[mine], out_ref.at[mine], send.at[2, b], recv.at[2, b], mate)
        copy.start()
        third.append(copy)
    for b in range(blocks):
        third[b].wait_recv()
    for b in range(blocks):
        first[b].wait_send()
        second[b].wait_send()
        third[b].wait_send()


def tensor_sum(part, collective_id, blocks=8):
    rows, width = part.shape
    return pl.pallas_call(
        functools.partial(psum_kernel, blocks),
        out_shape=jax.ShapeDtypeStruct(part.shape, part.dtype),
        in_specs=[VM],
        out_specs=VM,
        scratch_shapes=[pltpu.VMEM((rows // 2, width), part.dtype)] * 3
        + [pltpu.SemaphoreType.DMA((3, blocks))] * 2,
        compiler_params=pltpu.CompilerParams(
            collective_id=collective_id, has_side_effects=True, vmem_limit_bytes=40 << 20
        ),
        name="tensor_sum",
    )(part)


def swap_kernel(count, narrow, *refs):
    sources, results = refs[:count], refs[count : 2 * count]
    staged, send, recv, close_send, close_recv = refs[2 * count :]
    n = lax.axis_size("dp")
    me = lax.axis_index("dp")
    t = lax.axis_index("tensor")
    core, mate, across = tensor_peers()
    ranks = lax.axis_size("tensor")
    others = [lax.rem(me + k, n) for k in range(1, n)]
    greet([(other, t) for other in others] + [mate, across])
    seg = results[0].shape[0] // n
    part = seg // ranks
    far = lax.rem(t + 2, ranks)

    def at(place, rank):
        return pl.ds(pl.multiple_of(place * seg + rank * part, part), part)

    outgoing = []
    for i in range(count):
        for k in range(n):
            other = lax.rem(me + k, n)
            if k == 0:
                results[i][at(me, t)] = sources[i][at(me, t)].astype(jnp.float32)
                continue
            if narrow[i]:
                staged[i, k] = sources[i][at(other, t)].astype(jnp.float32)
                src = staged.at[i, k]
            else:
                src = sources[i].at[at(other, t)]
            copy = remote(src, results[i].at[at(me, t)], send.at[i, k], recv.at[i, k], (other, t))
            copy.start()
            outgoing.append(copy)
    close = []
    for i in range(count):
        for k in range(n):
            source = lax.rem(me + n - k, n)
            here = results[i].at[at(source, t)]
            if k:
                remote(here, here, send.at[i, k], recv.at[i, k], (source, t)).wait_recv()
            over = remote(here, here, close_send.at[0, i, k], close_recv.at[0, i, k], across)
            over.start()
            beside = remote(here, here, close_send.at[1, i, k], close_recv.at[1, i, k], mate)
            beside.start()
            close += [over, beside]
    last = []
    for i in range(count):
        for k in range(n):
            source = lax.rem(me + n - k, n)
            there = results[i].at[at(source, far)]
            remote(there, there, close_send.at[0, i, k], close_recv.at[0, i, k], across).wait_recv()
            copy = remote(there, there, close_send.at[2, i, k], close_recv.at[2, i, k], mate)
            copy.start()
            last.append(copy)
    for copy in outgoing:
        copy.wait_send()
    for j, copy in enumerate(close):
        copy.wait_send()
        if j % 2:
            copy.wait_recv()
    for copy in last:
        copy.wait()


def swap(arrays, n, collective_id):
    count = len(arrays)
    rows, width = arrays[0].shape
    narrow = [a.dtype != jnp.float32 for a in arrays]
    out = pl.pallas_call(
        functools.partial(swap_kernel, count, narrow),
        out_shape=[jax.ShapeDtypeStruct((rows, width), jnp.float32)] * count,
        in_specs=[VM] * count,
        out_specs=[VM] * count,
        scratch_shapes=[pltpu.VMEM((count, n, rows // n // 4, width), jnp.float32)]
        + [pltpu.SemaphoreType.DMA((count, n))] * 2
        + [pltpu.SemaphoreType.DMA((3, count, n))] * 2,
        compiler_params=pltpu.CompilerParams(
            collective_id=collective_id, has_side_effects=True, vmem_limit_bytes=40 << 20
        ),
        name="swap",
    )(*arrays)
    return out


SLOT = 80
DEPTH = 10
SPLIT = 3
WHOLE = 2


def grid_place():
    n = lax.axis_size("dp")
    me = lax.axis_index("dp")
    t = lax.axis_index("tensor")
    lines = n // 2
    z = lax.div(me, 2)
    x = lax.rem(me, 2)
    return n, lines, me, t, z, x


def reduce_slot(slot, chunks, data, split_rings, whole_rings, sems):
    n, lines, me, t, z, x = grid_place()
    mate = (me + 1 - 2 * x, t)
    send_x, recv_x, send_z, recv_z, send_d, recv_d, send_p, recv_p, send_s, recv_s = [sems.at[i] for i in range(10)]
    top = lines - 1
    finish = slot - 2 * lines - 1

    def ring(chunk):
        return lax.rem(chunk, DEPTH)

    def within(chunk):
        return (chunk >= 0) & (chunk < chunks)

    for stream in range(SPLIT):
        land_x, land_z, outgo, aside = split_rings
        up = stream % 2 == 0
        level = z if up else top - z
        after = (me + 2, t) if up else (me - 2, t)
        prior = (me - 2, t) if up else (me + 2, t)

        def rows(chunk, side):
            return pl.ds(pl.multiple_of(chunk * SLOT + 16 * stream + 8 * side, 8), 8)

        def spot(ref, chunk):
            return ref.at[stream, ring(chunk)]

        def copy(kind_send, kind_recv, chunk, src, dst, peer):
            at = (stream, ring(chunk))
            return remote(src, dst, kind_send.at[at], kind_recv.at[at], peer)

        def to_mate(chunk):
            return copy(send_x, recv_x, chunk, spot(aside, chunk), spot(land_x, chunk), mate)

        def to_after(chunk):
            return copy(send_z, recv_z, chunk, spot(outgo, chunk), spot(land_z, chunk), after)

        def result(chunk, peer):
            here = data.at[rows(chunk, x)]
            return copy(send_d, recv_d, chunk, here, here, peer)

        def close(chunk, side):
            here = data.at[rows(chunk, side)]
            return copy(send_p, recv_p, chunk, here, here, mate)

        def give_back(chunk):
            @pl.when(level > 0)
            def _():
                result(chunk, prior).start()

            close(chunk, x).start()

        @pl.when(slot < chunks)
        def _():
            aside[stream, ring(slot)] = data[rows(slot, 1 - x)]
            to_mate(slot).start()

        rise = slot - 1 - level

        @pl.when(within(rise))
        def _():
            here = rows(rise, x)
            at = ring(rise)
            to_mate(rise).wait_recv()

            @pl.when(level > 0)
            def _():
                to_after(rise).wait_recv()
                outgo[stream, at] = data[here] + land_x[stream, at] + land_z[stream, at]

            @pl.when(level == 0)
            def _():
                outgo[stream, at] = data[here] + land_x[stream, at]

            @pl.when(level < top)
            def _():
                to_after(rise).start()

            @pl.when(level == top)
            def _():
                data[here] = outgo[stream, at]
                give_back(rise)

        fall = slot - 1 - 2 * top + level

        @pl.when(within(fall) & (level < top))
        def _():
            result(fall, after).wait_recv()
            to_after(fall).wait_send()
            give_back(fall)

        @pl.when(within(finish))
        def _():
            @pl.when(level > 0)
            def _():
                result(finish, prior).wait_send()

            close(finish, x).wait_send()
            close(finish, 1 - x).wait_recv()
            to_mate(finish).wait_send()

    for stream in range(WHOLE):
        land_x, land_z, land_s, outgo = whole_rings
        line = z if stream == 0 else top - z
        step = 2 if stream == 0 else -2
        inner, outer = (me - step, t), (me + step, t)

        def rows(chunk):
            return pl.ds(pl.multiple_of(chunk * SLOT + 16 * (SPLIT + stream), 8), 16)

        def spot(ref, chunk):
            return ref.at[stream, ring(chunk)]

        def copy(kind_send, kind_recv, chunk, src, dst, peer):
            at = (ring(chunk),)
            return remote(
                src, dst, kind_send.at[SPLIT + stream, ring(chunk)], kind_recv.at[SPLIT + stream, ring(chunk)], peer
            )

        def inward(chunk):
            return copy(send_z, recv_z, chunk, spot(outgo, chunk), spot(land_z, chunk), inner)

        def outward(chunk):
            return copy(send_z, recv_s, chunk, spot(outgo, chunk), spot(land_s, chunk), outer)

        def to_mate(chunk):
            return copy(send_x, recv_x, chunk, spot(outgo, chunk), spot(land_x, chunk), mate)

        def result_out(chunk):
            here = data.at[rows(chunk)]
            return copy(send_d, recv_d, chunk, here, here, outer)

        def result_in(chunk):
            here = data.at[rows(chunk)]
            return copy(send_s, recv_d, chunk, here, here, inner)

        rise = slot - 1 - (top - line)
        root = lax.rem(jnp.maximum(rise, 0), 2)

        @pl.when(within(rise) & (line >= root))
        def _():
            here = rows(rise)
            at = ring(rise)

            @pl.when(line < top)
            def _():
                inward(rise).wait_recv()

            is_fork = (line == root) & (root > 0)

            @pl.when(is_fork)
            def _():
                outward(rise).wait_recv()
                outgo[stream, at] = data[here] + land_z[stream, at] + land_s[stream, at]

            @pl.when((line < top) & jnp.logical_not(is_fork))
            def _():
                outgo[stream, at] = data[here] + land_z[stream, at]

            @pl.when(line == top)
            def _():
                outgo[stream, at] = data[here]

            @pl.when(line > root)
            def _():
                inward(rise).start()

            @pl.when(line == root)
            def _():
                to_mate(rise).start()

        leaf = slot - 1

        @pl.when(within(leaf) & (line == 0) & (lax.rem(jnp.maximum(leaf, 0), 2) > 0))
        def _():
            outgo[stream, ring(leaf)] = data[rows(leaf)]
            outward(leaf).start()

        meet = slot - 2 - (top - line)
        meet_root = lax.rem(jnp.maximum(meet, 0), 2)

        @pl.when(within(meet) & (line == meet_root))
        def _():
            at = ring(meet)
            to_mate(meet).wait_recv()
            data[rows(meet)] = outgo[stream, at] + land_x[stream, at]
            result_out(meet).start()

            @pl.when(meet_root > 0)
            def _():
                result_in(meet).start()

        for parity in range(2):
            fall = slot - 2 - (top - parity) - (line - parity)

            @pl.when(within(fall) & (lax.rem(jnp.maximum(fall, 0), 2) == parity) & (line > parity))
            def _():
                result_out(fall).wait_recv()
                inward(fall).wait_send()

                @pl.when(line < top)
                def _():
                    result_out(fall).start()

        inside = slot - 2 - (top - 1) - 1

        @pl.when(within(inside) & (lax.rem(jnp.maximum(inside, 0), 2) > 0) & (line == 0))
        def _():
            result_in(inside).wait_recv()
            outward(inside).wait_send()

        end_root = lax.rem(jnp.maximum(finish, 0), 2)

        @pl.when(within(finish))
        def _():
            @pl.when((line >= end_root) & (line < top))
            def _():
                result_out(finish).wait_send()

            @pl.when(line == end_root)
            def _():
                to_mate(finish).wait_send()

                @pl.when(end_root > 0)
                def _():
                    result_in(finish).wait_send()


def settle(lines):
    return 2 * lines + 1


def reduce_scratch(width):
    return (
        [pltpu.VMEM((SPLIT, DEPTH, 8, width), jnp.float32)] * 4
        + [pltpu.VMEM((WHOLE, DEPTH, 16, width), jnp.float32)] * 4
        + [pltpu.SemaphoreType.DMA((10, SPLIT + WHOLE, DEPTH))]
    )


BLOCKS = 8


def dot_plain(left, right):
    return lax.dot_general(left, right, (((1,), (0,)), ((), ())), preferred_element_type=jnp.float32)


def dot_nt(left, right):
    return lax.dot_general(left, right, (((1,), (1,)), ((), ())), preferred_element_type=jnp.float32)


def dot_tn(left, right):
    return lax.dot_general(left, right, (((0,), (0,)), ((), ())), preferred_element_type=jnp.float32)


def aligned(start, size):
    return pl.ds(pl.multiple_of(start, size), size)


class TensorSum:
    def __init__(self, part, total, land_mate, land_across, half, send, recv):
        self.core, self.mate, self.across = tensor_peers()
        self.part, self.total, self.half = part, total, half
        self.land_mate, self.land_across = land_mate, land_across
        self.send, self.recv = send, recv
        self.rows = part.shape[0] // BLOCKS
        self.size = self.rows // 2

    def span(self, block, side):
        return aligned(block * self.rows + side * self.size, self.size)

    def slot(self, block):
        return aligned(block * self.size, self.size)

    def first(self, block):
        return remote(
            self.part.at[self.span(block, 1 - self.core)], self.land_mate.at[self.slot(block)],
            self.send.at[0, block], self.recv.at[0, block], self.mate,
        )

    def second(self, block):
        return remote(
            self.half.at[self.slot(block)], self.land_across.at[self.slot(block)],
            self.send.at[1, block], self.recv.at[1, block], self.across,
        )

    def third(self, block):
        mine = self.total.at[self.span(block, self.core)]
        return remote(mine, mine, self.send.at[2, block], self.recv.at[2, block], self.mate)

    def start(self):
        for block in range(BLOCKS):
            self.first(block).start()

    def cross(self, block):
        self.first(block).wait_recv()
        slot = self.slot(block)
        self.half[slot] = self.part[self.span(block, self.core)] + self.land_mate[slot]
        self.second(block).start()

    def share(self, block):
        self.second(block).wait_recv()
        slot = self.slot(block)
        self.total[self.span(block, self.core)] = self.half[slot] + self.land_across[slot]
        self.third(block).start()

    def finish(self):
        for block in range(BLOCKS):
            self.third(block).wait_recv()
        for block in range(BLOCKS):
            self.first(block).wait_send()
            self.second(block).wait_send()
            self.third(block).wait_send()


class Swap:
    def __init__(self, source, result, send, recv, close_send, close_recv):
        self.n = lax.axis_size("dp")
        self.me = lax.axis_index("dp")
        self.t = lax.axis_index("tensor")
        self.ranks = lax.axis_size("tensor")
        _, self.mate, self.across = tensor_peers()
        self.source, self.result = source, result
        self.sems = send, recv, close_send, close_recv
        self.seg = result.shape[0] // self.n
        self.part = self.seg // self.ranks

    def at(self, place, rank):
        return aligned(place * self.seg + rank * self.part, self.part)

    def out(self, k):
        other = lax.rem(self.me + k, self.n)
        return remote(
            self.source.at[self.at(other, self.t)], self.result.at[self.at(self.me, self.t)],
            self.sems[0].at[k], self.sems[1].at[k], (other, self.t),
        )

    def close(self, k, leg):
        origin = lax.rem(self.me + self.n - k, self.n)
        rank = lax.rem(self.t + 2, self.ranks) if leg == 2 else self.t
        here = self.result.at[self.at(origin, rank)]
        return remote(
            here, here, self.sems[2].at[leg, k], self.sems[3].at[leg, k], self.across if leg == 0 else self.mate
        )

    def start(self):
        mine = self.at(self.me, self.t)
        self.result[mine] = self.source[mine]
        for k in range(1, self.n):
            self.out(k).start()

    def gather(self, k):
        @pl.when(k > 0)
        def _():
            self.out(k).wait_recv()

        self.close(k, 0).start()
        self.close(k, 1).start()

    def forward(self, k):
        self.close(k, 0).wait_recv()
        self.close(k, 2).start()

    def sent(self):
        for k in range(1, self.n):
            self.out(k).wait_send()

    def finish(self):
        for k in range(self.n):
            self.close(k, 0).wait_send()
            self.close(k, 1).wait()
            self.close(k, 2).wait()


def tail_kernel(
    heads, key_dim, value_dim, ranges, chunks,
    part2_hbm, ffn_hbm, down_hbm, pre_hbm, core_hbm, update_hbm, state_hbm,
    resid1_ref, upstream_ref, resid_ref, mixed_ref, hidden1_ref, hidden2_ref, units_ref,
    w_out_ref, w_mix_ref, w_gate_ref, w_small_ref, norm1_ref, norm2_ref,
    gate_ref, small_ref, taps_ref, rate_ref, gain_ref, inverse_ref,
    data, output_ref, inputs_grad_ref,
    split_x, split_z, split_out, split_aside, whole_x, whole_z, whole_s, whole_out, sems,
    part, total, half, land_mate, land_across, sum_send, sum_recv,
    resid1_grad, resid1_low, mixed_grad, low, gate_low, small_low,
    taps_grad, gain_grad, rate_grad, norm1_grad, norm2_grad, ahead, pad, now,
    shuffled, swap_send, swap_recv, close_send, close_recv, load_sem,
):
    n, lines, me, t, z, x = grid_place()
    _, mate, across = tensor_peers()
    length, width = resid1_ref.shape
    qk = heads * key_dim
    values = heads * value_dim
    at_down, at_units, at_out, at_gate, at_mix, at_small, at_end, rows_all = ranges
    loads = [
        (part2_hbm, part),
        (down_hbm, data.at[pl.ds(at_down, at_units - at_down)]),
        (pre_hbm, data.at[pl.ds(at_mix, length)]),
        (core_hbm, data.at[pl.ds(at_mix + length, length), pl.ds(0, values)]),
        (update_hbm, data.at[pl.ds(at_mix + length, length), pl.ds(values, values)]),
        (state_hbm, data.at[pl.ds(at_gate, state_hbm.shape[0])]),
    ]
    loads = [pltpu.make_async_copy(src, dst, load_sem.at[i]) for i, (src, dst) in enumerate(loads)]
    load_ffn = pltpu.make_async_copy(ffn_hbm, part, load_sem.at[len(loads)])
    for load in loads:
        load.start()
    greet([(lax.rem(me + k, n), t) for k in range(1, n)] + [mate, across])
    refs = (
        data.at[pl.ds(at_mix, length)], gate_ref, small_ref, taps_ref, rate_ref, gain_ref,
        data.at[pl.ds(at_mix + length, length), pl.ds(0, values)],
        data.at[pl.ds(at_mix + length, length), pl.ds(values, values)],
        data.at[pl.ds(at_gate, state_hbm.shape[0])], inverse_ref, mixed_grad, low, gate_low, small_low, taps_grad, gain_grad, rate_grad,
        ahead, pad, now,
    )
    sums = [
        TensorSum(part, total, land_mate, land_across.at[i % 2], half, sum_send.at[i], sum_recv.at[i]) for i in range(3)
    ]
    swaps = [
        Swap(source, result, swap_send.at[i], swap_recv.at[i], close_send.at[i], close_recv.at[i])
        for i, (source, result) in enumerate([(total, shuffled), (resid1_grad, inputs_grad_ref)])
    ]
    norm1_grad[...] = jnp.zeros_like(norm1_grad)
    norm2_grad[...] = jnp.zeros_like(norm2_grad)
    backward_start(refs, SPAN)
    data[at_end:rows_all] = jnp.zeros((rows_all - at_end, width), jnp.float32)
    loads[0].wait()
    sums[0].start()
    loads[1].wait()

    def units_piece(i):
        data[pl.ds(pl.multiple_of(at_units + i * 128, 64), 128)] = dot_tn(
            units_ref[:, aligned(i * 128, 128)], hidden2_ref[...]
        )

    def wait_loads():
        for load in loads[2:]:
            load.wait()

    def norm_back(value, grad, gain, gain_grad_ref):
        scale = lax.rsqrt(jnp.mean(value * value, -1, keepdims=True) + EPS)
        normed = value * scale
        gain_grad_ref[...] += jnp.sum(grad * normed, 0, keepdims=True)
        scaled = grad * gain
        return scale * (scaled - normed * jnp.mean(scaled * normed, -1, keepdims=True))

    def norm2_piece(i):
        here = aligned(i * 64, 64)
        grad = upstream_ref[here].astype(jnp.float32) + norm_back(
            resid1_ref[here], total[here], norm2_ref[...], norm2_grad
        )
        resid1_grad[here] = grad
        resid1_low[here] = grad.astype(jnp.bfloat16)

    def mixed_piece(i):
        tile = aligned(i * 256, 256)
        mixed_grad[:, tile] = dot_nt(resid1_low[...], w_out_ref[tile])

    def out_piece(i):
        tile = aligned(i * 256, 256)
        data[pl.ds(pl.multiple_of(at_out + i * 256, 64), 256)] = dot_tn(
            mixed_ref[:, tile], resid1_low[...]
        )

    def gate_piece(i):
        tile = aligned(i * 256, 256)
        half_rows = width // 2
        data[pl.ds(pl.multiple_of(at_gate + i * 256, 64), 256), 0:values] = dot_tn(hidden1_ref[:, tile], gate_low[...])
        other = aligned(half_rows + i * 256, 256)
        data[pl.ds(pl.multiple_of(at_gate + i * 256, 64), 256), values : 2 * values] = dot_tn(
            hidden1_ref[:, other], gate_low[...]
        )

    def mix_piece(i):
        tile = aligned(i * 256, 256)
        data[pl.ds(pl.multiple_of(at_mix + i * 256, 64), 256)] = dot_tn(hidden1_ref[:, tile], low[...])

    def hidden_piece(i):
        tile = aligned(i * 256, 256)
        part[:, tile] = (
            dot_nt(low[...], w_mix_ref[tile]) + dot_nt(gate_low[...], w_gate_ref[tile])
            + dot_nt(small_low[...], w_small_ref[tile])
        )

    def output_piece(i):
        here = aligned(i * 64, 64)
        total[here] = total[here] + resid1_ref[here]

    def round_piece(i):
        here = aligned(i * 64, 64)
        output_ref[here] = shuffled[here].astype(output_ref.dtype)

    def norm1_piece(i):
        here = aligned(i * 64, 64)
        resid1_grad[here] = resid1_grad[here] + norm_back(
            resid_ref[here].astype(jnp.float32), total[here], norm1_ref[...], norm1_grad
        )

    def small_piece():
        base = at_small
        data[base : at_end] = jnp.zeros((at_end - base, width), jnp.float32)
        data[base : base + 4] = taps_grad[...]
        data[base + 4 : base + 5] = norm1_grad[...]
        data[base + 5 : base + 6] = norm2_grad[...]
        data[base + 6 : base + 7, 0:values] = gain_grad[...]
        data[base + 6 : base + 7, values : values + rate_grad.shape[1]] = rate_grad[...]
        data[base + 8 : base + 16] = dot_tn(small_low[...], hidden1_ref[...])[0:8]

    def start_ffn():
        load_ffn.start()
        load_ffn.wait()
        sums[1].start()

    pieces = []

    def plan(first, count, each, run):
        assert count % each == 0
        pieces.append((first, count, each, run))
        return first + -(-count // each)

    plan(0, (at_out - at_units) // 128, 1, units_piece)
    assert all(i + 1 <= (at_units + 128 * i) // SLOT for i in range((at_out - at_units) // 128))
    plan(0, 1, 1, lambda i: wait_loads())
    at = plan(0, BLOCKS, 2, sums[0].cross)
    at = plan(at, BLOCKS, 2, sums[0].share)
    at = plan(at, 1, 1, lambda i: sums[0].finish())
    at = plan(at, length // 64, 2, norm2_piece)
    at = plan(at, values // 256, 1, mixed_piece)
    side = at
    at = plan(at, values // 256, 1, out_piece)
    at_ready_out = at
    at = plan(at, length // SPAN, 1, lambda i: backward_chunk(heads, key_dim, value_dim, length // SPAN - 1 - i, refs))
    side = plan(side, 1, 1, lambda i: start_ffn())
    side = plan(side, BLOCKS, 2, sums[1].cross)
    side = plan(side, BLOCKS, 2, sums[1].share)
    side = plan(side, 1, 1, lambda i: sums[1].finish())
    part_free = side
    side = plan(side, length // 64, 4, output_piece)
    side = plan(side, 1, 1, lambda i: swaps[0].start())
    side = plan(side, n, 2, swaps[0].gather)
    side = plan(side, 1, 1, lambda i: swaps[0].sent())
    total_free = side
    side = plan(side, n, 2, swaps[0].forward)
    side = plan(side, 1, 1, lambda i: swaps[0].finish())
    side = plan(side, length // 64, 4, round_piece)
    at = plan(at, width // 512, 1, gate_piece)
    at_ready_gate = at
    at = plan(at, width // 256, 1, mix_piece)
    at_ready_mix = at
    at = plan(max(at, part_free), width // 256, 1, hidden_piece)
    at = plan(max(at, total_free), 1, 1, lambda i: sums[2].start())
    at = plan(at, BLOCKS, 2, sums[2].cross)
    at = plan(at, BLOCKS, 2, sums[2].share)
    at = plan(at, 1, 1, lambda i: sums[2].finish())
    at = plan(at, length // 64, 2, norm1_piece)
    at = plan(at, 1, 1, lambda i: small_piece())
    at_ready_small = at
    at = plan(at, 1, 1, lambda i: swaps[1].start())
    at = plan(at, n, 2, swaps[1].gather)
    plan(at, 1, 1, lambda i: swaps[1].sent())
    at = plan(at, n, 2, swaps[1].forward)
    at = plan(at, 1, 1, lambda i: swaps[1].finish())
    assert at_ready_out <= at_out // SLOT and at_ready_gate <= at_gate // SLOT
    assert at_ready_mix <= at_mix // SLOT and at_ready_small <= at_small // SLOT
    last = max(chunks + settle(lines), at, side)

    def step(slot, carry):
        reduce_slot(
            slot, chunks, data, (split_x, split_z, split_out, split_aside), (whole_x, whole_z, whole_s, whole_out), sems
        )
        for first, count, each, run in pieces:
            steps = -(-count // each)

            @pl.when((slot >= first) & (slot < first + steps))
            def _(first=first, each=each, run=run):
                if each == 1:
                    run(slot - first)
                else:
                    def inner(i, carry):
                        run((slot - first) * each + i)
                        return carry

                    lax.fori_loop(0, each, inner, 0)

        return carry

    lax.fori_loop(0, last, step, 0)


def tail(
    part2, ffn, down, pre, core, update, states, resid1, upstream, resid, mixed, hidden1, hidden2, units,
    w_out, w_mix, w_gate, w_small, norm1, norm2, gate, small, taps, rate, gain, inverses,
    heads, key_dim, value_dim, places, collective_id,
):
    length, width = resid1.shape
    values = heads * value_dim
    qk = heads * key_dim
    lanes = small.shape[1]
    heights = [down.shape[0], units.shape[1], values, values, width, 64]
    ranges = [0]
    for height in heights:
        ranges.append(ranges[-1] + height)
    rows_all = -(-ranges[-1] // SLOT) * SLOT
    chunks = rows_all // SLOT
    f32, bf = jnp.float32, jnp.bfloat16
    shape = jax.ShapeDtypeStruct
    out_shape = [
        pltpu.VMEM((rows_all, width), f32),
        pltpu.VMEM((length, width), bf),
        pltpu.VMEM((length, width), f32),
    ]
    vmem, any_ = VM, pl.BlockSpec(memory_space=pl.ANY)
    dma = pltpu.SemaphoreType.DMA
    scratch = (
        reduce_scratch(width)
        + [
            pltpu.VMEM((length, width), f32),
            pltpu.VMEM((length, width), f32),
            pltpu.VMEM((length // 2, width), f32),
            pltpu.VMEM((length // 2, width), f32),
            pltpu.VMEM((2, length // 2, width), f32),
            dma((3, 3, BLOCKS)),
            dma((3, 3, BLOCKS)),
            pltpu.VMEM((length, width), f32),
            pltpu.VMEM((length, width), bf),
            pltpu.VMEM((length, values), f32),
            pltpu.VMEM((length, width), bf),
            pltpu.VMEM((length, values), bf),
            pltpu.VMEM((length, lanes), bf),
            pltpu.VMEM(taps.shape, f32),
            pltpu.VMEM((1, values), f32),
            pltpu.VMEM((1, lanes), f32),
            pltpu.VMEM((1, width), f32),
            pltpu.VMEM((1, width), f32),
            pltpu.VMEM((HALO + SPAN, width), f32),
            pltpu.VMEM((HALO + SPAN, width), f32),
            pltpu.VMEM((heads, key_dim, value_dim), f32),
            pltpu.VMEM((length, width), f32),
            dma((2, places)),
            dma((2, places)),
            dma((2, 3, places)),
            dma((2, 3, places)),
            dma((9,)),
        ]
    )
    return pl.pallas_call(
        functools.partial(tail_kernel, heads, key_dim, value_dim, tuple(ranges) + (rows_all,), chunks),
        out_shape=out_shape,
        in_specs=[any_] * 7 + [vmem] * 19,
        out_specs=[vmem] * 3,
        scratch_shapes=scratch,
        compiler_params=pltpu.CompilerParams(
            collective_id=collective_id, has_side_effects=True,
            vmem_limit_bytes=67043328 - 4 * width * rows_all - 6 * width * length - (1 << 18),
        ),
        name="tail",
    )(
        part2, ffn, down, pre, core, update, states, resid1, upstream, resid, mixed, hidden1, hidden2, units,
        w_out, w_mix, w_gate, w_small, norm1, norm2, gate, small, taps, rate, gain, inverses,
    ), tuple(ranges)


def finish_kernel(heads, qk, values, ranges, data, output, inputs_grad, *refs):
    big, smalls, sems = refs[:10], refs[10:19], refs[19]
    at_down, at_units, at_out, at_gate, at_mix, at_small, _ = ranges
    width = data.shape[1]
    units = big[2].shape[0]

    def rows(start, height, left=0, wide=None):
        return data.at[pl.ds(start, height), pl.ds(left, width if wide is None else wide)]

    half = width // 2
    moves = [
        (output, big[0]),
        (inputs_grad, big[1]),
        (rows(at_units, units), big[2]),
        (rows(at_units + units, units), big[3]),
        (rows(at_down, units), big[4]),
        (rows(at_out, values), big[5]),
        (rows(at_gate, half, 0, values), big[6].at[pl.ds(0, half)]),
        (rows(at_gate, half, values, values), big[6].at[pl.ds(half, half)]),
        (rows(at_mix, width, 0, qk), big[7]),
        (rows(at_mix, width, qk, qk), big[8]),
        (rows(at_mix, width, 2 * qk, values), big[9]),
    ]
    moves = [pltpu.make_async_copy(src, dst, sems.at[i]) for i, (src, dst) in enumerate(moves)]
    for move in moves:
        move.start()
    norm1, norm2, head, rate, beta, decay, query, key, value = smalls
    small = data[at_small : at_small + 16]
    norm1[...] = small[4:5]
    norm2[...] = small[5:6]
    head[...] = small[6:7, 0:values]
    rate[...] = small[6:7, values : values + 2 * heads][:, heads:]
    beta[...] = small[8 : 8 + heads]
    decay[...] = small[8 + heads : 8 + 2 * heads]
    query[...] = small[0:4, 0:qk]
    key[...] = small[0:4, qk : 2 * qk]
    value[...] = small[0:4, 2 * qk :]
    for move in moves:
        move.wait()


def finish(data, output, inputs_grad, ranges, units, heads, qk, values):
    width = data.shape[1]
    length = output.shape[0]
    any_ = pl.BlockSpec(memory_space=pl.ANY)
    f32 = jnp.float32
    bigs = [
        (units, width), (units, width), (units, width), (values, width), (width, values), (width, qk), (width, qk), (width, values)
    ]
    smalls = [(1, width), (1, width), (1, values), (1, heads), (heads, width), (heads, width), (4, qk), (4, qk), (4, values)]
    held = [pltpu.with_memory_space_constraint(a, pltpu.VMEM) for a in (data, output, inputs_grad)]
    return pl.pallas_call(
        functools.partial(finish_kernel, heads, qk, values, ranges),
        out_shape=[jax.ShapeDtypeStruct((length, width), output.dtype), jax.ShapeDtypeStruct((length, width), f32)]
        + [jax.ShapeDtypeStruct(shape, f32) for shape in bigs + smalls],
        in_specs=[VM] * 3,
        out_specs=[any_] * 10 + [VM] * len(smalls),
        scratch_shapes=[pltpu.SemaphoreType.DMA((11,))],
        compiler_params=pltpu.CompilerParams(vmem_limit_bytes=8 << 20),
        name="finish",
    )(*held)


PAIR = 2


def unit_inverses(lowers, rows, cols):
    count = lowers[0].shape[0]
    near = (rows // 2 == cols // 2) & (rows > cols)
    inverses = [jnp.where(rows == cols, 1.0, jnp.where(near, -lower, 0.0)) for lower in lowers]
    block = 2
    while block < count:
        cross = (rows // (2 * block) == cols // (2 * block)) & (rows // block > cols // block)
        steps = [mm(inverse, jnp.where(cross, lower, 0.0)) for inverse, lower in zip(inverses, lowers)]
        inverses = [inverse - mm(step, inverse) for inverse, step in zip(inverses, steps)]
        block *= 2
    return inverses


def head_kernel(
    heads, key_dim, value_dim,
    pre_ref, gate_ref, small_ref, taps_ref, rate_ref, gain_ref, w_out_ref, resid_ref, cotangent_ref,
    mixed_ref, core_ref, update_ref, state_ref, inverse_ref, resid1_ref, upstream_ref,
    pad, now, solved_key, rise_query, key_tail, attend_all, ends,
    part, land_mate, land_across, half, sum_send, sum_recv,
    staged, arrived, swap_send, swap_recv, close_send, close_recv,
):
    length, width = pre_ref.shape
    span = SPAN
    chunks = length // span
    rows, cols = grids(span)
    qk = heads * key_dim
    n, _, me, t, _, _ = grid_place()
    _, mate, across = tensor_peers()
    greet([(lax.rem(me + k, n), t) for k in range(1, n)] + [mate, across])
    total = TensorSum(part, resid1_ref, land_mate, land_across, half, sum_send, sum_recv)
    swap = Swap(staged, arrived, swap_send, swap_recv, close_send, close_recv)
    for place in range(n):
        mine = swap.at(place, t)
        staged[mine] = cotangent_ref[mine].astype(jnp.float32)
    swap.start()
    pad[0:HALO] = jnp.zeros((HALO, width), jnp.float32)
    now[...] = jnp.zeros_like(now)

    def prepare_pair(turn, carry):
        items = []
        for k in range(PAIR):
            index = turn * PAIR + k
            here = aligned(index * span, span)
            pad[HALO : HALO + span] = pre_ref[here, :]
            total_pre = conv_window(pad[...], taps_ref[...], span)
            pad[0:HALO] = pad[span : span + HALO]
            active = total_pre * sigmoid(total_pre)
            beta, _, _, cumul = gates_of(small_ref[here, :], rate_ref[...], heads, rows, cols)
            beta_t = jnp.transpose(beta)
            cumul_t = jnp.transpose(cumul)
            for head in range(heads):
                query = active[:, head * key_dim : (head + 1) * key_dim]
                query = query * (lax.rsqrt(jnp.sum(query * query, -1, keepdims=True) + EPS) * key_dim ** (-0.5))
                key = active[:, qk + head * key_dim : qk + (head + 1) * key_dim]
                key = key * lax.rsqrt(jnp.sum(key * key, -1, keepdims=True) + EPS)
                value = active[:, 2 * qk + head * value_dim : 2 * qk + (head + 1) * value_dim]
                beta_col = beta[:, head : head + 1]
                cum_col = cumul[:, heads + head : heads + head + 1]
                cum_row = cumul_t[heads + head : heads + head + 1]
                within = cols <= rows
                decays = jnp.where(within, jnp.exp(jnp.where(within, cum_col - cum_row, 0.0)), 0.0)
                scaled = decays * beta_t[head : head + 1]
                products = mm_nt(jnp.concatenate([query, key], 0), key)
                lower = jnp.where(cols < rows, scaled * products[span:], 0.0)
                attend = scaled * products[:span]
                last = cum_col[span - 1 : span]
                rise = jnp.exp(cum_col)
                narrow = slice(head * key_dim, (head + 1) * key_dim)
                attend_all[index, head] = attend
                rise_query[here, narrow] = rise * query
                key_tail[here, narrow] = key * (jnp.exp(last - cum_col) * beta_col)
                ends[index, head] = jnp.broadcast_to(jnp.exp(last), (8, 128))
                items.append((index, head, here, lower, jnp.concatenate([value, rise * key], 1)))
        inverses = unit_inverses([item[3] for item in items], rows, cols)
        solved = [mm(inverse, item[4]) for inverse, item in zip(inverses, items)]
        for (index, head, here, _, _), inverse, solution_ in zip(items, inverses, solved):
            inverse_ref[index, head] = inverse
            update_ref[here, head * value_dim : (head + 1) * value_dim] = solution_[:, :value_dim]
            solved_key[here, head * key_dim : (head + 1) * key_dim] = solution_[:, value_dim:]
        for k in range(PAIR):
            swap.gather(turn * PAIR + k)
        return carry

    lax.fori_loop(0, chunks // PAIR, prepare_pair, 0)

    def project_out(index):
        here = aligned(index * span, span)
        part[here] = dot_plain(mixed_ref[here], w_out_ref[...])
        total.first(index).start()

    def chain(index, carry):
        @pl.when(index > 0)
        def _():
            project_out(index - 1)

        @pl.when(index > 1)
        def _():
            total.cross(index - 2)

        @pl.when(index > 3)
        def _():
            total.share(index - 4)

        here = aligned(index * span, span)
        gate = gate_ref[here, :]
        gated = gate * sigmoid(gate) * gain_ref[...]
        for head in range(heads):
            narrow = slice(head * key_dim, (head + 1) * key_dim)
            wide = slice(head * value_dim, (head + 1) * value_dim)
            state = now[head]
            state_ref[state_place(index, head, heads, key_dim, value_dim, width)] = state
            both = mm(jnp.concatenate([solved_key[here, narrow], rise_query[here, narrow]], 0), state)
            update = update_ref[here, wide] - both[:span]
            now[head] = ends[index, head][0:1, 0:1] * state + mm_tn(key_tail[here, narrow], update)
            core = both[span:] + mm(attend_all[index, head], update)
            update_ref[here, wide] = update
            core_ref[here, wide] = core
            normed = core * lax.rsqrt(jnp.mean(core * core, -1, keepdims=True) + EPS)
            mixed_ref[here, wide] = (normed * gated[:, wide]).astype(mixed_ref.dtype)
        swap.forward(index)
        return carry

    lax.fori_loop(0, chunks, chain, 0)
    project_out(chunks - 1)
    total.cross(chunks - 2)
    total.share(chunks - 4)
    total.cross(chunks - 1)
    total.share(chunks - 3)
    total.share(chunks - 2)
    total.share(chunks - 1)
    swap.sent()
    swap.finish()

    def turn_low(i, carry):
        here = aligned(i * 64, 64)
        upstream_ref[here] = arrived[here].astype(upstream_ref.dtype)
        return carry

    lax.fori_loop(0, length // 64, turn_low, 0)
    total.finish()

    def add_resid(i, carry):
        here = aligned(i * 64, 64)
        resid1_ref[here] = resid1_ref[here] + resid_ref[here]
        return carry

    lax.fori_loop(0, length // 64, add_resid, 0)


def head_part(
    pre, gate, small, taps, rate, gain, w_out, resid, cotangent, heads, key_dim, value_dim, places, collective_id
):
    length, width = pre.shape
    values = heads * value_dim
    qk = heads * key_dim
    chunks = length // SPAN
    f32, bf = jnp.float32, jnp.bfloat16
    shape = jax.ShapeDtypeStruct
    dma = pltpu.SemaphoreType.DMA
    return pl.pallas_call(
        functools.partial(head_kernel, heads, key_dim, value_dim),
        out_shape=[
            shape((length, values), bf),
            shape((length, values), f32),
            shape((length, values), f32),
            shape((chunks * heads * key_dim * value_dim // width, width), f32),
            shape((chunks, heads, SPAN, SPAN), f32),
            shape((length, width), f32),
            shape((length, width), bf),
        ],
        in_specs=[VM] * 9,
        out_specs=[VM] * 7,
        scratch_shapes=[
            pltpu.VMEM((HALO + SPAN, width), f32),
            pltpu.VMEM((heads, key_dim, value_dim), f32),
            pltpu.VMEM((length, qk), f32),
            pltpu.VMEM((length, qk), f32),
            pltpu.VMEM((length, qk), f32),
            pltpu.VMEM((chunks, heads, SPAN, SPAN), f32),
            pltpu.VMEM((chunks, heads, 8, 128), f32),
            pltpu.VMEM((length, width), f32),
            pltpu.VMEM((length // 2, width), f32),
            pltpu.VMEM((length // 2, width), f32),
            pltpu.VMEM((length // 2, width), f32),
            dma((3, BLOCKS)),
            dma((3, BLOCKS)),
            pltpu.VMEM((length, width), f32),
            pltpu.VMEM((length, width), f32),
            dma((places,)),
            dma((places,)),
            dma((3, places)),
            dma((3, places)),
        ],
        compiler_params=pltpu.CompilerParams(
            collective_id=collective_id, has_side_effects=True, vmem_limit_bytes=56 << 20
        ),
        name="head",
    )(pre, gate, small, taps, rate, gain, w_out, resid, cotangent)


def lane_pad(array, lanes):
    return jnp.pad(array, ((0, 0), (0, lanes - array.shape[1])))


def whole_sequences(
    inputs,
    norm1_gain,
    w_query,
    w_key,
    w_value,
    w_gate,
    w_beta,
    w_decay,
    decay_rate,
    conv_query,
    conv_key,
    conv_value,
    head_gain,
    w_out,
    norm2_gain,
    w_ffn_gate,
    w_ffn_up,
    w_ffn_down,
    cotangent,
):
    batch, seg, width = inputs.shape
    count = batch * seg
    heads = decay_rate.shape[0]
    key_dim = w_query.shape[1] // heads
    value_dim = w_value.shape[1] // heads
    qk_width = heads * key_dim
    lanes = 128
    bf = jnp.bfloat16
    places = lax.axis_size("dp")
    resid, = swap([inputs.reshape(count, width)], places, 1)
    hidden1 = rms_apply(resid, norm1_gain).astype(bf)
    w_mix = jnp.concatenate([w_query, w_key, w_value], axis=1)
    w_small = lane_pad(jnp.concatenate([w_beta, w_decay], axis=1), lanes)
    pre = project(hidden1, w_mix)
    gate_pre = project(hidden1, w_gate)
    small = project(hidden1, w_small)
    taps = jnp.concatenate([conv_query, conv_key, conv_value], axis=1)
    rate = lane_pad(jnp.pad(decay_rate, (heads, 0))[None], lanes)
    gain = head_gain[None]
    mixed, core, update, states, inverses, resid1, upstream = head_part(
        pre, gate_pre, small, taps, rate, gain, w_out, resid, cotangent.reshape(count, width),
        heads, key_dim, value_dim, places, 2,
    )
    hidden2 = rms_apply(resid1, norm2_gain).astype(bf)
    ffn_gate = project(hidden2, w_ffn_gate)
    ffn_up = project(hidden2, w_ffn_up)
    inner_full, swiglu_back = jax.vjp(swiglu, ffn_gate, ffn_up)
    inner = inner_full.astype(bf)
    grad_inner = back_project(upstream, w_ffn_down)
    grad_fgate, grad_fup = swiglu_back(grad_inner)
    grad_fgate = grad_fgate.astype(bf)
    grad_fup = grad_fup.astype(bf)
    part2 = back_project(grad_fgate, w_ffn_gate) + back_project(grad_fup, w_ffn_up)
    down = contract_rows(inner, upstream)
    ffn = project(inner, w_ffn_down)
    held, ranges = tail(
        part2, ffn, down, pre, core, update, states, resid1, upstream, resid.astype(bf), mixed, hidden1,
        hidden2, jnp.concatenate([grad_fgate, grad_fup], axis=1),
        w_out, w_mix, w_gate, w_small, norm1_gain[None], norm2_gain[None],
        gate_pre, small, taps, rate, gain, inverses,
        heads, key_dim, value_dim, places, 7,
    )
    (
        output, grad_inputs, fgate, fup, grad_down, grad_out_w, grad_gate_w, grad_query_w, grad_key_w, grad_value_w,
        grad_norm1_gain, grad_norm2_gain, grad_head, grad_rate, grad_beta_w, grad_decay_w,
        grad_convq, grad_convk, grad_convv,
    ) = finish(*held, ranges, inner.shape[1], heads, qk_width, heads * value_dim)
    return (
        output.reshape(batch, seg, width),
        grad_inputs.reshape(batch, seg, width),
        grad_norm1_gain[0],
        grad_query_w,
        grad_key_w,
        grad_value_w,
        grad_gate_w,
        grad_beta_w.T,
        grad_decay_w.T,
        grad_rate[0],
        grad_convq,
        grad_convk,
        grad_convv,
        grad_head[0],
        grad_out_w,
        grad_norm2_gain[0],
        fgate.T,
        fup.T,
        grad_down,
    )


def fits_whole(mesh, args):
    batch, length, width = args[0].shape
    places, ranks = mesh.shape["dp"], mesh.shape["tensor"]
    heads = args[8].shape[0] // ranks
    qk = args[2].shape[1] // ranks
    values = args[4].shape[1] // ranks
    units = args[15].shape[1] // ranks
    return (
        batch == places and places == 8 and ranks == 4 and length == places * SPAN and BLOCKS == places and heads <= 4
        and width == 2 * qk + values and width == 2 * values and width % 512 == 0 and length % 256 == 0
        and units % 64 == 0 and values % 256 == 0
        and length // SPAN * args[2].shape[1] // ranks * (values // heads) <= values * width
    )


def solution(mesh):
    placed = (
        P(None, "dp", None),
        P(),
        P(None, "tensor"),
        P(None, "tensor"),
        P(None, "tensor"),
        P(None, "tensor"),
        P(None, "tensor"),
        P(None, "tensor"),
        P("tensor"),
        P(None, "tensor"),
        P(None, "tensor"),
        P(None, "tensor"),
        P("tensor"),
        P("tensor", None),
        P(),
        P(None, "tensor"),
        P(None, "tensor"),
        P("tensor", None),
        P(None, "dp", None),
    )
    def step(*args):
        body = whole_sequences if fits_whole(mesh, args) else shards
        return placed_step(body)(*args)

    def placed_step(body):
      return jax.shard_map(
        body,
        mesh=mesh,
        in_specs=placed,
        out_specs=(
            P(None, "dp", None),
            P(None, "dp", None),
            P(),
            P(None, "tensor"),
            P(None, "tensor"),
            P(None, "tensor"),
            P(None, "tensor"),
            P(None, "tensor"),
            P(None, "tensor"),
            P("tensor"),
            P(None, "tensor"),
            P(None, "tensor"),
            P(None, "tensor"),
            P("tensor"),
            P("tensor", None),
            P(),
            P(None, "tensor"),
            P(None, "tensor"),
            P("tensor", None),
        ),
        check_vma=False,
    )

    return step
```

```python
import functools
from functools import partial

import jax
import jax.numpy as jnp
from jax import lax
from jax.experimental import pallas as pl
from jax.experimental.pallas import tpu as pltpu
from jax.sharding import PartitionSpec as P

SPAN = 64


EPS = 1e-06


def from_behind(shard, axis, by):
    count = lax.axis_size(axis)
    pairs = [(i, i + by) for i in range(count) if 0 <= i + by < count]
    return lax.ppermute(shard, axis, pairs)


def carried_in(part, axis, combine, identity, reverse):
    count = lax.axis_size(axis)
    place = lax.axis_index(axis)
    ahead = count - 1 - place if reverse else place
    gathered = jax.tree.map(lambda a: lax.all_gather(a, axis), part)
    state = jax.tree.map(lambda a, e: jnp.zeros_like(a) + jnp.asarray(e, a.dtype), part, identity)

    def one(turn, state):
        source = count - 1 - turn if reverse else turn
        return combine(
            state, jax.tree.map(lambda a: lax.dynamic_index_in_dim(a, source, 0, False), gathered)
        )

    return lax.fori_loop(0, ahead, one, state)


def exact(left, right):
    return jnp.matmul(left, right, precision=lax.Precision.HIGHEST)


def span_apply(state, inputs):
    query, key, values, beta, logdecay = inputs
    count = query.shape[0]
    cumul = jnp.cumsum(logdecay)
    row_ids = lax.broadcasted_iota(jnp.int32, (count, count), 0)
    col_ids = lax.broadcasted_iota(jnp.int32, (count, count), 1)
    within = col_ids <= row_ids
    strict = col_ids < row_ids
    spread = jnp.where(within, cumul[:, None] - cumul[None, :], 0.0)
    decays = jnp.where(within, jnp.exp(spread), 0.0)
    scaled = decays * beta[None, :]
    lower = jnp.where(strict, scaled * exact(key, key.T), 0.0)
    start_decay = jnp.exp(cumul)[:, None]
    right_side = values - start_decay * exact(key, state)
    system = jnp.eye(count, dtype=lower.dtype) + lower
    update = jax.scipy.linalg.solve_triangular(system, right_side, lower=True, unit_diagonal=True)
    output = start_decay * exact(query, state) + exact(scaled * exact(query, key.T), update)
    tail = jnp.exp(cumul[-1] - cumul) * beta
    new_state = jnp.exp(cumul[-1]) * state + exact((key * tail[:, None]).T, update)
    return (new_state, output)


def run_segment(query, key, values, beta, logdecay, state):
    length = query.shape[0]
    blocks = length // SPAN

    def split(array):
        return array.reshape((blocks, SPAN) + array.shape[1:])

    final, outputs = lax.scan(
        span_apply, state, (split(query), split(key), split(values), split(beta), split(logdecay))
    )
    return (outputs.reshape((length,) + outputs.shape[2:]), final)


def run_heads(query, key, values, beta, logdecay, state):
    return jax.vmap(jax.vmap(run_segment))(query, key, values, beta, logdecay, state)


def prepare(extended, beta_pre, decay_pre, conv_all, decay_rate, key_dim):
    batch, seg, heads = beta_pre.shape
    reach = conv_all.shape[0] - 1
    total = conv_all[0] * extended[:, 0:seg, :]
    for offset in range(1, reach + 1):
        total = total + conv_all[offset] * extended[:, offset : offset + seg, :]
    active = jax.nn.silu(total)
    qk_width = heads * key_dim
    query = active[..., :qk_width].reshape(batch, seg, heads, key_dim)
    key = active[..., qk_width : 2 * qk_width].reshape(batch, seg, heads, key_dim)
    values = active[..., 2 * qk_width :].reshape(batch, seg, heads, -1)
    query = query * lax.rsqrt(jnp.sum(query * query, -1, keepdims=True) + EPS) * key_dim ** (-0.5)
    key = key * lax.rsqrt(jnp.sum(key * key, -1, keepdims=True) + EPS)
    beta = jax.nn.sigmoid(beta_pre)
    logdecay = -decay_rate * jax.nn.softplus(decay_pre)
    return (
        jnp.moveaxis(query, 2, 1),
        jnp.moveaxis(key, 2, 1),
        jnp.moveaxis(values, 2, 1),
        jnp.moveaxis(beta, 2, 1),
        jnp.moveaxis(logdecay, 2, 1),
    )


def gate_norm(core, gate_pre, head_gain):
    normed = core * lax.rsqrt(jnp.mean(core * core, -1, keepdims=True) + EPS)
    return normed * head_gain * jax.nn.silu(gate_pre)


def rms_apply(resid, gain):
    return resid * lax.rsqrt(jnp.mean(resid * resid, -1, keepdims=True) + EPS) * gain


def swiglu(gate, upper):
    return jax.nn.silu(gate) * upper


def project(left, right):
    return jnp.dot(left, right, preferred_element_type=jnp.float32)


def contract_rows(left, right):
    return jnp.einsum("ra,rb->ab", left, right, preferred_element_type=jnp.float32)


def back_project(grad, weight):
    return jnp.einsum("rb,ab->ra", grad, weight, preferred_element_type=jnp.float32)


def compose(earlier, later):
    return (exact(later[0], earlier[0]), exact(later[0], earlier[1]) + later[1])


def shards(
    inputs,
    norm1_gain,
    w_query,
    w_key,
    w_value,
    w_gate,
    w_beta,
    w_decay,
    decay_rate,
    conv_query,
    conv_key,
    conv_value,
    head_gain,
    w_out,
    norm2_gain,
    w_ffn_gate,
    w_ffn_up,
    w_ffn_down,
    cotangent,
):
    batch, seg, width = inputs.shape
    count = batch * seg
    heads = decay_rate.shape[0]
    key_dim = w_query.shape[1] // heads
    value_dim = w_value.shape[1] // heads
    qk_width = heads * key_dim
    reach = conv_query.shape[0] - 1
    bf = jnp.bfloat16
    resid = inputs.reshape(count, width).astype(jnp.float32)
    normed1, norm1_back = jax.vjp(rms_apply, resid, norm1_gain)
    hidden1 = normed1.astype(bf)
    query_pre = project(hidden1, w_query)
    key_pre = project(hidden1, w_key)
    value_pre = project(hidden1, w_value)
    gate_pre = project(hidden1, w_gate)
    beta_pre = project(hidden1, w_beta)
    decay_pre = project(hidden1, w_decay)
    mixed_pre = jnp.concatenate([query_pre, key_pre, value_pre], axis=1).reshape(batch, seg, -1)
    rim = from_behind(mixed_pre[:, seg - reach :, :], "dp", 1)
    extended = jnp.concatenate([rim, mixed_pre], axis=1)
    conv_all = jnp.concatenate([conv_query, conv_key, conv_value], axis=1)
    features, prep_back = jax.vjp(
        partial(prepare, key_dim=key_dim),
        extended,
        beta_pre.reshape(batch, seg, heads),
        decay_pre.reshape(batch, seg, heads),
        conv_all,
        decay_rate,
    )
    query_h, key_h, value_h, beta_h, decay_h = features
    eye_block = jnp.broadcast_to(
        jnp.eye(key_dim, dtype=jnp.float32), (batch, heads, key_dim, key_dim)
    )
    zero_block = jnp.zeros((batch, heads, key_dim, value_dim), jnp.float32)
    values_aug = jnp.concatenate(
        [jnp.zeros(value_h.shape[:3] + (key_dim,), jnp.float32), value_h], axis=-1
    )
    state_aug = jnp.concatenate([eye_block, zero_block], axis=-1)
    outputs_aug, final_aug = run_heads(query_h, key_h, values_aug, beta_h, decay_h, state_aug)
    out_carry = outputs_aug[..., :key_dim]
    out_local = outputs_aug[..., key_dim:]
    transition = final_aug[..., :key_dim]
    offset_part = final_aug[..., key_dim:]
    prefix = carried_in((transition, offset_part), "dp", compose, (eye_block, zero_block), False)
    start_state = prefix[1]
    core = jnp.moveaxis(exact(out_carry, start_state) + out_local, 1, 2)
    gate4 = gate_pre.reshape(batch, seg, heads, value_dim)
    gated, gate_back = jax.vjp(gate_norm, core, gate4, head_gain.reshape(heads, value_dim))
    mixed = gated.reshape(count, heads * value_dim).astype(bf)
    attention = lax.psum(project(mixed, w_out), "tensor")
    resid1 = resid + attention
    normed2, norm2_back = jax.vjp(rms_apply, resid1, norm2_gain)
    hidden2 = normed2.astype(bf)
    ffn_gate = project(hidden2, w_ffn_gate)
    ffn_up = project(hidden2, w_ffn_up)
    inner_full, swiglu_back = jax.vjp(swiglu, ffn_gate, ffn_up)
    inner = inner_full.astype(bf)
    ffn = lax.psum(project(inner, w_ffn_down), "tensor")
    output = (resid1 + ffn).astype(bf).reshape(batch, seg, width)
    upstream = cotangent.reshape(count, width)
    grad_down = contract_rows(inner, upstream)
    grad_inner = back_project(upstream, w_ffn_down)
    grad_fgate, grad_fup = swiglu_back(grad_inner)
    grad_fgate = grad_fgate.astype(bf)
    grad_fup = grad_fup.astype(bf)
    grad_ffn_gate_w = contract_rows(hidden2, grad_fgate)
    grad_ffn_up_w = contract_rows(hidden2, grad_fup)
    grad_hidden2 = lax.psum(
        back_project(grad_fgate, w_ffn_gate) + back_project(grad_fup, w_ffn_up), "tensor"
    )
    grad_from_norm2, grad_norm2_gain = norm2_back(grad_hidden2)
    grad_resid1 = upstream.astype(jnp.float32) + grad_from_norm2
    grad_resid1_low = grad_resid1.astype(bf)
    grad_out_w = contract_rows(mixed, grad_resid1_low)
    grad_mixed = back_project(grad_resid1_low, w_out).reshape(batch, seg, heads, value_dim)
    grad_core, grad_gate4, grad_head_gain = gate_back(grad_mixed)
    grad_core_h = jnp.moveaxis(grad_core, 2, 1)
    carry_term = exact(jnp.swapaxes(out_carry, -1, -2), grad_core_h)
    suffix = carried_in(
        (jnp.swapaxes(transition, -1, -2), carry_term), "dp", compose, (eye_block, zero_block), True
    )

    def local_delta(query, key, values, beta, logdecay):
        return run_heads(query, key, values, beta, logdecay, start_state)

    recomputed, delta_back = jax.vjp(local_delta, query_h, key_h, value_h, beta_h, decay_h)
    feature_grads = delta_back((grad_core_h, suffix[1]))
    grad_ext, grad_beta_in, grad_decay_in, grad_conv, grad_rate = prep_back(feature_grads)
    returned = from_behind(grad_ext[:, :reach, :], "dp", -1)
    grad_mixed_pre = grad_ext[:, reach:, :] + jnp.pad(returned, ((0, 0), (seg - reach, 0), (0, 0)))
    grad_mixed_pre = grad_mixed_pre.reshape(count, -1)
    grad_query_low = grad_mixed_pre[:, :qk_width].astype(bf)
    grad_key_low = grad_mixed_pre[:, qk_width : 2 * qk_width].astype(bf)
    grad_value_low = grad_mixed_pre[:, 2 * qk_width :].astype(bf)
    grad_gate_low = grad_gate4.reshape(count, heads * value_dim).astype(bf)
    grad_beta_low = grad_beta_in.reshape(count, heads).astype(bf)
    grad_decay_low = grad_decay_in.reshape(count, heads).astype(bf)
    partial_hidden1 = (
        back_project(grad_query_low, w_query)
        + back_project(grad_key_low, w_key)
        + back_project(grad_value_low, w_value)
        + back_project(grad_gate_low, w_gate)
        + back_project(grad_beta_low, w_beta)
        + back_project(grad_decay_low, w_decay)
    )
    grad_hidden1 = lax.psum(partial_hidden1, "tensor")
    grad_from_norm1, grad_norm1_gain = norm1_back(grad_hidden1)
    grad_inputs = (grad_resid1 + grad_from_norm1).reshape(batch, seg, width)
    grad_query_w = contract_rows(hidden1, grad_query_low)
    grad_key_w = contract_rows(hidden1, grad_key_low)
    grad_value_w = contract_rows(hidden1, grad_value_low)
    grad_gate_w = contract_rows(hidden1, grad_gate_low)
    grad_beta_w = contract_rows(hidden1, grad_beta_low)
    grad_decay_w = contract_rows(hidden1, grad_decay_low)
    grad_convq = grad_conv[:, :qk_width]
    grad_convk = grad_conv[:, qk_width : 2 * qk_width]
    grad_convv = grad_conv[:, 2 * qk_width :]
    grad_head_flat = grad_head_gain.reshape(-1)
    (
        grad_norm1_gain,
        grad_query_w,
        grad_key_w,
        grad_value_w,
        grad_gate_w,
        grad_beta_w,
        grad_decay_w,
        grad_rate,
        grad_convq,
        grad_convk,
        grad_convv,
        grad_head_flat,
        grad_out_w,
        grad_norm2_gain,
        grad_ffn_gate_w,
        grad_ffn_up_w,
        grad_down,
    ) = lax.psum(
        (
            grad_norm1_gain,
            grad_query_w,
            grad_key_w,
            grad_value_w,
            grad_gate_w,
            grad_beta_w,
            grad_decay_w,
            grad_rate,
            grad_convq,
            grad_convk,
            grad_convv,
            grad_head_flat,
            grad_out_w,
            grad_norm2_gain,
            grad_ffn_gate_w,
            grad_ffn_up_w,
            grad_down,
        ),
        "dp",
    )
    return (
        output,
        grad_inputs,
        grad_norm1_gain,
        grad_query_w,
        grad_key_w,
        grad_value_w,
        grad_gate_w,
        grad_beta_w,
        grad_decay_w,
        grad_rate,
        grad_convq,
        grad_convk,
        grad_convv,
        grad_head_flat,
        grad_out_w,
        grad_norm2_gain,
        grad_ffn_gate_w,
        grad_ffn_up_w,
        grad_down,
    )


HALO = 8


def mm(left, right):
    return lax.dot_general(
        left, right, (((1,), (0,)), ((), ())),
        precision=lax.Precision.HIGHEST, preferred_element_type=jnp.float32,
    )


def mm_nt(left, right):
    return lax.dot_general(
        left, right, (((1,), (1,)), ((), ())),
        precision=lax.Precision.HIGHEST, preferred_element_type=jnp.float32,
    )


def mm_tn(left, right):
    return lax.dot_general(
        left, right, (((0,), (0,)), ((), ())),
        precision=lax.Precision.HIGHEST, preferred_element_type=jnp.float32,
    )


def grids(count):
    rows = lax.broadcasted_iota(jnp.int32, (count, count), 0)
    cols = lax.broadcasted_iota(jnp.int32, (count, count), 1)
    return rows, cols


def unit_inverse(lower, rows, cols):
    count = lower.shape[0]
    near = (rows // 2 == cols // 2) & (rows > cols)
    inverse = jnp.where(rows == cols, 1.0, jnp.where(near, -lower, 0.0))
    block = 2
    while block < count:
        cross = (rows // (2 * block) == cols // (2 * block)) & (rows // block > cols // block)
        inverse = inverse - mm(mm(inverse, jnp.where(cross, lower, 0.0)), inverse)
        block *= 2
    return inverse


def conv_window(halo_block, taps, span):
    reach = taps.shape[0] - 1
    total = None
    for offset in range(reach + 1):
        start = HALO - reach + offset
        term = taps[offset : offset + 1] * halo_block[start : start + span]
        total = term if total is None else total + term
    return total


def sigmoid(value):
    return 1.0 / (1.0 + jnp.exp(-value))


def softplus(value):
    return jnp.maximum(value, 0.0) + jnp.log(1.0 + jnp.exp(-jnp.abs(value)))


def gates_of(small, rate, heads, rows, cols):
    beta = sigmoid(small)
    slope = softplus(small)
    logdecay = -rate * slope
    cumul = mm(jnp.where(cols <= rows, 1.0, 0.0), logdecay)
    return beta, slope, logdecay, cumul


def state_place(index, head, heads, key_dim, value_dim, width):
    across = width // value_dim
    turn = index * heads + head
    return (
        pl.ds(pl.multiple_of(lax.div(turn, across) * key_dim, key_dim), key_dim),
        pl.ds(pl.multiple_of(lax.rem(turn, across) * value_dim, value_dim), value_dim),
    )


def chunk_terms(query, key, beta_col, beta_row, cum_col, cum_row, rows, cols):
    within = cols <= rows
    decays = jnp.where(within, jnp.exp(jnp.where(within, cum_col - cum_row, 0.0)), 0.0)
    scaled = decays * beta_row
    key_key = mm_nt(key, key)
    query_key = mm_nt(query, key)
    lower = jnp.where(cols < rows, scaled * key_key, 0.0)
    attend = scaled * query_key
    return decays, scaled, key_key, query_key, lower, attend


def forward_kernel(heads, key_dim, value_dim, pre_ref, gate_ref, small_ref, taps_ref, rate_ref, gain_ref,
                   mixed_ref, core_ref, update_ref, state_ref, inverse_ref, pad_ref, now_ref):
    length, width = pre_ref.shape
    span = SPAN
    chunks = length // span
    rows, cols = grids(span)
    qk = heads * key_dim
    pad_ref[0:HALO] = jnp.zeros((HALO, width), jnp.float32)
    for head in range(heads):
        now_ref[head] = jnp.zeros((key_dim, value_dim), jnp.float32)

    def chunk(index, carry):
        start = pl.multiple_of(index * span, span)
        here = pl.ds(start, span)
        pad_ref[HALO : HALO + span] = pre_ref[here, :]
        total = conv_window(pad_ref[...], taps_ref[...], span)
        pad_ref[0:HALO] = pad_ref[span : span + HALO]
        active = total * sigmoid(total)
        beta, _, _, cumul = gates_of(small_ref[here, :], rate_ref[...], heads, rows, cols)
        beta_t = jnp.transpose(beta)
        cumul_t = jnp.transpose(cumul)
        gate = gate_ref[here, :]
        gated = gate * sigmoid(gate) * gain_ref[...]
        for head in range(heads):
            query = active[:, head * key_dim : (head + 1) * key_dim]
            query = query * (lax.rsqrt(jnp.sum(query * query, -1, keepdims=True) + EPS) * key_dim ** (-0.5))
            key = active[:, qk + head * key_dim : qk + (head + 1) * key_dim]
            key = key * lax.rsqrt(jnp.sum(key * key, -1, keepdims=True) + EPS)
            value = active[:, 2 * qk + head * value_dim : 2 * qk + (head + 1) * value_dim]
            beta_col = beta[:, head : head + 1]
            beta_row = beta_t[head : head + 1]
            cum_col = cumul[:, heads + head : heads + head + 1]
            cum_row = cumul_t[heads + head : heads + head + 1]
            _, _, _, _, lower, attend = chunk_terms(query, key, beta_col, beta_row, cum_col, cum_row, rows, cols)
            inverse = unit_inverse(lower, rows, cols)
            state = now_ref[head]
            state_ref[state_place(index, head, heads, key_dim, value_dim, width)] = state
            rise = jnp.exp(cum_col)
            last = cum_col[span - 1 : span]
            update = mm(inverse, value) - mm(mm(inverse, rise * key), state)
            core = mm(rise * query, state) + mm(attend, update)
            tail = jnp.exp(last - cum_col) * beta_col
            now_ref[head] = jnp.exp(last) * state + mm_tn(key * tail, update)
            inverse_ref[index, head] = inverse
            wide = slice(head * value_dim, (head + 1) * value_dim)
            update_ref[here, wide] = update
            core_ref[here, wide] = core
            normed = core * lax.rsqrt(jnp.mean(core * core, -1, keepdims=True) + EPS)
            mixed_ref[here, wide] = (normed * gated[:, wide]).astype(mixed_ref.dtype)
        return carry

    lax.fori_loop(0, chunks, chunk, 0)


def delta_forward(pre, gate, small, taps, rate, gain, heads, key_dim, value_dim):
    length, width = pre.shape
    chunks = length // SPAN
    out_shape = (
        jax.ShapeDtypeStruct((length, heads * value_dim), jnp.bfloat16),
        jax.ShapeDtypeStruct((length, heads * value_dim), jnp.float32),
        jax.ShapeDtypeStruct((length, heads * value_dim), jnp.float32),
        jax.ShapeDtypeStruct((chunks * heads * key_dim * value_dim // width, width), jnp.float32),
        jax.ShapeDtypeStruct((chunks, heads, SPAN, SPAN), jnp.float32),
    )
    return pl.pallas_call(
        functools.partial(forward_kernel, heads, key_dim, value_dim),
        out_shape=out_shape,
        scratch_shapes=[
            pltpu.VMEM((HALO + SPAN, width), jnp.float32),
            pltpu.VMEM((heads, key_dim, value_dim), jnp.float32),
        ],
        compiler_params=pltpu.CompilerParams(vmem_limit_bytes=56 << 20),
        name="delta_forward",
    )(pre, gate, small, taps, rate, gain)


def backward_start(refs, span):
    (_, _, _, _, _, _, _, _, _, _, _, _, _, _, taps_grad_ref, gain_grad_ref, rate_grad_ref,
     _, pad_ref, now_ref) = refs
    now_ref[...] = jnp.zeros_like(now_ref)
    pad_ref[span : span + HALO] = jnp.zeros((HALO, pad_ref.shape[1]), jnp.float32)
    taps_grad_ref[...] = jnp.zeros_like(taps_grad_ref)
    gain_grad_ref[...] = jnp.zeros_like(gain_grad_ref)
    rate_grad_ref[...] = jnp.zeros_like(rate_grad_ref)


def backward_chunk(heads, key_dim, value_dim, index, refs):
    (pre_ref, gate_ref, small_ref, taps_ref, rate_ref, gain_ref,
     core_ref, update_ref, state_ref, inverse_ref, grad_ref,
     low_ref, gate_low_ref, small_low_ref, taps_grad_ref, gain_grad_ref, rate_grad_ref,
     ahead_ref, pad_ref, now_ref) = refs
    width = taps_ref.shape[1]
    span = SPAN
    rows, cols = grids(span)
    qk = heads * key_dim
    reach = taps_ref.shape[0] - 1
    lanes = small_ref.shape[1]
    lane = lax.broadcasted_iota(jnp.int32, (span, lanes), 1)
    start = pl.multiple_of(index * span, span)
    here = pl.ds(start, span)
    before = pl.ds(pl.multiple_of(jnp.maximum(start - HALO, 0), HALO), HALO)
    ahead_ref[0:HALO] = pre_ref[before, :] * jnp.where(index > 0, 1.0, 0.0)
    ahead_ref[HALO : HALO + span] = pre_ref[here, :]
    total = conv_window(ahead_ref[...], taps_ref[...], span)
    gain_of = sigmoid(total)
    active = total * gain_of
    bend = gain_of * (1.0 + total * (1.0 - gain_of))
    small = small_ref[here, :]
    beta, slope, _, cumul = gates_of(small, rate_ref[...], heads, rows, cols)
    beta_t = jnp.transpose(beta)
    cumul_t = jnp.transpose(cumul)
    gate = gate_ref[here, :]
    gate_sig = sigmoid(gate)
    gate_silu = gate * gate_sig
    gate_bend = gate_sig * (1.0 + gate * (1.0 - gate_sig))
    small_grad = jnp.zeros((span, lanes), jnp.float32)
    for head in range(heads):
        wide = slice(head * value_dim, (head + 1) * value_dim)
        core = core_ref[here, wide]
        grad_mixed = grad_ref[here, wide]
        gain = gain_ref[:, wide]
        scale = lax.rsqrt(jnp.mean(core * core, -1, keepdims=True) + EPS)
        normed = core * scale
        gate_low_ref[here, wide] = (grad_mixed * normed * gain * gate_bend[:, wide]).astype(gate_low_ref.dtype)
        with_gate = grad_mixed * gate_silu[:, wide]
        gain_grad_ref[:, wide] += jnp.sum(with_gate * normed, 0, keepdims=True)
        grad_normed = with_gate * gain
        grad_core = scale * (grad_normed - normed * jnp.mean(grad_normed * normed, -1, keepdims=True))
        query_act = active[:, head * key_dim : (head + 1) * key_dim]
        query_scale = lax.rsqrt(jnp.sum(query_act * query_act, -1, keepdims=True) + EPS)
        query = query_act * (query_scale * key_dim ** (-0.5))
        key_act = active[:, qk + head * key_dim : qk + (head + 1) * key_dim]
        key_scale = lax.rsqrt(jnp.sum(key_act * key_act, -1, keepdims=True) + EPS)
        key = key_act * key_scale
        beta_col = beta[:, head : head + 1]
        beta_row = beta_t[head : head + 1]
        cum_col = cumul[:, heads + head : heads + head + 1]
        cum_row = cumul_t[heads + head : heads + head + 1]
        decays, scaled, key_key, query_key, lower, attend = chunk_terms(
            query, key, beta_col, beta_row, cum_col, cum_row, rows, cols
        )
        state = state_ref[state_place(index, head, heads, key_dim, value_dim, width)]
        update = update_ref[here, wide]
        inverse = inverse_ref[index, head]
        grad_state = now_ref[head]
        rise = jnp.exp(cum_col)
        last = cum_col[span - 1 : span]
        fall = jnp.exp(last - cum_col)
        tail = fall * beta_col
        rise_query = rise * query
        rise_key = rise * key
        grad_update = mm_tn(attend, grad_core) + mm(key * tail, grad_state)
        grad_right = mm_tn(inverse, grad_update)
        now_ref[head] = jnp.exp(last) * grad_state + mm_tn(rise_query, grad_core) - mm_tn(rise_key, grad_right)
        grad_attend = jnp.where(cols <= rows, mm_nt(grad_core, update), 0.0)
        grad_lower = jnp.where(cols < rows, -mm_nt(grad_right, update), 0.0)
        core_state = mm_nt(grad_core, state)
        right_state = mm_nt(grad_right, state)
        grad_tail_key = mm_nt(update, grad_state)
        pair_query = grad_attend * scaled
        pair_key = grad_lower * scaled
        grad_query = rise * core_state + mm(pair_query, key)
        grad_key = (
            grad_tail_key * tail - rise * right_state + mm_tn(pair_query, query)
            + mm(pair_key, key) + mm_tn(pair_key, key)
        )
        grad_tail = jnp.sum(grad_tail_key * key, -1, keepdims=True)
        moved = grad_attend * query_key + grad_lower * key_key
        spread = moved * scaled
        by_row = jnp.sum(spread, -1, keepdims=True)
        sums = mm_tn(
            jnp.concatenate([moved * decays, spread], 1), jnp.ones((span, lanes), jnp.float32)
        )
        grad_beta = sums[:span, 0:1] + grad_tail * fall
        through_tail = grad_tail * tail
        grad_cum = (
            by_row - sums[span:, 0:1] - through_tail
            + rise * (jnp.sum(core_state * query, -1, keepdims=True) - jnp.sum(right_state * key, -1, keepdims=True))
        )
        end_grad = jnp.sum(through_tail, 0, keepdims=True) + jnp.exp(last) * jnp.sum(
            jnp.sum(state * grad_state, -1, keepdims=True), 0, keepdims=True
        )
        grad_cum = grad_cum + jnp.where(rows[:, 0:1] == span - 1, end_grad, 0.0)
        small_grad = small_grad + jnp.where(lane == head, grad_beta, 0.0)
        small_grad = small_grad + jnp.where(lane == heads + head, grad_cum, 0.0)
        grad_query = grad_query * key_dim ** (-0.5)
        unit = query_act * query_scale
        grad_query = query_scale * (grad_query - unit * jnp.sum(grad_query * unit, -1, keepdims=True))
        grad_key = key_scale * (grad_key - key * jnp.sum(grad_key * key, -1, keepdims=True))
        at = slice(head * key_dim, (head + 1) * key_dim)
        pad_ref[0:span, at] = grad_query * bend[:, at]
        at = slice(qk + head * key_dim, qk + (head + 1) * key_dim)
        pad_ref[0:span, at] = grad_key * bend[:, at]
        at = slice(2 * qk + head * value_dim, 2 * qk + (head + 1) * value_dim)
        pad_ref[0:span, at] = grad_right * bend[:, at]
    summed = mm(jnp.where(cols >= rows, 1.0, 0.0), small_grad)
    is_beta = lane < heads
    rate_grad_ref[...] += jnp.sum(jnp.where(is_beta, 0.0, -slope * summed), 0, keepdims=True)
    sig = beta
    small_low_ref[here, :] = jnp.where(
        is_beta, small_grad * sig * (1.0 - sig), -rate_ref[...] * sig * summed
    ).astype(small_low_ref.dtype)
    outer = pad_ref[...]
    dense = outer[0:span]
    block = ahead_ref[...]
    grad_pre = None
    for offset in range(reach + 1):
        behind = reach - offset
        taps_grad_ref[offset : offset + 1] += jnp.sum(
            dense * block[HALO - behind : HALO - behind + span], 0, keepdims=True
        )
        term = taps_ref[offset : offset + 1] * outer[behind : behind + span]
        grad_pre = term if grad_pre is None else grad_pre + term
    low_ref[here, :] = grad_pre.astype(low_ref.dtype)
    pad_ref[span : span + HALO] = pad_ref[0:HALO]


MESH = pl.DeviceIdType.MESH
VM = pl.BlockSpec(memory_space=pltpu.VMEM)


def call_out(peers):
    barrier = pltpu.get_barrier_semaphore()
    for peer in peers:
        pl.semaphore_signal(barrier, inc=1, device_id=peer, device_id_type=MESH)


def hear_all(peers):
    pl.semaphore_wait(pltpu.get_barrier_semaphore(), len(peers))


def greet(peers):
    call_out(peers)
    hear_all(peers)


def remote(src, dst, send, recv, peer):
    return pltpu.make_async_remote_copy(
        src_ref=src, dst_ref=dst, send_sem=send, recv_sem=recv, device_id=peer, device_id_type=MESH
    )


def tensor_peers():
    dp = lax.axis_index("dp")
    t = lax.axis_index("tensor")
    core = lax.rem(t, 2)
    mate = (dp, t + 1 - 2 * core)
    across = (dp, lax.rem(t + 2, 4))
    return core, mate, across


def psum_kernel(blocks, part_ref, out_ref, land_mate, land_across, half, send, recv):
    core, mate, across = tensor_peers()
    greet((mate, across))
    rows = part_ref.shape[0] // blocks
    part = rows // 2
    first = []
    for b in range(blocks):
        theirs = pl.ds(pl.multiple_of(b * rows + (1 - core) * part, part), part)
        copy = remote(part_ref.at[theirs], land_mate.at[pl.ds(b * part, part)], send.at[0, b], recv.at[0, b], mate)
        copy.start()
        first.append(copy)
    second = []
    for b in range(blocks):
        mine = pl.ds(pl.multiple_of(b * rows + core * part, part), part)
        slot = pl.ds(b * part, part)
        first[b].wait_recv()
        half[slot] = part_ref[mine] + land_mate[slot]
        copy = remote(half.at[slot], land_across.at[slot], send.at[1, b], recv.at[1, b], across)
        copy.start()
        second.append(copy)
    third = []
    for b in range(blocks):
        mine = pl.ds(pl.multiple_of(b * rows + core * part, part), part)
        slot = pl.ds(b * part, part)
        second[b].wait_recv()
        out_ref[mine] = half[slot] + land_across[slot]
        copy = remote(out_ref.at[mine], out_ref.at[mine], send.at[2, b], recv.at[2, b], mate)
        copy.start()
        third.append(copy)
    for b in range(blocks):
        third[b].wait_recv()
    for b in range(blocks):
        first[b].wait_send()
        second[b].wait_send()
        third[b].wait_send()


def tensor_sum(part, collective_id, blocks=8):
    rows, width = part.shape
    return pl.pallas_call(
        functools.partial(psum_kernel, blocks),
        out_shape=jax.ShapeDtypeStruct(part.shape, part.dtype),
        in_specs=[VM],
        out_specs=VM,
        scratch_shapes=[pltpu.VMEM((rows // 2, width), part.dtype)] * 3
        + [pltpu.SemaphoreType.DMA((3, blocks))] * 2,
        compiler_params=pltpu.CompilerParams(
            collective_id=collective_id, has_side_effects=True, vmem_limit_bytes=40 << 20
        ),
        name="tensor_sum",
    )(part)


def swap_kernel(count, narrow, *refs):
    sources, results = refs[:count], refs[count : 2 * count]
    staged, send, recv, close_send, close_recv = refs[2 * count :]
    n = lax.axis_size("dp")
    me = lax.axis_index("dp")
    t = lax.axis_index("tensor")
    core, mate, across = tensor_peers()
    ranks = lax.axis_size("tensor")
    others = [lax.rem(me + k, n) for k in range(1, n)]
    greet([(other, t) for other in others] + [mate, across])
    seg = results[0].shape[0] // n
    part = seg // ranks
    far = lax.rem(t + 2, ranks)

    def at(place, rank):
        return pl.ds(pl.multiple_of(place * seg + rank * part, part), part)

    outgoing = []
    for i in range(count):
        for k in range(n):
            other = lax.rem(me + k, n)
            if k == 0:
                results[i][at(me, t)] = sources[i][at(me, t)].astype(jnp.float32)
                continue
            if narrow[i]:
                staged[i, k] = sources[i][at(other, t)].astype(jnp.float32)
                src = staged.at[i, k]
            else:
                src = sources[i].at[at(other, t)]
            copy = remote(src, results[i].at[at(me, t)], send.at[i, k], recv.at[i, k], (other, t))
            copy.start()
            outgoing.append(copy)
    close = []
    for i in range(count):
        for k in range(n):
            source = lax.rem(me + n - k, n)
            here = results[i].at[at(source, t)]
            if k:
                remote(here, here, send.at[i, k], recv.at[i, k], (source, t)).wait_recv()
            over = remote(here, here, close_send.at[0, i, k], close_recv.at[0, i, k], across)
            over.start()
            beside = remote(here, here, close_send.at[1, i, k], close_recv.at[1, i, k], mate)
            beside.start()
            close += [over, beside]
    last = []
    for i in range(count):
        for k in range(n):
            source = lax.rem(me + n - k, n)
            there = results[i].at[at(source, far)]
            remote(there, there, close_send.at[0, i, k], close_recv.at[0, i, k], across).wait_recv()
            copy = remote(there, there, close_send.at[2, i, k], close_recv.at[2, i, k], mate)
            copy.start()
            last.append(copy)
    for copy in outgoing:
        copy.wait_send()
    for j, copy in enumerate(close):
        copy.wait_send()
        if j % 2:
            copy.wait_recv()
    for copy in last:
        copy.wait()


def swap(arrays, n, collective_id):
    count = len(arrays)
    rows, width = arrays[0].shape
    narrow = [a.dtype != jnp.float32 for a in arrays]
    out = pl.pallas_call(
        functools.partial(swap_kernel, count, narrow),
        out_shape=[jax.ShapeDtypeStruct((rows, width), jnp.float32)] * count,
        in_specs=[VM] * count,
        out_specs=[VM] * count,
        scratch_shapes=[pltpu.VMEM((count, n, rows // n // 4, width), jnp.float32)]
        + [pltpu.SemaphoreType.DMA((count, n))] * 2
        + [pltpu.SemaphoreType.DMA((3, count, n))] * 2,
        compiler_params=pltpu.CompilerParams(
            collective_id=collective_id, has_side_effects=True, vmem_limit_bytes=40 << 20
        ),
        name="swap",
    )(*arrays)
    return out


SLOT = 80
DEPTH = 10
SPLIT = 3
WHOLE = 2


def grid_place():
    n = lax.axis_size("dp")
    me = lax.axis_index("dp")
    t = lax.axis_index("tensor")
    lines = n // 2
    z = lax.div(me, 2)
    x = lax.rem(me, 2)
    return n, lines, me, t, z, x


def reduce_slot(slot, chunks, data, split_rings, whole_rings, sems):
    n, lines, me, t, z, x = grid_place()
    mate = (me + 1 - 2 * x, t)
    send_x, recv_x, send_z, recv_z, send_d, recv_d, send_p, recv_p, send_s, recv_s = [sems.at[i] for i in range(10)]
    top = lines - 1
    finish = slot - 2 * lines - 1

    def ring(chunk):
        return lax.rem(chunk, DEPTH)

    def within(chunk):
        return (chunk >= 0) & (chunk < chunks)

    for stream in range(SPLIT):
        land_x, land_z, outgo, aside = split_rings
        up = stream % 2 == 0
        level = z if up else top - z
        after = (me + 2, t) if up else (me - 2, t)
        prior = (me - 2, t) if up else (me + 2, t)

        def rows(chunk, side):
            return pl.ds(pl.multiple_of(chunk * SLOT + 16 * stream + 8 * side, 8), 8)

        def spot(ref, chunk):
            return ref.at[stream, ring(chunk)]

        def copy(kind_send, kind_recv, chunk, src, dst, peer):
            at = (stream, ring(chunk))
            return remote(src, dst, kind_send.at[at], kind_recv.at[at], peer)

        def to_mate(chunk):
            return copy(send_x, recv_x, chunk, spot(aside, chunk), spot(land_x, chunk), mate)

        def to_after(chunk):
            return copy(send_z, recv_z, chunk, spot(outgo, chunk), spot(land_z, chunk), after)

        def result(chunk, peer):
            here = data.at[rows(chunk, x)]
            return copy(send_d, recv_d, chunk, here, here, peer)

        def close(chunk, side):
            here = data.at[rows(chunk, side)]
            return copy(send_p, recv_p, chunk, here, here, mate)

        def give_back(chunk):
            @pl.when(level > 0)
            def _():
                result(chunk, prior).start()

            close(chunk, x).start()

        @pl.when(slot < chunks)
        def _():
            aside[stream, ring(slot)] = data[rows(slot, 1 - x)]
            to_mate(slot).start()

        rise = slot - 1 - level

        @pl.when(within(rise))
        def _():
            here = rows(rise, x)
            at = ring(rise)
            to_mate(rise).wait_recv()

            @pl.when(level > 0)
            def _():
                to_after(rise).wait_recv()
                outgo[stream, at] = data[here] + land_x[stream, at] + land_z[stream, at]

            @pl.when(level == 0)
            def _():
                outgo[stream, at] = data[here] + land_x[stream, at]

            @pl.when(level < top)
            def _():
                to_after(rise).start()

            @pl.when(level == top)
            def _():
                data[here] = outgo[stream, at]
                give_back(rise)

        fall = slot - 1 - 2 * top + level

        @pl.when(within(fall) & (level < top))
        def _():
            result(fall, after).wait_recv()
            to_after(fall).wait_send()
            give_back(fall)

        @pl.when(within(finish))
        def _():
            @pl.when(level > 0)
            def _():
                result(finish, prior).wait_send()

            close(finish, x).wait_send()
            close(finish, 1 - x).wait_recv()
            to_mate(finish).wait_send()

    for stream in range(WHOLE):
        land_x, land_z, land_s, outgo = whole_rings
        line = z if stream == 0 else top - z
        step = 2 if stream == 0 else -2
        inner, outer = (me - step, t), (me + step, t)

        def rows(chunk):
            return pl.ds(pl.multiple_of(chunk * SLOT + 16 * (SPLIT + stream), 8), 16)

        def spot(ref, chunk):
            return ref.at[stream, ring(chunk)]

        def copy(kind_send, kind_recv, chunk, src, dst, peer):
            at = (ring(chunk),)
            return remote(
                src, dst, kind_send.at[SPLIT + stream, ring(chunk)], kind_recv.at[SPLIT + stream, ring(chunk)], peer
            )

        def inward(chunk):
            return copy(send_z, recv_z, chunk, spot(outgo, chunk), spot(land_z, chunk), inner)

        def outward(chunk):
            return copy(send_z, recv_s, chunk, spot(outgo, chunk), spot(land_s, chunk), outer)

        def to_mate(chunk):
            return copy(send_x, recv_x, chunk, spot(outgo, chunk), spot(land_x, chunk), mate)

        def result_out(chunk):
            here = data.at[rows(chunk)]
            return copy(send_d, recv_d, chunk, here, here, outer)

        def result_in(chunk):
            here = data.at[rows(chunk)]
            return copy(send_s, recv_d, chunk, here, here, inner)

        rise = slot - 1 - (top - line)
        root = lax.rem(jnp.maximum(rise, 0), 2)

        @pl.when(within(rise) & (line >= root))
        def _():
            here = rows(rise)
            at = ring(rise)

            @pl.when(line < top)
            def _():
                inward(rise).wait_recv()

            is_fork = (line == root) & (root > 0)

            @pl.when(is_fork)
            def _():
                outward(rise).wait_recv()
                outgo[stream, at] = data[here] + land_z[stream, at] + land_s[stream, at]

            @pl.when((line < top) & jnp.logical_not(is_fork))
            def _():
                outgo[stream, at] = data[here] + land_z[stream, at]

            @pl.when(line == top)
            def _():
                outgo[stream, at] = data[here]

            @pl.when(line > root)
            def _():
                inward(rise).start()

            @pl.when(line == root)
            def _():
                to_mate(rise).start()

        leaf = slot - 1

        @pl.when(within(leaf) & (line == 0) & (lax.rem(jnp.maximum(leaf, 0), 2) > 0))
        def _():
            outgo[stream, ring(leaf)] = data[rows(leaf)]
            outward(leaf).start()

        meet = slot - 2 - (top - line)
        meet_root = lax.rem(jnp.maximum(meet, 0), 2)

        @pl.when(within(meet) & (line == meet_root))
        def _():
            at = ring(meet)
            to_mate(meet).wait_recv()
            data[rows(meet)] = outgo[stream, at] + land_x[stream, at]
            result_out(meet).start()

            @pl.when(meet_root > 0)
            def _():
                result_in(meet).start()

        for parity in range(2):
            fall = slot - 2 - (top - parity) - (line - parity)

            @pl.when(within(fall) & (lax.rem(jnp.maximum(fall, 0), 2) == parity) & (line > parity))
            def _():
                result_out(fall).wait_recv()
                inward(fall).wait_send()

                @pl.when(line < top)
                def _():
                    result_out(fall).start()

        inside = slot - 2 - (top - 1) - 1

        @pl.when(within(inside) & (lax.rem(jnp.maximum(inside, 0), 2) > 0) & (line == 0))
        def _():
            result_in(inside).wait_recv()
            outward(inside).wait_send()

        end_root = lax.rem(jnp.maximum(finish, 0), 2)

        @pl.when(within(finish))
        def _():
            @pl.when((line >= end_root) & (line < top))
            def _():
                result_out(finish).wait_send()

            @pl.when(line == end_root)
            def _():
                to_mate(finish).wait_send()

                @pl.when(end_root > 0)
                def _():
                    result_in(finish).wait_send()


def settle(lines):
    return 2 * lines + 1


def reduce_scratch(width):
    return (
        [pltpu.VMEM((SPLIT, DEPTH, 8, width), jnp.float32)] * 4
        + [pltpu.VMEM((WHOLE, DEPTH, 16, width), jnp.float32)] * 4
        + [pltpu.SemaphoreType.DMA((10, SPLIT + WHOLE, DEPTH))]
    )


BLOCKS = 8


def dot_plain(left, right):
    return lax.dot_general(left, right, (((1,), (0,)), ((), ())), preferred_element_type=jnp.float32)


def dot_nt(left, right):
    return lax.dot_general(left, right, (((1,), (1,)), ((), ())), preferred_element_type=jnp.float32)


def dot_tn(left, right):
    return lax.dot_general(left, right, (((0,), (0,)), ((), ())), preferred_element_type=jnp.float32)


def aligned(start, size):
    return pl.ds(pl.multiple_of(start, size), size)


class TensorSum:
    def __init__(self, part, total, land_mate, land_across, half, send, recv):
        self.core, self.mate, self.across = tensor_peers()
        self.part, self.total, self.half = part, total, half
        self.land_mate, self.land_across = land_mate, land_across
        self.send, self.recv = send, recv
        self.rows = part.shape[0] // BLOCKS
        self.size = self.rows // 2

    def span(self, block, side):
        return aligned(block * self.rows + side * self.size, self.size)

    def slot(self, block):
        return aligned(block * self.size, self.size)

    def first(self, block):
        return remote(
            self.part.at[self.span(block, 1 - self.core)], self.land_mate.at[self.slot(block)],
            self.send.at[0, block], self.recv.at[0, block], self.mate,
        )

    def second(self, block):
        return remote(
            self.half.at[self.slot(block)], self.land_across.at[self.slot(block)],
            self.send.at[1, block], self.recv.at[1, block], self.across,
        )

    def third(self, block):
        mine = self.total.at[self.span(block, self.core)]
        return remote(mine, mine, self.send.at[2, block], self.recv.at[2, block], self.mate)

    def start(self):
        for block in range(BLOCKS):
            self.first(block).start()

    def cross(self, block):
        self.first(block).wait_recv()
        slot = self.slot(block)
        self.half[slot] = self.part[self.span(block, self.core)] + self.land_mate[slot]
        self.second(block).start()

    def share(self, block, beside=None):
        self.second(block).wait_recv()
        slot = self.slot(block)
        mine = self.span(block, self.core)
        value = self.half[slot] + self.land_across[slot]
        self.total[mine] = value if beside is None else value + beside[mine].astype(value.dtype)
        self.third(block).start()

    def finish(self):
        for block in range(BLOCKS):
            self.third(block).wait_recv()
        for block in range(BLOCKS):
            self.first(block).wait_send()
            self.second(block).wait_send()
            self.third(block).wait_send()


class Swap:
    def __init__(self, source, result, send, recv, close_send, close_recv):
        self.n = lax.axis_size("dp")
        self.me = lax.axis_index("dp")
        self.t = lax.axis_index("tensor")
        self.ranks = lax.axis_size("tensor")
        _, self.mate, self.across = tensor_peers()
        self.source, self.result = source, result
        self.sems = send, recv, close_send, close_recv
        self.seg = result.shape[0] // self.n
        self.part = self.seg // self.ranks

    def at(self, place, rank):
        return aligned(place * self.seg + rank * self.part, self.part)

    def out(self, k):
        other = lax.rem(self.me + k, self.n)
        return remote(
            self.source.at[self.at(other, self.t)], self.result.at[self.at(self.me, self.t)],
            self.sems[0].at[k], self.sems[1].at[k], (other, self.t),
        )

    def close(self, k, leg):
        origin = lax.rem(self.me + self.n - k, self.n)
        rank = lax.rem(self.t + 2, self.ranks) if leg == 2 else self.t
        here = self.result.at[self.at(origin, rank)]
        return remote(
            here, here, self.sems[2].at[leg, k], self.sems[3].at[leg, k], self.across if leg == 0 else self.mate
        )

    def start(self):
        mine = self.at(self.me, self.t)
        self.result[mine] = self.source[mine]
        for k in range(1, self.n):
            self.out(k).start()

    def gather(self, k):
        @pl.when(k > 0)
        def _():
            self.out(k).wait_recv()

        self.close(k, 0).start()
        self.close(k, 1).start()

    def forward(self, k):
        self.close(k, 0).wait_recv()
        self.close(k, 2).start()

    def sent(self):
        for k in range(1, self.n):
            self.out(k).wait_send()

    def finish(self):
        for k in range(self.n):
            self.close(k, 0).wait_send()
            self.close(k, 1).wait()
            self.close(k, 2).wait()


class PlaneSwap(Swap):
    def __init__(self, source, result, send, recv, close_send, close_recv):
        super().__init__(source, result, send, recv, close_send, close_recv)
        self.core = lax.rem(self.t, 2)
        self.part = self.seg // 2

    def out(self, k):
        other = lax.rem(self.me + k, self.n)
        return remote(
            self.source.at[self.at(other, self.core)], self.result.at[self.at(self.me, self.core)],
            self.sems[0].at[k], self.sems[1].at[k], (other, self.t),
        )

    def close(self, k, leg):
        origin = lax.rem(self.me + self.n - k, self.n)
        here = self.result.at[self.at(origin, self.core)]
        return remote(here, here, self.sems[2].at[leg, k], self.sems[3].at[leg, k], self.mate)

    def start(self):
        mine = self.at(self.me, self.core)
        self.result[mine] = self.source[mine]
        for k in range(1, self.n):
            self.out(k).start()

    def gather(self, k):
        @pl.when(k > 0)
        def _():
            self.out(k).wait_recv()

        self.close(k, 1).start()

    def finish(self):
        for k in range(self.n):
            self.close(k, 1).wait()


def tail_kernel(
    heads, key_dim, value_dim, ranges, chunks,
    part2_hbm, ffn_hbm, pre_hbm, core_hbm, update_hbm, state_hbm,
    resid1_hbm, upstream_hbm, resid_hbm, mixed_hbm, hidden1_hbm, hidden2_hbm, units_hbm,
    w_out_hbm, query_hbm, key_hbm, value_hbm, w_gate_hbm, w_small_hbm, gate_hbm, small_hbm, inverse_hbm,
    norm1_ref, norm2_ref, taps_ref, rate_ref, gain_ref,
    data, output_ref, inputs_grad_ref,
    resid1_ref, upstream_ref, resid_ref, mixed_ref, hidden1_ref, hidden2_ref, units_ref,
    w_out_ref, w_mix_ref, w_gate_ref, w_small_ref, gate_ref, small_ref, inverse_ref,
    split_x, split_z, split_out, split_aside, whole_x, whole_z, whole_s, whole_out, sems,
    part, total, half, land_mate, land_across, sum_send, sum_recv,
    resid1_grad, resid1_low, mixed_grad, low, gate_low, small_low,
    taps_grad, gain_grad, rate_grad, norm1_grad, norm2_grad, ahead, pad, now,
    shuffled, swap_send, swap_recv, close_send, close_recv, load_sem,
):
    n, lines, me, t, z, x = grid_place()
    _, mate, across = tensor_peers()
    length, width = resid1_hbm.shape
    qk = heads * key_dim
    values = heads * value_dim
    at_down, at_units, at_out, at_gate, at_mix, at_small, at_end, rows_all = ranges
    loads = [
        (part2_hbm, part),
        (units_hbm, units_ref),
        (upstream_hbm, upstream_ref),
        (hidden2_hbm, hidden2_ref),
        (resid1_hbm, resid1_ref),
        (w_out_hbm, w_out_ref),
        (mixed_hbm, mixed_ref),
        (pre_hbm, data.at[pl.ds(at_mix, length)]),
        (core_hbm, data.at[pl.ds(at_mix + length, length), pl.ds(0, values)]),
        (update_hbm, data.at[pl.ds(at_mix + length, length), pl.ds(values, values)]),
        (state_hbm, data.at[pl.ds(at_gate, state_hbm.shape[0])]),
        (gate_hbm, gate_ref),
        (small_hbm, small_ref),
        (inverse_hbm, inverse_ref),
        (hidden1_hbm, hidden1_ref),
        (query_hbm, w_mix_ref.at[:, pl.ds(0, qk)]),
        (key_hbm, w_mix_ref.at[:, pl.ds(qk, qk)]),
        (value_hbm, w_mix_ref.at[:, pl.ds(2 * qk, values)]),
        (w_gate_hbm, w_gate_ref),
        (w_small_hbm, w_small_ref),
        (resid_hbm, resid_ref),
    ]
    loads = [pltpu.make_async_copy(src, dst, load_sem.at[i]) for i, (src, dst) in enumerate(loads)]
    load_ffn = pltpu.make_async_copy(ffn_hbm, part, load_sem.at[len(loads)])
    peers = [(lax.rem(me + k, n), t) for k in range(1, n)] + [mate, across]
    call_out(peers)
    for load in loads:
        load.start()
    refs = (
        data.at[pl.ds(at_mix, length)], gate_ref, small_ref, taps_ref, rate_ref, gain_ref,
        data.at[pl.ds(at_mix + length, length), pl.ds(0, values)],
        data.at[pl.ds(at_mix + length, length), pl.ds(values, values)],
        data.at[pl.ds(at_gate, state_hbm.shape[0])], inverse_ref, mixed_grad, low, gate_low, small_low, taps_grad, gain_grad, rate_grad,
        ahead, pad, now,
    )
    sums = [
        TensorSum(part, total, land_mate, land_across.at[i % 2], half, sum_send.at[i], sum_recv.at[i]) for i in range(3)
    ]
    swaps = [
        Swap(source, result, swap_send.at[i], swap_recv.at[i], close_send.at[i], close_recv.at[i])
        for i, (source, result) in enumerate([(total, shuffled), (resid1_grad, inputs_grad_ref)])
    ]
    norm1_grad[...] = jnp.zeros_like(norm1_grad)
    norm2_grad[...] = jnp.zeros_like(norm2_grad)
    backward_start(refs, SPAN)
    data[at_end:rows_all] = jnp.zeros((rows_all - at_end, width), jnp.float32)
    count_units = (at_units - at_down)
    tiles = units_ref.shape[2] // 128

    def units_piece(i):
        kind = lax.div(i, tiles)
        tile = lax.rem(i, tiles)
        left = units_ref[kind, :, aligned(tile * 128, 128)]
        start = at_down + kind * count_units + tile * 128

        def put(right):
            value = dot_tn(left, right)

            @pl.when(tile < tiles - 1)
            def _():
                data[pl.ds(pl.multiple_of(start, 64), 128)] = value

            @pl.when(tile == tiles - 1)
            def _():
                rest = count_units - (tiles - 1) * 128
                data[pl.ds(pl.multiple_of(start, 64), rest)] = value[0:rest]

        @pl.when(kind == 0)
        def _():
            put(upstream_ref[...])

        @pl.when(kind > 0)
        def _():
            put(hidden2_ref[...])

    loads[0].wait()
    hear_all(peers)
    sums[0].start()
    loads[1].wait()
    loads[2].wait()
    units_piece(0)

    def wait_loads():
        for load in loads[3:]:
            load.wait()

    def norm_back(value, grad, gain, gain_grad_ref):
        scale = lax.rsqrt(jnp.mean(value * value, -1, keepdims=True) + EPS)
        normed = value * scale
        gain_grad_ref[...] += jnp.sum(grad * normed, 0, keepdims=True)
        scaled = grad * gain
        return scale * (scaled - normed * jnp.mean(scaled * normed, -1, keepdims=True))

    def norm2_piece(i):
        here = aligned(i * 64, 64)
        grad = upstream_ref[here].astype(jnp.float32) + norm_back(
            resid1_ref[here], total[here], norm2_ref[...], norm2_grad
        )
        resid1_grad[here] = grad
        resid1_low[here] = grad.astype(jnp.bfloat16)

    def mixed_piece(i):
        tile = aligned(i * 256, 256)
        mixed_grad[:, tile] = dot_nt(resid1_low[...], w_out_ref[tile])

    def out_piece(i):
        tile = aligned(i * 256, 256)
        data[pl.ds(pl.multiple_of(at_out + i * 256, 64), 256)] = dot_tn(
            mixed_ref[:, tile], resid1_low[...]
        )

    def gate_piece(i):
        tile = aligned(i * 256, 256)
        half_rows = width // 2
        data[pl.ds(pl.multiple_of(at_gate + i * 256, 64), 256), 0:values] = dot_tn(hidden1_ref[:, tile], gate_low[...])
        other = aligned(half_rows + i * 256, 256)
        data[pl.ds(pl.multiple_of(at_gate + i * 256, 64), 256), values : 2 * values] = dot_tn(
            hidden1_ref[:, other], gate_low[...]
        )

    def mix_piece(i):
        tile = aligned(i * 256, 256)
        data[pl.ds(pl.multiple_of(at_mix + i * 256, 64), 256)] = dot_tn(hidden1_ref[:, tile], low[...])

    def hidden_piece(i):
        tile = aligned(i * 256, 256)
        part[:, tile] = (
            dot_nt(low[...], w_mix_ref[tile]) + dot_nt(gate_low[...], w_gate_ref[tile])
            + dot_plain(small_low[...], w_small_ref[:, tile])
        )

    def output_piece(i):
        here = aligned(i * 64, 64)
        total[here] = total[here] + resid1_ref[here]

    def round_piece(i):
        here = aligned(i * 64, 64)
        output_ref[here] = shuffled[here].astype(output_ref.dtype)

    def norm1_piece(i):
        here = aligned(i * 64, 64)
        resid1_grad[here] = resid1_grad[here] + norm_back(
            resid_ref[here].astype(jnp.float32), total[here], norm1_ref[...], norm1_grad
        )

    def small_piece():
        base = at_small
        data[base : at_end] = jnp.zeros((at_end - base, width), jnp.float32)
        data[base : base + 4] = taps_grad[...]
        data[base + 4 : base + 5] = norm1_grad[...]
        data[base + 5 : base + 6] = norm2_grad[...]
        data[base + 6 : base + 7, 0:values] = gain_grad[...]
        data[base + 6 : base + 7, values : values + rate_grad.shape[1]] = rate_grad[...]
        data[base + 8 : base + 16] = dot_tn(small_low[...], hidden1_ref[...])[0:8]

    def start_ffn():
        load_ffn.start()
        load_ffn.wait()
        sums[1].start()

    pieces = []

    def plan(first, count, each, run):
        assert count % each == 0
        pieces.append((first, count, each, run))
        return first + -(-count // each)

    plan(0, 1, 1, lambda i: wait_loads())
    plan(0, 3 * tiles - 1, 1, lambda i: units_piece(i + 1))
    for i in range(1, 3 * tiles):
        assert i <= (at_down + i // tiles * count_units + i % tiles * 128) // SLOT
    at = plan(0, BLOCKS, 2, sums[0].cross)
    at = plan(at, BLOCKS, 2, sums[0].share)
    at = plan(at, 1, 1, lambda i: sums[0].finish())
    at = plan(at, length // 64, 2, norm2_piece)
    at = plan(at, values // 256, 1, mixed_piece)
    side = at
    at = plan(at, values // 256, 1, out_piece)
    at_ready_out = at
    at = plan(at, length // SPAN, 1, lambda i: backward_chunk(heads, key_dim, value_dim, length // SPAN - 1 - i, refs))
    side = plan(side, 1, 1, lambda i: start_ffn())
    side = plan(side, BLOCKS, 2, sums[1].cross)
    side = plan(side, BLOCKS, 2, sums[1].share)
    side = plan(side, 1, 1, lambda i: sums[1].finish())
    part_free = side
    side = plan(side, length // 64, 4, output_piece)
    side = plan(side, 1, 1, lambda i: swaps[0].start())
    side = plan(side, n, 2, swaps[0].gather)
    side = plan(side, 1, 1, lambda i: swaps[0].sent())
    total_free = side
    side = plan(side, n, 2, swaps[0].forward)
    side = plan(side, 1, 1, lambda i: swaps[0].finish())
    side = plan(side, length // 64, 4, round_piece)
    at = plan(at, width // 512, 1, gate_piece)
    at_ready_gate = at
    at = plan(at, width // 256, 1, mix_piece)
    at_ready_mix = at
    at = plan(max(at, part_free), width // 256, 1, hidden_piece)
    at = plan(max(at, total_free), 1, 1, lambda i: sums[2].start())
    at = plan(at, BLOCKS, 2, sums[2].cross)
    at = plan(at, BLOCKS, 2, sums[2].share)
    at = plan(at, 1, 1, lambda i: sums[2].finish())
    at = plan(at, length // 64, 2, norm1_piece)
    at = plan(at, 1, 1, lambda i: small_piece())
    at_ready_small = at
    at = plan(at, 1, 1, lambda i: swaps[1].start())
    at = plan(at, n, 2, swaps[1].gather)
    plan(at, 1, 1, lambda i: swaps[1].sent())
    at = plan(at, n, 2, swaps[1].forward)
    at = plan(at, 1, 1, lambda i: swaps[1].finish())
    assert at_ready_out <= at_out // SLOT and at_ready_gate <= at_gate // SLOT
    assert at_ready_mix <= at_mix // SLOT and at_ready_small <= at_small // SLOT
    last = max(chunks + settle(lines), at, side)

    def step(slot, carry):
        reduce_slot(
            slot, chunks, data, (split_x, split_z, split_out, split_aside), (whole_x, whole_z, whole_s, whole_out), sems
        )
        for first, count, each, run in pieces:
            steps = -(-count // each)

            @pl.when((slot >= first) & (slot < first + steps))
            def _(first=first, each=each, run=run):
                if each == 1:
                    run(slot - first)
                else:
                    def inner(i, carry):
                        run((slot - first) * each + i)
                        return carry

                    lax.fori_loop(0, each, inner, 0)

        return carry

    lax.fori_loop(0, last, step, 0)


def tail(
    part2, ffn, pre, core, update, states, resid1, upstream, resid, mixed, hidden1, hidden2, units,
    w_out, w_query, w_key, w_value, w_gate, w_small, gate, small, inverses, norm1, norm2, taps, rate, gain,
    heads, key_dim, value_dim, count_units, places, collective_id,
):
    length, width = resid1.shape
    values = heads * value_dim
    qk = heads * key_dim
    lanes = small.shape[1]
    heights = [count_units, 2 * count_units, values, values, width, 64]
    ranges = [0]
    for height in heights:
        ranges.append(ranges[-1] + height)
    rows_all = -(-ranges[-1] // SLOT) * SLOT
    chunks = rows_all // SLOT
    f32, bf = jnp.float32, jnp.bfloat16
    shape = jax.ShapeDtypeStruct
    out_shape = [
        pltpu.VMEM((rows_all, width), f32),
        pltpu.VMEM((length, width), bf),
        pltpu.VMEM((length, width), f32),
    ]
    vmem, any_ = VM, pl.BlockSpec(memory_space=pl.ANY)
    dma = pltpu.SemaphoreType.DMA
    scratch = (
        [
            pltpu.VMEM(a.shape, a.dtype)
            for a in (
                resid1, upstream, resid, mixed, hidden1, hidden2, units, w_out, shape((width, width), bf), w_gate, w_small,
                gate, small, inverses,
            )
        ]
        + reduce_scratch(width)
        + [
            pltpu.VMEM((length, width), f32),
            pltpu.VMEM((length, width), f32),
            pltpu.VMEM((length // 2, width), f32),
            pltpu.VMEM((length // 2, width), f32),
            pltpu.VMEM((2, length // 2, width), f32),
            dma((3, 3, BLOCKS)),
            dma((3, 3, BLOCKS)),
            pltpu.VMEM((length, width), f32),
            pltpu.VMEM((length, width), bf),
            pltpu.VMEM((length, values), f32),
            pltpu.VMEM((length, width), bf),
            pltpu.VMEM((length, values), bf),
            pltpu.VMEM((length, lanes), bf),
            pltpu.VMEM(taps.shape, f32),
            pltpu.VMEM((1, values), f32),
            pltpu.VMEM((1, lanes), f32),
            pltpu.VMEM((1, width), f32),
            pltpu.VMEM((1, width), f32),
            pltpu.VMEM((HALO + SPAN, width), f32),
            pltpu.VMEM((HALO + SPAN, width), f32),
            pltpu.VMEM((heads, key_dim, value_dim), f32),
            pltpu.VMEM((length, width), f32),
            dma((2, places)),
            dma((2, places)),
            dma((2, 3, places)),
            dma((2, 3, places)),
            dma((24,)),
        ]
    )
    return pl.pallas_call(
        functools.partial(tail_kernel, heads, key_dim, value_dim, tuple(ranges) + (rows_all,), chunks),
        out_shape=out_shape,
        in_specs=[any_] * 22 + [vmem] * 5,
        out_specs=[vmem] * 3,
        scratch_shapes=scratch,
        compiler_params=pltpu.CompilerParams(
            collective_id=collective_id, has_side_effects=True,
            vmem_limit_bytes=67043328 - 4 * width * rows_all - 6 * width * length - (1 << 18),
        ),
        name="tail",
    )(
        part2, ffn, pre, core, update, states, resid1, upstream, resid, mixed, hidden1, hidden2, units,
        w_out, w_query, w_key, w_value, w_gate, w_small, gate, small, inverses, norm1, norm2, taps, rate, gain,
    ), tuple(ranges)


def finish_kernel(heads, qk, values, ranges, data, output, inputs_grad, *refs):
    big, smalls, sems = refs[:10], refs[10:19], refs[19]
    at_down, at_units, at_out, at_gate, at_mix, at_small, _ = ranges
    width = data.shape[1]
    units = big[2].shape[0]

    def rows(start, height, left=0, wide=None):
        return data.at[pl.ds(start, height), pl.ds(left, width if wide is None else wide)]

    half = width // 2
    moves = [
        (output, big[0]),
        (inputs_grad, big[1]),
        (rows(at_units, units), big[2]),
        (rows(at_units + units, units), big[3]),
        (rows(at_down, units), big[4]),
        (rows(at_out, values), big[5]),
        (rows(at_gate, half, 0, values), big[6].at[pl.ds(0, half)]),
        (rows(at_gate, half, values, values), big[6].at[pl.ds(half, half)]),
        (rows(at_mix, width, 0, qk), big[7]),
        (rows(at_mix, width, qk, qk), big[8]),
        (rows(at_mix, width, 2 * qk, values), big[9]),
    ]
    moves = [pltpu.make_async_copy(src, dst, sems.at[i]) for i, (src, dst) in enumerate(moves)]
    for move in moves:
        move.start()
    norm1, norm2, head, rate, beta, decay, query, key, value = smalls
    small = data[at_small : at_small + 16]
    norm1[...] = small[4:5]
    norm2[...] = small[5:6]
    head[...] = small[6:7, 0:values]
    rate[...] = small[6:7, values : values + 2 * heads][:, heads:]
    beta[...] = small[8 : 8 + heads]
    decay[...] = small[8 + heads : 8 + 2 * heads]
    query[...] = small[0:4, 0:qk]
    key[...] = small[0:4, qk : 2 * qk]
    value[...] = small[0:4, 2 * qk :]
    for move in moves:
        move.wait()


def finish(data, output, inputs_grad, ranges, units, heads, qk, values):
    width = data.shape[1]
    length = output.shape[0]
    any_ = pl.BlockSpec(memory_space=pl.ANY)
    f32 = jnp.float32
    bigs = [
        (units, width), (units, width), (units, width), (values, width), (width, values), (width, qk), (width, qk), (width, values)
    ]
    smalls = [(1, width), (1, width), (1, values), (1, heads), (heads, width), (heads, width), (4, qk), (4, qk), (4, values)]
    held = [pltpu.with_memory_space_constraint(a, pltpu.VMEM) for a in (data, output, inputs_grad)]
    return pl.pallas_call(
        functools.partial(finish_kernel, heads, qk, values, ranges),
        out_shape=[jax.ShapeDtypeStruct((length, width), output.dtype), jax.ShapeDtypeStruct((length, width), f32)]
        + [jax.ShapeDtypeStruct(shape, f32) for shape in bigs + smalls],
        in_specs=[VM] * 3,
        out_specs=[any_] * 10 + [VM] * len(smalls),
        scratch_shapes=[pltpu.SemaphoreType.DMA((11,))],
        compiler_params=pltpu.CompilerParams(vmem_limit_bytes=8 << 20),
        name="finish",
    )(*held)


PAIR = 2


def unit_inverses(lowers, rows, cols):
    count = lowers[0].shape[0]
    near = (rows // 2 == cols // 2) & (rows > cols)
    inverses = [jnp.where(rows == cols, 1.0, jnp.where(near, -lower, 0.0)) for lower in lowers]
    block = 2
    while block < count:
        cross = (rows // (2 * block) == cols // (2 * block)) & (rows // block > cols // block)
        steps = [mm(inverse, jnp.where(cross, lower, 0.0)) for inverse, lower in zip(inverses, lowers)]
        inverses = [inverse - mm(step, inverse) for inverse, step in zip(inverses, steps)]
        block *= 2
    return inverses


def head_kernel(
    heads, key_dim, value_dim,
    pre_ref, gate_ref, small_ref, taps_ref, rate_ref, gain_ref, w_out_ref, resid_ref, cotangent_ref,
    mixed_ref, core_ref, update_ref, state_ref, inverse_ref, resid1_ref, upstream_ref,
    pad, now, solved_key, rise_query, key_tail, attend_all, ends,
    part, land_mate, land_across, half, sum_send, sum_recv,
    staged, arrived, swap_send, swap_recv, close_send, close_recv,
):
    length, width = pre_ref.shape
    span = SPAN
    chunks = length // span
    rows, cols = grids(span)
    qk = heads * key_dim
    n, _, me, t, _, _ = grid_place()
    _, mate, across = tensor_peers()
    peers = [(lax.rem(me + k, n), t) for k in range(1, n)] + [mate, across]
    call_out(peers)
    total = TensorSum(part, resid1_ref, land_mate, land_across, half, sum_send, sum_recv)
    swap = PlaneSwap(staged, arrived, swap_send, swap_recv, close_send, close_recv)
    pad[0:HALO] = jnp.zeros((HALO, width), jnp.float32)
    now[...] = jnp.zeros_like(now)

    def prepare_pair(turn):
        items = []
        for k in range(PAIR):
            index = turn * PAIR + k
            here = aligned(index * span, span)
            pad[HALO : HALO + span] = pre_ref[here, :]
            total_pre = conv_window(pad[...], taps_ref[...], span)
            pad[0:HALO] = pad[span : span + HALO]
            active = total_pre * sigmoid(total_pre)
            beta, _, _, cumul = gates_of(small_ref[here, :], rate_ref[...], heads, rows, cols)
            beta_t = jnp.transpose(beta)
            cumul_t = jnp.transpose(cumul)
            for head in range(heads):
                query = active[:, head * key_dim : (head + 1) * key_dim]
                query = query * (lax.rsqrt(jnp.sum(query * query, -1, keepdims=True) + EPS) * key_dim ** (-0.5))
                key = active[:, qk + head * key_dim : qk + (head + 1) * key_dim]
                key = key * lax.rsqrt(jnp.sum(key * key, -1, keepdims=True) + EPS)
                value = active[:, 2 * qk + head * value_dim : 2 * qk + (head + 1) * value_dim]
                beta_col = beta[:, head : head + 1]
                cum_col = cumul[:, heads + head : heads + head + 1]
                cum_row = cumul_t[heads + head : heads + head + 1]
                within = cols <= rows
                decays = jnp.where(within, jnp.exp(jnp.where(within, cum_col - cum_row, 0.0)), 0.0)
                scaled = decays * beta_t[head : head + 1]
                products = mm_nt(jnp.concatenate([query, key], 0), key)
                lower = jnp.where(cols < rows, scaled * products[span:], 0.0)
                attend = scaled * products[:span]
                last = cum_col[span - 1 : span]
                rise = jnp.exp(cum_col)
                narrow = slice(head * key_dim, (head + 1) * key_dim)
                attend_all[index, head] = attend
                rise_query[here, narrow] = rise * query
                key_tail[here, narrow] = key * (jnp.exp(last - cum_col) * beta_col)
                ends[index, head] = jnp.broadcast_to(jnp.exp(last), (8, 128))
                items.append((index, head, here, lower, jnp.concatenate([value, rise * key], 1)))
        inverses = unit_inverses([item[3] for item in items], rows, cols)
        solved = [mm(inverse, item[4]) for inverse, item in zip(inverses, items)]
        for (index, head, here, _, _), inverse, solution_ in zip(items, inverses, solved):
            inverse_ref[index, head] = inverse
            update_ref[here, head * value_dim : (head + 1) * value_dim] = solution_[:, :value_dim]
            solved_key[here, head * key_dim : (head + 1) * key_dim] = solution_[:, value_dim:]

    def chain(index):
        here = aligned(index * span, span)
        gate = gate_ref[here, :]
        gated = gate * sigmoid(gate) * gain_ref[...]
        for head in range(heads):
            narrow = slice(head * key_dim, (head + 1) * key_dim)
            wide = slice(head * value_dim, (head + 1) * value_dim)
            state = now[head]
            state_ref[state_place(index, head, heads, key_dim, value_dim, width)] = state
            both = mm(jnp.concatenate([solved_key[here, narrow], rise_query[here, narrow]], 0), state)
            update = update_ref[here, wide] - both[:span]
            now[head] = ends[index, head][0:1, 0:1] * state + mm_tn(key_tail[here, narrow], update)
            core = both[span:] + mm(attend_all[index, head], update)
            update_ref[here, wide] = update
            core_ref[here, wide] = core
            normed = core * lax.rsqrt(jnp.mean(core * core, -1, keepdims=True) + EPS)
            mixed_ref[here, wide] = (normed * gated[:, wide]).astype(mixed_ref.dtype)

    def chain_pair(turn):
        for k in range(PAIR):
            chain(turn * PAIR + k)

    def send_pair(turn):
        here = aligned(turn * PAIR * span, PAIR * span)
        part[here] = dot_plain(mixed_ref[here], w_out_ref[...])
        for k in range(PAIR):
            total.first(turn * PAIR + k).start()

    def cross_pair(turn):
        for k in range(PAIR):
            total.cross(turn * PAIR + k)

    def share_pair(turn):
        for k in range(PAIR):
            total.share(turn * PAIR + k, resid_ref)

    pairs = chunks // PAIR
    for place in range(n):
        mine = swap.at(place, swap.core)
        staged[mine] = cotangent_ref[mine].astype(jnp.float32)
    prepare_pair(0)
    hear_all(peers)
    swap.start()

    def step(turn, carry):
        chain_pair(turn - 1)
        prepare_pair(turn)
        send_pair(turn - 1)

        cross_pair(turn - 1)

        @pl.when(turn > 1)
        def _():
            share_pair(turn - 2)

        return carry

    lax.fori_loop(1, pairs, step, 0)
    chain_pair(pairs - 1)
    send_pair(pairs - 1)
    cross_pair(pairs - 1)
    share_pair(pairs - 2)

    def gather(k, carry):
        swap.gather(k)
        return carry

    lax.fori_loop(0, n, gather, 0)

    share_pair(pairs - 1)
    swap.sent()
    swap.finish()

    def turn_low(i, carry):
        here = aligned(i * 64, 64)
        upstream_ref[here] = arrived[here].astype(upstream_ref.dtype)
        return carry

    lax.fori_loop(0, length // 64, turn_low, 0)
    total.finish()


def head_part(
    pre, gate, small, taps, rate, gain, w_out, resid, cotangent, heads, key_dim, value_dim, places, collective_id
):
    length, width = pre.shape
    values = heads * value_dim
    qk = heads * key_dim
    chunks = length // SPAN
    f32, bf = jnp.float32, jnp.bfloat16
    shape = jax.ShapeDtypeStruct
    dma = pltpu.SemaphoreType.DMA
    return pl.pallas_call(
        functools.partial(head_kernel, heads, key_dim, value_dim),
        out_shape=[
            shape((length, values), bf),
            shape((length, values), f32),
            shape((length, values), f32),
            shape((chunks * heads * key_dim * value_dim // width, width), f32),
            shape((chunks, heads, SPAN, SPAN), f32),
            shape((length, width), f32),
            shape((length, width), bf),
        ],
        in_specs=[VM] * 9,
        out_specs=[VM] * 7,
        scratch_shapes=[
            pltpu.VMEM((HALO + SPAN, width), f32),
            pltpu.VMEM((heads, key_dim, value_dim), f32),
            pltpu.VMEM((length, qk), f32),
            pltpu.VMEM((length, qk), f32),
            pltpu.VMEM((length, qk), f32),
            pltpu.VMEM((chunks, heads, SPAN, SPAN), f32),
            pltpu.VMEM((chunks, heads, 8, 128), f32),
            pltpu.VMEM((length, width), f32),
            pltpu.VMEM((length // 2, width), f32),
            pltpu.VMEM((length // 2, width), f32),
            pltpu.VMEM((length // 2, width), f32),
            dma((3, BLOCKS)),
            dma((3, BLOCKS)),
            pltpu.VMEM((length, width), f32),
            pltpu.VMEM((length, width), f32),
            dma((places,)),
            dma((places,)),
            dma((3, places)),
            dma((3, places)),
        ],
        compiler_params=pltpu.CompilerParams(
            collective_id=collective_id, has_side_effects=True, vmem_limit_bytes=67043328
        ),
        name="head",
    )(pre, gate, small, taps, rate, gain, w_out, resid, cotangent)


def prep_kernel(
    heads,
    x_ref, norm1_ref, query_hbm, key_hbm, value_hbm, gate_hbm, beta_ref, decay_ref, rate_ref, taps_q, taps_k, taps_v,
    low_ref, hidden_ref, pre_ref, gate_pre_ref, small_ref, w_small_ref, taps_ref, rate_row_ref,
    w_mix, w_gate, rows16, staged, arrived, send, recv, close_send, close_recv, load_sem,
):
    length, width = x_ref.shape
    qk = query_hbm.shape[1]
    values = value_hbm.shape[1]
    n, _, me, t, _, _ = grid_place()
    _, mate, across = tensor_peers()
    peers = [(lax.rem(me + k, n), t) for k in range(1, n)] + [mate, across]
    call_out(peers)
    loads = [
        (query_hbm, w_mix.at[:, pl.ds(0, qk)]),
        (key_hbm, w_mix.at[:, pl.ds(qk, qk)]),
        (value_hbm, w_mix.at[:, pl.ds(2 * qk, values)]),
        (gate_hbm, w_gate),
    ]
    loads = [pltpu.make_async_copy(src, dst, load_sem.at[i]) for i, (src, dst) in enumerate(loads)]
    for load in loads:
        load.start()
    swap = Swap(staged, arrived, send, recv, close_send, close_recv)
    for place in range(n):
        mine = swap.at(place, t)
        staged[mine] = x_ref[mine].astype(jnp.float32)
    hear_all(peers)
    swap.start()
    taps_ref[:, 0:qk] = taps_q[...]
    taps_ref[:, qk : 2 * qk] = taps_k[...]
    taps_ref[:, 2 * qk :] = taps_v[...]
    lanes = rate_row_ref.shape[1]
    lane = lax.broadcasted_iota(jnp.int32, (1, lanes), 1)
    row = jnp.zeros((1, lanes), jnp.float32)
    for head in range(heads):
        row = jnp.where(lane == heads + head, rate_ref[:, head : head + 1], row)
    rate_row_ref[...] = row
    rows16[...] = jnp.zeros_like(rows16)
    rows16[0:heads] = beta_ref[...].astype(jnp.float32)
    rows16[heads : 2 * heads] = decay_ref[...].astype(jnp.float32)
    w_small_ref[...] = jnp.zeros_like(w_small_ref)
    w_small_ref[0:16] = rows16[...].astype(w_small_ref.dtype)

    def gather(k, carry):
        swap.gather(k)
        return carry

    def forward(k, carry):
        swap.forward(k)
        return carry

    lax.fori_loop(0, n, gather, 0)
    lax.fori_loop(0, n, forward, 0)
    for load in loads:
        load.wait()
    swap.sent()
    swap.finish()

    def norm(i, carry):
        here = aligned(i * 64, 64)
        value = arrived[here]
        low_ref[here] = value.astype(low_ref.dtype)
        scale = lax.rsqrt(jnp.mean(value * value, -1, keepdims=True) + EPS)
        hidden_ref[here] = (value * scale * norm1_ref[...]).astype(hidden_ref.dtype)
        return carry

    lax.fori_loop(0, length // 64, norm, 0)

    def mix_tile(i, carry):
        tile = aligned(i * 256, 256)
        pre_ref[:, tile] = dot_plain(hidden_ref[...], w_mix[:, tile])
        return carry

    def gate_tile(i, carry):
        tile = aligned(i * 256, 256)
        gate_pre_ref[:, tile] = dot_plain(hidden_ref[...], w_gate[:, tile])
        return carry

    lax.fori_loop(0, width // 256, mix_tile, 0)
    lax.fori_loop(0, values // 256, gate_tile, 0)
    small_ref[...] = dot_nt(hidden_ref[...], w_small_ref[...])


def prep(x, norm1, w_query, w_key, w_value, w_gate, w_beta_t, w_decay_t, rate, taps_q, taps_k, taps_v, places, collective_id):
    length, width = x.shape
    heads = rate.shape[1]
    values = w_value.shape[1]
    lanes = 128
    f32, bf = jnp.float32, jnp.bfloat16
    shape = jax.ShapeDtypeStruct
    dma = pltpu.SemaphoreType.DMA
    any_ = pl.BlockSpec(memory_space=pl.ANY)
    return pl.pallas_call(
        functools.partial(prep_kernel, heads),
        out_shape=[
            shape((length, width), bf),
            shape((length, width), bf),
            shape((length, width), f32),
            shape((length, values), f32),
            shape((length, lanes), f32),
            shape((lanes, width), bf),
            shape((taps_q.shape[0], width), f32),
            shape((1, lanes), f32),
        ],
        in_specs=[VM] * 2 + [any_] * 4 + [VM] * 6,
        out_specs=[VM] * 8,
        scratch_shapes=[
            pltpu.VMEM((width, width), bf),
            pltpu.VMEM((width, values), bf),
            pltpu.VMEM((16, width), f32),
            pltpu.VMEM((length, width), f32),
            pltpu.VMEM((length, width), f32),
            dma((places,)),
            dma((places,)),
            dma((3, places)),
            dma((3, places)),
            dma((4,)),
        ],
        compiler_params=pltpu.CompilerParams(
            collective_id=collective_id, has_side_effects=True, vmem_limit_bytes=67043328
        ),
        name="prep",
    )(x, norm1, w_query, w_key, w_value, w_gate, w_beta_t, w_decay_t, rate, taps_q, taps_k, taps_v)


def feed_kernel(
    resid1_ref, norm2_ref, upstream_hbm, gate_hbm, up_hbm, down_hbm,
    hidden_ref, units_ref, part2_ref, ffn_ref,
    upstream, w_gate, w_up, w_down, gate_pre, up_pre, inner_grad, load_sem,
):
    length, width = resid1_ref.shape
    units = w_gate.shape[0]
    loads = [(gate_hbm, w_gate), (up_hbm, w_up), (upstream_hbm, upstream), (down_hbm, w_down)]
    loads = [pltpu.make_async_copy(src, dst, load_sem.at[i]) for i, (src, dst) in enumerate(loads)]
    for load in loads:
        load.start()

    def norm(i, carry):
        here = aligned(i * 64, 64)
        value = resid1_ref[here]
        scale = lax.rsqrt(jnp.mean(value * value, -1, keepdims=True) + EPS)
        hidden_ref[here] = (value * scale * norm2_ref[...]).astype(hidden_ref.dtype)
        return carry

    lax.fori_loop(0, length // 64, norm, 0)
    loads[0].wait()
    gate_pre[...] = dot_nt(hidden_ref[...], w_gate[...])
    loads[1].wait()
    up_pre[...] = dot_nt(hidden_ref[...], w_up[...])
    loads[2].wait()
    loads[3].wait()
    inner_grad[...] = dot_nt(upstream[...], w_down[...])
    units_ref[:, :, units // 128 * 128 :] = jnp.zeros((3, length, units_ref.shape[2] - units // 128 * 128), units_ref.dtype)

    def bend(i, carry):
        here = aligned(i * 64, 64)
        gate = gate_pre[here]
        upper = up_pre[here]
        grad = inner_grad[here]
        sig = sigmoid(gate)
        silu = gate * sig
        low = units_ref.dtype
        units_ref[0, here, 0:units] = (silu * upper).astype(low)
        units_ref[1, here, 0:units] = (grad * upper * (sig * (1.0 + gate * (1.0 - sig)))).astype(low)
        units_ref[2, here, 0:units] = (grad * silu).astype(low)
        return carry

    lax.fori_loop(0, length // 64, bend, 0)
    part2_ref[...] = dot_plain(units_ref[1, :, 0:units], w_gate[...]) + dot_plain(units_ref[2, :, 0:units], w_up[...])
    ffn_ref[...] = dot_plain(units_ref[0, :, 0:units], w_down[...])


def feed(resid1, norm2, upstream, w_gate_t, w_up_t, w_down):
    length, width = resid1.shape
    units = w_down.shape[0]
    padded = -(-units // 128) * 128
    f32, bf = jnp.float32, jnp.bfloat16
    shape = jax.ShapeDtypeStruct
    any_ = pl.BlockSpec(memory_space=pl.ANY)
    return pl.pallas_call(
        feed_kernel,
        out_shape=[
            shape((length, width), bf),
            shape((3, length, padded), bf),
            shape((length, width), f32),
            shape((length, width), f32),
        ],
        in_specs=[VM] * 2 + [any_] * 4,
        out_specs=[VM] * 4,
        scratch_shapes=[
            pltpu.VMEM((length, width), bf),
            pltpu.VMEM((units, width), bf),
            pltpu.VMEM((units, width), bf),
            pltpu.VMEM((units, width), bf),
            pltpu.VMEM((length, units), f32),
            pltpu.VMEM((length, units), f32),
            pltpu.VMEM((length, units), f32),
            pltpu.SemaphoreType.DMA((4,)),
        ],
        compiler_params=pltpu.CompilerParams(vmem_limit_bytes=67043328),
        name="feed",
    )(resid1, norm2, upstream, w_gate_t, w_up_t, w_down)


def whole_sequences(
    inputs,
    norm1_gain,
    w_query,
    w_key,
    w_value,
    w_gate,
    w_beta,
    w_decay,
    decay_rate,
    conv_query,
    conv_key,
    conv_value,
    head_gain,
    w_out,
    norm2_gain,
    w_ffn_gate,
    w_ffn_up,
    w_ffn_down,
    cotangent,
):
    batch, seg, width = inputs.shape
    count = batch * seg
    heads = decay_rate.shape[0]
    key_dim = w_query.shape[1] // heads
    value_dim = w_value.shape[1] // heads
    qk_width = heads * key_dim
    places = lax.axis_size("dp")
    resid, hidden1, pre, gate_pre, small, w_small, taps, rate = prep(
        inputs.reshape(count, width), norm1_gain[None], w_query, w_key, w_value, w_gate, w_beta.T, w_decay.T,
        decay_rate[None], conv_query, conv_key, conv_value, places, 1,
    )
    gain = head_gain[None]
    mixed, core, update, states, inverses, resid1, upstream = head_part(
        pre, gate_pre, small, taps, rate, gain, w_out, resid, cotangent.reshape(count, width),
        heads, key_dim, value_dim, places, 2,
    )
    hidden2, units, part2, ffn = feed(
        resid1, norm2_gain[None], upstream, w_ffn_gate.T, w_ffn_up.T, w_ffn_down
    )
    held, ranges = tail(
        part2, ffn, pre, core, update, states, resid1, upstream, resid, mixed, hidden1, hidden2, units,
        w_out, w_query, w_key, w_value, w_gate, w_small, gate_pre, small, inverses,
        norm1_gain[None], norm2_gain[None], taps, rate, gain,
        heads, key_dim, value_dim, w_ffn_down.shape[0], places, 7,
    )
    (
        output, grad_inputs, fgate, fup, grad_down, grad_out_w, grad_gate_w, grad_query_w, grad_key_w, grad_value_w,
        grad_norm1_gain, grad_norm2_gain, grad_head, grad_rate, grad_beta_w, grad_decay_w,
        grad_convq, grad_convk, grad_convv,
    ) = finish(*held, ranges, w_ffn_down.shape[0], heads, qk_width, heads * value_dim)
    return (
        output.reshape(batch, seg, width),
        grad_inputs.reshape(batch, seg, width),
        grad_norm1_gain[0],
        grad_query_w,
        grad_key_w,
        grad_value_w,
        grad_gate_w,
        grad_beta_w.T,
        grad_decay_w.T,
        grad_rate[0],
        grad_convq,
        grad_convk,
        grad_convv,
        grad_head[0],
        grad_out_w,
        grad_norm2_gain[0],
        fgate.T,
        fup.T,
        grad_down,
    )


def fits_whole(mesh, args):
    batch, length, width = args[0].shape
    places, ranks = mesh.shape["dp"], mesh.shape["tensor"]
    heads = args[8].shape[0] // ranks
    qk = args[2].shape[1] // ranks
    values = args[4].shape[1] // ranks
    units = args[15].shape[1] // ranks
    return (
        batch == places and places == 8 and ranks == 4 and length == places * SPAN and BLOCKS == places and heads <= 4
        and width == 2 * qk + values and width == 2 * values and width % 512 == 0 and length % 256 == 0
        and units % 64 == 0 and values % 256 == 0
        and length // SPAN * args[2].shape[1] // ranks * (values // heads) <= values * width
    )


def solution(mesh):
    placed = (
        P(None, "dp", None),
        P(),
        P(None, "tensor"),
        P(None, "tensor"),
        P(None, "tensor"),
        P(None, "tensor"),
        P(None, "tensor"),
        P(None, "tensor"),
        P("tensor"),
        P(None, "tensor"),
        P(None, "tensor"),
        P(None, "tensor"),
        P("tensor"),
        P("tensor", None),
        P(),
        P(None, "tensor"),
        P(None, "tensor"),
        P("tensor", None),
        P(None, "dp", None),
    )
    def step(*args):
        body = whole_sequences if fits_whole(mesh, args) else shards
        return placed_step(body)(*args)

    def placed_step(body):
      return jax.shard_map(
        body,
        mesh=mesh,
        in_specs=placed,
        out_specs=(
            P(None, "dp", None),
            P(None, "dp", None),
            P(),
            P(None, "tensor"),
            P(None, "tensor"),
            P(None, "tensor"),
            P(None, "tensor"),
            P(None, "tensor"),
            P(None, "tensor"),
            P("tensor"),
            P(None, "tensor"),
            P(None, "tensor"),
            P(None, "tensor"),
            P("tensor"),
            P("tensor", None),
            P(),
            P(None, "tensor"),
            P(None, "tensor"),
            P("tensor", None),
        ),
        check_vma=False,
    )

    return step
```

```python
import functools
from functools import partial

import jax
import jax.numpy as jnp
from jax import lax
from jax.experimental import pallas as pl
from jax.experimental.pallas import tpu as pltpu
from jax.sharding import PartitionSpec as P

SPAN = 64


EPS = 1e-06


def from_behind(shard, axis, by):
    count = lax.axis_size(axis)
    pairs = [(i, i + by) for i in range(count) if 0 <= i + by < count]
    return lax.ppermute(shard, axis, pairs)


def carried_in(part, axis, combine, identity, reverse):
    count = lax.axis_size(axis)
    place = lax.axis_index(axis)
    ahead = count - 1 - place if reverse else place
    gathered = jax.tree.map(lambda a: lax.all_gather(a, axis), part)
    state = jax.tree.map(lambda a, e: jnp.zeros_like(a) + jnp.asarray(e, a.dtype), part, identity)

    def one(turn, state):
        source = count - 1 - turn if reverse else turn
        return combine(
            state, jax.tree.map(lambda a: lax.dynamic_index_in_dim(a, source, 0, False), gathered)
        )

    return lax.fori_loop(0, ahead, one, state)


def exact(left, right):
    return jnp.matmul(left, right, precision=lax.Precision.HIGHEST)


def span_apply(state, inputs):
    query, key, values, beta, logdecay = inputs
    count = query.shape[0]
    cumul = jnp.cumsum(logdecay)
    row_ids = lax.broadcasted_iota(jnp.int32, (count, count), 0)
    col_ids = lax.broadcasted_iota(jnp.int32, (count, count), 1)
    within = col_ids <= row_ids
    strict = col_ids < row_ids
    spread = jnp.where(within, cumul[:, None] - cumul[None, :], 0.0)
    decays = jnp.where(within, jnp.exp(spread), 0.0)
    scaled = decays * beta[None, :]
    lower = jnp.where(strict, scaled * exact(key, key.T), 0.0)
    start_decay = jnp.exp(cumul)[:, None]
    right_side = values - start_decay * exact(key, state)
    system = jnp.eye(count, dtype=lower.dtype) + lower
    update = jax.scipy.linalg.solve_triangular(system, right_side, lower=True, unit_diagonal=True)
    output = start_decay * exact(query, state) + exact(scaled * exact(query, key.T), update)
    tail = jnp.exp(cumul[-1] - cumul) * beta
    new_state = jnp.exp(cumul[-1]) * state + exact((key * tail[:, None]).T, update)
    return (new_state, output)


def run_segment(query, key, values, beta, logdecay, state):
    length = query.shape[0]
    blocks = length // SPAN

    def split(array):
        return array.reshape((blocks, SPAN) + array.shape[1:])

    final, outputs = lax.scan(
        span_apply, state, (split(query), split(key), split(values), split(beta), split(logdecay))
    )
    return (outputs.reshape((length,) + outputs.shape[2:]), final)


def run_heads(query, key, values, beta, logdecay, state):
    return jax.vmap(jax.vmap(run_segment))(query, key, values, beta, logdecay, state)


def prepare(extended, beta_pre, decay_pre, conv_all, decay_rate, key_dim):
    batch, seg, heads = beta_pre.shape
    reach = conv_all.shape[0] - 1
    total = conv_all[0] * extended[:, 0:seg, :]
    for offset in range(1, reach + 1):
        total = total + conv_all[offset] * extended[:, offset : offset + seg, :]
    active = jax.nn.silu(total)
    qk_width = heads * key_dim
    query = active[..., :qk_width].reshape(batch, seg, heads, key_dim)
    key = active[..., qk_width : 2 * qk_width].reshape(batch, seg, heads, key_dim)
    values = active[..., 2 * qk_width :].reshape(batch, seg, heads, -1)
    query = query * lax.rsqrt(jnp.sum(query * query, -1, keepdims=True) + EPS) * key_dim ** (-0.5)
    key = key * lax.rsqrt(jnp.sum(key * key, -1, keepdims=True) + EPS)
    beta = jax.nn.sigmoid(beta_pre)
    logdecay = -decay_rate * jax.nn.softplus(decay_pre)
    return (
        jnp.moveaxis(query, 2, 1),
        jnp.moveaxis(key, 2, 1),
        jnp.moveaxis(values, 2, 1),
        jnp.moveaxis(beta, 2, 1),
        jnp.moveaxis(logdecay, 2, 1),
    )


def gate_norm(core, gate_pre, head_gain):
    normed = core * lax.rsqrt(jnp.mean(core * core, -1, keepdims=True) + EPS)
    return normed * head_gain * jax.nn.silu(gate_pre)


def rms_apply(resid, gain):
    return resid * lax.rsqrt(jnp.mean(resid * resid, -1, keepdims=True) + EPS) * gain


def swiglu(gate, upper):
    return jax.nn.silu(gate) * upper


def project(left, right):
    return jnp.dot(left, right, preferred_element_type=jnp.float32)


def contract_rows(left, right):
    return jnp.einsum("ra,rb->ab", left, right, preferred_element_type=jnp.float32)


def back_project(grad, weight):
    return jnp.einsum("rb,ab->ra", grad, weight, preferred_element_type=jnp.float32)


def compose(earlier, later):
    return (exact(later[0], earlier[0]), exact(later[0], earlier[1]) + later[1])


def shards(
    inputs,
    norm1_gain,
    w_query,
    w_key,
    w_value,
    w_gate,
    w_beta,
    w_decay,
    decay_rate,
    conv_query,
    conv_key,
    conv_value,
    head_gain,
    w_out,
    norm2_gain,
    w_ffn_gate,
    w_ffn_up,
    w_ffn_down,
    cotangent,
):
    batch, seg, width = inputs.shape
    count = batch * seg
    heads = decay_rate.shape[0]
    key_dim = w_query.shape[1] // heads
    value_dim = w_value.shape[1] // heads
    qk_width = heads * key_dim
    reach = conv_query.shape[0] - 1
    bf = jnp.bfloat16
    resid = inputs.reshape(count, width).astype(jnp.float32)
    normed1, norm1_back = jax.vjp(rms_apply, resid, norm1_gain)
    hidden1 = normed1.astype(bf)
    query_pre = project(hidden1, w_query)
    key_pre = project(hidden1, w_key)
    value_pre = project(hidden1, w_value)
    gate_pre = project(hidden1, w_gate)
    beta_pre = project(hidden1, w_beta)
    decay_pre = project(hidden1, w_decay)
    mixed_pre = jnp.concatenate([query_pre, key_pre, value_pre], axis=1).reshape(batch, seg, -1)
    rim = from_behind(mixed_pre[:, seg - reach :, :], "dp", 1)
    extended = jnp.concatenate([rim, mixed_pre], axis=1)
    conv_all = jnp.concatenate([conv_query, conv_key, conv_value], axis=1)
    features, prep_back = jax.vjp(
        partial(prepare, key_dim=key_dim),
        extended,
        beta_pre.reshape(batch, seg, heads),
        decay_pre.reshape(batch, seg, heads),
        conv_all,
        decay_rate,
    )
    query_h, key_h, value_h, beta_h, decay_h = features
    eye_block = jnp.broadcast_to(
        jnp.eye(key_dim, dtype=jnp.float32), (batch, heads, key_dim, key_dim)
    )
    zero_block = jnp.zeros((batch, heads, key_dim, value_dim), jnp.float32)
    values_aug = jnp.concatenate(
        [jnp.zeros(value_h.shape[:3] + (key_dim,), jnp.float32), value_h], axis=-1
    )
    state_aug = jnp.concatenate([eye_block, zero_block], axis=-1)
    outputs_aug, final_aug = run_heads(query_h, key_h, values_aug, beta_h, decay_h, state_aug)
    out_carry = outputs_aug[..., :key_dim]
    out_local = outputs_aug[..., key_dim:]
    transition = final_aug[..., :key_dim]
    offset_part = final_aug[..., key_dim:]
    prefix = carried_in((transition, offset_part), "dp", compose, (eye_block, zero_block), False)
    start_state = prefix[1]
    core = jnp.moveaxis(exact(out_carry, start_state) + out_local, 1, 2)
    gate4 = gate_pre.reshape(batch, seg, heads, value_dim)
    gated, gate_back = jax.vjp(gate_norm, core, gate4, head_gain.reshape(heads, value_dim))
    mixed = gated.reshape(count, heads * value_dim).astype(bf)
    attention = lax.psum(project(mixed, w_out), "tensor")
    resid1 = resid + attention
    normed2, norm2_back = jax.vjp(rms_apply, resid1, norm2_gain)
    hidden2 = normed2.astype(bf)
    ffn_gate = project(hidden2, w_ffn_gate)
    ffn_up = project(hidden2, w_ffn_up)
    inner_full, swiglu_back = jax.vjp(swiglu, ffn_gate, ffn_up)
    inner = inner_full.astype(bf)
    ffn = lax.psum(project(inner, w_ffn_down), "tensor")
    output = (resid1 + ffn).astype(bf).reshape(batch, seg, width)
    upstream = cotangent.reshape(count, width)
    grad_down = contract_rows(inner, upstream)
    grad_inner = back_project(upstream, w_ffn_down)
    grad_fgate, grad_fup = swiglu_back(grad_inner)
    grad_fgate = grad_fgate.astype(bf)
    grad_fup = grad_fup.astype(bf)
    grad_ffn_gate_w = contract_rows(hidden2, grad_fgate)
    grad_ffn_up_w = contract_rows(hidden2, grad_fup)
    grad_hidden2 = lax.psum(
        back_project(grad_fgate, w_ffn_gate) + back_project(grad_fup, w_ffn_up), "tensor"
    )
    grad_from_norm2, grad_norm2_gain = norm2_back(grad_hidden2)
    grad_resid1 = upstream.astype(jnp.float32) + grad_from_norm2
    grad_resid1_low = grad_resid1.astype(bf)
    grad_out_w = contract_rows(mixed, grad_resid1_low)
    grad_mixed = back_project(grad_resid1_low, w_out).reshape(batch, seg, heads, value_dim)
    grad_core, grad_gate4, grad_head_gain = gate_back(grad_mixed)
    grad_core_h = jnp.moveaxis(grad_core, 2, 1)
    carry_term = exact(jnp.swapaxes(out_carry, -1, -2), grad_core_h)
    suffix = carried_in(
        (jnp.swapaxes(transition, -1, -2), carry_term), "dp", compose, (eye_block, zero_block), True
    )

    def local_delta(query, key, values, beta, logdecay):
        return run_heads(query, key, values, beta, logdecay, start_state)

    recomputed, delta_back = jax.vjp(local_delta, query_h, key_h, value_h, beta_h, decay_h)
    feature_grads = delta_back((grad_core_h, suffix[1]))
    grad_ext, grad_beta_in, grad_decay_in, grad_conv, grad_rate = prep_back(feature_grads)
    returned = from_behind(grad_ext[:, :reach, :], "dp", -1)
    grad_mixed_pre = grad_ext[:, reach:, :] + jnp.pad(returned, ((0, 0), (seg - reach, 0), (0, 0)))
    grad_mixed_pre = grad_mixed_pre.reshape(count, -1)
    grad_query_low = grad_mixed_pre[:, :qk_width].astype(bf)
    grad_key_low = grad_mixed_pre[:, qk_width : 2 * qk_width].astype(bf)
    grad_value_low = grad_mixed_pre[:, 2 * qk_width :].astype(bf)
    grad_gate_low = grad_gate4.reshape(count, heads * value_dim).astype(bf)
    grad_beta_low = grad_beta_in.reshape(count, heads).astype(bf)
    grad_decay_low = grad_decay_in.reshape(count, heads).astype(bf)
    partial_hidden1 = (
        back_project(grad_query_low, w_query)
        + back_project(grad_key_low, w_key)
        + back_project(grad_value_low, w_value)
        + back_project(grad_gate_low, w_gate)
        + back_project(grad_beta_low, w_beta)
        + back_project(grad_decay_low, w_decay)
    )
    grad_hidden1 = lax.psum(partial_hidden1, "tensor")
    grad_from_norm1, grad_norm1_gain = norm1_back(grad_hidden1)
    grad_inputs = (grad_resid1 + grad_from_norm1).reshape(batch, seg, width)
    grad_query_w = contract_rows(hidden1, grad_query_low)
    grad_key_w = contract_rows(hidden1, grad_key_low)
    grad_value_w = contract_rows(hidden1, grad_value_low)
    grad_gate_w = contract_rows(hidden1, grad_gate_low)
    grad_beta_w = contract_rows(hidden1, grad_beta_low)
    grad_decay_w = contract_rows(hidden1, grad_decay_low)
    grad_convq = grad_conv[:, :qk_width]
    grad_convk = grad_conv[:, qk_width : 2 * qk_width]
    grad_convv = grad_conv[:, 2 * qk_width :]
    grad_head_flat = grad_head_gain.reshape(-1)
    (
        grad_norm1_gain,
        grad_query_w,
        grad_key_w,
        grad_value_w,
        grad_gate_w,
        grad_beta_w,
        grad_decay_w,
        grad_rate,
        grad_convq,
        grad_convk,
        grad_convv,
        grad_head_flat,
        grad_out_w,
        grad_norm2_gain,
        grad_ffn_gate_w,
        grad_ffn_up_w,
        grad_down,
    ) = lax.psum(
        (
            grad_norm1_gain,
            grad_query_w,
            grad_key_w,
            grad_value_w,
            grad_gate_w,
            grad_beta_w,
            grad_decay_w,
            grad_rate,
            grad_convq,
            grad_convk,
            grad_convv,
            grad_head_flat,
            grad_out_w,
            grad_norm2_gain,
            grad_ffn_gate_w,
            grad_ffn_up_w,
            grad_down,
        ),
        "dp",
    )
    return (
        output,
        grad_inputs,
        grad_norm1_gain,
        grad_query_w,
        grad_key_w,
        grad_value_w,
        grad_gate_w,
        grad_beta_w,
        grad_decay_w,
        grad_rate,
        grad_convq,
        grad_convk,
        grad_convv,
        grad_head_flat,
        grad_out_w,
        grad_norm2_gain,
        grad_ffn_gate_w,
        grad_ffn_up_w,
        grad_down,
    )


HALO = 8


def mm(left, right):
    return lax.dot_general(
        left, right, (((1,), (0,)), ((), ())),
        precision=lax.Precision.HIGHEST, preferred_element_type=jnp.float32,
    )


def mm_nt(left, right):
    return lax.dot_general(
        left, right, (((1,), (1,)), ((), ())),
        precision=lax.Precision.HIGHEST, preferred_element_type=jnp.float32,
    )


def mm_tn(left, right):
    return lax.dot_general(
        left, right, (((0,), (0,)), ((), ())),
        precision=lax.Precision.HIGHEST, preferred_element_type=jnp.float32,
    )


def grids(count):
    rows = lax.broadcasted_iota(jnp.int32, (count, count), 0)
    cols = lax.broadcasted_iota(jnp.int32, (count, count), 1)
    return rows, cols


def unit_inverse(lower, rows, cols):
    count = lower.shape[0]
    near = (rows // 2 == cols // 2) & (rows > cols)
    inverse = jnp.where(rows == cols, 1.0, jnp.where(near, -lower, 0.0))
    block = 2
    while block < count:
        cross = (rows // (2 * block) == cols // (2 * block)) & (rows // block > cols // block)
        inverse = inverse - mm(mm(inverse, jnp.where(cross, lower, 0.0)), inverse)
        block *= 2
    return inverse


def conv_window(halo_block, taps, span):
    reach = taps.shape[0] - 1
    total = None
    for offset in range(reach + 1):
        start = HALO - reach + offset
        term = taps[offset : offset + 1] * halo_block[start : start + span]
        total = term if total is None else total + term
    return total


def sigmoid(value):
    return 1.0 / (1.0 + jnp.exp(-value))


def softplus(value):
    return jnp.maximum(value, 0.0) + jnp.log(1.0 + jnp.exp(-jnp.abs(value)))


def gates_of(small, rate, heads, rows, cols):
    beta = sigmoid(small)
    slope = softplus(small)
    logdecay = -rate * slope
    cumul = mm(jnp.where(cols <= rows, 1.0, 0.0), logdecay)
    return beta, slope, logdecay, cumul


def state_place(index, head, heads, key_dim, value_dim, width):
    across = width // value_dim
    turn = index * heads + head
    return (
        pl.ds(pl.multiple_of(lax.div(turn, across) * key_dim, key_dim), key_dim),
        pl.ds(pl.multiple_of(lax.rem(turn, across) * value_dim, value_dim), value_dim),
    )


def chunk_terms(query, key, beta_col, beta_row, cum_col, cum_row, rows, cols):
    within = cols <= rows
    decays = jnp.where(within, jnp.exp(jnp.where(within, cum_col - cum_row, 0.0)), 0.0)
    scaled = decays * beta_row
    key_key = mm_nt(key, key)
    query_key = mm_nt(query, key)
    lower = jnp.where(cols < rows, scaled * key_key, 0.0)
    attend = scaled * query_key
    return decays, scaled, key_key, query_key, lower, attend


def forward_kernel(heads, key_dim, value_dim, pre_ref, gate_ref, small_ref, taps_ref, rate_ref, gain_ref,
                   mixed_ref, core_ref, update_ref, state_ref, inverse_ref, pad_ref, now_ref):
    length, width = pre_ref.shape
    span = SPAN
    chunks = length // span
    rows, cols = grids(span)
    qk = heads * key_dim
    pad_ref[0:HALO] = jnp.zeros((HALO, width), jnp.float32)
    for head in range(heads):
        now_ref[head] = jnp.zeros((key_dim, value_dim), jnp.float32)

    def chunk(index, carry):
        start = pl.multiple_of(index * span, span)
        here = pl.ds(start, span)
        pad_ref[HALO : HALO + span] = pre_ref[here, :]
        total = conv_window(pad_ref[...], taps_ref[...], span)
        pad_ref[0:HALO] = pad_ref[span : span + HALO]
        active = total * sigmoid(total)
        beta, _, _, cumul = gates_of(small_ref[here, :], rate_ref[...], heads, rows, cols)
        beta_t = jnp.transpose(beta)
        cumul_t = jnp.transpose(cumul)
        gate = gate_ref[here, :]
        gated = gate * sigmoid(gate) * gain_ref[...]
        for head in range(heads):
            query = active[:, head * key_dim : (head + 1) * key_dim]
            query = query * (lax.rsqrt(jnp.sum(query * query, -1, keepdims=True) + EPS) * key_dim ** (-0.5))
            key = active[:, qk + head * key_dim : qk + (head + 1) * key_dim]
            key = key * lax.rsqrt(jnp.sum(key * key, -1, keepdims=True) + EPS)
            value = active[:, 2 * qk + head * value_dim : 2 * qk + (head + 1) * value_dim]
            beta_col = beta[:, head : head + 1]
            beta_row = beta_t[head : head + 1]
            cum_col = cumul[:, heads + head : heads + head + 1]
            cum_row = cumul_t[heads + head : heads + head + 1]
            _, _, _, _, lower, attend = chunk_terms(query, key, beta_col, beta_row, cum_col, cum_row, rows, cols)
            inverse = unit_inverse(lower, rows, cols)
            state = now_ref[head]
            state_ref[state_place(index, head, heads, key_dim, value_dim, width)] = state
            rise = jnp.exp(cum_col)
            last = cum_col[span - 1 : span]
            update = mm(inverse, value) - mm(mm(inverse, rise * key), state)
            core = mm(rise * query, state) + mm(attend, update)
            tail = jnp.exp(last - cum_col) * beta_col
            now_ref[head] = jnp.exp(last) * state + mm_tn(key * tail, update)
            inverse_ref[index, head] = inverse
            wide = slice(head * value_dim, (head + 1) * value_dim)
            update_ref[here, wide] = update
            core_ref[here, wide] = core
            normed = core * lax.rsqrt(jnp.mean(core * core, -1, keepdims=True) + EPS)
            mixed_ref[here, wide] = (normed * gated[:, wide]).astype(mixed_ref.dtype)
        return carry

    lax.fori_loop(0, chunks, chunk, 0)


def delta_forward(pre, gate, small, taps, rate, gain, heads, key_dim, value_dim):
    length, width = pre.shape
    chunks = length // SPAN
    out_shape = (
        jax.ShapeDtypeStruct((length, heads * value_dim), jnp.bfloat16),
        jax.ShapeDtypeStruct((length, heads * value_dim), jnp.float32),
        jax.ShapeDtypeStruct((length, heads * value_dim), jnp.float32),
        jax.ShapeDtypeStruct((chunks * heads * key_dim * value_dim // width, width), jnp.float32),
        jax.ShapeDtypeStruct((chunks, heads, SPAN, SPAN), jnp.float32),
    )
    return pl.pallas_call(
        functools.partial(forward_kernel, heads, key_dim, value_dim),
        out_shape=out_shape,
        scratch_shapes=[
            pltpu.VMEM((HALO + SPAN, width), jnp.float32),
            pltpu.VMEM((heads, key_dim, value_dim), jnp.float32),
        ],
        compiler_params=pltpu.CompilerParams(vmem_limit_bytes=56 << 20),
        name="delta_forward",
    )(pre, gate, small, taps, rate, gain)


def backward_start(refs, span):
    (_, _, _, _, _, _, _, _, _, _, _, _, _, _, taps_grad_ref, gain_grad_ref, rate_grad_ref,
     _, pad_ref, now_ref) = refs
    now_ref[...] = jnp.zeros_like(now_ref)
    pad_ref[span : span + HALO] = jnp.zeros((HALO, pad_ref.shape[1]), jnp.float32)
    taps_grad_ref[...] = jnp.zeros_like(taps_grad_ref)
    gain_grad_ref[...] = jnp.zeros_like(gain_grad_ref)
    rate_grad_ref[...] = jnp.zeros_like(rate_grad_ref)


def backward_chunk(heads, key_dim, value_dim, index, refs):
    (pre_ref, gate_ref, small_ref, taps_ref, rate_ref, gain_ref,
     core_ref, update_ref, state_ref, inverse_ref, grad_ref,
     low_ref, gate_low_ref, small_low_ref, taps_grad_ref, gain_grad_ref, rate_grad_ref,
     ahead_ref, pad_ref, now_ref) = refs
    width = taps_ref.shape[1]
    span = SPAN
    rows, cols = grids(span)
    qk = heads * key_dim
    reach = taps_ref.shape[0] - 1
    lanes = small_ref.shape[1]
    lane = lax.broadcasted_iota(jnp.int32, (span, lanes), 1)
    start = pl.multiple_of(index * span, span)
    here = pl.ds(start, span)
    before = pl.ds(pl.multiple_of(jnp.maximum(start - HALO, 0), HALO), HALO)
    ahead_ref[0:HALO] = pre_ref[before, :] * jnp.where(index > 0, 1.0, 0.0)
    ahead_ref[HALO : HALO + span] = pre_ref[here, :]
    total = conv_window(ahead_ref[...], taps_ref[...], span)
    gain_of = sigmoid(total)
    active = total * gain_of
    bend = gain_of * (1.0 + total * (1.0 - gain_of))
    small = small_ref[here, :]
    beta, slope, _, cumul = gates_of(small, rate_ref[...], heads, rows, cols)
    beta_t = jnp.transpose(beta)
    cumul_t = jnp.transpose(cumul)
    gate = gate_ref[here, :]
    gate_sig = sigmoid(gate)
    gate_silu = gate * gate_sig
    gate_bend = gate_sig * (1.0 + gate * (1.0 - gate_sig))
    small_grad = jnp.zeros((span, lanes), jnp.float32)
    for head in range(heads):
        wide = slice(head * value_dim, (head + 1) * value_dim)
        core = core_ref[here, wide]
        grad_mixed = grad_ref[here, wide]
        gain = gain_ref[:, wide]
        scale = lax.rsqrt(jnp.mean(core * core, -1, keepdims=True) + EPS)
        normed = core * scale
        gate_low_ref[here, wide] = (grad_mixed * normed * gain * gate_bend[:, wide]).astype(gate_low_ref.dtype)
        with_gate = grad_mixed * gate_silu[:, wide]
        gain_grad_ref[:, wide] += jnp.sum(with_gate * normed, 0, keepdims=True)
        grad_normed = with_gate * gain
        grad_core = scale * (grad_normed - normed * jnp.mean(grad_normed * normed, -1, keepdims=True))
        query_act = active[:, head * key_dim : (head + 1) * key_dim]
        query_scale = lax.rsqrt(jnp.sum(query_act * query_act, -1, keepdims=True) + EPS)
        query = query_act * (query_scale * key_dim ** (-0.5))
        key_act = active[:, qk + head * key_dim : qk + (head + 1) * key_dim]
        key_scale = lax.rsqrt(jnp.sum(key_act * key_act, -1, keepdims=True) + EPS)
        key = key_act * key_scale
        beta_col = beta[:, head : head + 1]
        beta_row = beta_t[head : head + 1]
        cum_col = cumul[:, heads + head : heads + head + 1]
        cum_row = cumul_t[heads + head : heads + head + 1]
        decays, scaled, key_key, query_key, lower, attend = chunk_terms(
            query, key, beta_col, beta_row, cum_col, cum_row, rows, cols
        )
        state = state_ref[state_place(index, head, heads, key_dim, value_dim, width)]
        update = update_ref[here, wide]
        inverse = inverse_ref[index, head]
        grad_state = now_ref[head]
        rise = jnp.exp(cum_col)
        last = cum_col[span - 1 : span]
        fall = jnp.exp(last - cum_col)
        tail = fall * beta_col
        rise_query = rise * query
        rise_key = rise * key
        grad_update = mm_tn(attend, grad_core) + mm(key * tail, grad_state)
        grad_right = mm_tn(inverse, grad_update)
        now_ref[head] = jnp.exp(last) * grad_state + mm_tn(rise_query, grad_core) - mm_tn(rise_key, grad_right)
        grad_attend = jnp.where(cols <= rows, mm_nt(grad_core, update), 0.0)
        grad_lower = jnp.where(cols < rows, -mm_nt(grad_right, update), 0.0)
        core_state = mm_nt(grad_core, state)
        right_state = mm_nt(grad_right, state)
        grad_tail_key = mm_nt(update, grad_state)
        pair_query = grad_attend * scaled
        pair_key = grad_lower * scaled
        grad_query = rise * core_state + mm(pair_query, key)
        grad_key = (
            grad_tail_key * tail - rise * right_state + mm_tn(pair_query, query)
            + mm(pair_key, key) + mm_tn(pair_key, key)
        )
        grad_tail = jnp.sum(grad_tail_key * key, -1, keepdims=True)
        moved = grad_attend * query_key + grad_lower * key_key
        spread = moved * scaled
        by_row = jnp.sum(spread, -1, keepdims=True)
        sums = mm_tn(
            jnp.concatenate([moved * decays, spread], 1), jnp.ones((span, lanes), jnp.float32)
        )
        grad_beta = sums[:span, 0:1] + grad_tail * fall
        through_tail = grad_tail * tail
        grad_cum = (
            by_row - sums[span:, 0:1] - through_tail
            + rise * (jnp.sum(core_state * query, -1, keepdims=True) - jnp.sum(right_state * key, -1, keepdims=True))
        )
        end_grad = jnp.sum(through_tail, 0, keepdims=True) + jnp.exp(last) * jnp.sum(
            jnp.sum(state * grad_state, -1, keepdims=True), 0, keepdims=True
        )
        grad_cum = grad_cum + jnp.where(rows[:, 0:1] == span - 1, end_grad, 0.0)
        small_grad = small_grad + jnp.where(lane == head, grad_beta, 0.0)
        small_grad = small_grad + jnp.where(lane == heads + head, grad_cum, 0.0)
        grad_query = grad_query * key_dim ** (-0.5)
        unit = query_act * query_scale
        grad_query = query_scale * (grad_query - unit * jnp.sum(grad_query * unit, -1, keepdims=True))
        grad_key = key_scale * (grad_key - key * jnp.sum(grad_key * key, -1, keepdims=True))
        at = slice(head * key_dim, (head + 1) * key_dim)
        pad_ref[0:span, at] = grad_query * bend[:, at]
        at = slice(qk + head * key_dim, qk + (head + 1) * key_dim)
        pad_ref[0:span, at] = grad_key * bend[:, at]
        at = slice(2 * qk + head * value_dim, 2 * qk + (head + 1) * value_dim)
        pad_ref[0:span, at] = grad_right * bend[:, at]
    summed = mm(jnp.where(cols >= rows, 1.0, 0.0), small_grad)
    is_beta = lane < heads
    rate_grad_ref[...] += jnp.sum(jnp.where(is_beta, 0.0, -slope * summed), 0, keepdims=True)
    sig = beta
    small_low_ref[here, :] = jnp.where(
        is_beta, small_grad * sig * (1.0 - sig), -rate_ref[...] * sig * summed
    ).astype(small_low_ref.dtype)
    outer = pad_ref[...]
    dense = outer[0:span]
    block = ahead_ref[...]
    grad_pre = None
    for offset in range(reach + 1):
        behind = reach - offset
        taps_grad_ref[offset : offset + 1] += jnp.sum(
            dense * block[HALO - behind : HALO - behind + span], 0, keepdims=True
        )
        term = taps_ref[offset : offset + 1] * outer[behind : behind + span]
        grad_pre = term if grad_pre is None else grad_pre + term
    low_ref[here, :] = grad_pre.astype(low_ref.dtype)
    pad_ref[span : span + HALO] = pad_ref[0:HALO]


MESH = pl.DeviceIdType.MESH
VM = pl.BlockSpec(memory_space=pltpu.VMEM)


def call_out(peers):
    barrier = pltpu.get_barrier_semaphore()
    for peer in peers:
        pl.semaphore_signal(barrier, inc=1, device_id=peer, device_id_type=MESH)


def hear_all(peers):
    pl.semaphore_wait(pltpu.get_barrier_semaphore(), len(peers))


def greet(peers):
    call_out(peers)
    hear_all(peers)


def remote(src, dst, send, recv, peer):
    return pltpu.make_async_remote_copy(
        src_ref=src, dst_ref=dst, send_sem=send, recv_sem=recv, device_id=peer, device_id_type=MESH
    )


def tensor_peers():
    dp = lax.axis_index("dp")
    t = lax.axis_index("tensor")
    core = lax.rem(t, 2)
    mate = (dp, t + 1 - 2 * core)
    across = (dp, lax.rem(t + 2, 4))
    return core, mate, across


def psum_kernel(blocks, part_ref, out_ref, land_mate, land_across, half, send, recv):
    core, mate, across = tensor_peers()
    greet((mate, across))
    rows = part_ref.shape[0] // blocks
    part = rows // 2
    first = []
    for b in range(blocks):
        theirs = pl.ds(pl.multiple_of(b * rows + (1 - core) * part, part), part)
        copy = remote(part_ref.at[theirs], land_mate.at[pl.ds(b * part, part)], send.at[0, b], recv.at[0, b], mate)
        copy.start()
        first.append(copy)
    second = []
    for b in range(blocks):
        mine = pl.ds(pl.multiple_of(b * rows + core * part, part), part)
        slot = pl.ds(b * part, part)
        first[b].wait_recv()
        half[slot] = part_ref[mine] + land_mate[slot]
        copy = remote(half.at[slot], land_across.at[slot], send.at[1, b], recv.at[1, b], across)
        copy.start()
        second.append(copy)
    third = []
    for b in range(blocks):
        mine = pl.ds(pl.multiple_of(b * rows + core * part, part), part)
        slot = pl.ds(b * part, part)
        second[b].wait_recv()
        out_ref[mine] = half[slot] + land_across[slot]
        copy = remote(out_ref.at[mine], out_ref.at[mine], send.at[2, b], recv.at[2, b], mate)
        copy.start()
        third.append(copy)
    for b in range(blocks):
        third[b].wait_recv()
    for b in range(blocks):
        first[b].wait_send()
        second[b].wait_send()
        third[b].wait_send()


def tensor_sum(part, collective_id, blocks=8):
    rows, width = part.shape
    return pl.pallas_call(
        functools.partial(psum_kernel, blocks),
        out_shape=jax.ShapeDtypeStruct(part.shape, part.dtype),
        in_specs=[VM],
        out_specs=VM,
        scratch_shapes=[pltpu.VMEM((rows // 2, width), part.dtype)] * 3
        + [pltpu.SemaphoreType.DMA((3, blocks))] * 2,
        compiler_params=pltpu.CompilerParams(
            collective_id=collective_id, has_side_effects=True, vmem_limit_bytes=40 << 20
        ),
        name="tensor_sum",
    )(part)


def swap_kernel(count, narrow, *refs):
    sources, results = refs[:count], refs[count : 2 * count]
    staged, send, recv, close_send, close_recv = refs[2 * count :]
    n = lax.axis_size("dp")
    me = lax.axis_index("dp")
    t = lax.axis_index("tensor")
    core, mate, across = tensor_peers()
    ranks = lax.axis_size("tensor")
    others = [lax.rem(me + k, n) for k in range(1, n)]
    greet([(other, t) for other in others] + [mate, across])
    seg = results[0].shape[0] // n
    part = seg // ranks
    far = lax.rem(t + 2, ranks)

    def at(place, rank):
        return pl.ds(pl.multiple_of(place * seg + rank * part, part), part)

    outgoing = []
    for i in range(count):
        for k in range(n):
            other = lax.rem(me + k, n)
            if k == 0:
                results[i][at(me, t)] = sources[i][at(me, t)].astype(jnp.float32)
                continue
            if narrow[i]:
                staged[i, k] = sources[i][at(other, t)].astype(jnp.float32)
                src = staged.at[i, k]
            else:
                src = sources[i].at[at(other, t)]
            copy = remote(src, results[i].at[at(me, t)], send.at[i, k], recv.at[i, k], (other, t))
            copy.start()
            outgoing.append(copy)
    close = []
    for i in range(count):
        for k in range(n):
            source = lax.rem(me + n - k, n)
            here = results[i].at[at(source, t)]
            if k:
                remote(here, here, send.at[i, k], recv.at[i, k], (source, t)).wait_recv()
            over = remote(here, here, close_send.at[0, i, k], close_recv.at[0, i, k], across)
            over.start()
            beside = remote(here, here, close_send.at[1, i, k], close_recv.at[1, i, k], mate)
            beside.start()
            close += [over, beside]
    last = []
    for i in range(count):
        for k in range(n):
            source = lax.rem(me + n - k, n)
            there = results[i].at[at(source, far)]
            remote(there, there, close_send.at[0, i, k], close_recv.at[0, i, k], across).wait_recv()
            copy = remote(there, there, close_send.at[2, i, k], close_recv.at[2, i, k], mate)
            copy.start()
            last.append(copy)
    for copy in outgoing:
        copy.wait_send()
    for j, copy in enumerate(close):
        copy.wait_send()
        if j % 2:
            copy.wait_recv()
    for copy in last:
        copy.wait()


def swap(arrays, n, collective_id):
    count = len(arrays)
    rows, width = arrays[0].shape
    narrow = [a.dtype != jnp.float32 for a in arrays]
    out = pl.pallas_call(
        functools.partial(swap_kernel, count, narrow),
        out_shape=[jax.ShapeDtypeStruct((rows, width), jnp.float32)] * count,
        in_specs=[VM] * count,
        out_specs=[VM] * count,
        scratch_shapes=[pltpu.VMEM((count, n, rows // n // 4, width), jnp.float32)]
        + [pltpu.SemaphoreType.DMA((count, n))] * 2
        + [pltpu.SemaphoreType.DMA((3, count, n))] * 2,
        compiler_params=pltpu.CompilerParams(
            collective_id=collective_id, has_side_effects=True, vmem_limit_bytes=40 << 20
        ),
        name="swap",
    )(*arrays)
    return out


SLOT = 80
DEPTH = 10
SPLIT = 3
WHOLE = 2


def grid_place():
    n = lax.axis_size("dp")
    me = lax.axis_index("dp")
    t = lax.axis_index("tensor")
    lines = n // 2
    z = lax.div(me, 2)
    x = lax.rem(me, 2)
    return n, lines, me, t, z, x


def reduce_slot(slot, chunks, data, split_rings, whole_rings, sems):
    n, lines, me, t, z, x = grid_place()
    mate = (me + 1 - 2 * x, t)
    send_x, recv_x, send_z, recv_z, send_d, recv_d, send_p, recv_p, send_s, recv_s = [sems.at[i] for i in range(10)]
    top = lines - 1
    finish = slot - 2 * lines - 1

    def ring(chunk):
        return lax.rem(chunk, DEPTH)

    def within(chunk):
        return (chunk >= 0) & (chunk < chunks)

    for stream in range(SPLIT):
        land_x, land_z, outgo, aside = split_rings
        up = stream % 2 == 0
        level = z if up else top - z
        after = (me + 2, t) if up else (me - 2, t)
        prior = (me - 2, t) if up else (me + 2, t)

        def rows(chunk, side):
            return pl.ds(pl.multiple_of(chunk * SLOT + 16 * stream + 8 * side, 8), 8)

        def spot(ref, chunk):
            return ref.at[stream, ring(chunk)]

        def copy(kind_send, kind_recv, chunk, src, dst, peer):
            at = (stream, ring(chunk))
            return remote(src, dst, kind_send.at[at], kind_recv.at[at], peer)

        def to_mate(chunk):
            return copy(send_x, recv_x, chunk, spot(aside, chunk), spot(land_x, chunk), mate)

        def to_after(chunk):
            return copy(send_z, recv_z, chunk, spot(outgo, chunk), spot(land_z, chunk), after)

        def result(chunk, peer):
            here = data.at[rows(chunk, x)]
            return copy(send_d, recv_d, chunk, here, here, peer)

        def close(chunk, side):
            here = data.at[rows(chunk, side)]
            return copy(send_p, recv_p, chunk, here, here, mate)

        def give_back(chunk):
            @pl.when(level > 0)
            def _():
                result(chunk, prior).start()

            close(chunk, x).start()

        @pl.when(slot < chunks)
        def _():
            aside[stream, ring(slot)] = data[rows(slot, 1 - x)]
            to_mate(slot).start()

        rise = slot - 1 - level

        @pl.when(within(rise))
        def _():
            here = rows(rise, x)
            at = ring(rise)
            to_mate(rise).wait_recv()

            @pl.when(level > 0)
            def _():
                to_after(rise).wait_recv()
                outgo[stream, at] = data[here] + land_x[stream, at] + land_z[stream, at]

            @pl.when(level == 0)
            def _():
                outgo[stream, at] = data[here] + land_x[stream, at]

            @pl.when(level < top)
            def _():
                to_after(rise).start()

            @pl.when(level == top)
            def _():
                data[here] = outgo[stream, at]
                give_back(rise)

        fall = slot - 1 - 2 * top + level

        @pl.when(within(fall) & (level < top))
        def _():
            result(fall, after).wait_recv()
            to_after(fall).wait_send()
            give_back(fall)

        @pl.when(within(finish))
        def _():
            @pl.when(level > 0)
            def _():
                result(finish, prior).wait_send()

            close(finish, x).wait_send()
            close(finish, 1 - x).wait_recv()
            to_mate(finish).wait_send()

    for stream in range(WHOLE):
        land_x, land_z, land_s, outgo = whole_rings
        line = z if stream == 0 else top - z
        step = 2 if stream == 0 else -2
        inner, outer = (me - step, t), (me + step, t)

        def rows(chunk):
            return pl.ds(pl.multiple_of(chunk * SLOT + 16 * (SPLIT + stream), 8), 16)

        def spot(ref, chunk):
            return ref.at[stream, ring(chunk)]

        def copy(kind_send, kind_recv, chunk, src, dst, peer):
            at = (ring(chunk),)
            return remote(
                src, dst, kind_send.at[SPLIT + stream, ring(chunk)], kind_recv.at[SPLIT + stream, ring(chunk)], peer
            )

        def inward(chunk):
            return copy(send_z, recv_z, chunk, spot(outgo, chunk), spot(land_z, chunk), inner)

        def outward(chunk):
            return copy(send_z, recv_s, chunk, spot(outgo, chunk), spot(land_s, chunk), outer)

        def to_mate(chunk):
            return copy(send_x, recv_x, chunk, spot(outgo, chunk), spot(land_x, chunk), mate)

        def result_out(chunk):
            here = data.at[rows(chunk)]
            return copy(send_d, recv_d, chunk, here, here, outer)

        def result_in(chunk):
            here = data.at[rows(chunk)]
            return copy(send_s, recv_d, chunk, here, here, inner)

        rise = slot - 1 - (top - line)
        root = lax.rem(jnp.maximum(rise, 0), 2)

        @pl.when(within(rise) & (line >= root))
        def _():
            here = rows(rise)
            at = ring(rise)

            @pl.when(line < top)
            def _():
                inward(rise).wait_recv()

            is_fork = (line == root) & (root > 0)

            @pl.when(is_fork)
            def _():
                outward(rise).wait_recv()
                outgo[stream, at] = data[here] + land_z[stream, at] + land_s[stream, at]

            @pl.when((line < top) & jnp.logical_not(is_fork))
            def _():
                outgo[stream, at] = data[here] + land_z[stream, at]

            @pl.when(line == top)
            def _():
                outgo[stream, at] = data[here]

            @pl.when(line > root)
            def _():
                inward(rise).start()

            @pl.when(line == root)
            def _():
                to_mate(rise).start()

        leaf = slot - 1

        @pl.when(within(leaf) & (line == 0) & (lax.rem(jnp.maximum(leaf, 0), 2) > 0))
        def _():
            outgo[stream, ring(leaf)] = data[rows(leaf)]
            outward(leaf).start()

        meet = slot - 2 - (top - line)
        meet_root = lax.rem(jnp.maximum(meet, 0), 2)

        @pl.when(within(meet) & (line == meet_root))
        def _():
            at = ring(meet)
            to_mate(meet).wait_recv()
            data[rows(meet)] = outgo[stream, at] + land_x[stream, at]
            result_out(meet).start()

            @pl.when(meet_root > 0)
            def _():
                result_in(meet).start()

        for parity in range(2):
            fall = slot - 2 - (top - parity) - (line - parity)

            @pl.when(within(fall) & (lax.rem(jnp.maximum(fall, 0), 2) == parity) & (line > parity))
            def _():
                result_out(fall).wait_recv()
                inward(fall).wait_send()

                @pl.when(line < top)
                def _():
                    result_out(fall).start()

        inside = slot - 2 - (top - 1) - 1

        @pl.when(within(inside) & (lax.rem(jnp.maximum(inside, 0), 2) > 0) & (line == 0))
        def _():
            result_in(inside).wait_recv()
            outward(inside).wait_send()

        end_root = lax.rem(jnp.maximum(finish, 0), 2)

        @pl.when(within(finish))
        def _():
            @pl.when((line >= end_root) & (line < top))
            def _():
                result_out(finish).wait_send()

            @pl.when(line == end_root)
            def _():
                to_mate(finish).wait_send()

                @pl.when(end_root > 0)
                def _():
                    result_in(finish).wait_send()


def settle(lines):
    return 2 * lines + 1


def reduce_scratch(width):
    return (
        [pltpu.VMEM((SPLIT, DEPTH, 8, width), jnp.float32)] * 4
        + [pltpu.VMEM((WHOLE, DEPTH, 16, width), jnp.float32)] * 4
        + [pltpu.SemaphoreType.DMA((10, SPLIT + WHOLE, DEPTH))]
    )


BLOCKS = 8


def dot_plain(left, right):
    return lax.dot_general(left, right, (((1,), (0,)), ((), ())), preferred_element_type=jnp.float32)


def dot_nt(left, right):
    return lax.dot_general(left, right, (((1,), (1,)), ((), ())), preferred_element_type=jnp.float32)


def dot_tn(left, right):
    return lax.dot_general(left, right, (((0,), (0,)), ((), ())), preferred_element_type=jnp.float32)


def aligned(start, size):
    return pl.ds(pl.multiple_of(start, size), size)


class TensorSum:
    def __init__(self, part, total, land_mate, land_across, half, send, recv):
        self.core, self.mate, self.across = tensor_peers()
        self.part, self.total, self.half = part, total, half
        self.land_mate, self.land_across = land_mate, land_across
        self.send, self.recv = send, recv
        self.rows = part.shape[0] // BLOCKS
        self.size = self.rows // 2

    def span(self, block, side):
        return aligned(block * self.rows + side * self.size, self.size)

    def slot(self, block):
        return aligned(block * self.size, self.size)

    def first(self, block):
        return remote(
            self.part.at[self.span(block, 1 - self.core)], self.land_mate.at[self.slot(block)],
            self.send.at[0, block], self.recv.at[0, block], self.mate,
        )

    def second(self, block):
        return remote(
            self.half.at[self.slot(block)], self.land_across.at[self.slot(block)],
            self.send.at[1, block], self.recv.at[1, block], self.across,
        )

    def third(self, block):
        mine = self.total.at[self.span(block, self.core)]
        return remote(mine, mine, self.send.at[2, block], self.recv.at[2, block], self.mate)

    def start(self):
        for block in range(BLOCKS):
            self.first(block).start()

    def cross(self, block):
        self.first(block).wait_recv()
        slot = self.slot(block)
        self.half[slot] = self.part[self.span(block, self.core)] + self.land_mate[slot]
        self.second(block).start()

    def share(self, block, beside=None):
        self.second(block).wait_recv()
        slot = self.slot(block)
        mine = self.span(block, self.core)
        value = self.half[slot] + self.land_across[slot]
        self.total[mine] = value if beside is None else value + beside[mine].astype(value.dtype)
        self.third(block).start()

    def finish(self, had=0):
        for block in range(had, BLOCKS):
            self.third(block).wait_recv()
        for block in range(BLOCKS):
            self.first(block).wait_send()
            self.second(block).wait_send()
            self.third(block).wait_send()


class Swap:
    def __init__(self, source, result, send, recv, close_send, close_recv):
        self.n = lax.axis_size("dp")
        self.me = lax.axis_index("dp")
        self.t = lax.axis_index("tensor")
        self.ranks = lax.axis_size("tensor")
        _, self.mate, self.across = tensor_peers()
        self.source, self.result = source, result
        self.sems = send, recv, close_send, close_recv
        self.seg = result.shape[0] // self.n
        self.part = self.seg // self.ranks

    def at(self, place, rank):
        return aligned(place * self.seg + rank * self.part, self.part)

    def out(self, k):
        other = lax.rem(self.me + k, self.n)
        return remote(
            self.source.at[self.at(other, self.t)], self.result.at[self.at(self.me, self.t)],
            self.sems[0].at[k], self.sems[1].at[k], (other, self.t),
        )

    def close(self, k, leg):
        origin = lax.rem(self.me + self.n - k, self.n)
        rank = lax.rem(self.t + 2, self.ranks) if leg == 2 else self.t
        here = self.result.at[self.at(origin, rank)]
        return remote(
            here, here, self.sems[2].at[leg, k], self.sems[3].at[leg, k], self.across if leg == 0 else self.mate
        )

    def start(self):
        mine = self.at(self.me, self.t)
        self.result[mine] = self.source[mine]
        for k in range(1, self.n):
            self.out(k).start()

    def gather(self, k):
        @pl.when(k > 0)
        def _():
            self.out(k).wait_recv()

        self.close(k, 0).start()
        self.close(k, 1).start()

    def forward(self, k):
        self.close(k, 0).wait_recv()
        self.close(k, 2).start()

    def sent(self):
        for k in range(1, self.n):
            self.out(k).wait_send()

    def finish(self):
        for k in range(self.n):
            self.close(k, 0).wait_send()
            self.close(k, 1).wait()
            self.close(k, 2).wait()


class PlaneSwap(Swap):
    def __init__(self, source, result, send, recv, close_send, close_recv):
        super().__init__(source, result, send, recv, close_send, close_recv)
        self.core = lax.rem(self.t, 2)
        self.part = self.seg // 2

    def out(self, k):
        other = lax.rem(self.me + k, self.n)
        return remote(
            self.source.at[self.at(other, self.core)], self.result.at[self.at(self.me, self.core)],
            self.sems[0].at[k], self.sems[1].at[k], (other, self.t),
        )

    def close(self, k, leg):
        origin = lax.rem(self.me + self.n - k, self.n)
        here = self.result.at[self.at(origin, self.core)]
        return remote(here, here, self.sems[2].at[leg, k], self.sems[3].at[leg, k], self.mate)

    def start(self):
        mine = self.at(self.me, self.core)
        self.result[mine] = self.source[mine]
        for k in range(1, self.n):
            self.out(k).start()

    def gather(self, k):
        @pl.when(k > 0)
        def _():
            self.out(k).wait_recv()

        self.close(k, 1).start()

    def finish(self):
        for k in range(self.n):
            self.close(k, 1).wait()


def tail_kernel(
    heads, key_dim, value_dim, ranges, chunks,
    part2_hbm, ffn_hbm, pre_hbm, core_hbm, update_hbm, state_hbm,
    resid1_hbm, upstream_hbm, resid_hbm, mixed_hbm, hidden1_hbm, hidden2_hbm, units_hbm,
    w_out_hbm, query_hbm, key_hbm, value_hbm, w_gate_hbm, w_small_hbm, gate_hbm, small_hbm, inverse_hbm,
    norm1_ref, norm2_ref, taps_ref, rate_ref, gain_ref,
    data, output_ref, inputs_grad_ref,
    resid1_ref, upstream_ref, resid_ref, mixed_ref, hidden1_ref, hidden2_ref, units_ref,
    w_out_ref, w_mix_ref, w_gate_ref, w_small_ref, gate_ref, small_ref, inverse_ref,
    split_x, split_z, split_out, split_aside, whole_x, whole_z, whole_s, whole_out, sems,
    part, total, half, land_mate, land_across, sum_send, sum_recv,
    resid1_grad, resid1_low, mixed_grad, low, gate_low, small_low,
    taps_grad, gain_grad, rate_grad, norm1_grad, norm2_grad, ahead, pad, now,
    shuffled, swap_send, swap_recv, close_send, close_recv, load_sem,
):
    n, lines, me, t, z, x = grid_place()
    _, mate, across = tensor_peers()
    length, width = resid1_hbm.shape
    qk = heads * key_dim
    values = heads * value_dim
    at_down, at_units, at_out, at_gate, at_mix, at_small, at_end, rows_all = ranges
    loads = [
        (part2_hbm, part),
        (units_hbm, units_ref),
        (upstream_hbm, upstream_ref),
        (hidden2_hbm, hidden2_ref),
        (resid1_hbm, resid1_ref),
        (w_out_hbm, w_out_ref),
        (mixed_hbm, mixed_ref),
        (pre_hbm, data.at[pl.ds(at_mix, length)]),
        (core_hbm, data.at[pl.ds(at_mix + length, length), pl.ds(0, values)]),
        (update_hbm, data.at[pl.ds(at_mix + length, length), pl.ds(values, values)]),
        (state_hbm, data.at[pl.ds(at_gate, state_hbm.shape[0])]),
        (gate_hbm, gate_ref),
        (small_hbm, small_ref),
        (inverse_hbm, inverse_ref),
        (hidden1_hbm, hidden1_ref),
        (query_hbm, w_mix_ref.at[:, pl.ds(0, qk)]),
        (key_hbm, w_mix_ref.at[:, pl.ds(qk, qk)]),
        (value_hbm, w_mix_ref.at[:, pl.ds(2 * qk, values)]),
        (w_gate_hbm, w_gate_ref),
        (w_small_hbm, w_small_ref),
        (resid_hbm, resid_ref),
    ]
    loads = [pltpu.make_async_copy(src, dst, load_sem.at[i]) for i, (src, dst) in enumerate(loads)]
    load_ffn = pltpu.make_async_copy(ffn_hbm, part, load_sem.at[len(loads)])
    peers = [(lax.rem(me + k, n), t) for k in range(1, n)] + [mate, across]
    call_out(peers)
    for load in loads:
        load.start()
    refs = (
        data.at[pl.ds(at_mix, length)], gate_ref, small_ref, taps_ref, rate_ref, gain_ref,
        data.at[pl.ds(at_mix + length, length), pl.ds(0, values)],
        data.at[pl.ds(at_mix + length, length), pl.ds(values, values)],
        data.at[pl.ds(at_gate, state_hbm.shape[0])], inverse_ref, mixed_grad, low, gate_low, small_low, taps_grad, gain_grad, rate_grad,
        ahead, pad, now,
    )
    sums = [
        TensorSum(part, total, land_mate, land_across.at[i % 2], half, sum_send.at[i], sum_recv.at[i]) for i in range(3)
    ]
    swaps = [
        Swap(source, result, swap_send.at[i], swap_recv.at[i], close_send.at[i], close_recv.at[i])
        for i, (source, result) in enumerate([(total, shuffled), (resid1_grad, inputs_grad_ref)])
    ]
    norm1_grad[...] = jnp.zeros_like(norm1_grad)
    norm2_grad[...] = jnp.zeros_like(norm2_grad)
    backward_start(refs, SPAN)
    data[at_end:rows_all] = jnp.zeros((rows_all - at_end, width), jnp.float32)
    count_units = (at_units - at_down)
    tiles = units_ref.shape[2] // 128

    def units_piece(i):
        kind = lax.div(i, tiles)
        tile = lax.rem(i, tiles)
        left = units_ref[kind, :, aligned(tile * 128, 128)]
        start = at_down + kind * count_units + tile * 128

        def put(right):
            value = dot_tn(left, right)

            @pl.when(tile < tiles - 1)
            def _():
                data[pl.ds(pl.multiple_of(start, 64), 128)] = value

            @pl.when(tile == tiles - 1)
            def _():
                rest = count_units - (tiles - 1) * 128
                data[pl.ds(pl.multiple_of(start, 64), rest)] = value[0:rest]

        @pl.when(kind == 0)
        def _():
            put(upstream_ref[...])

        @pl.when(kind > 0)
        def _():
            put(hidden2_ref[...])

    loads[0].wait()
    hear_all(peers)
    sums[0].start()
    loads[1].wait()
    loads[2].wait()
    units_piece(0)

    def wait_loads():
        for load in loads[3:]:
            load.wait()

    def norm_back(value, grad, gain, gain_grad_ref):
        scale = lax.rsqrt(jnp.mean(value * value, -1, keepdims=True) + EPS)
        normed = value * scale
        gain_grad_ref[...] += jnp.sum(grad * normed, 0, keepdims=True)
        scaled = grad * gain
        return scale * (scaled - normed * jnp.mean(scaled * normed, -1, keepdims=True))

    def norm2_piece(i):
        here = aligned(i * 64, 64)
        grad = upstream_ref[here].astype(jnp.float32) + norm_back(
            resid1_ref[here], total[here], norm2_ref[...], norm2_grad
        )
        resid1_grad[here] = grad
        resid1_low[here] = grad.astype(jnp.bfloat16)

    def mixed_piece(i):
        tile = aligned(i * 256, 256)
        mixed_grad[:, tile] = dot_nt(resid1_low[...], w_out_ref[tile])

    def out_piece(i):
        tile = aligned(i * 256, 256)
        data[pl.ds(pl.multiple_of(at_out + i * 256, 64), 256)] = dot_tn(
            mixed_ref[:, tile], resid1_low[...]
        )

    def gate_piece(i):
        tile = aligned(i * 256, 256)
        half_rows = width // 2
        data[pl.ds(pl.multiple_of(at_gate + i * 256, 64), 256), 0:values] = dot_tn(hidden1_ref[:, tile], gate_low[...])
        other = aligned(half_rows + i * 256, 256)
        data[pl.ds(pl.multiple_of(at_gate + i * 256, 64), 256), values : 2 * values] = dot_tn(
            hidden1_ref[:, other], gate_low[...]
        )

    def mix_piece(i):
        tile = aligned(i * 256, 256)
        data[pl.ds(pl.multiple_of(at_mix + i * 256, 64), 256)] = dot_tn(hidden1_ref[:, tile], low[...])

    def hidden_piece(i):
        tile = aligned(i * 256, 256)
        part[:, tile] = (
            dot_nt(low[...], w_mix_ref[tile]) + dot_nt(gate_low[...], w_gate_ref[tile])
            + dot_plain(small_low[...], w_small_ref[:, tile])
        )

    def output_piece(i):
        here = aligned(i * 64, 64)
        total[here] = total[here] + resid1_ref[here]

    def round_piece(i):
        here = aligned(i * 64, 64)
        output_ref[here] = shuffled[here].astype(output_ref.dtype)

    def norm1_piece(i):
        here = aligned(i * 64, 64)
        resid1_grad[here] = resid1_grad[here] + norm_back(
            resid_ref[here].astype(jnp.float32), total[here], norm1_ref[...], norm1_grad
        )

    def small_piece():
        base = at_small
        data[base : at_end] = jnp.zeros((at_end - base, width), jnp.float32)
        data[base : base + 4] = taps_grad[...]
        data[base + 4 : base + 5] = norm1_grad[...]
        data[base + 5 : base + 6] = norm2_grad[...]
        data[base + 6 : base + 7, 0:values] = gain_grad[...]
        data[base + 6 : base + 7, values : values + rate_grad.shape[1]] = rate_grad[...]
        data[base + 8 : base + 16] = dot_tn(small_low[...], hidden1_ref[...])[0:8]

    def start_ffn():
        load_ffn.start()
        load_ffn.wait()
        sums[1].start()

    pieces = []

    def plan(first, count, each, run):
        assert count % each == 0
        pieces.append((first, count, each, run))
        return first + -(-count // each)

    plan(0, 1, 1, lambda i: wait_loads())
    plan(0, 3 * tiles - 1, 1, lambda i: units_piece(i + 1))
    for i in range(1, 3 * tiles):
        assert i <= (at_down + i // tiles * count_units + i % tiles * 128) // SLOT
    at = plan(0, BLOCKS, 2, sums[0].cross)
    at = plan(at, BLOCKS, 2, sums[0].share)
    at = plan(at, 1, 1, lambda i: sums[0].finish())
    at = plan(at, length // 64, 2, norm2_piece)
    at = plan(at, values // 256, 1, mixed_piece)
    side = at
    at = plan(at, values // 256, 1, out_piece)
    at_ready_out = at
    at = plan(at, length // SPAN, 1, lambda i: backward_chunk(heads, key_dim, value_dim, length // SPAN - 1 - i, refs))
    side = plan(side, 1, 1, lambda i: start_ffn())
    side = plan(side, BLOCKS, 2, sums[1].cross)
    side = plan(side, BLOCKS, 2, sums[1].share)
    side = plan(side, 1, 1, lambda i: sums[1].finish())
    part_free = side
    side = plan(side, length // 64, 4, output_piece)
    side = plan(side, 1, 1, lambda i: swaps[0].start())
    side = plan(side, n, 2, swaps[0].gather)
    side = plan(side, 1, 1, lambda i: swaps[0].sent())
    total_free = side
    side = plan(side, n, 2, swaps[0].forward)
    side = plan(side, 1, 1, lambda i: swaps[0].finish())
    side = plan(side, length // 64, 4, round_piece)
    at = plan(at, width // 512, 1, gate_piece)
    at_ready_gate = at
    at = plan(at, width // 256, 1, mix_piece)
    at_ready_mix = at
    at = plan(max(at, part_free), width // 256, 1, hidden_piece)
    at = plan(max(at, total_free), 1, 1, lambda i: sums[2].start())
    at = plan(at, BLOCKS, 2, sums[2].cross)
    at = plan(at, BLOCKS, 2, sums[2].share)
    at = plan(at, 1, 1, lambda i: sums[2].finish())
    at = plan(at, length // 64, 2, norm1_piece)
    at = plan(at, 1, 1, lambda i: small_piece())
    at_ready_small = at
    at = plan(at, 1, 1, lambda i: swaps[1].start())
    at = plan(at, n, 2, swaps[1].gather)
    plan(at, 1, 1, lambda i: swaps[1].sent())
    at = plan(at, n, 2, swaps[1].forward)
    at = plan(at, 1, 1, lambda i: swaps[1].finish())
    assert at_ready_out <= at_out // SLOT and at_ready_gate <= at_gate // SLOT
    assert at_ready_mix <= at_mix // SLOT and at_ready_small <= at_small // SLOT
    last = max(chunks + settle(lines), at, side)

    def step(slot, carry):
        reduce_slot(
            slot, chunks, data, (split_x, split_z, split_out, split_aside), (whole_x, whole_z, whole_s, whole_out), sems
        )
        for first, count, each, run in pieces:
            steps = -(-count // each)

            @pl.when((slot >= first) & (slot < first + steps))
            def _(first=first, each=each, run=run):
                if each == 1:
                    run(slot - first)
                else:
                    def inner(i, carry):
                        run((slot - first) * each + i)
                        return carry

                    lax.fori_loop(0, each, inner, 0)

        return carry

    lax.fori_loop(0, last, step, 0)


def tail(
    part2, ffn, pre, core, update, states, resid1, upstream, resid, mixed, hidden1, hidden2, units,
    w_out, w_query, w_key, w_value, w_gate, w_small, gate, small, inverses, norm1, norm2, taps, rate, gain,
    heads, key_dim, value_dim, count_units, places, collective_id,
):
    length, width = resid1.shape
    values = heads * value_dim
    qk = heads * key_dim
    lanes = small.shape[1]
    heights = [count_units, 2 * count_units, values, values, width, 64]
    ranges = [0]
    for height in heights:
        ranges.append(ranges[-1] + height)
    rows_all = -(-ranges[-1] // SLOT) * SLOT
    chunks = rows_all // SLOT
    f32, bf = jnp.float32, jnp.bfloat16
    shape = jax.ShapeDtypeStruct
    out_shape = [
        pltpu.VMEM((rows_all, width), f32),
        pltpu.VMEM((length, width), bf),
        pltpu.VMEM((length, width), f32),
    ]
    vmem, any_ = VM, pl.BlockSpec(memory_space=pl.ANY)
    dma = pltpu.SemaphoreType.DMA
    scratch = (
        [
            pltpu.VMEM(a.shape, a.dtype)
            for a in (
                resid1, upstream, resid, mixed, hidden1, hidden2, units, w_out, shape((width, width), bf), w_gate, w_small,
                gate, small, inverses,
            )
        ]
        + reduce_scratch(width)
        + [
            pltpu.VMEM((length, width), f32),
            pltpu.VMEM((length, width), f32),
            pltpu.VMEM((length // 2, width), f32),
            pltpu.VMEM((length // 2, width), f32),
            pltpu.VMEM((2, length // 2, width), f32),
            dma((3, 3, BLOCKS)),
            dma((3, 3, BLOCKS)),
            pltpu.VMEM((length, width), f32),
            pltpu.VMEM((length, width), bf),
            pltpu.VMEM((length, values), f32),
            pltpu.VMEM((length, width), bf),
            pltpu.VMEM((length, values), bf),
            pltpu.VMEM((length, lanes), bf),
            pltpu.VMEM(taps.shape, f32),
            pltpu.VMEM((1, values), f32),
            pltpu.VMEM((1, lanes), f32),
            pltpu.VMEM((1, width), f32),
            pltpu.VMEM((1, width), f32),
            pltpu.VMEM((HALO + SPAN, width), f32),
            pltpu.VMEM((HALO + SPAN, width), f32),
            pltpu.VMEM((heads, key_dim, value_dim), f32),
            pltpu.VMEM((length, width), f32),
            dma((2, places)),
            dma((2, places)),
            dma((2, 3, places)),
            dma((2, 3, places)),
            dma((24,)),
        ]
    )
    return pl.pallas_call(
        functools.partial(tail_kernel, heads, key_dim, value_dim, tuple(ranges) + (rows_all,), chunks),
        out_shape=out_shape,
        in_specs=[any_] * 22 + [vmem] * 5,
        out_specs=[vmem] * 3,
        scratch_shapes=scratch,
        compiler_params=pltpu.CompilerParams(
            collective_id=collective_id, has_side_effects=True,
            vmem_limit_bytes=67043328 - 4 * width * rows_all - 6 * width * length - (1 << 18),
        ),
        name="tail",
    )(
        part2, ffn, pre, core, update, states, resid1, upstream, resid, mixed, hidden1, hidden2, units,
        w_out, w_query, w_key, w_value, w_gate, w_small, gate, small, inverses, norm1, norm2, taps, rate, gain,
    ), tuple(ranges)


def finish_kernel(heads, qk, values, ranges, data, output, inputs_grad, *refs):
    big, smalls, sems = refs[:10], refs[10:19], refs[19]
    at_down, at_units, at_out, at_gate, at_mix, at_small, _ = ranges
    width = data.shape[1]
    units = big[2].shape[0]

    def rows(start, height, left=0, wide=None):
        return data.at[pl.ds(start, height), pl.ds(left, width if wide is None else wide)]

    half = width // 2
    moves = [
        (output, big[0]),
        (inputs_grad, big[1]),
        (rows(at_units, units), big[2]),
        (rows(at_units + units, units), big[3]),
        (rows(at_down, units), big[4]),
        (rows(at_out, values), big[5]),
        (rows(at_gate, half, 0, values), big[6].at[pl.ds(0, half)]),
        (rows(at_gate, half, values, values), big[6].at[pl.ds(half, half)]),
        (rows(at_mix, width, 0, qk), big[7]),
        (rows(at_mix, width, qk, qk), big[8]),
        (rows(at_mix, width, 2 * qk, values), big[9]),
    ]
    moves = [pltpu.make_async_copy(src, dst, sems.at[i]) for i, (src, dst) in enumerate(moves)]
    for move in moves:
        move.start()
    norm1, norm2, head, rate, beta, decay, query, key, value = smalls
    small = data[at_small : at_small + 16]
    norm1[...] = small[4:5]
    norm2[...] = small[5:6]
    head[...] = small[6:7, 0:values]
    rate[...] = small[6:7, values : values + 2 * heads][:, heads:]
    beta[...] = small[8 : 8 + heads]
    decay[...] = small[8 + heads : 8 + 2 * heads]
    query[...] = small[0:4, 0:qk]
    key[...] = small[0:4, qk : 2 * qk]
    value[...] = small[0:4, 2 * qk :]
    for move in moves:
        move.wait()


def finish(data, output, inputs_grad, ranges, units, heads, qk, values):
    width = data.shape[1]
    length = output.shape[0]
    any_ = pl.BlockSpec(memory_space=pl.ANY)
    f32 = jnp.float32
    bigs = [
        (units, width), (units, width), (units, width), (values, width), (width, values), (width, qk), (width, qk), (width, values)
    ]
    smalls = [(1, width), (1, width), (1, values), (1, heads), (heads, width), (heads, width), (4, qk), (4, qk), (4, values)]
    held = [pltpu.with_memory_space_constraint(a, pltpu.VMEM) for a in (data, output, inputs_grad)]
    return pl.pallas_call(
        functools.partial(finish_kernel, heads, qk, values, ranges),
        out_shape=[jax.ShapeDtypeStruct((length, width), output.dtype), jax.ShapeDtypeStruct((length, width), f32)]
        + [jax.ShapeDtypeStruct(shape, f32) for shape in bigs + smalls],
        in_specs=[VM] * 3,
        out_specs=[any_] * 10 + [VM] * len(smalls),
        scratch_shapes=[pltpu.SemaphoreType.DMA((11,))],
        compiler_params=pltpu.CompilerParams(vmem_limit_bytes=8 << 20),
        name="finish",
    )(*held)


PAIR = 2


def unit_inverses(lowers, rows, cols):
    count = lowers[0].shape[0]
    near = (rows // 2 == cols // 2) & (rows > cols)
    inverses = [jnp.where(rows == cols, 1.0, jnp.where(near, -lower, 0.0)) for lower in lowers]
    block = 2
    while block < count:
        cross = (rows // (2 * block) == cols // (2 * block)) & (rows // block > cols // block)
        steps = [mm(inverse, jnp.where(cross, lower, 0.0)) for inverse, lower in zip(inverses, lowers)]
        inverses = [inverse - mm(step, inverse) for inverse, step in zip(inverses, steps)]
        block *= 2
    return inverses


def head_body(
    heads, key_dim, value_dim, begin, early, halfway,
    pre_ref, gate_ref, small_ref, taps_ref, rate_ref, gain_ref, w_out_ref, resid_ref, norm2_ref,
    w_gate_hbm, w_up_hbm, w_down_hbm,
    mixed_ref, core_ref, update_ref, state_ref, inverse_ref, resid1_ref, upstream_ref, hidden_ref, units_ref, part2_ref, ffn_ref,
    pad, now, solved_key, rise_query, key_tail, attend_all, ends,
    part, land_mate, land_across, half, sum_send, sum_recv,
    arrived, w_gate, w_up, w_down, gate_pre, up_pre, inner_grad, load_sem,
):
    length, width = pre_ref.shape
    span = SPAN
    chunks = length // span
    rows, cols = grids(span)
    qk = heads * key_dim
    n, _, me, t, _, _ = grid_place()
    _, mate, across = tensor_peers()
    loads = [(w_gate_hbm, w_gate), (w_up_hbm, w_up), (w_down_hbm, w_down)]
    loads = [pltpu.make_async_copy(src, dst, load_sem.at[i]) for i, (src, dst) in enumerate(loads)]
    for load in loads:
        load.start()
    total = TensorSum(part, resid1_ref, land_mate, land_across, half, sum_send, sum_recv)
    swap = begin
    pad[0:HALO] = jnp.zeros((HALO, width), jnp.float32)
    now[...] = jnp.zeros_like(now)

    def prepare_pair(turn):
        items = []
        for k in range(PAIR):
            index = turn * PAIR + k
            here = aligned(index * span, span)
            pad[HALO : HALO + span] = pre_ref[here, :]
            total_pre = conv_window(pad[...], taps_ref[...], span)
            pad[0:HALO] = pad[span : span + HALO]
            active = total_pre * sigmoid(total_pre)
            beta, _, _, cumul = gates_of(small_ref[here, :], rate_ref[...], heads, rows, cols)
            beta_t = jnp.transpose(beta)
            cumul_t = jnp.transpose(cumul)
            for head in range(heads):
                query = active[:, head * key_dim : (head + 1) * key_dim]
                query = query * (lax.rsqrt(jnp.sum(query * query, -1, keepdims=True) + EPS) * key_dim ** (-0.5))
                key = active[:, qk + head * key_dim : qk + (head + 1) * key_dim]
                key = key * lax.rsqrt(jnp.sum(key * key, -1, keepdims=True) + EPS)
                value = active[:, 2 * qk + head * value_dim : 2 * qk + (head + 1) * value_dim]
                beta_col = beta[:, head : head + 1]
                cum_col = cumul[:, heads + head : heads + head + 1]
                cum_row = cumul_t[heads + head : heads + head + 1]
                within = cols <= rows
                decays = jnp.where(within, jnp.exp(jnp.where(within, cum_col - cum_row, 0.0)), 0.0)
                scaled = decays * beta_t[head : head + 1]
                products = mm_nt(jnp.concatenate([query, key], 0), key)
                lower = jnp.where(cols < rows, scaled * products[span:], 0.0)
                attend = scaled * products[:span]
                last = cum_col[span - 1 : span]
                rise = jnp.exp(cum_col)
                narrow = slice(head * key_dim, (head + 1) * key_dim)
                attend_all[index, head] = attend
                rise_query[here, narrow] = rise * query
                key_tail[here, narrow] = key * (jnp.exp(last - cum_col) * beta_col)
                ends[index, head] = jnp.broadcast_to(jnp.exp(last), (8, 128))
                items.append((index, head, here, lower, jnp.concatenate([value, rise * key], 1)))
        inverses = unit_inverses([item[3] for item in items], rows, cols)
        solved = [mm(inverse, item[4]) for inverse, item in zip(inverses, items)]
        for (index, head, here, _, _), inverse, solution_ in zip(items, inverses, solved):
            inverse_ref[index, head] = inverse
            update_ref[here, head * value_dim : (head + 1) * value_dim] = solution_[:, :value_dim]
            solved_key[here, head * key_dim : (head + 1) * key_dim] = solution_[:, value_dim:]

    def chain(index):
        here = aligned(index * span, span)
        gate = gate_ref[here, :]
        gated = gate * sigmoid(gate) * gain_ref[...]
        for head in range(heads):
            narrow = slice(head * key_dim, (head + 1) * key_dim)
            wide = slice(head * value_dim, (head + 1) * value_dim)
            state = now[head]
            state_ref[state_place(index, head, heads, key_dim, value_dim, width)] = state
            both = mm(jnp.concatenate([solved_key[here, narrow], rise_query[here, narrow]], 0), state)
            update = update_ref[here, wide] - both[:span]
            now[head] = ends[index, head][0:1, 0:1] * state + mm_tn(key_tail[here, narrow], update)
            core = both[span:] + mm(attend_all[index, head], update)
            update_ref[here, wide] = update
            core_ref[here, wide] = core
            normed = core * lax.rsqrt(jnp.mean(core * core, -1, keepdims=True) + EPS)
            mixed_ref[here, wide] = (normed * gated[:, wide]).astype(mixed_ref.dtype)

    def chain_pair(turn):
        for k in range(PAIR):
            chain(turn * PAIR + k)

    def send_pair(turn):
        here = aligned(turn * PAIR * span, PAIR * span)
        part[here] = dot_plain(mixed_ref[here], w_out_ref[...])
        for k in range(PAIR):
            total.first(turn * PAIR + k).start()

    def cross_pair(turn):
        for k in range(PAIR):
            total.cross(turn * PAIR + k)

    def share_pair(turn):
        for k in range(PAIR):
            total.share(turn * PAIR + k, resid_ref)

    pairs = chunks // PAIR
    prepare_pair(0)

    def step(turn, carry):
        chain_pair(turn - 1)
        prepare_pair(turn)
        send_pair(turn - 1)

        cross_pair(turn - 1)

        @pl.when(turn > 1)
        def _():
            share_pair(turn - 2)

        return carry

    lax.fori_loop(1, pairs, step, 0)
    chain_pair(pairs - 1)
    send_pair(pairs - 1)
    cross_pair(pairs - 1)
    share_pair(pairs - 2)

    def gather(k, carry):
        swap.gather(k)
        return carry

    lax.fori_loop(0, n, gather, 0)

    swap.sent()
    swap.finish()

    def turn_low(i, carry):
        here = aligned(i * 64, 64)
        upstream_ref[here] = arrived[here].astype(upstream_ref.dtype)
        return carry

    lax.fori_loop(0, length // 64, turn_low, 0)
    for load in loads:
        load.wait()
    units = w_gate.shape[0]
    whole = units // 128 * 128
    low = units_ref.dtype
    units_ref[:, :, whole:] = jnp.zeros((3, length, units_ref.shape[2] - whole), low)
    some = length // 2

    def feed(first):
        def norm(i, carry):
            here = aligned(first + i * 64, 64)
            value = resid1_ref[here]
            scale = lax.rsqrt(jnp.mean(value * value, -1, keepdims=True) + EPS)
            hidden_ref[here] = (value * scale * norm2_ref[...]).astype(low)
            return carry

        lax.fori_loop(0, some // 64, norm, 0)
        block = pl.ds(first, some)
        gate_pre[...] = dot_nt(hidden_ref[block], w_gate[...])
        up_pre[...] = dot_nt(hidden_ref[block], w_up[...])
        inner_grad[...] = dot_nt(upstream_ref[block], w_down[...])

        def bend(i, carry):
            at = aligned(i * 64, 64)
            here = aligned(first + i * 64, 64)
            gate = gate_pre[at]
            upper = up_pre[at]
            grad = inner_grad[at]
            sig = sigmoid(gate)
            silu = gate * sig
            units_ref[0, here, 0:units] = (silu * upper).astype(low)
            units_ref[1, here, 0:units] = (grad * upper * (sig * (1.0 + gate * (1.0 - sig)))).astype(low)
            units_ref[2, here, 0:units] = (grad * silu).astype(low)
            return carry

        lax.fori_loop(0, some // 64, bend, 0)
        part2_ref[block] = dot_plain(units_ref[1, block, 0:units], w_gate[...]) + dot_plain(
            units_ref[2, block, 0:units], w_up[...]
        )
        ffn_ref[block] = dot_plain(units_ref[0, block, 0:units], w_down[...])

    early()
    for block in range(BLOCKS // 2):
        total.third(block).wait_recv()
    feed(0)
    halfway()
    share_pair(pairs - 1)
    total.finish(BLOCKS // 2)
    feed(some)


def front_kernel(
    heads, key_dim, value_dim,
    x_ref, norm1_ref, beta_ref, decay_ref, rate_ref, taps_q, taps_k, taps_v, gain_ref, cotangent_ref, norm2_ref,
    query_hbm, key_hbm, value_hbm, gate_hbm, w_out_hbm, w_gate_hbm, w_up_hbm, w_down_hbm,
    low_out, hidden1_out, pre_out, gate_out, small_out, w_small_out,
    mixed_out, core_out, update_out, state_out, inverse_out, upstream_out, resid1_out,
    hidden2_out, units_out, part2_out, ffn_out, taps_ref, rate_row_ref,
    low, hidden1, pre, gate_pre, small, w_small, mixed, core, update, state, inverse, upstream, resid1,
    hidden2, units, part2, ffn, w_out,
    w_mix, w_gate_mix, rows16, staged, arrived, send, recv, close_send, close_recv, load_sem,
    pad, now, solved_key, rise_query, key_tail, attend_all, ends,
    part, land_mate, land_across, half, sum_send, sum_recv,
    staged2, arrived2, send2, recv2, close_send2, close_recv2,
    w_gate, w_up, w_down, gate_in, up_in, inner_grad, load_sem2, out_sem,
):
    load_w_out = pltpu.make_async_copy(w_out_hbm, w_out, out_sem.at[0])
    load_w_out.start()
    cotangents = PlaneSwap(staged2, arrived2, send2, recv2, close_send2, close_recv2)

    def between():
        for place in range(cotangents.n):
            mine = cotangents.at(place, cotangents.core)
            staged2[mine] = cotangent_ref[mine].astype(jnp.float32)
        cotangents.start()

    prep_part(
        heads, between, x_ref, norm1_ref, query_hbm, key_hbm, value_hbm, gate_hbm, beta_ref, decay_ref, rate_ref,
        taps_q, taps_k, taps_v, low, hidden1, pre, gate_pre, small, w_small, taps_ref, rate_row_ref,
        w_mix, w_gate_mix, rows16, staged, arrived, send, recv, close_send, close_recv, load_sem,
    )
    pairs = [
        (low, low_out), (hidden1, hidden1_out), (pre, pre_out), (gate_pre, gate_out), (small, small_out),
        (w_small, w_small_out),
    ]
    later = [
        (mixed, mixed_out), (core, core_out), (update, update_out), (state, state_out), (inverse, inverse_out),
        (upstream, upstream_out),
    ]
    rows = hidden2.shape[0]
    halves = [pl.ds(0, rows // 2), pl.ds(rows // 2, rows // 2)]
    last = [
        [
            (hidden2.at[span], hidden2_out.at[span]), (part2.at[span], part2_out.at[span]), (ffn.at[span], ffn_out.at[span]),
            (resid1.at[span], resid1_out.at[span]),
        ]
        + [(units.at[k, span], units_out.at[k, span]) for k in range(3)]
        for span in halves
    ]
    every = pairs + later + last[0] + last[1]
    copies = [pltpu.make_async_copy(src, dst, out_sem.at[1 + i]) for i, (src, dst) in enumerate(every)]
    one, two, three = len(pairs), len(pairs) + len(later), len(pairs) + len(later) + len(last[0])

    def begin_copies(start, stop):
        for copy in copies[start:stop]:
            copy.start()

    begin_copies(0, one)
    load_w_out.wait()
    head_body(
        heads, key_dim, value_dim, cotangents, lambda: begin_copies(one, two), lambda: begin_copies(two, three),
        pre, gate_pre, small, taps_ref, rate_row_ref, gain_ref, w_out, low, norm2_ref, w_gate_hbm, w_up_hbm, w_down_hbm,
        mixed, core, update, state, inverse, resid1, upstream, hidden2, units, part2, ffn,
        pad, now, solved_key, rise_query, key_tail, attend_all, ends,
        part, land_mate, land_across, half, sum_send, sum_recv,
        arrived2, w_gate, w_up, w_down, gate_in, up_in, inner_grad, load_sem2,
    )
    begin_copies(three, len(copies))
    for copy in copies:
        copy.wait()


def front(
    x, cotangent, norm1, norm2, w_query, w_key, w_value, w_gate, w_beta_t, w_decay_t, rate, taps_q, taps_k, taps_v, gain,
    w_out, w_gate_t, w_up_t, w_down, heads, key_dim, value_dim, places, collective_id,
):
    length, width = x.shape
    values = heads * value_dim
    qk = heads * key_dim
    lanes = 128
    chunks = length // SPAN
    units = w_down.shape[0]
    padded = -(-units // 128) * 128
    f32, bf = jnp.float32, jnp.bfloat16
    dma = pltpu.SemaphoreType.DMA
    any_ = pl.BlockSpec(memory_space=pl.ANY)
    shapes = [
        ((length, width), bf),
        ((length, width), bf),
        ((length, width), f32),
        ((length, values), f32),
        ((length, lanes), f32),
        ((lanes, width), bf),
        ((length, values), bf),
        ((length, values), f32),
        ((length, values), f32),
        ((chunks * heads * key_dim * value_dim // width, width), f32),
        ((chunks, heads, SPAN, SPAN), f32),
        ((length, width), bf),
        ((length, width), f32),
        ((length, width), bf),
        ((3, length, padded), bf),
        ((length, width), f32),
        ((length, width), f32),
    ]
    smalls = [((taps_q.shape[0], width), f32), ((1, lanes), f32)]
    vmem = [
        (w_out.shape, bf),
        ((width, width), bf),
        ((width, values), bf),
        ((16, width), f32),
        ((length, width), f32),
        ((length, width), f32),
    ]
    swap_sems = [dma((places,)), dma((places,)), dma((3, places)), dma((3, places))]
    more = [
        ((HALO + SPAN, width), f32),
        ((heads, key_dim, value_dim), f32),
        ((length, qk), f32),
        ((length, qk), f32),
        ((length, qk), f32),
        ((chunks, heads, SPAN, SPAN), f32),
        ((chunks, heads, 8, 128), f32),
        ((length, width), f32),
        ((length // 2, width), f32),
        ((length // 2, width), f32),
        ((length // 2, width), f32),
    ]
    last = [((units, width), bf)] * 3 + [((length // 2, units), f32)] * 3

    def scratch(items):
        return [pltpu.VMEM(shape, kind) for shape, kind in items]

    return pl.pallas_call(
        functools.partial(front_kernel, heads, key_dim, value_dim),
        out_shape=[jax.ShapeDtypeStruct(shape, kind) for shape, kind in shapes + smalls],
        in_specs=[VM] * 11 + [any_] * 8,
        out_specs=[any_] * len(shapes) + [VM] * len(smalls),
        scratch_shapes=scratch(shapes) + scratch(vmem) + swap_sems + [dma((4,))] + scratch(more)
        + [dma((3, BLOCKS)), dma((3, BLOCKS))] + scratch([((length, width), f32)] * 2) + swap_sems + scratch(last)
        + [dma((3,)), dma((32,))],
        compiler_params=pltpu.CompilerParams(
            collective_id=collective_id, has_side_effects=True, vmem_limit_bytes=67043328
        ),
        name="front",
    )(
        x, norm1, w_beta_t, w_decay_t, rate, taps_q, taps_k, taps_v, gain, cotangent, norm2,
        w_query, w_key, w_value, w_gate, w_out, w_gate_t, w_up_t, w_down,
    )


def prep_part(
    heads, between,
    x_ref, norm1_ref, query_hbm, key_hbm, value_hbm, gate_hbm, beta_ref, decay_ref, rate_ref, taps_q, taps_k, taps_v,
    low_ref, hidden_ref, pre_ref, gate_pre_ref, small_ref, w_small_ref, taps_ref, rate_row_ref,
    w_mix, w_gate, rows16, staged, arrived, send, recv, close_send, close_recv, load_sem,
):
    length, width = x_ref.shape
    qk = query_hbm.shape[1]
    values = value_hbm.shape[1]
    n, _, me, t, _, _ = grid_place()
    _, mate, across = tensor_peers()
    peers = [(lax.rem(me + k, n), t) for k in range(1, n)] + [mate, across]
    call_out(peers)
    loads = [
        (query_hbm, w_mix.at[:, pl.ds(0, qk)]),
        (key_hbm, w_mix.at[:, pl.ds(qk, qk)]),
        (value_hbm, w_mix.at[:, pl.ds(2 * qk, values)]),
        (gate_hbm, w_gate),
    ]
    loads = [pltpu.make_async_copy(src, dst, load_sem.at[i]) for i, (src, dst) in enumerate(loads)]
    for load in loads:
        load.start()
    swap = Swap(staged, arrived, send, recv, close_send, close_recv)
    for place in range(n):
        mine = swap.at(place, t)
        staged[mine] = x_ref[mine].astype(jnp.float32)
    hear_all(peers)
    swap.start()
    taps_ref[:, 0:qk] = taps_q[...]
    taps_ref[:, qk : 2 * qk] = taps_k[...]
    taps_ref[:, 2 * qk :] = taps_v[...]
    lanes = rate_row_ref.shape[1]
    lane = lax.broadcasted_iota(jnp.int32, (1, lanes), 1)
    row = jnp.zeros((1, lanes), jnp.float32)
    for head in range(heads):
        row = jnp.where(lane == heads + head, rate_ref[:, head : head + 1], row)
    rate_row_ref[...] = row
    rows16[...] = jnp.zeros_like(rows16)
    rows16[0:heads] = beta_ref[...].astype(jnp.float32)
    rows16[heads : 2 * heads] = decay_ref[...].astype(jnp.float32)
    w_small_ref[...] = jnp.zeros_like(w_small_ref)
    w_small_ref[0:16] = rows16[...].astype(w_small_ref.dtype)

    def gather(k, carry):
        swap.gather(k)
        return carry

    def forward(k, carry):
        swap.forward(k)
        return carry

    lax.fori_loop(0, n, gather, 0)
    between()
    lax.fori_loop(0, n, forward, 0)
    for load in loads:
        load.wait()
    swap.sent()
    swap.finish()

    def norm(i, carry):
        here = aligned(i * 64, 64)
        value = arrived[here]
        low_ref[here] = value.astype(low_ref.dtype)
        scale = lax.rsqrt(jnp.mean(value * value, -1, keepdims=True) + EPS)
        hidden_ref[here] = (value * scale * norm1_ref[...]).astype(hidden_ref.dtype)
        return carry

    lax.fori_loop(0, length // 64, norm, 0)

    def mix_tile(i, carry):
        tile = aligned(i * 256, 256)
        pre_ref[:, tile] = dot_plain(hidden_ref[...], w_mix[:, tile])
        return carry

    def gate_tile(i, carry):
        tile = aligned(i * 256, 256)
        gate_pre_ref[:, tile] = dot_plain(hidden_ref[...], w_gate[:, tile])
        return carry

    lax.fori_loop(0, width // 256, mix_tile, 0)
    lax.fori_loop(0, values // 256, gate_tile, 0)
    small_ref[...] = dot_nt(hidden_ref[...], w_small_ref[...])


def whole_sequences(
    inputs,
    norm1_gain,
    w_query,
    w_key,
    w_value,
    w_gate,
    w_beta,
    w_decay,
    decay_rate,
    conv_query,
    conv_key,
    conv_value,
    head_gain,
    w_out,
    norm2_gain,
    w_ffn_gate,
    w_ffn_up,
    w_ffn_down,
    cotangent,
):
    batch, seg, width = inputs.shape
    count = batch * seg
    heads = decay_rate.shape[0]
    key_dim = w_query.shape[1] // heads
    value_dim = w_value.shape[1] // heads
    qk_width = heads * key_dim
    places = lax.axis_size("dp")
    gain = head_gain[None]
    (
        resid, hidden1, pre, gate_pre, small, w_small, mixed, core, update, states, inverses, upstream, resid1,
        hidden2, units, part2, ffn, taps, rate,
    ) = front(
        inputs.reshape(count, width), cotangent.reshape(count, width), norm1_gain[None], norm2_gain[None],
        w_query, w_key, w_value, w_gate, w_beta.T, w_decay.T, decay_rate[None], conv_query, conv_key, conv_value, gain,
        w_out, w_ffn_gate.T, w_ffn_up.T, w_ffn_down, heads, key_dim, value_dim, places, 2,
    )
    held, ranges = tail(
        part2, ffn, pre, core, update, states, resid1, upstream, resid, mixed, hidden1, hidden2, units,
        w_out, w_query, w_key, w_value, w_gate, w_small, gate_pre, small, inverses,
        norm1_gain[None], norm2_gain[None], taps, rate, gain,
        heads, key_dim, value_dim, w_ffn_down.shape[0], places, 7,
    )
    (
        output, grad_inputs, fgate, fup, grad_down, grad_out_w, grad_gate_w, grad_query_w, grad_key_w, grad_value_w,
        grad_norm1_gain, grad_norm2_gain, grad_head, grad_rate, grad_beta_w, grad_decay_w,
        grad_convq, grad_convk, grad_convv,
    ) = finish(*held, ranges, w_ffn_down.shape[0], heads, qk_width, heads * value_dim)
    return (
        output.reshape(batch, seg, width),
        grad_inputs.reshape(batch, seg, width),
        grad_norm1_gain[0],
        grad_query_w,
        grad_key_w,
        grad_value_w,
        grad_gate_w,
        grad_beta_w.T,
        grad_decay_w.T,
        grad_rate[0],
        grad_convq,
        grad_convk,
        grad_convv,
        grad_head[0],
        grad_out_w,
        grad_norm2_gain[0],
        fgate.T,
        fup.T,
        grad_down,
    )


def fits_whole(mesh, args):
    batch, length, width = args[0].shape
    places, ranks = mesh.shape["dp"], mesh.shape["tensor"]
    heads = args[8].shape[0] // ranks
    qk = args[2].shape[1] // ranks
    values = args[4].shape[1] // ranks
    units = args[15].shape[1] // ranks
    return (
        batch == places and places == 8 and ranks == 4 and length == places * SPAN and BLOCKS == places and heads <= 4
        and width == 2 * qk + values and width == 2 * values and width % 512 == 0 and length % 256 == 0
        and units % 64 == 0 and values % 256 == 0
        and length // SPAN * args[2].shape[1] // ranks * (values // heads) <= values * width
    )


def solution(mesh):
    placed = (
        P(None, "dp", None),
        P(),
        P(None, "tensor"),
        P(None, "tensor"),
        P(None, "tensor"),
        P(None, "tensor"),
        P(None, "tensor"),
        P(None, "tensor"),
        P("tensor"),
        P(None, "tensor"),
        P(None, "tensor"),
        P(None, "tensor"),
        P("tensor"),
        P("tensor", None),
        P(),
        P(None, "tensor"),
        P(None, "tensor"),
        P("tensor", None),
        P(None, "dp", None),
    )
    def step(*args):
        body = whole_sequences if fits_whole(mesh, args) else shards
        return placed_step(body)(*args)

    def placed_step(body):
      return jax.shard_map(
        body,
        mesh=mesh,
        in_specs=placed,
        out_specs=(
            P(None, "dp", None),
            P(None, "dp", None),
            P(),
            P(None, "tensor"),
            P(None, "tensor"),
            P(None, "tensor"),
            P(None, "tensor"),
            P(None, "tensor"),
            P(None, "tensor"),
            P("tensor"),
            P(None, "tensor"),
            P(None, "tensor"),
            P(None, "tensor"),
            P("tensor"),
            P("tensor", None),
            P(),
            P(None, "tensor"),
            P(None, "tensor"),
            P("tensor", None),
        ),
        check_vma=False,
    )

    return step
```

```python
import functools
from functools import partial

import jax
import jax.numpy as jnp
from jax import lax
from jax.experimental import pallas as pl
from jax.experimental.pallas import tpu as pltpu
from jax.sharding import PartitionSpec as P

SPAN = 64


EPS = 1e-06


def from_behind(shard, axis, by):
    count = lax.axis_size(axis)
    pairs = [(i, i + by) for i in range(count) if 0 <= i + by < count]
    return lax.ppermute(shard, axis, pairs)


def carried_in(part, axis, combine, identity, reverse):
    count = lax.axis_size(axis)
    place = lax.axis_index(axis)
    ahead = count - 1 - place if reverse else place
    gathered = jax.tree.map(lambda a: lax.all_gather(a, axis), part)
    state = jax.tree.map(lambda a, e: jnp.zeros_like(a) + jnp.asarray(e, a.dtype), part, identity)

    def one(turn, state):
        source = count - 1 - turn if reverse else turn
        return combine(
            state, jax.tree.map(lambda a: lax.dynamic_index_in_dim(a, source, 0, False), gathered)
        )

    return lax.fori_loop(0, ahead, one, state)


def exact(left, right):
    return jnp.matmul(left, right, precision=lax.Precision.HIGHEST)


def span_apply(state, inputs):
    query, key, values, beta, logdecay = inputs
    count = query.shape[0]
    cumul = jnp.cumsum(logdecay)
    row_ids = lax.broadcasted_iota(jnp.int32, (count, count), 0)
    col_ids = lax.broadcasted_iota(jnp.int32, (count, count), 1)
    within = col_ids <= row_ids
    strict = col_ids < row_ids
    spread = jnp.where(within, cumul[:, None] - cumul[None, :], 0.0)
    decays = jnp.where(within, jnp.exp(spread), 0.0)
    scaled = decays * beta[None, :]
    lower = jnp.where(strict, scaled * exact(key, key.T), 0.0)
    start_decay = jnp.exp(cumul)[:, None]
    right_side = values - start_decay * exact(key, state)
    system = jnp.eye(count, dtype=lower.dtype) + lower
    update = jax.scipy.linalg.solve_triangular(system, right_side, lower=True, unit_diagonal=True)
    output = start_decay * exact(query, state) + exact(scaled * exact(query, key.T), update)
    tail = jnp.exp(cumul[-1] - cumul) * beta
    new_state = jnp.exp(cumul[-1]) * state + exact((key * tail[:, None]).T, update)
    return (new_state, output)


def run_segment(query, key, values, beta, logdecay, state):
    length = query.shape[0]
    blocks = length // SPAN

    def split(array):
        return array.reshape((blocks, SPAN) + array.shape[1:])

    final, outputs = lax.scan(
        span_apply, state, (split(query), split(key), split(values), split(beta), split(logdecay))
    )
    return (outputs.reshape((length,) + outputs.shape[2:]), final)


def run_heads(query, key, values, beta, logdecay, state):
    return jax.vmap(jax.vmap(run_segment))(query, key, values, beta, logdecay, state)


def prepare(extended, beta_pre, decay_pre, conv_all, decay_rate, key_dim):
    batch, seg, heads = beta_pre.shape
    reach = conv_all.shape[0] - 1
    total = conv_all[0] * extended[:, 0:seg, :]
    for offset in range(1, reach + 1):
        total = total + conv_all[offset] * extended[:, offset : offset + seg, :]
    active = jax.nn.silu(total)
    qk_width = heads * key_dim
    query = active[..., :qk_width].reshape(batch, seg, heads, key_dim)
    key = active[..., qk_width : 2 * qk_width].reshape(batch, seg, heads, key_dim)
    values = active[..., 2 * qk_width :].reshape(batch, seg, heads, -1)
    query = query * lax.rsqrt(jnp.sum(query * query, -1, keepdims=True) + EPS) * key_dim ** (-0.5)
    key = key * lax.rsqrt(jnp.sum(key * key, -1, keepdims=True) + EPS)
    beta = jax.nn.sigmoid(beta_pre)
    logdecay = -decay_rate * jax.nn.softplus(decay_pre)
    return (
        jnp.moveaxis(query, 2, 1),
        jnp.moveaxis(key, 2, 1),
        jnp.moveaxis(values, 2, 1),
        jnp.moveaxis(beta, 2, 1),
        jnp.moveaxis(logdecay, 2, 1),
    )


def gate_norm(core, gate_pre, head_gain):
    normed = core * lax.rsqrt(jnp.mean(core * core, -1, keepdims=True) + EPS)
    return normed * head_gain * jax.nn.silu(gate_pre)


def rms_apply(resid, gain):
    return resid * lax.rsqrt(jnp.mean(resid * resid, -1, keepdims=True) + EPS) * gain


def swiglu(gate, upper):
    return jax.nn.silu(gate) * upper


def project(left, right):
    return jnp.dot(left, right, preferred_element_type=jnp.float32)


def contract_rows(left, right):
    return jnp.einsum("ra,rb->ab", left, right, preferred_element_type=jnp.float32)


def back_project(grad, weight):
    return jnp.einsum("rb,ab->ra", grad, weight, preferred_element_type=jnp.float32)


def compose(earlier, later):
    return (exact(later[0], earlier[0]), exact(later[0], earlier[1]) + later[1])


def shards(
    inputs,
    norm1_gain,
    w_query,
    w_key,
    w_value,
    w_gate,
    w_beta,
    w_decay,
    decay_rate,
    conv_query,
    conv_key,
    conv_value,
    head_gain,
    w_out,
    norm2_gain,
    w_ffn_gate,
    w_ffn_up,
    w_ffn_down,
    cotangent,
):
    batch, seg, width = inputs.shape
    count = batch * seg
    heads = decay_rate.shape[0]
    key_dim = w_query.shape[1] // heads
    value_dim = w_value.shape[1] // heads
    qk_width = heads * key_dim
    reach = conv_query.shape[0] - 1
    bf = jnp.bfloat16
    resid = inputs.reshape(count, width).astype(jnp.float32)
    normed1, norm1_back = jax.vjp(rms_apply, resid, norm1_gain)
    hidden1 = normed1.astype(bf)
    query_pre = project(hidden1, w_query)
    key_pre = project(hidden1, w_key)
    value_pre = project(hidden1, w_value)
    gate_pre = project(hidden1, w_gate)
    beta_pre = project(hidden1, w_beta)
    decay_pre = project(hidden1, w_decay)
    mixed_pre = jnp.concatenate([query_pre, key_pre, value_pre], axis=1).reshape(batch, seg, -1)
    rim = from_behind(mixed_pre[:, seg - reach :, :], "dp", 1)
    extended = jnp.concatenate([rim, mixed_pre], axis=1)
    conv_all = jnp.concatenate([conv_query, conv_key, conv_value], axis=1)
    features, prep_back = jax.vjp(
        partial(prepare, key_dim=key_dim),
        extended,
        beta_pre.reshape(batch, seg, heads),
        decay_pre.reshape(batch, seg, heads),
        conv_all,
        decay_rate,
    )
    query_h, key_h, value_h, beta_h, decay_h = features
    eye_block = jnp.broadcast_to(
        jnp.eye(key_dim, dtype=jnp.float32), (batch, heads, key_dim, key_dim)
    )
    zero_block = jnp.zeros((batch, heads, key_dim, value_dim), jnp.float32)
    values_aug = jnp.concatenate(
        [jnp.zeros(value_h.shape[:3] + (key_dim,), jnp.float32), value_h], axis=-1
    )
    state_aug = jnp.concatenate([eye_block, zero_block], axis=-1)
    outputs_aug, final_aug = run_heads(query_h, key_h, values_aug, beta_h, decay_h, state_aug)
    out_carry = outputs_aug[..., :key_dim]
    out_local = outputs_aug[..., key_dim:]
    transition = final_aug[..., :key_dim]
    offset_part = final_aug[..., key_dim:]
    prefix = carried_in((transition, offset_part), "dp", compose, (eye_block, zero_block), False)
    start_state = prefix[1]
    core = jnp.moveaxis(exact(out_carry, start_state) + out_local, 1, 2)
    gate4 = gate_pre.reshape(batch, seg, heads, value_dim)
    gated, gate_back = jax.vjp(gate_norm, core, gate4, head_gain.reshape(heads, value_dim))
    mixed = gated.reshape(count, heads * value_dim).astype(bf)
    attention = lax.psum(project(mixed, w_out), "tensor")
    resid1 = resid + attention
    normed2, norm2_back = jax.vjp(rms_apply, resid1, norm2_gain)
    hidden2 = normed2.astype(bf)
    ffn_gate = project(hidden2, w_ffn_gate)
    ffn_up = project(hidden2, w_ffn_up)
    inner_full, swiglu_back = jax.vjp(swiglu, ffn_gate, ffn_up)
    inner = inner_full.astype(bf)
    ffn = lax.psum(project(inner, w_ffn_down), "tensor")
    output = (resid1 + ffn).astype(bf).reshape(batch, seg, width)
    upstream = cotangent.reshape(count, width)
    grad_down = contract_rows(inner, upstream)
    grad_inner = back_project(upstream, w_ffn_down)
    grad_fgate, grad_fup = swiglu_back(grad_inner)
    grad_fgate = grad_fgate.astype(bf)
    grad_fup = grad_fup.astype(bf)
    grad_ffn_gate_w = contract_rows(hidden2, grad_fgate)
    grad_ffn_up_w = contract_rows(hidden2, grad_fup)
    grad_hidden2 = lax.psum(
        back_project(grad_fgate, w_ffn_gate) + back_project(grad_fup, w_ffn_up), "tensor"
    )
    grad_from_norm2, grad_norm2_gain = norm2_back(grad_hidden2)
    grad_resid1 = upstream.astype(jnp.float32) + grad_from_norm2
    grad_resid1_low = grad_resid1.astype(bf)
    grad_out_w = contract_rows(mixed, grad_resid1_low)
    grad_mixed = back_project(grad_resid1_low, w_out).reshape(batch, seg, heads, value_dim)
    grad_core, grad_gate4, grad_head_gain = gate_back(grad_mixed)
    grad_core_h = jnp.moveaxis(grad_core, 2, 1)
    carry_term = exact(jnp.swapaxes(out_carry, -1, -2), grad_core_h)
    suffix = carried_in(
        (jnp.swapaxes(transition, -1, -2), carry_term), "dp", compose, (eye_block, zero_block), True
    )

    def local_delta(query, key, values, beta, logdecay):
        return run_heads(query, key, values, beta, logdecay, start_state)

    recomputed, delta_back = jax.vjp(local_delta, query_h, key_h, value_h, beta_h, decay_h)
    feature_grads = delta_back((grad_core_h, suffix[1]))
    grad_ext, grad_beta_in, grad_decay_in, grad_conv, grad_rate = prep_back(feature_grads)
    returned = from_behind(grad_ext[:, :reach, :], "dp", -1)
    grad_mixed_pre = grad_ext[:, reach:, :] + jnp.pad(returned, ((0, 0), (seg - reach, 0), (0, 0)))
    grad_mixed_pre = grad_mixed_pre.reshape(count, -1)
    grad_query_low = grad_mixed_pre[:, :qk_width].astype(bf)
    grad_key_low = grad_mixed_pre[:, qk_width : 2 * qk_width].astype(bf)
    grad_value_low = grad_mixed_pre[:, 2 * qk_width :].astype(bf)
    grad_gate_low = grad_gate4.reshape(count, heads * value_dim).astype(bf)
    grad_beta_low = grad_beta_in.reshape(count, heads).astype(bf)
    grad_decay_low = grad_decay_in.reshape(count, heads).astype(bf)
    partial_hidden1 = (
        back_project(grad_query_low, w_query)
        + back_project(grad_key_low, w_key)
        + back_project(grad_value_low, w_value)
        + back_project(grad_gate_low, w_gate)
        + back_project(grad_beta_low, w_beta)
        + back_project(grad_decay_low, w_decay)
    )
    grad_hidden1 = lax.psum(partial_hidden1, "tensor")
    grad_from_norm1, grad_norm1_gain = norm1_back(grad_hidden1)
    grad_inputs = (grad_resid1 + grad_from_norm1).reshape(batch, seg, width)
    grad_query_w = contract_rows(hidden1, grad_query_low)
    grad_key_w = contract_rows(hidden1, grad_key_low)
    grad_value_w = contract_rows(hidden1, grad_value_low)
    grad_gate_w = contract_rows(hidden1, grad_gate_low)
    grad_beta_w = contract_rows(hidden1, grad_beta_low)
    grad_decay_w = contract_rows(hidden1, grad_decay_low)
    grad_convq = grad_conv[:, :qk_width]
    grad_convk = grad_conv[:, qk_width : 2 * qk_width]
    grad_convv = grad_conv[:, 2 * qk_width :]
    grad_head_flat = grad_head_gain.reshape(-1)
    (
        grad_norm1_gain,
        grad_query_w,
        grad_key_w,
        grad_value_w,
        grad_gate_w,
        grad_beta_w,
        grad_decay_w,
        grad_rate,
        grad_convq,
        grad_convk,
        grad_convv,
        grad_head_flat,
        grad_out_w,
        grad_norm2_gain,
        grad_ffn_gate_w,
        grad_ffn_up_w,
        grad_down,
    ) = lax.psum(
        (
            grad_norm1_gain,
            grad_query_w,
            grad_key_w,
            grad_value_w,
            grad_gate_w,
            grad_beta_w,
            grad_decay_w,
            grad_rate,
            grad_convq,
            grad_convk,
            grad_convv,
            grad_head_flat,
            grad_out_w,
            grad_norm2_gain,
            grad_ffn_gate_w,
            grad_ffn_up_w,
            grad_down,
        ),
        "dp",
    )
    return (
        output,
        grad_inputs,
        grad_norm1_gain,
        grad_query_w,
        grad_key_w,
        grad_value_w,
        grad_gate_w,
        grad_beta_w,
        grad_decay_w,
        grad_rate,
        grad_convq,
        grad_convk,
        grad_convv,
        grad_head_flat,
        grad_out_w,
        grad_norm2_gain,
        grad_ffn_gate_w,
        grad_ffn_up_w,
        grad_down,
    )


HALO = 8


def mm(left, right):
    return lax.dot_general(
        left, right, (((1,), (0,)), ((), ())),
        precision=lax.Precision.HIGHEST, preferred_element_type=jnp.float32,
    )


def mm_nt(left, right):
    return lax.dot_general(
        left, right, (((1,), (1,)), ((), ())),
        precision=lax.Precision.HIGHEST, preferred_element_type=jnp.float32,
    )


def mm_tn(left, right):
    return lax.dot_general(
        left, right, (((0,), (0,)), ((), ())),
        precision=lax.Precision.HIGHEST, preferred_element_type=jnp.float32,
    )


def grids(count):
    rows = lax.broadcasted_iota(jnp.int32, (count, count), 0)
    cols = lax.broadcasted_iota(jnp.int32, (count, count), 1)
    return rows, cols


def unit_inverse(lower, rows, cols):
    count = lower.shape[0]
    near = (rows // 2 == cols // 2) & (rows > cols)
    inverse = jnp.where(rows == cols, 1.0, jnp.where(near, -lower, 0.0))
    block = 2
    while block < count:
        cross = (rows // (2 * block) == cols // (2 * block)) & (rows // block > cols // block)
        inverse = inverse - mm(mm(inverse, jnp.where(cross, lower, 0.0)), inverse)
        block *= 2
    return inverse


def conv_window(halo_block, taps, span):
    reach = taps.shape[0] - 1
    total = None
    for offset in range(reach + 1):
        start = HALO - reach + offset
        term = taps[offset : offset + 1] * halo_block[start : start + span]
        total = term if total is None else total + term
    return total


def sigmoid(value):
    return 1.0 / (1.0 + jnp.exp(-value))


def softplus(value):
    return jnp.maximum(value, 0.0) + jnp.log(1.0 + jnp.exp(-jnp.abs(value)))


def gates_of(small, rate, heads, rows, cols):
    beta = sigmoid(small)
    slope = softplus(small)
    logdecay = -rate * slope
    cumul = mm(jnp.where(cols <= rows, 1.0, 0.0), logdecay)
    return beta, slope, logdecay, cumul


def state_place(index, head, heads, key_dim, value_dim, width):
    across = width // value_dim
    turn = index * heads + head
    return (
        pl.ds(pl.multiple_of(lax.div(turn, across) * key_dim, key_dim), key_dim),
        pl.ds(pl.multiple_of(lax.rem(turn, across) * value_dim, value_dim), value_dim),
    )


def chunk_terms(query, key, beta_col, beta_row, cum_col, cum_row, rows, cols):
    within = cols <= rows
    decays = jnp.where(within, jnp.exp(jnp.where(within, cum_col - cum_row, 0.0)), 0.0)
    scaled = decays * beta_row
    key_key = mm_nt(key, key)
    query_key = mm_nt(query, key)
    lower = jnp.where(cols < rows, scaled * key_key, 0.0)
    attend = scaled * query_key
    return decays, scaled, key_key, query_key, lower, attend


def forward_kernel(heads, key_dim, value_dim, pre_ref, gate_ref, small_ref, taps_ref, rate_ref, gain_ref,
                   mixed_ref, core_ref, update_ref, state_ref, inverse_ref, pad_ref, now_ref):
    length, width = pre_ref.shape
    span = SPAN
    chunks = length // span
    rows, cols = grids(span)
    qk = heads * key_dim
    pad_ref[0:HALO] = jnp.zeros((HALO, width), jnp.float32)
    for head in range(heads):
        now_ref[head] = jnp.zeros((key_dim, value_dim), jnp.float32)

    def chunk(index, carry):
        start = pl.multiple_of(index * span, span)
        here = pl.ds(start, span)
        pad_ref[HALO : HALO + span] = pre_ref[here, :]
        total = conv_window(pad_ref[...], taps_ref[...], span)
        pad_ref[0:HALO] = pad_ref[span : span + HALO]
        active = total * sigmoid(total)
        beta, _, _, cumul = gates_of(small_ref[here, :], rate_ref[...], heads, rows, cols)
        beta_t = jnp.transpose(beta)
        cumul_t = jnp.transpose(cumul)
        gate = gate_ref[here, :]
        gated = gate * sigmoid(gate) * gain_ref[...]
        for head in range(heads):
            query = active[:, head * key_dim : (head + 1) * key_dim]
            query = query * (lax.rsqrt(jnp.sum(query * query, -1, keepdims=True) + EPS) * key_dim ** (-0.5))
            key = active[:, qk + head * key_dim : qk + (head + 1) * key_dim]
            key = key * lax.rsqrt(jnp.sum(key * key, -1, keepdims=True) + EPS)
            value = active[:, 2 * qk + head * value_dim : 2 * qk + (head + 1) * value_dim]
            beta_col = beta[:, head : head + 1]
            beta_row = beta_t[head : head + 1]
            cum_col = cumul[:, heads + head : heads + head + 1]
            cum_row = cumul_t[heads + head : heads + head + 1]
            _, _, _, _, lower, attend = chunk_terms(query, key, beta_col, beta_row, cum_col, cum_row, rows, cols)
            inverse = unit_inverse(lower, rows, cols)
            state = now_ref[head]
            state_ref[state_place(index, head, heads, key_dim, value_dim, width)] = state
            rise = jnp.exp(cum_col)
            last = cum_col[span - 1 : span]
            update = mm(inverse, value) - mm(mm(inverse, rise * key), state)
            core = mm(rise * query, state) + mm(attend, update)
            tail = jnp.exp(last - cum_col) * beta_col
            now_ref[head] = jnp.exp(last) * state + mm_tn(key * tail, update)
            inverse_ref[index, head] = inverse
            wide = slice(head * value_dim, (head + 1) * value_dim)
            update_ref[here, wide] = update
            core_ref[here, wide] = core
            normed = core * lax.rsqrt(jnp.mean(core * core, -1, keepdims=True) + EPS)
            mixed_ref[here, wide] = (normed * gated[:, wide]).astype(mixed_ref.dtype)
        return carry

    lax.fori_loop(0, chunks, chunk, 0)


def delta_forward(pre, gate, small, taps, rate, gain, heads, key_dim, value_dim):
    length, width = pre.shape
    chunks = length // SPAN
    out_shape = (
        jax.ShapeDtypeStruct((length, heads * value_dim), jnp.bfloat16),
        jax.ShapeDtypeStruct((length, heads * value_dim), jnp.float32),
        jax.ShapeDtypeStruct((length, heads * value_dim), jnp.float32),
        jax.ShapeDtypeStruct((chunks * heads * key_dim * value_dim // width, width), jnp.float32),
        jax.ShapeDtypeStruct((chunks, heads, SPAN, SPAN), jnp.float32),
    )
    return pl.pallas_call(
        functools.partial(forward_kernel, heads, key_dim, value_dim),
        out_shape=out_shape,
        scratch_shapes=[
            pltpu.VMEM((HALO + SPAN, width), jnp.float32),
            pltpu.VMEM((heads, key_dim, value_dim), jnp.float32),
        ],
        compiler_params=pltpu.CompilerParams(vmem_limit_bytes=56 << 20),
        name="delta_forward",
    )(pre, gate, small, taps, rate, gain)


def backward_start(refs, span):
    (_, _, _, _, _, _, _, _, _, _, _, _, _, _, taps_grad_ref, gain_grad_ref, rate_grad_ref,
     _, pad_ref, now_ref) = refs
    now_ref[...] = jnp.zeros_like(now_ref)
    pad_ref[span : span + HALO] = jnp.zeros((HALO, pad_ref.shape[1]), jnp.float32)
    taps_grad_ref[...] = jnp.zeros_like(taps_grad_ref)
    gain_grad_ref[...] = jnp.zeros_like(gain_grad_ref)
    rate_grad_ref[...] = jnp.zeros_like(rate_grad_ref)


def backward_chunk(heads, key_dim, value_dim, index, refs):
    (pre_ref, gate_ref, small_ref, taps_ref, rate_ref, gain_ref,
     core_ref, update_ref, state_ref, inverse_ref, grad_ref,
     low_ref, gate_low_ref, small_low_ref, taps_grad_ref, gain_grad_ref, rate_grad_ref,
     ahead_ref, pad_ref, now_ref) = refs
    width = taps_ref.shape[1]
    span = SPAN
    rows, cols = grids(span)
    qk = heads * key_dim
    reach = taps_ref.shape[0] - 1
    lanes = small_ref.shape[1]
    lane = lax.broadcasted_iota(jnp.int32, (span, lanes), 1)
    start = pl.multiple_of(index * span, span)
    here = pl.ds(start, span)
    before = pl.ds(pl.multiple_of(jnp.maximum(start - HALO, 0), HALO), HALO)
    ahead_ref[0:HALO] = pre_ref[before, :] * jnp.where(index > 0, 1.0, 0.0)
    ahead_ref[HALO : HALO + span] = pre_ref[here, :]
    total = conv_window(ahead_ref[...], taps_ref[...], span)
    gain_of = sigmoid(total)
    active = total * gain_of
    bend = gain_of * (1.0 + total * (1.0 - gain_of))
    small = small_ref[here, :]
    beta, slope, _, cumul = gates_of(small, rate_ref[...], heads, rows, cols)
    beta_t = jnp.transpose(beta)
    cumul_t = jnp.transpose(cumul)
    gate = gate_ref[here, :]
    gate_sig = sigmoid(gate)
    gate_silu = gate * gate_sig
    gate_bend = gate_sig * (1.0 + gate * (1.0 - gate_sig))
    small_grad = jnp.zeros((span, lanes), jnp.float32)
    for head in range(heads):
        wide = slice(head * value_dim, (head + 1) * value_dim)
        core = core_ref[here, wide]
        grad_mixed = grad_ref[here, wide]
        gain = gain_ref[:, wide]
        scale = lax.rsqrt(jnp.mean(core * core, -1, keepdims=True) + EPS)
        normed = core * scale
        gate_low_ref[here, wide] = (grad_mixed * normed * gain * gate_bend[:, wide]).astype(gate_low_ref.dtype)
        with_gate = grad_mixed * gate_silu[:, wide]
        gain_grad_ref[:, wide] += jnp.sum(with_gate * normed, 0, keepdims=True)
        grad_normed = with_gate * gain
        grad_core = scale * (grad_normed - normed * jnp.mean(grad_normed * normed, -1, keepdims=True))
        query_act = active[:, head * key_dim : (head + 1) * key_dim]
        query_scale = lax.rsqrt(jnp.sum(query_act * query_act, -1, keepdims=True) + EPS)
        query = query_act * (query_scale * key_dim ** (-0.5))
        key_act = active[:, qk + head * key_dim : qk + (head + 1) * key_dim]
        key_scale = lax.rsqrt(jnp.sum(key_act * key_act, -1, keepdims=True) + EPS)
        key = key_act * key_scale
        beta_col = beta[:, head : head + 1]
        beta_row = beta_t[head : head + 1]
        cum_col = cumul[:, heads + head : heads + head + 1]
        cum_row = cumul_t[heads + head : heads + head + 1]
        decays, scaled, key_key, query_key, lower, attend = chunk_terms(
            query, key, beta_col, beta_row, cum_col, cum_row, rows, cols
        )
        state = state_ref[state_place(index, head, heads, key_dim, value_dim, width)]
        update = update_ref[here, wide]
        inverse = inverse_ref[index, head]
        grad_state = now_ref[head]
        rise = jnp.exp(cum_col)
        last = cum_col[span - 1 : span]
        fall = jnp.exp(last - cum_col)
        tail = fall * beta_col
        rise_query = rise * query
        rise_key = rise * key
        grad_update = mm_tn(attend, grad_core) + mm(key * tail, grad_state)
        grad_right = mm_tn(inverse, grad_update)
        now_ref[head] = jnp.exp(last) * grad_state + mm_tn(rise_query, grad_core) - mm_tn(rise_key, grad_right)
        grad_attend = jnp.where(cols <= rows, mm_nt(grad_core, update), 0.0)
        grad_lower = jnp.where(cols < rows, -mm_nt(grad_right, update), 0.0)
        core_state = mm_nt(grad_core, state)
        right_state = mm_nt(grad_right, state)
        grad_tail_key = mm_nt(update, grad_state)
        pair_query = grad_attend * scaled
        pair_key = grad_lower * scaled
        grad_query = rise * core_state + mm(pair_query, key)
        grad_key = (
            grad_tail_key * tail - rise * right_state + mm_tn(pair_query, query)
            + mm(pair_key, key) + mm_tn(pair_key, key)
        )
        grad_tail = jnp.sum(grad_tail_key * key, -1, keepdims=True)
        moved = grad_attend * query_key + grad_lower * key_key
        spread = moved * scaled
        by_row = jnp.sum(spread, -1, keepdims=True)
        sums = mm_tn(
            jnp.concatenate([moved * decays, spread], 1), jnp.ones((span, lanes), jnp.float32)
        )
        grad_beta = sums[:span, 0:1] + grad_tail * fall
        through_tail = grad_tail * tail
        grad_cum = (
            by_row - sums[span:, 0:1] - through_tail
            + rise * (jnp.sum(core_state * query, -1, keepdims=True) - jnp.sum(right_state * key, -1, keepdims=True))
        )
        end_grad = jnp.sum(through_tail, 0, keepdims=True) + jnp.exp(last) * jnp.sum(
            jnp.sum(state * grad_state, -1, keepdims=True), 0, keepdims=True
        )
        grad_cum = grad_cum + jnp.where(rows[:, 0:1] == span - 1, end_grad, 0.0)
        small_grad = small_grad + jnp.where(lane == head, grad_beta, 0.0)
        small_grad = small_grad + jnp.where(lane == heads + head, grad_cum, 0.0)
        grad_query = grad_query * key_dim ** (-0.5)
        unit = query_act * query_scale
        grad_query = query_scale * (grad_query - unit * jnp.sum(grad_query * unit, -1, keepdims=True))
        grad_key = key_scale * (grad_key - key * jnp.sum(grad_key * key, -1, keepdims=True))
        at = slice(head * key_dim, (head + 1) * key_dim)
        pad_ref[0:span, at] = grad_query * bend[:, at]
        at = slice(qk + head * key_dim, qk + (head + 1) * key_dim)
        pad_ref[0:span, at] = grad_key * bend[:, at]
        at = slice(2 * qk + head * value_dim, 2 * qk + (head + 1) * value_dim)
        pad_ref[0:span, at] = grad_right * bend[:, at]
    summed = mm(jnp.where(cols >= rows, 1.0, 0.0), small_grad)
    is_beta = lane < heads
    rate_grad_ref[...] += jnp.sum(jnp.where(is_beta, 0.0, -slope * summed), 0, keepdims=True)
    sig = beta
    small_low_ref[here, :] = jnp.where(
        is_beta, small_grad * sig * (1.0 - sig), -rate_ref[...] * sig * summed
    ).astype(small_low_ref.dtype)
    outer = pad_ref[...]
    dense = outer[0:span]
    block = ahead_ref[...]
    grad_pre = None
    for offset in range(reach + 1):
        behind = reach - offset
        taps_grad_ref[offset : offset + 1] += jnp.sum(
            dense * block[HALO - behind : HALO - behind + span], 0, keepdims=True
        )
        term = taps_ref[offset : offset + 1] * outer[behind : behind + span]
        grad_pre = term if grad_pre is None else grad_pre + term
    low_ref[here, :] = grad_pre.astype(low_ref.dtype)
    pad_ref[span : span + HALO] = pad_ref[0:HALO]


MESH = pl.DeviceIdType.MESH
VM = pl.BlockSpec(memory_space=pltpu.VMEM)


def call_out(peers):
    barrier = pltpu.get_barrier_semaphore()
    for peer in peers:
        pl.semaphore_signal(barrier, inc=1, device_id=peer, device_id_type=MESH)


def hear_all(peers):
    pl.semaphore_wait(pltpu.get_barrier_semaphore(), len(peers))


def greet(peers):
    call_out(peers)
    hear_all(peers)


def remote(src, dst, send, recv, peer):
    return pltpu.make_async_remote_copy(
        src_ref=src, dst_ref=dst, send_sem=send, recv_sem=recv, device_id=peer, device_id_type=MESH
    )


def tensor_peers():
    dp = lax.axis_index("dp")
    t = lax.axis_index("tensor")
    core = lax.rem(t, 2)
    mate = (dp, t + 1 - 2 * core)
    across = (dp, lax.rem(t + 2, 4))
    return core, mate, across


def psum_kernel(blocks, part_ref, out_ref, land_mate, land_across, half, send, recv):
    core, mate, across = tensor_peers()
    greet((mate, across))
    rows = part_ref.shape[0] // blocks
    part = rows // 2
    first = []
    for b in range(blocks):
        theirs = pl.ds(pl.multiple_of(b * rows + (1 - core) * part, part), part)
        copy = remote(part_ref.at[theirs], land_mate.at[pl.ds(b * part, part)], send.at[0, b], recv.at[0, b], mate)
        copy.start()
        first.append(copy)
    second = []
    for b in range(blocks):
        mine = pl.ds(pl.multiple_of(b * rows + core * part, part), part)
        slot = pl.ds(b * part, part)
        first[b].wait_recv()
        half[slot] = part_ref[mine] + land_mate[slot]
        copy = remote(half.at[slot], land_across.at[slot], send.at[1, b], recv.at[1, b], across)
        copy.start()
        second.append(copy)
    third = []
    for b in range(blocks):
        mine = pl.ds(pl.multiple_of(b * rows + core * part, part), part)
        slot = pl.ds(b * part, part)
        second[b].wait_recv()
        out_ref[mine] = half[slot] + land_across[slot]
        copy = remote(out_ref.at[mine], out_ref.at[mine], send.at[2, b], recv.at[2, b], mate)
        copy.start()
        third.append(copy)
    for b in range(blocks):
        third[b].wait_recv()
    for b in range(blocks):
        first[b].wait_send()
        second[b].wait_send()
        third[b].wait_send()


def tensor_sum(part, collective_id, blocks=8):
    rows, width = part.shape
    return pl.pallas_call(
        functools.partial(psum_kernel, blocks),
        out_shape=jax.ShapeDtypeStruct(part.shape, part.dtype),
        in_specs=[VM],
        out_specs=VM,
        scratch_shapes=[pltpu.VMEM((rows // 2, width), part.dtype)] * 3
        + [pltpu.SemaphoreType.DMA((3, blocks))] * 2,
        compiler_params=pltpu.CompilerParams(
            collective_id=collective_id, has_side_effects=True, vmem_limit_bytes=40 << 20
        ),
        name="tensor_sum",
    )(part)


def swap_kernel(count, narrow, *refs):
    sources, results = refs[:count], refs[count : 2 * count]
    staged, send, recv, close_send, close_recv = refs[2 * count :]
    n = lax.axis_size("dp")
    me = lax.axis_index("dp")
    t = lax.axis_index("tensor")
    core, mate, across = tensor_peers()
    ranks = lax.axis_size("tensor")
    others = [lax.rem(me + k, n) for k in range(1, n)]
    greet([(other, t) for other in others] + [mate, across])
    seg = results[0].shape[0] // n
    part = seg // ranks
    far = lax.rem(t + 2, ranks)

    def at(place, rank):
        return pl.ds(pl.multiple_of(place * seg + rank * part, part), part)

    outgoing = []
    for i in range(count):
        for k in range(n):
            other = lax.rem(me + k, n)
            if k == 0:
                results[i][at(me, t)] = sources[i][at(me, t)].astype(jnp.float32)
                continue
            if narrow[i]:
                staged[i, k] = sources[i][at(other, t)].astype(jnp.float32)
                src = staged.at[i, k]
            else:
                src = sources[i].at[at(other, t)]
            copy = remote(src, results[i].at[at(me, t)], send.at[i, k], recv.at[i, k], (other, t))
            copy.start()
            outgoing.append(copy)
    close = []
    for i in range(count):
        for k in range(n):
            source = lax.rem(me + n - k, n)
            here = results[i].at[at(source, t)]
            if k:
                remote(here, here, send.at[i, k], recv.at[i, k], (source, t)).wait_recv()
            over = remote(here, here, close_send.at[0, i, k], close_recv.at[0, i, k], across)
            over.start()
            beside = remote(here, here, close_send.at[1, i, k], close_recv.at[1, i, k], mate)
            beside.start()
            close += [over, beside]
    last = []
    for i in range(count):
        for k in range(n):
            source = lax.rem(me + n - k, n)
            there = results[i].at[at(source, far)]
            remote(there, there, close_send.at[0, i, k], close_recv.at[0, i, k], across).wait_recv()
            copy = remote(there, there, close_send.at[2, i, k], close_recv.at[2, i, k], mate)
            copy.start()
            last.append(copy)
    for copy in outgoing:
        copy.wait_send()
    for j, copy in enumerate(close):
        copy.wait_send()
        if j % 2:
            copy.wait_recv()
    for copy in last:
        copy.wait()


def swap(arrays, n, collective_id):
    count = len(arrays)
    rows, width = arrays[0].shape
    narrow = [a.dtype != jnp.float32 for a in arrays]
    out = pl.pallas_call(
        functools.partial(swap_kernel, count, narrow),
        out_shape=[jax.ShapeDtypeStruct((rows, width), jnp.float32)] * count,
        in_specs=[VM] * count,
        out_specs=[VM] * count,
        scratch_shapes=[pltpu.VMEM((count, n, rows // n // 4, width), jnp.float32)]
        + [pltpu.SemaphoreType.DMA((count, n))] * 2
        + [pltpu.SemaphoreType.DMA((3, count, n))] * 2,
        compiler_params=pltpu.CompilerParams(
            collective_id=collective_id, has_side_effects=True, vmem_limit_bytes=40 << 20
        ),
        name="swap",
    )(*arrays)
    return out


SLOT = 80
DEPTH = 10
SPLIT = 3
WHOLE = 2
ORDER = (0, 1, 2, 3)


def grid_place():
    n = lax.axis_size("dp")
    me = lax.axis_index("dp")
    t = lax.axis_index("tensor")
    lines = n // 2
    z = lax.div(me, 2)
    x = lax.rem(me, 2)
    return n, lines, me, t, z, x


def reduce_slot(slot, chunks, data, split_rings, whole_rings, sems):
    n, lines, me, t, z, x = grid_place()
    mate = (me + 1 - 2 * x, t)
    send_x, recv_x, send_z, recv_z, send_d, recv_d, send_p, recv_p, send_s, recv_s = [sems.at[i] for i in range(10)]
    top = lines - 1
    finish = slot - 2 * lines - 1

    def ring(chunk):
        return lax.rem(chunk, DEPTH)

    def within(chunk):
        return (chunk >= 0) & (chunk < chunks)

    def split_stream(stream):
        land_x, land_z, outgo, aside = split_rings
        up = stream % 2 == 0
        level = z if up else top - z
        after = (me + 2, t) if up else (me - 2, t)
        prior = (me - 2, t) if up else (me + 2, t)

        def rows(chunk, side):
            return pl.ds(pl.multiple_of(chunk * SLOT + 16 * stream + 8 * side, 8), 8)

        def spot(ref, chunk):
            return ref.at[stream, ring(chunk)]

        def copy(kind_send, kind_recv, chunk, src, dst, peer):
            at = (stream, ring(chunk))
            return remote(src, dst, kind_send.at[at], kind_recv.at[at], peer)

        def to_mate(chunk):
            return copy(send_x, recv_x, chunk, spot(aside, chunk), spot(land_x, chunk), mate)

        def to_after(chunk):
            return copy(send_z, recv_z, chunk, spot(outgo, chunk), spot(land_z, chunk), after)

        def result(chunk, peer):
            here = data.at[rows(chunk, x)]
            return copy(send_d, recv_d, chunk, here, here, peer)

        def close(chunk, side):
            here = data.at[rows(chunk, side)]
            return copy(send_p, recv_p, chunk, here, here, mate)

        def give_back(chunk):
            @pl.when(level > 0)
            def _():
                result(chunk, prior).start()

            close(chunk, x).start()

        def enter():
          @pl.when(slot < chunks)
          def _():
            aside[stream, ring(slot)] = data[rows(slot, 1 - x)]
            to_mate(slot).start()

        def climb():
            rise = slot - 1 - level

            @pl.when(within(rise))
            def _():
                here = rows(rise, x)
                at = ring(rise)
                to_mate(rise).wait_recv()

                @pl.when(level > 0)
                def _():
                    to_after(rise).wait_recv()
                    outgo[stream, at] = data[here] + land_x[stream, at] + land_z[stream, at]

                @pl.when(level == 0)
                def _():
                    outgo[stream, at] = data[here] + land_x[stream, at]

                @pl.when(level < top)
                def _():
                    to_after(rise).start()

                @pl.when(level == top)
                def _():
                    data[here] = outgo[stream, at]
                    give_back(rise)

        def descend():
            fall = slot - 1 - 2 * top + level

            @pl.when(within(fall) & (level < top))
            def _():
                result(fall, after).wait_recv()
                to_after(fall).wait_send()
                give_back(fall)

        def leave():
            @pl.when(within(finish))
            def _():
                @pl.when(level > 0)
                def _():
                    result(finish, prior).wait_send()

                close(finish, x).wait_send()
                close(finish, 1 - x).wait_recv()
                to_mate(finish).wait_send()

        return enter, climb, descend, leave

    def whole_stream(stream):
        land_x, land_z, land_s, outgo = whole_rings
        line = z if stream == 0 else top - z
        step = 2 if stream == 0 else -2
        inner, outer = (me - step, t), (me + step, t)

        def rows(chunk):
            return pl.ds(pl.multiple_of(chunk * SLOT + 16 * (SPLIT + stream), 8), 16)

        def spot(ref, chunk):
            return ref.at[stream, ring(chunk)]

        def copy(kind_send, kind_recv, chunk, src, dst, peer):
            at = (ring(chunk),)
            return remote(
                src, dst, kind_send.at[SPLIT + stream, ring(chunk)], kind_recv.at[SPLIT + stream, ring(chunk)], peer
            )

        def inward(chunk):
            return copy(send_z, recv_z, chunk, spot(outgo, chunk), spot(land_z, chunk), inner)

        def outward(chunk):
            return copy(send_z, recv_s, chunk, spot(outgo, chunk), spot(land_s, chunk), outer)

        def to_mate(chunk):
            return copy(send_x, recv_x, chunk, spot(outgo, chunk), spot(land_x, chunk), mate)

        def result_out(chunk):
            here = data.at[rows(chunk)]
            return copy(send_d, recv_d, chunk, here, here, outer)

        def result_in(chunk):
            here = data.at[rows(chunk)]
            return copy(send_s, recv_d, chunk, here, here, inner)

        def enter():
            leaf = slot - 1

            @pl.when(within(leaf) & (line == 0) & (lax.rem(jnp.maximum(leaf, 0), 2) > 0))
            def _():
                outgo[stream, ring(leaf)] = data[rows(leaf)]
                outward(leaf).start()

        def climb():
            rise = slot - 1 - (top - line)
            root = lax.rem(jnp.maximum(rise, 0), 2)

            @pl.when(within(rise) & (line >= root))
            def _():
                here = rows(rise)
                at = ring(rise)

                @pl.when(line < top)
                def _():
                    inward(rise).wait_recv()

                is_fork = (line == root) & (root > 0)

                @pl.when(is_fork)
                def _():
                    outward(rise).wait_recv()
                    outgo[stream, at] = data[here] + land_z[stream, at] + land_s[stream, at]

                @pl.when((line < top) & jnp.logical_not(is_fork))
                def _():
                    outgo[stream, at] = data[here] + land_z[stream, at]

                @pl.when(line == top)
                def _():
                    outgo[stream, at] = data[here]

                @pl.when(line > root)
                def _():
                    inward(rise).start()

                @pl.when(line == root)
                def _():
                    to_mate(rise).start()

        def descend():
            meet = slot - 2 - (top - line)
            meet_root = lax.rem(jnp.maximum(meet, 0), 2)

            @pl.when(within(meet) & (line == meet_root))
            def _():
                at = ring(meet)
                to_mate(meet).wait_recv()
                data[rows(meet)] = outgo[stream, at] + land_x[stream, at]
                result_out(meet).start()

                @pl.when(meet_root > 0)
                def _():
                    result_in(meet).start()

            for parity in range(2):
                fall = slot - 2 - (top - parity) - (line - parity)

                @pl.when(within(fall) & (lax.rem(jnp.maximum(fall, 0), 2) == parity) & (line > parity))
                def _():
                    result_out(fall).wait_recv()
                    inward(fall).wait_send()

                    @pl.when(line < top)
                    def _():
                        result_out(fall).start()

            inside = slot - 2 - (top - 1) - 1

            @pl.when(within(inside) & (lax.rem(jnp.maximum(inside, 0), 2) > 0) & (line == 0))
            def _():
                result_in(inside).wait_recv()
                outward(inside).wait_send()

        def leave():
            end_root = lax.rem(jnp.maximum(finish, 0), 2)

            @pl.when(within(finish))
            def _():
                @pl.when((line >= end_root) & (line < top))
                def _():
                    result_out(finish).wait_send()

                @pl.when(line == end_root)
                def _():
                    to_mate(finish).wait_send()

                    @pl.when(end_root > 0)
                    def _():
                        result_in(finish).wait_send()

        return enter, climb, descend, leave

    streams = [whole_stream(stream) for stream in range(WHOLE)] + [split_stream(stream) for stream in range(SPLIT)]
    for stream in streams:
        for phase in ORDER:
            stream[phase]()


def settle(lines):
    return 2 * lines + 1


def reduce_scratch(width):
    return (
        [pltpu.VMEM((SPLIT, DEPTH, 8, width), jnp.float32)] * 4
        + [pltpu.VMEM((WHOLE, DEPTH, 16, width), jnp.float32)] * 4
        + [pltpu.SemaphoreType.DMA((10, SPLIT + WHOLE, DEPTH))]
    )


BLOCKS = 8


def dot_plain(left, right):
    return lax.dot_general(left, right, (((1,), (0,)), ((), ())), preferred_element_type=jnp.float32)


def dot_nt(left, right):
    return lax.dot_general(left, right, (((1,), (1,)), ((), ())), preferred_element_type=jnp.float32)


def dot_tn(left, right):
    return lax.dot_general(left, right, (((0,), (0,)), ((), ())), preferred_element_type=jnp.float32)


def aligned(start, size):
    return pl.ds(pl.multiple_of(start, size), size)


class TensorSum:
    def __init__(self, part, total, land_mate, land_across, half, send, recv):
        self.core, self.mate, self.across = tensor_peers()
        self.part, self.total, self.half = part, total, half
        self.land_mate, self.land_across = land_mate, land_across
        self.send, self.recv = send, recv
        self.rows = part.shape[0] // BLOCKS
        self.size = self.rows // 2

    def span(self, block, side):
        return aligned(block * self.rows + side * self.size, self.size)

    def slot(self, block):
        return aligned(block * self.size, self.size)

    def first(self, block):
        return remote(
            self.part.at[self.span(block, 1 - self.core)], self.land_mate.at[self.slot(block)],
            self.send.at[0, block], self.recv.at[0, block], self.mate,
        )

    def second(self, block):
        return remote(
            self.half.at[self.slot(block)], self.land_across.at[self.slot(block)],
            self.send.at[1, block], self.recv.at[1, block], self.across,
        )

    def third(self, block):
        mine = self.total.at[self.span(block, self.core)]
        return remote(mine, mine, self.send.at[2, block], self.recv.at[2, block], self.mate)

    def start(self):
        for block in range(BLOCKS):
            self.first(block).start()

    def cross(self, block):
        self.first(block).wait_recv()
        slot = self.slot(block)
        self.half[slot] = self.part[self.span(block, self.core)] + self.land_mate[slot]
        self.second(block).start()

    def share(self, block, beside=None):
        self.second(block).wait_recv()
        slot = self.slot(block)
        mine = self.span(block, self.core)
        value = self.half[slot] + self.land_across[slot]
        self.total[mine] = value if beside is None else value + beside[mine].astype(value.dtype)
        self.third(block).start()

    def finish(self, had=0):
        for block in range(had, BLOCKS):
            self.third(block).wait_recv()
        for block in range(BLOCKS):
            self.first(block).wait_send()
            self.second(block).wait_send()
            self.third(block).wait_send()


class Swap:
    def __init__(self, source, result, send, recv, close_send, close_recv):
        self.n = lax.axis_size("dp")
        self.me = lax.axis_index("dp")
        self.t = lax.axis_index("tensor")
        self.ranks = lax.axis_size("tensor")
        _, self.mate, self.across = tensor_peers()
        self.source, self.result = source, result
        self.sems = send, recv, close_send, close_recv
        self.seg = result.shape[0] // self.n
        self.part = self.seg // self.ranks

    def at(self, place, rank):
        return aligned(place * self.seg + rank * self.part, self.part)

    def out(self, k):
        other = lax.rem(self.me + k, self.n)
        return remote(
            self.source.at[self.at(other, self.t)], self.result.at[self.at(self.me, self.t)],
            self.sems[0].at[k], self.sems[1].at[k], (other, self.t),
        )

    def close(self, k, leg):
        origin = lax.rem(self.me + self.n - k, self.n)
        rank = lax.rem(self.t + 2, self.ranks) if leg == 2 else self.t
        here = self.result.at[self.at(origin, rank)]
        return remote(
            here, here, self.sems[2].at[leg, k], self.sems[3].at[leg, k], self.across if leg == 0 else self.mate
        )

    def start(self):
        mine = self.at(self.me, self.t)
        self.result[mine] = self.source[mine]
        for k in range(1, self.n):
            self.out(k).start()

    def gather(self, k):
        @pl.when(k > 0)
        def _():
            self.out(k).wait_recv()

        self.close(k, 0).start()
        self.close(k, 1).start()

    def forward(self, k):
        self.close(k, 0).wait_recv()
        self.close(k, 2).start()

    def sent(self):
        for k in range(1, self.n):
            self.out(k).wait_send()

    def finish(self):
        for k in range(self.n):
            self.close(k, 0).wait_send()
            self.close(k, 1).wait()
            self.close(k, 2).wait()


class PlaneSwap(Swap):
    def __init__(self, source, result, send, recv, close_send, close_recv):
        super().__init__(source, result, send, recv, close_send, close_recv)
        self.core = lax.rem(self.t, 2)
        self.part = self.seg // 2

    def out(self, k):
        other = lax.rem(self.me + k, self.n)
        return remote(
            self.source.at[self.at(other, self.core)], self.result.at[self.at(self.me, self.core)],
            self.sems[0].at[k], self.sems[1].at[k], (other, self.t),
        )

    def close(self, k, leg):
        origin = lax.rem(self.me + self.n - k, self.n)
        here = self.result.at[self.at(origin, self.core)]
        return remote(here, here, self.sems[2].at[leg, k], self.sems[3].at[leg, k], self.mate)

    def start(self):
        mine = self.at(self.me, self.core)
        self.result[mine] = self.source[mine]
        for k in range(1, self.n):
            self.out(k).start()

    def gather(self, k):
        @pl.when(k > 0)
        def _():
            self.out(k).wait_recv()

        self.close(k, 1).start()

    def finish(self):
        for k in range(self.n):
            self.close(k, 1).wait()


def tail_kernel(
    heads, key_dim, value_dim, ranges, chunks,
    part2_hbm, ffn_hbm, pre_hbm, core_hbm, update_hbm, state_hbm,
    resid1_hbm, upstream_hbm, resid_hbm, mixed_hbm, hidden1_hbm, hidden2_hbm, units_hbm,
    w_out_hbm, query_hbm, key_hbm, value_hbm, w_gate_hbm, w_small_hbm, gate_hbm, small_hbm, inverse_hbm,
    norm1_ref, norm2_ref, taps_ref, rate_ref, gain_ref,
    data, output_ref, inputs_grad_ref,
    resid1_ref, upstream_ref, resid_ref, mixed_ref, hidden1_ref, hidden2_ref, units_ref,
    w_out_ref, w_mix_ref, w_gate_ref, w_small_ref, gate_ref, small_ref, inverse_ref,
    split_x, split_z, split_out, split_aside, whole_x, whole_z, whole_s, whole_out, sems,
    part, total, half, land_mate, land_across, sum_send, sum_recv,
    resid1_grad, resid1_low, mixed_grad, low, gate_low, small_low,
    taps_grad, gain_grad, rate_grad, norm1_grad, norm2_grad, ahead, pad, now,
    shuffled, swap_send, swap_recv, close_send, close_recv, load_sem,
):
    n, lines, me, t, z, x = grid_place()
    _, mate, across = tensor_peers()
    length, width = resid1_hbm.shape
    qk = heads * key_dim
    values = heads * value_dim
    at_down, at_units, at_out, at_gate, at_mix, at_small, at_end, rows_all = ranges
    loads = [
        (part2_hbm, part),
        (units_hbm, units_ref),
        (upstream_hbm, upstream_ref),
        (hidden2_hbm, hidden2_ref),
        (resid1_hbm, resid1_ref),
        (w_out_hbm, w_out_ref),
        (mixed_hbm, mixed_ref),
        (pre_hbm, data.at[pl.ds(at_mix, length)]),
        (core_hbm, data.at[pl.ds(at_mix + length, length), pl.ds(0, values)]),
        (update_hbm, data.at[pl.ds(at_mix + length, length), pl.ds(values, values)]),
        (state_hbm, data.at[pl.ds(at_gate, state_hbm.shape[0])]),
        (gate_hbm, gate_ref),
        (small_hbm, small_ref),
        (inverse_hbm, inverse_ref),
        (hidden1_hbm, hidden1_ref),
        (query_hbm, w_mix_ref.at[:, pl.ds(0, qk)]),
        (key_hbm, w_mix_ref.at[:, pl.ds(qk, qk)]),
        (value_hbm, w_mix_ref.at[:, pl.ds(2 * qk, values)]),
        (w_gate_hbm, w_gate_ref),
        (w_small_hbm, w_small_ref),
        (resid_hbm, resid_ref),
    ]
    loads = [pltpu.make_async_copy(src, dst, load_sem.at[i]) for i, (src, dst) in enumerate(loads)]
    load_ffn = pltpu.make_async_copy(ffn_hbm, part, load_sem.at[len(loads)])
    peers = [(lax.rem(me + k, n), t) for k in range(1, n)] + [mate, across]
    call_out(peers)
    for load in loads:
        load.start()
    refs = (
        data.at[pl.ds(at_mix, length)], gate_ref, small_ref, taps_ref, rate_ref, gain_ref,
        data.at[pl.ds(at_mix + length, length), pl.ds(0, values)],
        data.at[pl.ds(at_mix + length, length), pl.ds(values, values)],
        data.at[pl.ds(at_gate, state_hbm.shape[0])], inverse_ref, mixed_grad, low, gate_low, small_low, taps_grad, gain_grad, rate_grad,
        ahead, pad, now,
    )
    sums = [
        TensorSum(part, total, land_mate, land_across.at[i % 2], half, sum_send.at[i], sum_recv.at[i]) for i in range(3)
    ]
    swaps = [
        Swap(source, result, swap_send.at[i], swap_recv.at[i], close_send.at[i], close_recv.at[i])
        for i, (source, result) in enumerate([(total, shuffled), (resid1_grad, inputs_grad_ref)])
    ]
    norm1_grad[...] = jnp.zeros_like(norm1_grad)
    norm2_grad[...] = jnp.zeros_like(norm2_grad)
    backward_start(refs, SPAN)
    data[at_end:rows_all] = jnp.zeros((rows_all - at_end, width), jnp.float32)
    count_units = (at_units - at_down)
    tiles = units_ref.shape[2] // 128

    def units_piece(i):
        kind = lax.div(i, tiles)
        tile = lax.rem(i, tiles)
        left = units_ref[kind, :, aligned(tile * 128, 128)]
        start = at_down + kind * count_units + tile * 128

        def put(right):
            value = dot_tn(left, right)

            @pl.when(tile < tiles - 1)
            def _():
                data[pl.ds(pl.multiple_of(start, 64), 128)] = value

            @pl.when(tile == tiles - 1)
            def _():
                rest = count_units - (tiles - 1) * 128
                data[pl.ds(pl.multiple_of(start, 64), rest)] = value[0:rest]

        @pl.when(kind == 0)
        def _():
            put(upstream_ref[...])

        @pl.when(kind > 0)
        def _():
            put(hidden2_ref[...])

    loads[0].wait()
    hear_all(peers)
    sums[0].start()
    loads[1].wait()
    loads[2].wait()
    units_piece(0)

    def wait_loads():
        for load in loads[3:]:
            load.wait()

    def norm_back(value, grad, gain, gain_grad_ref):
        scale = lax.rsqrt(jnp.mean(value * value, -1, keepdims=True) + EPS)
        normed = value * scale
        gain_grad_ref[...] += jnp.sum(grad * normed, 0, keepdims=True)
        scaled = grad * gain
        return scale * (scaled - normed * jnp.mean(scaled * normed, -1, keepdims=True))

    def norm2_piece(i):
        here = aligned(i * 64, 64)
        grad = upstream_ref[here].astype(jnp.float32) + norm_back(
            resid1_ref[here], total[here], norm2_ref[...], norm2_grad
        )
        resid1_grad[here] = grad
        resid1_low[here] = grad.astype(jnp.bfloat16)

    def mixed_piece(i):
        tile = aligned(i * 256, 256)
        mixed_grad[:, tile] = dot_nt(resid1_low[...], w_out_ref[tile])

    def out_piece(i):
        tile = aligned(i * 256, 256)
        data[pl.ds(pl.multiple_of(at_out + i * 256, 64), 256)] = dot_tn(
            mixed_ref[:, tile], resid1_low[...]
        )

    def gate_piece(i):
        tile = aligned(i * 256, 256)
        half_rows = width // 2
        data[pl.ds(pl.multiple_of(at_gate + i * 256, 64), 256), 0:values] = dot_tn(hidden1_ref[:, tile], gate_low[...])
        other = aligned(half_rows + i * 256, 256)
        data[pl.ds(pl.multiple_of(at_gate + i * 256, 64), 256), values : 2 * values] = dot_tn(
            hidden1_ref[:, other], gate_low[...]
        )

    def mix_piece(i):
        tile = aligned(i * 256, 256)
        data[pl.ds(pl.multiple_of(at_mix + i * 256, 64), 256)] = dot_tn(hidden1_ref[:, tile], low[...])

    def hidden_piece(i):
        tile = aligned(i * 256, 256)
        part[:, tile] = (
            dot_nt(low[...], w_mix_ref[tile]) + dot_nt(gate_low[...], w_gate_ref[tile])
            + dot_plain(small_low[...], w_small_ref[:, tile])
        )

    def output_piece(i):
        here = aligned(i * 64, 64)
        total[here] = total[here] + resid1_ref[here]

    def round_piece(i):
        here = aligned(i * 64, 64)
        output_ref[here] = shuffled[here].astype(output_ref.dtype)

    def norm1_piece(i):
        here = aligned(i * 64, 64)
        resid1_grad[here] = resid1_grad[here] + norm_back(
            resid_ref[here].astype(jnp.float32), total[here], norm1_ref[...], norm1_grad
        )

    def small_piece():
        base = at_small
        data[base : at_end] = jnp.zeros((at_end - base, width), jnp.float32)
        data[base : base + 4] = taps_grad[...]
        data[base + 4 : base + 5] = norm1_grad[...]
        data[base + 5 : base + 6] = norm2_grad[...]
        data[base + 6 : base + 7, 0:values] = gain_grad[...]
        data[base + 6 : base + 7, values : values + rate_grad.shape[1]] = rate_grad[...]
        data[base + 8 : base + 16] = dot_tn(small_low[...], hidden1_ref[...])[0:8]

    def start_ffn():
        load_ffn.start()
        load_ffn.wait()
        sums[1].start()

    pieces = []

    def plan(first, count, each, run):
        assert count % each == 0
        pieces.append((first, count, each, run))
        return first + -(-count // each)

    plan(0, 1, 1, lambda i: wait_loads())
    plan(0, 3 * tiles - 1, 1, lambda i: units_piece(i + 1))
    for i in range(1, 3 * tiles):
        assert i <= (at_down + i // tiles * count_units + i % tiles * 128) // SLOT
    at = plan(0, BLOCKS, 2, sums[0].cross)
    at = plan(at, BLOCKS, 2, sums[0].share)
    at = plan(at, 1, 1, lambda i: sums[0].finish())
    at = plan(at, length // 64, 2, norm2_piece)
    at = plan(at, values // 256, 1, mixed_piece)
    side = at
    at = plan(at, values // 256, 1, out_piece)
    at_ready_out = at
    at = plan(at, length // SPAN, 1, lambda i: backward_chunk(heads, key_dim, value_dim, length // SPAN - 1 - i, refs))
    side = plan(side, 1, 1, lambda i: start_ffn())
    side = plan(side, BLOCKS, 2, sums[1].cross)
    side = plan(side, BLOCKS, 2, sums[1].share)
    side = plan(side, 1, 1, lambda i: sums[1].finish())
    part_free = side
    side = plan(side, length // 64, 4, output_piece)
    side = plan(side, 1, 1, lambda i: swaps[0].start())
    side = plan(side, n, 2, swaps[0].gather)
    side = plan(side, 1, 1, lambda i: swaps[0].sent())
    total_free = side
    side = plan(side, n, 2, swaps[0].forward)
    side = plan(side, 1, 1, lambda i: swaps[0].finish())
    side = plan(side, length // 64, 4, round_piece)
    at = plan(at, width // 512, 1, gate_piece)
    at_ready_gate = at
    at = plan(at, width // 256, 1, mix_piece)
    at_ready_mix = at
    at = plan(max(at, part_free), width // 256, 1, hidden_piece)
    at = plan(max(at, total_free), 1, 1, lambda i: sums[2].start())
    at = plan(at, BLOCKS, 2, sums[2].cross)
    at = plan(at, BLOCKS, 2, sums[2].share)
    at = plan(at, 1, 1, lambda i: sums[2].finish())
    at = plan(at, length // 64, 2, norm1_piece)
    at = plan(at, 1, 1, lambda i: small_piece())
    at_ready_small = at
    at = plan(at, 1, 1, lambda i: swaps[1].start())
    at = plan(at, n, 2, swaps[1].gather)
    plan(at, 1, 1, lambda i: swaps[1].sent())
    at = plan(at, n, 2, swaps[1].forward)
    at = plan(at, 1, 1, lambda i: swaps[1].finish())
    assert at_ready_out <= at_out // SLOT and at_ready_gate <= at_gate // SLOT
    assert at_ready_mix <= at_mix // SLOT and at_ready_small <= at_small // SLOT
    last = max(chunks + settle(lines), at, side)

    def step(slot, carry):
        reduce_slot(
            slot, chunks, data, (split_x, split_z, split_out, split_aside), (whole_x, whole_z, whole_s, whole_out), sems
        )
        for first, count, each, run in pieces:
            steps = -(-count // each)

            @pl.when((slot >= first) & (slot < first + steps))
            def _(first=first, each=each, run=run):
                if each == 1:
                    run(slot - first)
                else:
                    def inner(i, carry):
                        run((slot - first) * each + i)
                        return carry

                    lax.fori_loop(0, each, inner, 0)

        return carry

    lax.fori_loop(0, last, step, 0)


def tail(
    part2, ffn, pre, core, update, states, resid1, upstream, resid, mixed, hidden1, hidden2, units,
    w_out, w_query, w_key, w_value, w_gate, w_small, gate, small, inverses, norm1, norm2, taps, rate, gain,
    heads, key_dim, value_dim, count_units, places, collective_id,
):
    length, width = resid1.shape
    values = heads * value_dim
    qk = heads * key_dim
    lanes = small.shape[1]
    heights = [count_units, 2 * count_units, values, values, width, 64]
    ranges = [0]
    for height in heights:
        ranges.append(ranges[-1] + height)
    rows_all = -(-ranges[-1] // SLOT) * SLOT
    chunks = rows_all // SLOT
    f32, bf = jnp.float32, jnp.bfloat16
    shape = jax.ShapeDtypeStruct
    out_shape = [
        pltpu.VMEM((rows_all, width), f32),
        pltpu.VMEM((length, width), bf),
        pltpu.VMEM((length, width), f32),
    ]
    vmem, any_ = VM, pl.BlockSpec(memory_space=pl.ANY)
    dma = pltpu.SemaphoreType.DMA
    scratch = (
        [
            pltpu.VMEM(a.shape, a.dtype)
            for a in (
                resid1, upstream, resid, mixed, hidden1, hidden2, units, w_out, shape((width, width), bf), w_gate, w_small,
                gate, small, inverses,
            )
        ]
        + reduce_scratch(width)
        + [
            pltpu.VMEM((length, width), f32),
            pltpu.VMEM((length, width), f32),
            pltpu.VMEM((length // 2, width), f32),
            pltpu.VMEM((length // 2, width), f32),
            pltpu.VMEM((2, length // 2, width), f32),
            dma((3, 3, BLOCKS)),
            dma((3, 3, BLOCKS)),
            pltpu.VMEM((length, width), f32),
            pltpu.VMEM((length, width), bf),
            pltpu.VMEM((length, values), f32),
            pltpu.VMEM((length, width), bf),
            pltpu.VMEM((length, values), bf),
            pltpu.VMEM((length, lanes), bf),
            pltpu.VMEM(taps.shape, f32),
            pltpu.VMEM((1, values), f32),
            pltpu.VMEM((1, lanes), f32),
            pltpu.VMEM((1, width), f32),
            pltpu.VMEM((1, width), f32),
            pltpu.VMEM((HALO + SPAN, width), f32),
            pltpu.VMEM((HALO + SPAN, width), f32),
            pltpu.VMEM((heads, key_dim, value_dim), f32),
            pltpu.VMEM((length, width), f32),
            dma((2, places)),
            dma((2, places)),
            dma((2, 3, places)),
            dma((2, 3, places)),
            dma((24,)),
        ]
    )
    return pl.pallas_call(
        functools.partial(tail_kernel, heads, key_dim, value_dim, tuple(ranges) + (rows_all,), chunks),
        out_shape=out_shape,
        in_specs=[any_] * 22 + [vmem] * 5,
        out_specs=[vmem] * 3,
        scratch_shapes=scratch,
        compiler_params=pltpu.CompilerParams(
            collective_id=collective_id, has_side_effects=True,
            vmem_limit_bytes=67043328 - 4 * width * rows_all - 6 * width * length - (1 << 18),
        ),
        name="tail",
    )(
        part2, ffn, pre, core, update, states, resid1, upstream, resid, mixed, hidden1, hidden2, units,
        w_out, w_query, w_key, w_value, w_gate, w_small, gate, small, inverses, norm1, norm2, taps, rate, gain,
    ), tuple(ranges)


def finish_kernel(heads, qk, values, ranges, data, output, inputs_grad, *refs):
    big, smalls, sems = refs[:10], refs[10:19], refs[19]
    at_down, at_units, at_out, at_gate, at_mix, at_small, _ = ranges
    width = data.shape[1]
    units = big[2].shape[0]

    def rows(start, height, left=0, wide=None):
        return data.at[pl.ds(start, height), pl.ds(left, width if wide is None else wide)]

    half = width // 2
    moves = [
        (output, big[0]),
        (inputs_grad, big[1]),
        (rows(at_units, units), big[2]),
        (rows(at_units + units, units), big[3]),
        (rows(at_down, units), big[4]),
        (rows(at_out, values), big[5]),
        (rows(at_gate, half, 0, values), big[6].at[pl.ds(0, half)]),
        (rows(at_gate, half, values, values), big[6].at[pl.ds(half, half)]),
        (rows(at_mix, width, 0, qk), big[7]),
        (rows(at_mix, width, qk, qk), big[8]),
        (rows(at_mix, width, 2 * qk, values), big[9]),
    ]
    moves = [pltpu.make_async_copy(src, dst, sems.at[i]) for i, (src, dst) in enumerate(moves)]
    for move in moves:
        move.start()
    norm1, norm2, head, rate, beta, decay, query, key, value = smalls
    small = data[at_small : at_small + 16]
    norm1[...] = small[4:5]
    norm2[...] = small[5:6]
    head[...] = small[6:7, 0:values]
    rate[...] = small[6:7, values : values + 2 * heads][:, heads:]
    beta[...] = small[8 : 8 + heads]
    decay[...] = small[8 + heads : 8 + 2 * heads]
    query[...] = small[0:4, 0:qk]
    key[...] = small[0:4, qk : 2 * qk]
    value[...] = small[0:4, 2 * qk :]
    for move in moves:
        move.wait()


def finish(data, output, inputs_grad, ranges, units, heads, qk, values):
    width = data.shape[1]
    length = output.shape[0]
    any_ = pl.BlockSpec(memory_space=pl.ANY)
    f32 = jnp.float32
    bigs = [
        (units, width), (units, width), (units, width), (values, width), (width, values), (width, qk), (width, qk), (width, values)
    ]
    smalls = [(1, width), (1, width), (1, values), (1, heads), (heads, width), (heads, width), (4, qk), (4, qk), (4, values)]
    held = [pltpu.with_memory_space_constraint(a, pltpu.VMEM) for a in (data, output, inputs_grad)]
    return pl.pallas_call(
        functools.partial(finish_kernel, heads, qk, values, ranges),
        out_shape=[jax.ShapeDtypeStruct((length, width), output.dtype), jax.ShapeDtypeStruct((length, width), f32)]
        + [jax.ShapeDtypeStruct(shape, f32) for shape in bigs + smalls],
        in_specs=[VM] * 3,
        out_specs=[any_] * 10 + [VM] * len(smalls),
        scratch_shapes=[pltpu.SemaphoreType.DMA((11,))],
        compiler_params=pltpu.CompilerParams(vmem_limit_bytes=8 << 20),
        name="finish",
    )(*held)


PAIR = 2


def unit_inverses(lowers, rows, cols):
    count = lowers[0].shape[0]
    near = (rows // 2 == cols // 2) & (rows > cols)
    inverses = [jnp.where(rows == cols, 1.0, jnp.where(near, -lower, 0.0)) for lower in lowers]
    block = 2
    while block < count:
        cross = (rows // (2 * block) == cols // (2 * block)) & (rows // block > cols // block)
        steps = [mm(inverse, jnp.where(cross, lower, 0.0)) for inverse, lower in zip(inverses, lowers)]
        inverses = [inverse - mm(step, inverse) for inverse, step in zip(inverses, steps)]
        block *= 2
    return inverses


def head_body(
    heads, key_dim, value_dim, begin, early, halfway,
    pre_ref, gate_ref, small_ref, taps_ref, rate_ref, gain_ref, w_out_ref, resid_ref, norm2_ref,
    w_gate_hbm, w_up_hbm, w_down_hbm,
    mixed_ref, core_ref, update_ref, state_ref, inverse_ref, resid1_ref, upstream_ref, hidden_ref, units_ref, part2_ref, ffn_ref,
    pad, now, solved_key, rise_query, key_tail, attend_all, ends,
    part, land_mate, land_across, half, sum_send, sum_recv,
    arrived, w_gate, w_up, w_down, gate_pre, up_pre, inner_grad, load_sem,
):
    length, width = pre_ref.shape
    span = SPAN
    chunks = length // span
    rows, cols = grids(span)
    qk = heads * key_dim
    n, _, me, t, _, _ = grid_place()
    _, mate, across = tensor_peers()
    loads = [(w_gate_hbm, w_gate), (w_up_hbm, w_up), (w_down_hbm, w_down)]
    loads = [pltpu.make_async_copy(src, dst, load_sem.at[i]) for i, (src, dst) in enumerate(loads)]
    for load in loads:
        load.start()
    total = TensorSum(part, resid1_ref, land_mate, land_across, half, sum_send, sum_recv)
    swap = begin
    pad[0:HALO] = jnp.zeros((HALO, width), jnp.float32)
    now[...] = jnp.zeros_like(now)

    def prepare_pair(turn):
        items = []
        for k in range(PAIR):
            index = turn * PAIR + k
            here = aligned(index * span, span)
            pad[HALO : HALO + span] = pre_ref[here, :]
            total_pre = conv_window(pad[...], taps_ref[...], span)
            pad[0:HALO] = pad[span : span + HALO]
            active = total_pre * sigmoid(total_pre)
            beta, _, _, cumul = gates_of(small_ref[here, :], rate_ref[...], heads, rows, cols)
            beta_t = jnp.transpose(beta)
            cumul_t = jnp.transpose(cumul)
            for head in range(heads):
                query = active[:, head * key_dim : (head + 1) * key_dim]
                query = query * (lax.rsqrt(jnp.sum(query * query, -1, keepdims=True) + EPS) * key_dim ** (-0.5))
                key = active[:, qk + head * key_dim : qk + (head + 1) * key_dim]
                key = key * lax.rsqrt(jnp.sum(key * key, -1, keepdims=True) + EPS)
                value = active[:, 2 * qk + head * value_dim : 2 * qk + (head + 1) * value_dim]
                beta_col = beta[:, head : head + 1]
                cum_col = cumul[:, heads + head : heads + head + 1]
                cum_row = cumul_t[heads + head : heads + head + 1]
                within = cols <= rows
                decays = jnp.where(within, jnp.exp(jnp.where(within, cum_col - cum_row, 0.0)), 0.0)
                scaled = decays * beta_t[head : head + 1]
                products = mm_nt(jnp.concatenate([query, key], 0), key)
                lower = jnp.where(cols < rows, scaled * products[span:], 0.0)
                attend = scaled * products[:span]
                last = cum_col[span - 1 : span]
                rise = jnp.exp(cum_col)
                narrow = slice(head * key_dim, (head + 1) * key_dim)
                attend_all[index, head] = attend
                rise_query[here, narrow] = rise * query
                key_tail[here, narrow] = key * (jnp.exp(last - cum_col) * beta_col)
                ends[index, head] = jnp.broadcast_to(jnp.exp(last), (8, 128))
                items.append((index, head, here, lower, jnp.concatenate([value, rise * key], 1)))
        inverses = unit_inverses([item[3] for item in items], rows, cols)
        solved = [mm(inverse, item[4]) for inverse, item in zip(inverses, items)]
        for (index, head, here, _, _), inverse, solution_ in zip(items, inverses, solved):
            inverse_ref[index, head] = inverse
            update_ref[here, head * value_dim : (head + 1) * value_dim] = solution_[:, :value_dim]
            solved_key[here, head * key_dim : (head + 1) * key_dim] = solution_[:, value_dim:]

    def chain(index):
        here = aligned(index * span, span)
        gate = gate_ref[here, :]
        gated = gate * sigmoid(gate) * gain_ref[...]
        for head in range(heads):
            narrow = slice(head * key_dim, (head + 1) * key_dim)
            wide = slice(head * value_dim, (head + 1) * value_dim)
            state = now[head]
            state_ref[state_place(index, head, heads, key_dim, value_dim, width)] = state
            both = mm(jnp.concatenate([solved_key[here, narrow], rise_query[here, narrow]], 0), state)
            update = update_ref[here, wide] - both[:span]
            now[head] = ends[index, head][0:1, 0:1] * state + mm_tn(key_tail[here, narrow], update)
            core = both[span:] + mm(attend_all[index, head], update)
            update_ref[here, wide] = update
            core_ref[here, wide] = core
            normed = core * lax.rsqrt(jnp.mean(core * core, -1, keepdims=True) + EPS)
            mixed_ref[here, wide] = (normed * gated[:, wide]).astype(mixed_ref.dtype)

    def chain_pair(turn):
        for k in range(PAIR):
            chain(turn * PAIR + k)

    def send_pair(turn):
        here = aligned(turn * PAIR * span, PAIR * span)
        part[here] = dot_plain(mixed_ref[here], w_out_ref[...])
        for k in range(PAIR):
            total.first(turn * PAIR + k).start()

    def cross_pair(turn):
        for k in range(PAIR):
            total.cross(turn * PAIR + k)

    def share_pair(turn):
        for k in range(PAIR):
            total.share(turn * PAIR + k, resid_ref)

    pairs = chunks // PAIR
    prepare_pair(0)

    def step(turn, carry):
        chain_pair(turn - 1)
        prepare_pair(turn)
        send_pair(turn - 1)

        cross_pair(turn - 1)

        @pl.when(turn > 1)
        def _():
            share_pair(turn - 2)

        return carry

    lax.fori_loop(1, pairs, step, 0)
    chain_pair(pairs - 1)
    send_pair(pairs - 1)
    cross_pair(pairs - 1)
    share_pair(pairs - 2)

    def gather(k, carry):
        swap.gather(k)
        return carry

    lax.fori_loop(0, n, gather, 0)

    swap.sent()
    swap.finish()

    def turn_low(i, carry):
        here = aligned(i * 64, 64)
        upstream_ref[here] = arrived[here].astype(upstream_ref.dtype)
        return carry

    lax.fori_loop(0, length // 64, turn_low, 0)
    for load in loads:
        load.wait()
    units = w_gate.shape[0]
    whole = units // 128 * 128
    low = units_ref.dtype
    units_ref[:, :, whole:] = jnp.zeros((3, length, units_ref.shape[2] - whole), low)
    some = length // 2

    def feed(first):
        def norm(i, carry):
            here = aligned(first + i * 64, 64)
            value = resid1_ref[here]
            scale = lax.rsqrt(jnp.mean(value * value, -1, keepdims=True) + EPS)
            hidden_ref[here] = (value * scale * norm2_ref[...]).astype(low)
            return carry

        lax.fori_loop(0, some // 64, norm, 0)
        block = pl.ds(first, some)
        gate_pre[...] = dot_nt(hidden_ref[block], w_gate[...])
        up_pre[...] = dot_nt(hidden_ref[block], w_up[...])
        inner_grad[...] = dot_nt(upstream_ref[block], w_down[...])

        def bend(i, carry):
            at = aligned(i * 64, 64)
            here = aligned(first + i * 64, 64)
            gate = gate_pre[at]
            upper = up_pre[at]
            grad = inner_grad[at]
            sig = sigmoid(gate)
            silu = gate * sig
            units_ref[0, here, 0:units] = (silu * upper).astype(low)
            units_ref[1, here, 0:units] = (grad * upper * (sig * (1.0 + gate * (1.0 - sig)))).astype(low)
            units_ref[2, here, 0:units] = (grad * silu).astype(low)
            return carry

        lax.fori_loop(0, some // 64, bend, 0)
        part2_ref[block] = dot_plain(units_ref[1, block, 0:units], w_gate[...]) + dot_plain(
            units_ref[2, block, 0:units], w_up[...]
        )
        ffn_ref[block] = dot_plain(units_ref[0, block, 0:units], w_down[...])

    early()
    for block in range(BLOCKS // 2):
        total.third(block).wait_recv()
    feed(0)
    halfway()
    share_pair(pairs - 1)
    total.finish(BLOCKS // 2)
    feed(some)


def front_kernel(
    heads, key_dim, value_dim,
    x_ref, norm1_ref, beta_ref, decay_ref, rate_ref, taps_q, taps_k, taps_v, gain_ref, cotangent_ref, norm2_ref,
    query_hbm, key_hbm, value_hbm, gate_hbm, w_out_hbm, w_gate_hbm, w_up_hbm, w_down_hbm,
    low_out, hidden1_out, pre_out, gate_out, small_out, w_small_out,
    mixed_out, core_out, update_out, state_out, inverse_out, upstream_out, resid1_out,
    hidden2_out, units_out, part2_out, ffn_out, taps_ref, rate_row_ref,
    low, hidden1, pre, gate_pre, small, w_small, mixed, core, update, state, inverse, upstream, resid1,
    hidden2, units, part2, ffn, w_out,
    w_mix, w_gate_mix, rows16, staged, arrived, send, recv, close_send, close_recv, load_sem,
    pad, now, solved_key, rise_query, key_tail, attend_all, ends,
    part, land_mate, land_across, half, sum_send, sum_recv,
    staged2, arrived2, send2, recv2, close_send2, close_recv2,
    w_gate, w_up, w_down, gate_in, up_in, inner_grad, load_sem2, out_sem,
):
    load_w_out = pltpu.make_async_copy(w_out_hbm, w_out, out_sem.at[0])
    load_w_out.start()
    cotangents = PlaneSwap(staged2, arrived2, send2, recv2, close_send2, close_recv2)

    def between():
        for place in range(cotangents.n):
            mine = cotangents.at(place, cotangents.core)
            staged2[mine] = cotangent_ref[mine].astype(jnp.float32)
        cotangents.start()

    prep_part(
        heads, between, x_ref, norm1_ref, query_hbm, key_hbm, value_hbm, gate_hbm, beta_ref, decay_ref, rate_ref,
        taps_q, taps_k, taps_v, low, hidden1, pre, gate_pre, small, w_small, taps_ref, rate_row_ref,
        w_mix, w_gate_mix, rows16, staged, arrived, send, recv, close_send, close_recv, load_sem,
    )
    pairs = [
        (low, low_out), (hidden1, hidden1_out), (pre, pre_out), (gate_pre, gate_out), (small, small_out),
        (w_small, w_small_out),
    ]
    later = [
        (mixed, mixed_out), (core, core_out), (update, update_out), (state, state_out), (inverse, inverse_out),
        (upstream, upstream_out),
    ]
    rows = hidden2.shape[0]
    halves = [pl.ds(0, rows // 2), pl.ds(rows // 2, rows // 2)]
    last = [
        [
            (hidden2.at[span], hidden2_out.at[span]), (part2.at[span], part2_out.at[span]), (ffn.at[span], ffn_out.at[span]),
            (resid1.at[span], resid1_out.at[span]),
        ]
        + [(units.at[k, span], units_out.at[k, span]) for k in range(3)]
        for span in halves
    ]
    every = pairs + later + last[0] + last[1]
    copies = [pltpu.make_async_copy(src, dst, out_sem.at[1 + i]) for i, (src, dst) in enumerate(every)]
    one, two, three = len(pairs), len(pairs) + len(later), len(pairs) + len(later) + len(last[0])

    def begin_copies(start, stop):
        for copy in copies[start:stop]:
            copy.start()

    begin_copies(0, one)
    load_w_out.wait()
    head_body(
        heads, key_dim, value_dim, cotangents, lambda: begin_copies(one, two), lambda: begin_copies(two, three),
        pre, gate_pre, small, taps_ref, rate_row_ref, gain_ref, w_out, low, norm2_ref, w_gate_hbm, w_up_hbm, w_down_hbm,
        mixed, core, update, state, inverse, resid1, upstream, hidden2, units, part2, ffn,
        pad, now, solved_key, rise_query, key_tail, attend_all, ends,
        part, land_mate, land_across, half, sum_send, sum_recv,
        arrived2, w_gate, w_up, w_down, gate_in, up_in, inner_grad, load_sem2,
    )
    begin_copies(three, len(copies))
    for copy in copies:
        copy.wait()


def front(
    x, cotangent, norm1, norm2, w_query, w_key, w_value, w_gate, w_beta_t, w_decay_t, rate, taps_q, taps_k, taps_v, gain,
    w_out, w_gate_t, w_up_t, w_down, heads, key_dim, value_dim, places, collective_id,
):
    length, width = x.shape
    values = heads * value_dim
    qk = heads * key_dim
    lanes = 128
    chunks = length // SPAN
    units = w_down.shape[0]
    padded = -(-units // 128) * 128
    f32, bf = jnp.float32, jnp.bfloat16
    dma = pltpu.SemaphoreType.DMA
    any_ = pl.BlockSpec(memory_space=pl.ANY)
    shapes = [
        ((length, width), bf),
        ((length, width), bf),
        ((length, width), f32),
        ((length, values), f32),
        ((length, lanes), f32),
        ((lanes, width), bf),
        ((length, values), bf),
        ((length, values), f32),
        ((length, values), f32),
        ((chunks * heads * key_dim * value_dim // width, width), f32),
        ((chunks, heads, SPAN, SPAN), f32),
        ((length, width), bf),
        ((length, width), f32),
        ((length, width), bf),
        ((3, length, padded), bf),
        ((length, width), f32),
        ((length, width), f32),
    ]
    smalls = [((taps_q.shape[0], width), f32), ((1, lanes), f32)]
    vmem = [
        (w_out.shape, bf),
        ((width, width), bf),
        ((width, values), bf),
        ((16, width), f32),
        ((length, width), f32),
        ((length, width), f32),
    ]
    swap_sems = [dma((places,)), dma((places,)), dma((3, places)), dma((3, places))]
    more = [
        ((HALO + SPAN, width), f32),
        ((heads, key_dim, value_dim), f32),
        ((length, qk), f32),
        ((length, qk), f32),
        ((length, qk), f32),
        ((chunks, heads, SPAN, SPAN), f32),
        ((chunks, heads, 8, 128), f32),
        ((length, width), f32),
        ((length // 2, width), f32),
        ((length // 2, width), f32),
        ((length // 2, width), f32),
    ]
    last = [((units, width), bf)] * 3 + [((length // 2, units), f32)] * 3

    def scratch(items):
        return [pltpu.VMEM(shape, kind) for shape, kind in items]

    return pl.pallas_call(
        functools.partial(front_kernel, heads, key_dim, value_dim),
        out_shape=[jax.ShapeDtypeStruct(shape, kind) for shape, kind in shapes + smalls],
        in_specs=[VM] * 11 + [any_] * 8,
        out_specs=[any_] * len(shapes) + [VM] * len(smalls),
        scratch_shapes=scratch(shapes) + scratch(vmem) + swap_sems + [dma((4,))] + scratch(more)
        + [dma((3, BLOCKS)), dma((3, BLOCKS))] + scratch([((length, width), f32)] * 2) + swap_sems + scratch(last)
        + [dma((3,)), dma((32,))],
        compiler_params=pltpu.CompilerParams(
            collective_id=collective_id, has_side_effects=True, vmem_limit_bytes=67043328
        ),
        name="front",
    )(
        x, norm1, w_beta_t, w_decay_t, rate, taps_q, taps_k, taps_v, gain, cotangent, norm2,
        w_query, w_key, w_value, w_gate, w_out, w_gate_t, w_up_t, w_down,
    )


def prep_part(
    heads, between,
    x_ref, norm1_ref, query_hbm, key_hbm, value_hbm, gate_hbm, beta_ref, decay_ref, rate_ref, taps_q, taps_k, taps_v,
    low_ref, hidden_ref, pre_ref, gate_pre_ref, small_ref, w_small_ref, taps_ref, rate_row_ref,
    w_mix, w_gate, rows16, staged, arrived, send, recv, close_send, close_recv, load_sem,
):
    length, width = x_ref.shape
    qk = query_hbm.shape[1]
    values = value_hbm.shape[1]
    n, _, me, t, _, _ = grid_place()
    _, mate, across = tensor_peers()
    peers = [(lax.rem(me + k, n), t) for k in range(1, n)] + [mate, across]
    call_out(peers)
    loads = [
        (query_hbm, w_mix.at[:, pl.ds(0, qk)]),
        (key_hbm, w_mix.at[:, pl.ds(qk, qk)]),
        (value_hbm, w_mix.at[:, pl.ds(2 * qk, values)]),
        (gate_hbm, w_gate),
    ]
    loads = [pltpu.make_async_copy(src, dst, load_sem.at[i]) for i, (src, dst) in enumerate(loads)]
    for load in loads:
        load.start()
    swap = Swap(staged, arrived, send, recv, close_send, close_recv)
    for place in range(n):
        mine = swap.at(place, t)
        staged[mine] = x_ref[mine].astype(jnp.float32)
    hear_all(peers)
    swap.start()
    taps_ref[:, 0:qk] = taps_q[...]
    taps_ref[:, qk : 2 * qk] = taps_k[...]
    taps_ref[:, 2 * qk :] = taps_v[...]
    lanes = rate_row_ref.shape[1]
    lane = lax.broadcasted_iota(jnp.int32, (1, lanes), 1)
    row = jnp.zeros((1, lanes), jnp.float32)
    for head in range(heads):
        row = jnp.where(lane == heads + head, rate_ref[:, head : head + 1], row)
    rate_row_ref[...] = row
    rows16[...] = jnp.zeros_like(rows16)
    rows16[0:heads] = beta_ref[...].astype(jnp.float32)
    rows16[heads : 2 * heads] = decay_ref[...].astype(jnp.float32)
    w_small_ref[...] = jnp.zeros_like(w_small_ref)
    w_small_ref[0:16] = rows16[...].astype(w_small_ref.dtype)

    def gather(k, carry):
        swap.gather(k)
        return carry

    def forward(k, carry):
        swap.forward(k)
        return carry

    lax.fori_loop(0, n, gather, 0)
    between()
    lax.fori_loop(0, n, forward, 0)
    for load in loads:
        load.wait()
    swap.sent()
    swap.finish()

    def norm(i, carry):
        here = aligned(i * 64, 64)
        value = arrived[here]
        low_ref[here] = value.astype(low_ref.dtype)
        scale = lax.rsqrt(jnp.mean(value * value, -1, keepdims=True) + EPS)
        hidden_ref[here] = (value * scale * norm1_ref[...]).astype(hidden_ref.dtype)
        return carry

    lax.fori_loop(0, length // 64, norm, 0)

    def mix_tile(i, carry):
        tile = aligned(i * 256, 256)
        pre_ref[:, tile] = dot_plain(hidden_ref[...], w_mix[:, tile])
        return carry

    def gate_tile(i, carry):
        tile = aligned(i * 256, 256)
        gate_pre_ref[:, tile] = dot_plain(hidden_ref[...], w_gate[:, tile])
        return carry

    lax.fori_loop(0, width // 256, mix_tile, 0)
    lax.fori_loop(0, values // 256, gate_tile, 0)
    small_ref[...] = dot_nt(hidden_ref[...], w_small_ref[...])


def whole_sequences(
    inputs,
    norm1_gain,
    w_query,
    w_key,
    w_value,
    w_gate,
    w_beta,
    w_decay,
    decay_rate,
    conv_query,
    conv_key,
    conv_value,
    head_gain,
    w_out,
    norm2_gain,
    w_ffn_gate,
    w_ffn_up,
    w_ffn_down,
    cotangent,
):
    batch, seg, width = inputs.shape
    count = batch * seg
    heads = decay_rate.shape[0]
    key_dim = w_query.shape[1] // heads
    value_dim = w_value.shape[1] // heads
    qk_width = heads * key_dim
    places = lax.axis_size("dp")
    gain = head_gain[None]
    (
        resid, hidden1, pre, gate_pre, small, w_small, mixed, core, update, states, inverses, upstream, resid1,
        hidden2, units, part2, ffn, taps, rate,
    ) = front(
        inputs.reshape(count, width), cotangent.reshape(count, width), norm1_gain[None], norm2_gain[None],
        w_query, w_key, w_value, w_gate, w_beta.T, w_decay.T, decay_rate[None], conv_query, conv_key, conv_value, gain,
        w_out, w_ffn_gate.T, w_ffn_up.T, w_ffn_down, heads, key_dim, value_dim, places, 2,
    )
    held, ranges = tail(
        part2, ffn, pre, core, update, states, resid1, upstream, resid, mixed, hidden1, hidden2, units,
        w_out, w_query, w_key, w_value, w_gate, w_small, gate_pre, small, inverses,
        norm1_gain[None], norm2_gain[None], taps, rate, gain,
        heads, key_dim, value_dim, w_ffn_down.shape[0], places, 7,
    )
    (
        output, grad_inputs, fgate, fup, grad_down, grad_out_w, grad_gate_w, grad_query_w, grad_key_w, grad_value_w,
        grad_norm1_gain, grad_norm2_gain, grad_head, grad_rate, grad_beta_w, grad_decay_w,
        grad_convq, grad_convk, grad_convv,
    ) = finish(*held, ranges, w_ffn_down.shape[0], heads, qk_width, heads * value_dim)
    return (
        output.reshape(batch, seg, width),
        grad_inputs.reshape(batch, seg, width),
        grad_norm1_gain[0],
        grad_query_w,
        grad_key_w,
        grad_value_w,
        grad_gate_w,
        grad_beta_w.T,
        grad_decay_w.T,
        grad_rate[0],
        grad_convq,
        grad_convk,
        grad_convv,
        grad_head[0],
        grad_out_w,
        grad_norm2_gain[0],
        fgate.T,
        fup.T,
        grad_down,
    )


def fits_whole(mesh, args):
    batch, length, width = args[0].shape
    places, ranks = mesh.shape["dp"], mesh.shape["tensor"]
    heads = args[8].shape[0] // ranks
    qk = args[2].shape[1] // ranks
    values = args[4].shape[1] // ranks
    units = args[15].shape[1] // ranks
    return (
        batch == places and places == 8 and ranks == 4 and length == places * SPAN and BLOCKS == places and heads <= 4
        and width == 2 * qk + values and width == 2 * values and width % 512 == 0 and length % 256 == 0
        and units % 64 == 0 and values % 256 == 0
        and length // SPAN * args[2].shape[1] // ranks * (values // heads) <= values * width
    )


def solution(mesh):
    placed = (
        P(None, "dp", None),
        P(),
        P(None, "tensor"),
        P(None, "tensor"),
        P(None, "tensor"),
        P(None, "tensor"),
        P(None, "tensor"),
        P(None, "tensor"),
        P("tensor"),
        P(None, "tensor"),
        P(None, "tensor"),
        P(None, "tensor"),
        P("tensor"),
        P("tensor", None),
        P(),
        P(None, "tensor"),
        P(None, "tensor"),
        P("tensor", None),
        P(None, "dp", None),
    )
    def step(*args):
        body = whole_sequences if fits_whole(mesh, args) else shards
        return placed_step(body)(*args)

    def placed_step(body):
      return jax.shard_map(
        body,
        mesh=mesh,
        in_specs=placed,
        out_specs=(
            P(None, "dp", None),
            P(None, "dp", None),
            P(),
            P(None, "tensor"),
            P(None, "tensor"),
            P(None, "tensor"),
            P(None, "tensor"),
            P(None, "tensor"),
            P(None, "tensor"),
            P("tensor"),
            P(None, "tensor"),
            P(None, "tensor"),
            P(None, "tensor"),
            P("tensor"),
            P("tensor", None),
            P(),
            P(None, "tensor"),
            P(None, "tensor"),
            P("tensor", None),
        ),
        check_vma=False,
    )

    return step
```

```python
import functools
from functools import partial

import jax
import jax.numpy as jnp
from jax import lax
from jax.experimental import pallas as pl
from jax.experimental.pallas import tpu as pltpu
from jax.sharding import PartitionSpec as P

SPAN = 64


EPS = 1e-06


def from_behind(shard, axis, by):
    count = lax.axis_size(axis)
    pairs = [(i, i + by) for i in range(count) if 0 <= i + by < count]
    return lax.ppermute(shard, axis, pairs)


def carried_in(part, axis, combine, identity, reverse):
    count = lax.axis_size(axis)
    place = lax.axis_index(axis)
    ahead = count - 1 - place if reverse else place
    gathered = jax.tree.map(lambda a: lax.all_gather(a, axis), part)
    state = jax.tree.map(lambda a, e: jnp.zeros_like(a) + jnp.asarray(e, a.dtype), part, identity)

    def one(turn, state):
        source = count - 1 - turn if reverse else turn
        return combine(
            state, jax.tree.map(lambda a: lax.dynamic_index_in_dim(a, source, 0, False), gathered)
        )

    return lax.fori_loop(0, ahead, one, state)


def exact(left, right):
    return jnp.matmul(left, right, precision=lax.Precision.HIGHEST)


def span_apply(state, inputs):
    query, key, values, beta, logdecay = inputs
    count = query.shape[0]
    cumul = jnp.cumsum(logdecay)
    row_ids = lax.broadcasted_iota(jnp.int32, (count, count), 0)
    col_ids = lax.broadcasted_iota(jnp.int32, (count, count), 1)
    within = col_ids <= row_ids
    strict = col_ids < row_ids
    spread = jnp.where(within, cumul[:, None] - cumul[None, :], 0.0)
    decays = jnp.where(within, jnp.exp(spread), 0.0)
    scaled = decays * beta[None, :]
    lower = jnp.where(strict, scaled * exact(key, key.T), 0.0)
    start_decay = jnp.exp(cumul)[:, None]
    right_side = values - start_decay * exact(key, state)
    system = jnp.eye(count, dtype=lower.dtype) + lower
    update = jax.scipy.linalg.solve_triangular(system, right_side, lower=True, unit_diagonal=True)
    output = start_decay * exact(query, state) + exact(scaled * exact(query, key.T), update)
    tail = jnp.exp(cumul[-1] - cumul) * beta
    new_state = jnp.exp(cumul[-1]) * state + exact((key * tail[:, None]).T, update)
    return (new_state, output)


def run_segment(query, key, values, beta, logdecay, state):
    length = query.shape[0]
    blocks = length // SPAN

    def split(array):
        return array.reshape((blocks, SPAN) + array.shape[1:])

    final, outputs = lax.scan(
        span_apply, state, (split(query), split(key), split(values), split(beta), split(logdecay))
    )
    return (outputs.reshape((length,) + outputs.shape[2:]), final)


def run_heads(query, key, values, beta, logdecay, state):
    return jax.vmap(jax.vmap(run_segment))(query, key, values, beta, logdecay, state)


def prepare(extended, beta_pre, decay_pre, conv_all, decay_rate, key_dim):
    batch, seg, heads = beta_pre.shape
    reach = conv_all.shape[0] - 1
    total = conv_all[0] * extended[:, 0:seg, :]
    for offset in range(1, reach + 1):
        total = total + conv_all[offset] * extended[:, offset : offset + seg, :]
    active = jax.nn.silu(total)
    qk_width = heads * key_dim
    query = active[..., :qk_width].reshape(batch, seg, heads, key_dim)
    key = active[..., qk_width : 2 * qk_width].reshape(batch, seg, heads, key_dim)
    values = active[..., 2 * qk_width :].reshape(batch, seg, heads, -1)
    query = query * lax.rsqrt(jnp.sum(query * query, -1, keepdims=True) + EPS) * key_dim ** (-0.5)
    key = key * lax.rsqrt(jnp.sum(key * key, -1, keepdims=True) + EPS)
    beta = jax.nn.sigmoid(beta_pre)
    logdecay = -decay_rate * jax.nn.softplus(decay_pre)
    return (
        jnp.moveaxis(query, 2, 1),
        jnp.moveaxis(key, 2, 1),
        jnp.moveaxis(values, 2, 1),
        jnp.moveaxis(beta, 2, 1),
        jnp.moveaxis(logdecay, 2, 1),
    )


def gate_norm(core, gate_pre, head_gain):
    normed = core * lax.rsqrt(jnp.mean(core * core, -1, keepdims=True) + EPS)
    return normed * head_gain * jax.nn.silu(gate_pre)


def rms_apply(resid, gain):
    return resid * lax.rsqrt(jnp.mean(resid * resid, -1, keepdims=True) + EPS) * gain


def swiglu(gate, upper):
    return jax.nn.silu(gate) * upper


def project(left, right):
    return jnp.dot(left, right, preferred_element_type=jnp.float32)


def contract_rows(left, right):
    return jnp.einsum("ra,rb->ab", left, right, preferred_element_type=jnp.float32)


def back_project(grad, weight):
    return jnp.einsum("rb,ab->ra", grad, weight, preferred_element_type=jnp.float32)


def compose(earlier, later):
    return (exact(later[0], earlier[0]), exact(later[0], earlier[1]) + later[1])


def shards(
    inputs,
    norm1_gain,
    w_query,
    w_key,
    w_value,
    w_gate,
    w_beta,
    w_decay,
    decay_rate,
    conv_query,
    conv_key,
    conv_value,
    head_gain,
    w_out,
    norm2_gain,
    w_ffn_gate,
    w_ffn_up,
    w_ffn_down,
    cotangent,
):
    batch, seg, width = inputs.shape
    count = batch * seg
    heads = decay_rate.shape[0]
    key_dim = w_query.shape[1] // heads
    value_dim = w_value.shape[1] // heads
    qk_width = heads * key_dim
    reach = conv_query.shape[0] - 1
    bf = jnp.bfloat16
    resid = inputs.reshape(count, width).astype(jnp.float32)
    normed1, norm1_back = jax.vjp(rms_apply, resid, norm1_gain)
    hidden1 = normed1.astype(bf)
    query_pre = project(hidden1, w_query)
    key_pre = project(hidden1, w_key)
    value_pre = project(hidden1, w_value)
    gate_pre = project(hidden1, w_gate)
    beta_pre = project(hidden1, w_beta)
    decay_pre = project(hidden1, w_decay)
    mixed_pre = jnp.concatenate([query_pre, key_pre, value_pre], axis=1).reshape(batch, seg, -1)
    rim = from_behind(mixed_pre[:, seg - reach :, :], "dp", 1)
    extended = jnp.concatenate([rim, mixed_pre], axis=1)
    conv_all = jnp.concatenate([conv_query, conv_key, conv_value], axis=1)
    features, prep_back = jax.vjp(
        partial(prepare, key_dim=key_dim),
        extended,
        beta_pre.reshape(batch, seg, heads),
        decay_pre.reshape(batch, seg, heads),
        conv_all,
        decay_rate,
    )
    query_h, key_h, value_h, beta_h, decay_h = features
    eye_block = jnp.broadcast_to(
        jnp.eye(key_dim, dtype=jnp.float32), (batch, heads, key_dim, key_dim)
    )
    zero_block = jnp.zeros((batch, heads, key_dim, value_dim), jnp.float32)
    values_aug = jnp.concatenate(
        [jnp.zeros(value_h.shape[:3] + (key_dim,), jnp.float32), value_h], axis=-1
    )
    state_aug = jnp.concatenate([eye_block, zero_block], axis=-1)
    outputs_aug, final_aug = run_heads(query_h, key_h, values_aug, beta_h, decay_h, state_aug)
    out_carry = outputs_aug[..., :key_dim]
    out_local = outputs_aug[..., key_dim:]
    transition = final_aug[..., :key_dim]
    offset_part = final_aug[..., key_dim:]
    prefix = carried_in((transition, offset_part), "dp", compose, (eye_block, zero_block), False)
    start_state = prefix[1]
    core = jnp.moveaxis(exact(out_carry, start_state) + out_local, 1, 2)
    gate4 = gate_pre.reshape(batch, seg, heads, value_dim)
    gated, gate_back = jax.vjp(gate_norm, core, gate4, head_gain.reshape(heads, value_dim))
    mixed = gated.reshape(count, heads * value_dim).astype(bf)
    attention = lax.psum(project(mixed, w_out), "tensor")
    resid1 = resid + attention
    normed2, norm2_back = jax.vjp(rms_apply, resid1, norm2_gain)
    hidden2 = normed2.astype(bf)
    ffn_gate = project(hidden2, w_ffn_gate)
    ffn_up = project(hidden2, w_ffn_up)
    inner_full, swiglu_back = jax.vjp(swiglu, ffn_gate, ffn_up)
    inner = inner_full.astype(bf)
    ffn = lax.psum(project(inner, w_ffn_down), "tensor")
    output = (resid1 + ffn).astype(bf).reshape(batch, seg, width)
    upstream = cotangent.reshape(count, width)
    grad_down = contract_rows(inner, upstream)
    grad_inner = back_project(upstream, w_ffn_down)
    grad_fgate, grad_fup = swiglu_back(grad_inner)
    grad_fgate = grad_fgate.astype(bf)
    grad_fup = grad_fup.astype(bf)
    grad_ffn_gate_w = contract_rows(hidden2, grad_fgate)
    grad_ffn_up_w = contract_rows(hidden2, grad_fup)
    grad_hidden2 = lax.psum(
        back_project(grad_fgate, w_ffn_gate) + back_project(grad_fup, w_ffn_up), "tensor"
    )
    grad_from_norm2, grad_norm2_gain = norm2_back(grad_hidden2)
    grad_resid1 = upstream.astype(jnp.float32) + grad_from_norm2
    grad_resid1_low = grad_resid1.astype(bf)
    grad_out_w = contract_rows(mixed, grad_resid1_low)
    grad_mixed = back_project(grad_resid1_low, w_out).reshape(batch, seg, heads, value_dim)
    grad_core, grad_gate4, grad_head_gain = gate_back(grad_mixed)
    grad_core_h = jnp.moveaxis(grad_core, 2, 1)
    carry_term = exact(jnp.swapaxes(out_carry, -1, -2), grad_core_h)
    suffix = carried_in(
        (jnp.swapaxes(transition, -1, -2), carry_term), "dp", compose, (eye_block, zero_block), True
    )

    def local_delta(query, key, values, beta, logdecay):
        return run_heads(query, key, values, beta, logdecay, start_state)

    recomputed, delta_back = jax.vjp(local_delta, query_h, key_h, value_h, beta_h, decay_h)
    feature_grads = delta_back((grad_core_h, suffix[1]))
    grad_ext, grad_beta_in, grad_decay_in, grad_conv, grad_rate = prep_back(feature_grads)
    returned = from_behind(grad_ext[:, :reach, :], "dp", -1)
    grad_mixed_pre = grad_ext[:, reach:, :] + jnp.pad(returned, ((0, 0), (seg - reach, 0), (0, 0)))
    grad_mixed_pre = grad_mixed_pre.reshape(count, -1)
    grad_query_low = grad_mixed_pre[:, :qk_width].astype(bf)
    grad_key_low = grad_mixed_pre[:, qk_width : 2 * qk_width].astype(bf)
    grad_value_low = grad_mixed_pre[:, 2 * qk_width :].astype(bf)
    grad_gate_low = grad_gate4.reshape(count, heads * value_dim).astype(bf)
    grad_beta_low = grad_beta_in.reshape(count, heads).astype(bf)
    grad_decay_low = grad_decay_in.reshape(count, heads).astype(bf)
    partial_hidden1 = (
        back_project(grad_query_low, w_query)
        + back_project(grad_key_low, w_key)
        + back_project(grad_value_low, w_value)
        + back_project(grad_gate_low, w_gate)
        + back_project(grad_beta_low, w_beta)
        + back_project(grad_decay_low, w_decay)
    )
    grad_hidden1 = lax.psum(partial_hidden1, "tensor")
    grad_from_norm1, grad_norm1_gain = norm1_back(grad_hidden1)
    grad_inputs = (grad_resid1 + grad_from_norm1).reshape(batch, seg, width)
    grad_query_w = contract_rows(hidden1, grad_query_low)
    grad_key_w = contract_rows(hidden1, grad_key_low)
    grad_value_w = contract_rows(hidden1, grad_value_low)
    grad_gate_w = contract_rows(hidden1, grad_gate_low)
    grad_beta_w = contract_rows(hidden1, grad_beta_low)
    grad_decay_w = contract_rows(hidden1, grad_decay_low)
    grad_convq = grad_conv[:, :qk_width]
    grad_convk = grad_conv[:, qk_width : 2 * qk_width]
    grad_convv = grad_conv[:, 2 * qk_width :]
    grad_head_flat = grad_head_gain.reshape(-1)
    (
        grad_norm1_gain,
        grad_query_w,
        grad_key_w,
        grad_value_w,
        grad_gate_w,
        grad_beta_w,
        grad_decay_w,
        grad_rate,
        grad_convq,
        grad_convk,
        grad_convv,
        grad_head_flat,
        grad_out_w,
        grad_norm2_gain,
        grad_ffn_gate_w,
        grad_ffn_up_w,
        grad_down,
    ) = lax.psum(
        (
            grad_norm1_gain,
            grad_query_w,
            grad_key_w,
            grad_value_w,
            grad_gate_w,
            grad_beta_w,
            grad_decay_w,
            grad_rate,
            grad_convq,
            grad_convk,
            grad_convv,
            grad_head_flat,
            grad_out_w,
            grad_norm2_gain,
            grad_ffn_gate_w,
            grad_ffn_up_w,
            grad_down,
        ),
        "dp",
    )
    return (
        output,
        grad_inputs,
        grad_norm1_gain,
        grad_query_w,
        grad_key_w,
        grad_value_w,
        grad_gate_w,
        grad_beta_w,
        grad_decay_w,
        grad_rate,
        grad_convq,
        grad_convk,
        grad_convv,
        grad_head_flat,
        grad_out_w,
        grad_norm2_gain,
        grad_ffn_gate_w,
        grad_ffn_up_w,
        grad_down,
    )


HALO = 8


def mm(left, right):
    return lax.dot_general(
        left, right, (((1,), (0,)), ((), ())),
        precision=lax.Precision.HIGHEST, preferred_element_type=jnp.float32,
    )


def mm_nt(left, right):
    return lax.dot_general(
        left, right, (((1,), (1,)), ((), ())),
        precision=lax.Precision.HIGHEST, preferred_element_type=jnp.float32,
    )


def mm_tn(left, right):
    return lax.dot_general(
        left, right, (((0,), (0,)), ((), ())),
        precision=lax.Precision.HIGHEST, preferred_element_type=jnp.float32,
    )


def grids(count):
    rows = lax.broadcasted_iota(jnp.int32, (count, count), 0)
    cols = lax.broadcasted_iota(jnp.int32, (count, count), 1)
    return rows, cols


def unit_inverse(lower, rows, cols):
    count = lower.shape[0]
    near = (rows // 2 == cols // 2) & (rows > cols)
    inverse = jnp.where(rows == cols, 1.0, jnp.where(near, -lower, 0.0))
    block = 2
    while block < count:
        cross = (rows // (2 * block) == cols // (2 * block)) & (rows // block > cols // block)
        inverse = inverse - mm(mm(inverse, jnp.where(cross, lower, 0.0)), inverse)
        block *= 2
    return inverse


def conv_window(halo_block, taps, span):
    reach = taps.shape[0] - 1
    total = None
    for offset in range(reach + 1):
        start = HALO - reach + offset
        term = taps[offset : offset + 1] * halo_block[start : start + span]
        total = term if total is None else total + term
    return total


def sigmoid(value):
    return 1.0 / (1.0 + jnp.exp(-value))


def softplus(value):
    return jnp.maximum(value, 0.0) + jnp.log(1.0 + jnp.exp(-jnp.abs(value)))


def gates_of(small, rate, heads, rows, cols):
    beta = sigmoid(small)
    slope = softplus(small)
    logdecay = -rate * slope
    cumul = mm(jnp.where(cols <= rows, 1.0, 0.0), logdecay)
    return beta, slope, logdecay, cumul


def state_place(index, head, heads, key_dim, value_dim, width):
    across = width // value_dim
    turn = index * heads + head
    return (
        pl.ds(pl.multiple_of(lax.div(turn, across) * key_dim, key_dim), key_dim),
        pl.ds(pl.multiple_of(lax.rem(turn, across) * value_dim, value_dim), value_dim),
    )


def chunk_terms(query, key, beta_col, beta_row, cum_col, cum_row, rows, cols):
    within = cols <= rows
    decays = jnp.where(within, jnp.exp(jnp.where(within, cum_col - cum_row, 0.0)), 0.0)
    scaled = decays * beta_row
    key_key = mm_nt(key, key)
    query_key = mm_nt(query, key)
    lower = jnp.where(cols < rows, scaled * key_key, 0.0)
    attend = scaled * query_key
    return decays, scaled, key_key, query_key, lower, attend


def forward_kernel(heads, key_dim, value_dim, pre_ref, gate_ref, small_ref, taps_ref, rate_ref, gain_ref,
                   mixed_ref, core_ref, update_ref, state_ref, inverse_ref, pad_ref, now_ref):
    length, width = pre_ref.shape
    span = SPAN
    chunks = length // span
    rows, cols = grids(span)
    qk = heads * key_dim
    pad_ref[0:HALO] = jnp.zeros((HALO, width), jnp.float32)
    for head in range(heads):
        now_ref[head] = jnp.zeros((key_dim, value_dim), jnp.float32)

    def chunk(index, carry):
        start = pl.multiple_of(index * span, span)
        here = pl.ds(start, span)
        pad_ref[HALO : HALO + span] = pre_ref[here, :]
        total = conv_window(pad_ref[...], taps_ref[...], span)
        pad_ref[0:HALO] = pad_ref[span : span + HALO]
        active = total * sigmoid(total)
        beta, _, _, cumul = gates_of(small_ref[here, :], rate_ref[...], heads, rows, cols)
        beta_t = jnp.transpose(beta)
        cumul_t = jnp.transpose(cumul)
        gate = gate_ref[here, :]
        gated = gate * sigmoid(gate) * gain_ref[...]
        for head in range(heads):
            query = active[:, head * key_dim : (head + 1) * key_dim]
            query = query * (lax.rsqrt(jnp.sum(query * query, -1, keepdims=True) + EPS) * key_dim ** (-0.5))
            key = active[:, qk + head * key_dim : qk + (head + 1) * key_dim]
            key = key * lax.rsqrt(jnp.sum(key * key, -1, keepdims=True) + EPS)
            value = active[:, 2 * qk + head * value_dim : 2 * qk + (head + 1) * value_dim]
            beta_col = beta[:, head : head + 1]
            beta_row = beta_t[head : head + 1]
            cum_col = cumul[:, heads + head : heads + head + 1]
            cum_row = cumul_t[heads + head : heads + head + 1]
            _, _, _, _, lower, attend = chunk_terms(query, key, beta_col, beta_row, cum_col, cum_row, rows, cols)
            inverse = unit_inverse(lower, rows, cols)
            state = now_ref[head]
            state_ref[state_place(index, head, heads, key_dim, value_dim, width)] = state
            rise = jnp.exp(cum_col)
            last = cum_col[span - 1 : span]
            update = mm(inverse, value) - mm(mm(inverse, rise * key), state)
            core = mm(rise * query, state) + mm(attend, update)
            tail = jnp.exp(last - cum_col) * beta_col
            now_ref[head] = jnp.exp(last) * state + mm_tn(key * tail, update)
            inverse_ref[index, head] = inverse
            wide = slice(head * value_dim, (head + 1) * value_dim)
            update_ref[here, wide] = update
            core_ref[here, wide] = core
            normed = core * lax.rsqrt(jnp.mean(core * core, -1, keepdims=True) + EPS)
            mixed_ref[here, wide] = (normed * gated[:, wide]).astype(mixed_ref.dtype)
        return carry

    lax.fori_loop(0, chunks, chunk, 0)


def delta_forward(pre, gate, small, taps, rate, gain, heads, key_dim, value_dim):
    length, width = pre.shape
    chunks = length // SPAN
    out_shape = (
        jax.ShapeDtypeStruct((length, heads * value_dim), jnp.bfloat16),
        jax.ShapeDtypeStruct((length, heads * value_dim), jnp.float32),
        jax.ShapeDtypeStruct((length, heads * value_dim), jnp.float32),
        jax.ShapeDtypeStruct((chunks * heads * key_dim * value_dim // width, width), jnp.float32),
        jax.ShapeDtypeStruct((chunks, heads, SPAN, SPAN), jnp.float32),
    )
    return pl.pallas_call(
        functools.partial(forward_kernel, heads, key_dim, value_dim),
        out_shape=out_shape,
        scratch_shapes=[
            pltpu.VMEM((HALO + SPAN, width), jnp.float32),
            pltpu.VMEM((heads, key_dim, value_dim), jnp.float32),
        ],
        compiler_params=pltpu.CompilerParams(vmem_limit_bytes=56 << 20),
        name="delta_forward",
    )(pre, gate, small, taps, rate, gain)


def backward_start(refs, span):
    (_, _, _, _, _, _, _, _, _, _, _, _, _, _, taps_grad_ref, gain_grad_ref, rate_grad_ref,
     _, pad_ref, now_ref) = refs
    now_ref[...] = jnp.zeros_like(now_ref)
    pad_ref[span : span + HALO] = jnp.zeros((HALO, pad_ref.shape[1]), jnp.float32)
    taps_grad_ref[...] = jnp.zeros_like(taps_grad_ref)
    gain_grad_ref[...] = jnp.zeros_like(gain_grad_ref)
    rate_grad_ref[...] = jnp.zeros_like(rate_grad_ref)


def backward_chunk(heads, key_dim, value_dim, index, refs):
    (pre_ref, gate_ref, small_ref, taps_ref, rate_ref, gain_ref,
     core_ref, update_ref, state_ref, inverse_ref, grad_ref,
     low_ref, gate_low_ref, small_low_ref, taps_grad_ref, gain_grad_ref, rate_grad_ref,
     ahead_ref, pad_ref, now_ref) = refs
    width = taps_ref.shape[1]
    span = SPAN
    rows, cols = grids(span)
    qk = heads * key_dim
    reach = taps_ref.shape[0] - 1
    lanes = small_ref.shape[1]
    lane = lax.broadcasted_iota(jnp.int32, (span, lanes), 1)
    start = pl.multiple_of(index * span, span)
    here = pl.ds(start, span)
    before = pl.ds(pl.multiple_of(jnp.maximum(start - HALO, 0), HALO), HALO)
    ahead_ref[0:HALO] = pre_ref[before, :] * jnp.where(index > 0, 1.0, 0.0)
    ahead_ref[HALO : HALO + span] = pre_ref[here, :]
    total = conv_window(ahead_ref[...], taps_ref[...], span)
    gain_of = sigmoid(total)
    active = total * gain_of
    bend = gain_of * (1.0 + total * (1.0 - gain_of))
    small = small_ref[here, :]
    beta, slope, _, cumul = gates_of(small, rate_ref[...], heads, rows, cols)
    beta_t = jnp.transpose(beta)
    cumul_t = jnp.transpose(cumul)
    gate = gate_ref[here, :]
    gate_sig = sigmoid(gate)
    gate_silu = gate * gate_sig
    gate_bend = gate_sig * (1.0 + gate * (1.0 - gate_sig))
    small_grad = jnp.zeros((span, lanes), jnp.float32)
    for head in range(heads):
        wide = slice(head * value_dim, (head + 1) * value_dim)
        core = core_ref[here, wide]
        grad_mixed = grad_ref[here, wide]
        gain = gain_ref[:, wide]
        scale = lax.rsqrt(jnp.mean(core * core, -1, keepdims=True) + EPS)
        normed = core * scale
        gate_low_ref[here, wide] = (grad_mixed * normed * gain * gate_bend[:, wide]).astype(gate_low_ref.dtype)
        with_gate = grad_mixed * gate_silu[:, wide]
        gain_grad_ref[:, wide] += jnp.sum(with_gate * normed, 0, keepdims=True)
        grad_normed = with_gate * gain
        grad_core = scale * (grad_normed - normed * jnp.mean(grad_normed * normed, -1, keepdims=True))
        query_act = active[:, head * key_dim : (head + 1) * key_dim]
        query_scale = lax.rsqrt(jnp.sum(query_act * query_act, -1, keepdims=True) + EPS)
        query = query_act * (query_scale * key_dim ** (-0.5))
        key_act = active[:, qk + head * key_dim : qk + (head + 1) * key_dim]
        key_scale = lax.rsqrt(jnp.sum(key_act * key_act, -1, keepdims=True) + EPS)
        key = key_act * key_scale
        beta_col = beta[:, head : head + 1]
        beta_row = beta_t[head : head + 1]
        cum_col = cumul[:, heads + head : heads + head + 1]
        cum_row = cumul_t[heads + head : heads + head + 1]
        decays, scaled, key_key, query_key, lower, attend = chunk_terms(
            query, key, beta_col, beta_row, cum_col, cum_row, rows, cols
        )
        state = state_ref[state_place(index, head, heads, key_dim, value_dim, width)]
        update = update_ref[here, wide]
        inverse = inverse_ref[index, head]
        grad_state = now_ref[head]
        rise = jnp.exp(cum_col)
        last = cum_col[span - 1 : span]
        fall = jnp.exp(last - cum_col)
        tail = fall * beta_col
        rise_query = rise * query
        rise_key = rise * key
        grad_update = mm_tn(attend, grad_core) + mm(key * tail, grad_state)
        grad_right = mm_tn(inverse, grad_update)
        now_ref[head] = jnp.exp(last) * grad_state + mm_tn(rise_query, grad_core) - mm_tn(rise_key, grad_right)
        grad_attend = jnp.where(cols <= rows, mm_nt(grad_core, update), 0.0)
        grad_lower = jnp.where(cols < rows, -mm_nt(grad_right, update), 0.0)
        core_state = mm_nt(grad_core, state)
        right_state = mm_nt(grad_right, state)
        grad_tail_key = mm_nt(update, grad_state)
        pair_query = grad_attend * scaled
        pair_key = grad_lower * scaled
        grad_query = rise * core_state + mm(pair_query, key)
        grad_key = (
            grad_tail_key * tail - rise * right_state + mm_tn(pair_query, query)
            + mm(pair_key, key) + mm_tn(pair_key, key)
        )
        grad_tail = jnp.sum(grad_tail_key * key, -1, keepdims=True)
        moved = grad_attend * query_key + grad_lower * key_key
        spread = moved * scaled
        by_row = jnp.sum(spread, -1, keepdims=True)
        sums = mm_tn(
            jnp.concatenate([moved * decays, spread], 1), jnp.ones((span, lanes), jnp.float32)
        )
        grad_beta = sums[:span, 0:1] + grad_tail * fall
        through_tail = grad_tail * tail
        grad_cum = (
            by_row - sums[span:, 0:1] - through_tail
            + rise * (jnp.sum(core_state * query, -1, keepdims=True) - jnp.sum(right_state * key, -1, keepdims=True))
        )
        end_grad = jnp.sum(through_tail, 0, keepdims=True) + jnp.exp(last) * jnp.sum(
            jnp.sum(state * grad_state, -1, keepdims=True), 0, keepdims=True
        )
        grad_cum = grad_cum + jnp.where(rows[:, 0:1] == span - 1, end_grad, 0.0)
        small_grad = small_grad + jnp.where(lane == head, grad_beta, 0.0)
        small_grad = small_grad + jnp.where(lane == heads + head, grad_cum, 0.0)
        grad_query = grad_query * key_dim ** (-0.5)
        unit = query_act * query_scale
        grad_query = query_scale * (grad_query - unit * jnp.sum(grad_query * unit, -1, keepdims=True))
        grad_key = key_scale * (grad_key - key * jnp.sum(grad_key * key, -1, keepdims=True))
        at = slice(head * key_dim, (head + 1) * key_dim)
        pad_ref[0:span, at] = grad_query * bend[:, at]
        at = slice(qk + head * key_dim, qk + (head + 1) * key_dim)
        pad_ref[0:span, at] = grad_key * bend[:, at]
        at = slice(2 * qk + head * value_dim, 2 * qk + (head + 1) * value_dim)
        pad_ref[0:span, at] = grad_right * bend[:, at]
    summed = mm(jnp.where(cols >= rows, 1.0, 0.0), small_grad)
    is_beta = lane < heads
    rate_grad_ref[...] += jnp.sum(jnp.where(is_beta, 0.0, -slope * summed), 0, keepdims=True)
    sig = beta
    small_low_ref[here, :] = jnp.where(
        is_beta, small_grad * sig * (1.0 - sig), -rate_ref[...] * sig * summed
    ).astype(small_low_ref.dtype)
    outer = pad_ref[...]
    dense = outer[0:span]
    block = ahead_ref[...]
    grad_pre = None
    for offset in range(reach + 1):
        behind = reach - offset
        taps_grad_ref[offset : offset + 1] += jnp.sum(
            dense * block[HALO - behind : HALO - behind + span], 0, keepdims=True
        )
        term = taps_ref[offset : offset + 1] * outer[behind : behind + span]
        grad_pre = term if grad_pre is None else grad_pre + term
    low_ref[here, :] = grad_pre.astype(low_ref.dtype)
    pad_ref[span : span + HALO] = pad_ref[0:HALO]


MESH = pl.DeviceIdType.MESH
VM = pl.BlockSpec(memory_space=pltpu.VMEM)


def call_out(peers):
    barrier = pltpu.get_barrier_semaphore()
    for peer in peers:
        pl.semaphore_signal(barrier, inc=1, device_id=peer, device_id_type=MESH)


def hear_all(peers):
    pl.semaphore_wait(pltpu.get_barrier_semaphore(), len(peers))


def greet(peers):
    call_out(peers)
    hear_all(peers)


def remote(src, dst, send, recv, peer):
    return pltpu.make_async_remote_copy(
        src_ref=src, dst_ref=dst, send_sem=send, recv_sem=recv, device_id=peer, device_id_type=MESH
    )


def tensor_peers():
    dp = lax.axis_index("dp")
    t = lax.axis_index("tensor")
    core = lax.rem(t, 2)
    mate = (dp, t + 1 - 2 * core)
    across = (dp, lax.rem(t + 2, 4))
    return core, mate, across


def psum_kernel(blocks, part_ref, out_ref, land_mate, land_across, half, send, recv):
    core, mate, across = tensor_peers()
    greet((mate, across))
    rows = part_ref.shape[0] // blocks
    part = rows // 2
    first = []
    for b in range(blocks):
        theirs = pl.ds(pl.multiple_of(b * rows + (1 - core) * part, part), part)
        copy = remote(part_ref.at[theirs], land_mate.at[pl.ds(b * part, part)], send.at[0, b], recv.at[0, b], mate)
        copy.start()
        first.append(copy)
    second = []
    for b in range(blocks):
        mine = pl.ds(pl.multiple_of(b * rows + core * part, part), part)
        slot = pl.ds(b * part, part)
        first[b].wait_recv()
        half[slot] = part_ref[mine] + land_mate[slot]
        copy = remote(half.at[slot], land_across.at[slot], send.at[1, b], recv.at[1, b], across)
        copy.start()
        second.append(copy)
    third = []
    for b in range(blocks):
        mine = pl.ds(pl.multiple_of(b * rows + core * part, part), part)
        slot = pl.ds(b * part, part)
        second[b].wait_recv()
        out_ref[mine] = half[slot] + land_across[slot]
        copy = remote(out_ref.at[mine], out_ref.at[mine], send.at[2, b], recv.at[2, b], mate)
        copy.start()
        third.append(copy)
    for b in range(blocks):
        third[b].wait_recv()
    for b in range(blocks):
        first[b].wait_send()
        second[b].wait_send()
        third[b].wait_send()


def tensor_sum(part, collective_id, blocks=8):
    rows, width = part.shape
    return pl.pallas_call(
        functools.partial(psum_kernel, blocks),
        out_shape=jax.ShapeDtypeStruct(part.shape, part.dtype),
        in_specs=[VM],
        out_specs=VM,
        scratch_shapes=[pltpu.VMEM((rows // 2, width), part.dtype)] * 3
        + [pltpu.SemaphoreType.DMA((3, blocks))] * 2,
        compiler_params=pltpu.CompilerParams(
            collective_id=collective_id, has_side_effects=True, vmem_limit_bytes=40 << 20
        ),
        name="tensor_sum",
    )(part)


def swap_kernel(count, narrow, *refs):
    sources, results = refs[:count], refs[count : 2 * count]
    staged, send, recv, close_send, close_recv = refs[2 * count :]
    n = lax.axis_size("dp")
    me = lax.axis_index("dp")
    t = lax.axis_index("tensor")
    core, mate, across = tensor_peers()
    ranks = lax.axis_size("tensor")
    others = [lax.rem(me + k, n) for k in range(1, n)]
    greet([(other, t) for other in others] + [mate, across])
    seg = results[0].shape[0] // n
    part = seg // ranks
    far = lax.rem(t + 2, ranks)

    def at(place, rank):
        return pl.ds(pl.multiple_of(place * seg + rank * part, part), part)

    outgoing = []
    for i in range(count):
        for k in range(n):
            other = lax.rem(me + k, n)
            if k == 0:
                results[i][at(me, t)] = sources[i][at(me, t)].astype(jnp.float32)
                continue
            if narrow[i]:
                staged[i, k] = sources[i][at(other, t)].astype(jnp.float32)
                src = staged.at[i, k]
            else:
                src = sources[i].at[at(other, t)]
            copy = remote(src, results[i].at[at(me, t)], send.at[i, k], recv.at[i, k], (other, t))
            copy.start()
            outgoing.append(copy)
    close = []
    for i in range(count):
        for k in range(n):
            source = lax.rem(me + n - k, n)
            here = results[i].at[at(source, t)]
            if k:
                remote(here, here, send.at[i, k], recv.at[i, k], (source, t)).wait_recv()
            over = remote(here, here, close_send.at[0, i, k], close_recv.at[0, i, k], across)
            over.start()
            beside = remote(here, here, close_send.at[1, i, k], close_recv.at[1, i, k], mate)
            beside.start()
            close += [over, beside]
    last = []
    for i in range(count):
        for k in range(n):
            source = lax.rem(me + n - k, n)
            there = results[i].at[at(source, far)]
            remote(there, there, close_send.at[0, i, k], close_recv.at[0, i, k], across).wait_recv()
            copy = remote(there, there, close_send.at[2, i, k], close_recv.at[2, i, k], mate)
            copy.start()
            last.append(copy)
    for copy in outgoing:
        copy.wait_send()
    for j, copy in enumerate(close):
        copy.wait_send()
        if j % 2:
            copy.wait_recv()
    for copy in last:
        copy.wait()


def swap(arrays, n, collective_id):
    count = len(arrays)
    rows, width = arrays[0].shape
    narrow = [a.dtype != jnp.float32 for a in arrays]
    out = pl.pallas_call(
        functools.partial(swap_kernel, count, narrow),
        out_shape=[jax.ShapeDtypeStruct((rows, width), jnp.float32)] * count,
        in_specs=[VM] * count,
        out_specs=[VM] * count,
        scratch_shapes=[pltpu.VMEM((count, n, rows // n // 4, width), jnp.float32)]
        + [pltpu.SemaphoreType.DMA((count, n))] * 2
        + [pltpu.SemaphoreType.DMA((3, count, n))] * 2,
        compiler_params=pltpu.CompilerParams(
            collective_id=collective_id, has_side_effects=True, vmem_limit_bytes=40 << 20
        ),
        name="swap",
    )(*arrays)
    return out


SLOT = 80
DEPTH = 10
SPLIT = 3
WHOLE = 2
ORDER = (0, 1, 2, 3)


def grid_place():
    n = lax.axis_size("dp")
    me = lax.axis_index("dp")
    t = lax.axis_index("tensor")
    lines = n // 2
    z = lax.div(me, 2)
    x = lax.rem(me, 2)
    return n, lines, me, t, z, x


def reduce_slot(slot, chunks, data, split_rings, whole_rings, sems):
    n, lines, me, t, z, x = grid_place()
    mate = (me + 1 - 2 * x, t)
    send_x, recv_x, send_z, recv_z, send_d, recv_d, send_p, recv_p, send_s, recv_s = [sems.at[i] for i in range(10)]
    top = lines - 1
    finish = slot - 2 * lines - 1

    def ring(chunk):
        return lax.rem(chunk, DEPTH)

    def within(chunk):
        return (chunk >= 0) & (chunk < chunks)

    def split_stream(stream):
        land_x, land_z, outgo, aside = split_rings
        up = stream % 2 == 0
        level = z if up else top - z
        after = (me + 2, t) if up else (me - 2, t)
        prior = (me - 2, t) if up else (me + 2, t)

        def rows(chunk, side):
            return pl.ds(pl.multiple_of(chunk * SLOT + 16 * stream + 8 * side, 8), 8)

        def spot(ref, chunk):
            return ref.at[stream, ring(chunk)]

        def copy(kind_send, kind_recv, chunk, src, dst, peer):
            at = (stream, ring(chunk))
            return remote(src, dst, kind_send.at[at], kind_recv.at[at], peer)

        def to_mate(chunk):
            return copy(send_x, recv_x, chunk, spot(aside, chunk), spot(land_x, chunk), mate)

        def to_after(chunk):
            return copy(send_z, recv_z, chunk, spot(outgo, chunk), spot(land_z, chunk), after)

        def result(chunk, peer):
            here = data.at[rows(chunk, x)]
            return copy(send_d, recv_d, chunk, here, here, peer)

        def close(chunk, side):
            here = data.at[rows(chunk, side)]
            return copy(send_p, recv_p, chunk, here, here, mate)

        def give_back(chunk):
            @pl.when(level > 0)
            def _():
                result(chunk, prior).start()

            close(chunk, x).start()

        def enter():
          @pl.when(slot < chunks)
          def _():
            aside[stream, ring(slot)] = data[rows(slot, 1 - x)]
            to_mate(slot).start()

        def climb():
            rise = slot - 1 - level

            @pl.when(within(rise))
            def _():
                here = rows(rise, x)
                at = ring(rise)
                to_mate(rise).wait_recv()

                @pl.when(level > 0)
                def _():
                    to_after(rise).wait_recv()
                    outgo[stream, at] = data[here] + land_x[stream, at] + land_z[stream, at]

                @pl.when(level == 0)
                def _():
                    outgo[stream, at] = data[here] + land_x[stream, at]

                @pl.when(level < top)
                def _():
                    to_after(rise).start()

                @pl.when(level == top)
                def _():
                    data[here] = outgo[stream, at]
                    give_back(rise)

        def descend():
            fall = slot - 1 - 2 * top + level

            @pl.when(within(fall) & (level < top))
            def _():
                result(fall, after).wait_recv()
                to_after(fall).wait_send()
                give_back(fall)

        def leave():
            @pl.when(within(finish))
            def _():
                @pl.when(level > 0)
                def _():
                    result(finish, prior).wait_send()

                close(finish, x).wait_send()
                close(finish, 1 - x).wait_recv()
                to_mate(finish).wait_send()

        return enter, climb, descend, leave

    def whole_stream(stream):
        land_x, land_z, land_s, outgo = whole_rings
        line = z if stream == 0 else top - z
        step = 2 if stream == 0 else -2
        inner, outer = (me - step, t), (me + step, t)

        def rows(chunk):
            return pl.ds(pl.multiple_of(chunk * SLOT + 16 * (SPLIT + stream), 8), 16)

        def spot(ref, chunk):
            return ref.at[stream, ring(chunk)]

        def copy(kind_send, kind_recv, chunk, src, dst, peer):
            at = (ring(chunk),)
            return remote(
                src, dst, kind_send.at[SPLIT + stream, ring(chunk)], kind_recv.at[SPLIT + stream, ring(chunk)], peer
            )

        def inward(chunk):
            return copy(send_z, recv_z, chunk, spot(outgo, chunk), spot(land_z, chunk), inner)

        def outward(chunk):
            return copy(send_z, recv_s, chunk, spot(outgo, chunk), spot(land_s, chunk), outer)

        def to_mate(chunk):
            return copy(send_x, recv_x, chunk, spot(outgo, chunk), spot(land_x, chunk), mate)

        def result_out(chunk):
            here = data.at[rows(chunk)]
            return copy(send_d, recv_d, chunk, here, here, outer)

        def result_in(chunk):
            here = data.at[rows(chunk)]
            return copy(send_s, recv_d, chunk, here, here, inner)

        def enter():
            leaf = slot - 1

            @pl.when(within(leaf) & (line == 0) & (lax.rem(jnp.maximum(leaf, 0), 2) > 0))
            def _():
                outgo[stream, ring(leaf)] = data[rows(leaf)]
                outward(leaf).start()

        def climb():
            rise = slot - 1 - (top - line)
            root = lax.rem(jnp.maximum(rise, 0), 2)

            @pl.when(within(rise) & (line >= root))
            def _():
                here = rows(rise)
                at = ring(rise)

                @pl.when(line < top)
                def _():
                    inward(rise).wait_recv()

                is_fork = (line == root) & (root > 0)

                @pl.when(is_fork)
                def _():
                    outward(rise).wait_recv()
                    outgo[stream, at] = data[here] + land_z[stream, at] + land_s[stream, at]

                @pl.when((line < top) & jnp.logical_not(is_fork))
                def _():
                    outgo[stream, at] = data[here] + land_z[stream, at]

                @pl.when(line == top)
                def _():
                    outgo[stream, at] = data[here]

                @pl.when(line > root)
                def _():
                    inward(rise).start()

                @pl.when(line == root)
                def _():
                    to_mate(rise).start()

        def descend():
            meet = slot - 2 - (top - line)
            meet_root = lax.rem(jnp.maximum(meet, 0), 2)

            @pl.when(within(meet) & (line == meet_root))
            def _():
                at = ring(meet)
                to_mate(meet).wait_recv()
                data[rows(meet)] = outgo[stream, at] + land_x[stream, at]
                result_out(meet).start()

                @pl.when(meet_root > 0)
                def _():
                    result_in(meet).start()

            for parity in range(2):
                fall = slot - 2 - (top - parity) - (line - parity)

                @pl.when(within(fall) & (lax.rem(jnp.maximum(fall, 0), 2) == parity) & (line > parity))
                def _():
                    result_out(fall).wait_recv()
                    inward(fall).wait_send()

                    @pl.when(line < top)
                    def _():
                        result_out(fall).start()

            inside = slot - 2 - (top - 1) - 1

            @pl.when(within(inside) & (lax.rem(jnp.maximum(inside, 0), 2) > 0) & (line == 0))
            def _():
                result_in(inside).wait_recv()
                outward(inside).wait_send()

        def leave():
            end_root = lax.rem(jnp.maximum(finish, 0), 2)

            @pl.when(within(finish))
            def _():
                @pl.when((line >= end_root) & (line < top))
                def _():
                    result_out(finish).wait_send()

                @pl.when(line == end_root)
                def _():
                    to_mate(finish).wait_send()

                    @pl.when(end_root > 0)
                    def _():
                        result_in(finish).wait_send()

        return enter, climb, descend, leave

    streams = [whole_stream(stream) for stream in range(WHOLE)] + [split_stream(stream) for stream in range(SPLIT)]
    for stream in streams:
        for phase in ORDER:
            stream[phase]()


def settle(lines):
    return 2 * lines + 1


def reduce_scratch(width):
    return (
        [pltpu.VMEM((SPLIT, DEPTH, 8, width), jnp.float32)] * 4
        + [pltpu.VMEM((WHOLE, DEPTH, 16, width), jnp.float32)] * 4
        + [pltpu.SemaphoreType.DMA((10, SPLIT + WHOLE, DEPTH))]
    )


BLOCKS = 8


def dot_plain(left, right):
    return lax.dot_general(left, right, (((1,), (0,)), ((), ())), preferred_element_type=jnp.float32)


def dot_nt(left, right):
    return lax.dot_general(left, right, (((1,), (1,)), ((), ())), preferred_element_type=jnp.float32)


def dot_tn(left, right):
    return lax.dot_general(left, right, (((0,), (0,)), ((), ())), preferred_element_type=jnp.float32)


def aligned(start, size):
    return pl.ds(pl.multiple_of(start, size), size)


class TensorSum:
    def __init__(self, part, total, land_mate, land_across, half, send, recv):
        self.core, self.mate, self.across = tensor_peers()
        self.part, self.total, self.half = part, total, half
        self.land_mate, self.land_across = land_mate, land_across
        self.send, self.recv = send, recv
        self.rows = part.shape[0] // BLOCKS
        self.size = self.rows // 2

    def span(self, block, side):
        return aligned(block * self.rows + side * self.size, self.size)

    def slot(self, block):
        return aligned(block * self.size, self.size)

    def first(self, block):
        return remote(
            self.part.at[self.span(block, 1 - self.core)], self.land_mate.at[self.slot(block)],
            self.send.at[0, block], self.recv.at[0, block], self.mate,
        )

    def second(self, block):
        return remote(
            self.half.at[self.slot(block)], self.land_across.at[self.slot(block)],
            self.send.at[1, block], self.recv.at[1, block], self.across,
        )

    def third(self, block):
        mine = self.total.at[self.span(block, self.core)]
        return remote(mine, mine, self.send.at[2, block], self.recv.at[2, block], self.mate)

    def start(self):
        for block in range(BLOCKS):
            self.first(block).start()

    def cross(self, block):
        self.first(block).wait_recv()
        slot = self.slot(block)
        self.half[slot] = self.part[self.span(block, self.core)] + self.land_mate[slot]
        self.second(block).start()

    def share(self, block, beside=None):
        self.second(block).wait_recv()
        slot = self.slot(block)
        mine = self.span(block, self.core)
        value = self.half[slot] + self.land_across[slot]
        self.total[mine] = value if beside is None else value + beside[mine].astype(value.dtype)
        self.third(block).start()

    def finish(self, had=0):
        for block in range(had, BLOCKS):
            self.third(block).wait_recv()
        for block in range(BLOCKS):
            self.first(block).wait_send()
            self.second(block).wait_send()
            self.third(block).wait_send()


class Swap:
    def __init__(self, source, result, send, recv, close_send, close_recv):
        self.n = lax.axis_size("dp")
        self.me = lax.axis_index("dp")
        self.t = lax.axis_index("tensor")
        self.ranks = lax.axis_size("tensor")
        _, self.mate, self.across = tensor_peers()
        self.source, self.result = source, result
        self.sems = send, recv, close_send, close_recv
        self.seg = result.shape[0] // self.n
        self.part = self.seg // self.ranks

    def at(self, place, rank):
        return aligned(place * self.seg + rank * self.part, self.part)

    def out(self, k):
        other = lax.rem(self.me + k, self.n)
        return remote(
            self.source.at[self.at(other, self.t)], self.result.at[self.at(self.me, self.t)],
            self.sems[0].at[k], self.sems[1].at[k], (other, self.t),
        )

    def close(self, k, leg):
        origin = lax.rem(self.me + self.n - k, self.n)
        rank = lax.rem(self.t + 2, self.ranks) if leg == 2 else self.t
        here = self.result.at[self.at(origin, rank)]
        return remote(
            here, here, self.sems[2].at[leg, k], self.sems[3].at[leg, k], self.across if leg == 0 else self.mate
        )

    def start(self):
        mine = self.at(self.me, self.t)
        self.result[mine] = self.source[mine]
        for k in range(1, self.n):
            self.out(k).start()

    def gather(self, k):
        @pl.when(k > 0)
        def _():
            self.out(k).wait_recv()

        self.close(k, 0).start()
        self.close(k, 1).start()

    def forward(self, k):
        self.close(k, 0).wait_recv()
        self.close(k, 2).start()

    def sent(self):
        for k in range(1, self.n):
            self.out(k).wait_send()

    def finish(self):
        for k in range(self.n):
            self.close(k, 0).wait_send()
            self.close(k, 1).wait()
            self.close(k, 2).wait()


class PlaneSwap(Swap):
    def __init__(self, source, result, send, recv, close_send, close_recv):
        super().__init__(source, result, send, recv, close_send, close_recv)
        self.core = lax.rem(self.t, 2)
        self.part = self.seg // 2

    def out(self, k):
        other = lax.rem(self.me + k, self.n)
        return remote(
            self.source.at[self.at(other, self.core)], self.result.at[self.at(self.me, self.core)],
            self.sems[0].at[k], self.sems[1].at[k], (other, self.t),
        )

    def close(self, k, leg):
        origin = lax.rem(self.me + self.n - k, self.n)
        here = self.result.at[self.at(origin, self.core)]
        return remote(here, here, self.sems[2].at[leg, k], self.sems[3].at[leg, k], self.mate)

    def start(self):
        mine = self.at(self.me, self.core)
        self.result[mine] = self.source[mine]
        for k in range(1, self.n):
            self.out(k).start()

    def gather(self, k):
        @pl.when(k > 0)
        def _():
            self.out(k).wait_recv()

        self.close(k, 1).start()

    def finish(self):
        for k in range(self.n):
            self.close(k, 1).wait()


def tail_kernel(
    heads, key_dim, value_dim, ranges, chunks,
    part2_hbm, ffn_hbm, pre_hbm, core_hbm, update_hbm, state_hbm,
    resid1_hbm, upstream_hbm, resid_hbm, mixed_hbm, hidden1_hbm, hidden2_hbm, units_hbm,
    w_out_hbm, query_hbm, key_hbm, value_hbm, w_gate_hbm, w_small_hbm, gate_hbm, small_hbm, inverse_hbm,
    norm1_ref, norm2_ref, taps_ref, rate_ref, gain_ref,
    data, output_ref, inputs_grad_ref,
    resid1_ref, upstream_ref, resid_ref, mixed_ref, hidden1_ref, hidden2_ref, units_ref,
    w_out_ref, w_mix_ref, w_gate_ref, w_small_ref, gate_ref, small_ref, inverse_ref,
    split_x, split_z, split_out, split_aside, whole_x, whole_z, whole_s, whole_out, sems,
    part, total, half, land_mate, land_across, sum_send, sum_recv,
    resid1_grad, resid1_low, mixed_grad, low, gate_low, small_low,
    taps_grad, gain_grad, rate_grad, norm1_grad, norm2_grad, ahead, pad, now,
    shuffled, swap_send, swap_recv, close_send, close_recv, load_sem,
):
    n, lines, me, t, z, x = grid_place()
    _, mate, across = tensor_peers()
    length, width = resid1_hbm.shape
    qk = heads * key_dim
    values = heads * value_dim
    at_down, at_units, at_out, at_gate, at_mix, at_small, at_end, rows_all = ranges
    loads = [
        (units_hbm, units_ref),
        (upstream_hbm, upstream_ref),
        (part2_hbm, part),
        (hidden2_hbm, hidden2_ref),
        (resid1_hbm, resid1_ref),
        (w_out_hbm, w_out_ref),
        (mixed_hbm, mixed_ref),
        (pre_hbm, data.at[pl.ds(at_mix, length)]),
        (core_hbm, data.at[pl.ds(at_mix + length, length), pl.ds(0, values)]),
        (update_hbm, data.at[pl.ds(at_mix + length, length), pl.ds(values, values)]),
        (state_hbm, data.at[pl.ds(at_gate, state_hbm.shape[0])]),
        (gate_hbm, gate_ref),
        (small_hbm, small_ref),
        (inverse_hbm, inverse_ref),
        (hidden1_hbm, hidden1_ref),
        (query_hbm, w_mix_ref.at[:, pl.ds(0, qk)]),
        (key_hbm, w_mix_ref.at[:, pl.ds(qk, qk)]),
        (value_hbm, w_mix_ref.at[:, pl.ds(2 * qk, values)]),
        (w_gate_hbm, w_gate_ref),
        (w_small_hbm, w_small_ref),
        (resid_hbm, resid_ref),
    ]
    loads = [pltpu.make_async_copy(src, dst, load_sem.at[i]) for i, (src, dst) in enumerate(loads)]
    load_ffn = pltpu.make_async_copy(ffn_hbm, part, load_sem.at[len(loads)])
    peers = [(lax.rem(me + k, n), t) for k in range(1, n)] + [mate, across]
    call_out(peers)
    for load in loads:
        load.start()
    refs = (
        data.at[pl.ds(at_mix, length)], gate_ref, small_ref, taps_ref, rate_ref, gain_ref,
        data.at[pl.ds(at_mix + length, length), pl.ds(0, values)],
        data.at[pl.ds(at_mix + length, length), pl.ds(values, values)],
        data.at[pl.ds(at_gate, state_hbm.shape[0])], inverse_ref, mixed_grad, low, gate_low, small_low, taps_grad, gain_grad, rate_grad,
        ahead, pad, now,
    )
    sums = [
        TensorSum(part, total, land_mate, land_across.at[i % 2], half, sum_send.at[i], sum_recv.at[i]) for i in range(3)
    ]
    swaps = [
        Swap(source, result, swap_send.at[i], swap_recv.at[i], close_send.at[i], close_recv.at[i])
        for i, (source, result) in enumerate([(total, shuffled), (resid1_grad, inputs_grad_ref)])
    ]
    norm1_grad[...] = jnp.zeros_like(norm1_grad)
    norm2_grad[...] = jnp.zeros_like(norm2_grad)
    backward_start(refs, SPAN)
    data[at_end:rows_all] = jnp.zeros((rows_all - at_end, width), jnp.float32)
    count_units = (at_units - at_down)
    tiles = units_ref.shape[2] // 128

    def units_piece(i):
        kind = lax.div(i, tiles)
        tile = lax.rem(i, tiles)
        left = units_ref[kind, :, aligned(tile * 128, 128)]
        start = at_down + kind * count_units + tile * 128

        def put(right):
            value = dot_tn(left, right)

            @pl.when(tile < tiles - 1)
            def _():
                data[pl.ds(pl.multiple_of(start, 64), 128)] = value

            @pl.when(tile == tiles - 1)
            def _():
                rest = count_units - (tiles - 1) * 128
                data[pl.ds(pl.multiple_of(start, 64), rest)] = value[0:rest]

        @pl.when(kind == 0)
        def _():
            put(upstream_ref[...])

        @pl.when(kind > 0)
        def _():
            put(hidden2_ref[...])

    loads[0].wait()
    loads[1].wait()
    units_piece(0)
    loads[2].wait()
    hear_all(peers)
    sums[0].start()

    def wait_loads():
        for load in loads[3:]:
            load.wait()

    def norm_back(value, grad, gain, gain_grad_ref):
        scale = lax.rsqrt(jnp.mean(value * value, -1, keepdims=True) + EPS)
        normed = value * scale
        gain_grad_ref[...] += jnp.sum(grad * normed, 0, keepdims=True)
        scaled = grad * gain
        return scale * (scaled - normed * jnp.mean(scaled * normed, -1, keepdims=True))

    def norm2_piece(i):
        here = aligned(i * 64, 64)
        grad = upstream_ref[here].astype(jnp.float32) + norm_back(
            resid1_ref[here], total[here], norm2_ref[...], norm2_grad
        )
        resid1_grad[here] = grad
        resid1_low[here] = grad.astype(jnp.bfloat16)

    def mixed_piece(i):
        tile = aligned(i * 256, 256)
        mixed_grad[:, tile] = dot_nt(resid1_low[...], w_out_ref[tile])

    def out_piece(i):
        tile = aligned(i * 256, 256)
        data[pl.ds(pl.multiple_of(at_out + i * 256, 64), 256)] = dot_tn(
            mixed_ref[:, tile], resid1_low[...]
        )

    def gate_piece(i):
        tile = aligned(i * 256, 256)
        half_rows = width // 2
        data[pl.ds(pl.multiple_of(at_gate + i * 256, 64), 256), 0:values] = dot_tn(hidden1_ref[:, tile], gate_low[...])
        other = aligned(half_rows + i * 256, 256)
        data[pl.ds(pl.multiple_of(at_gate + i * 256, 64), 256), values : 2 * values] = dot_tn(
            hidden1_ref[:, other], gate_low[...]
        )

    def mix_piece(i):
        tile = aligned(i * 256, 256)
        data[pl.ds(pl.multiple_of(at_mix + i * 256, 64), 256)] = dot_tn(hidden1_ref[:, tile], low[...])

    def hidden_piece(i):
        tile = aligned(i * 256, 256)
        part[:, tile] = (
            dot_nt(low[...], w_mix_ref[tile]) + dot_nt(gate_low[...], w_gate_ref[tile])
            + dot_plain(small_low[...], w_small_ref[:, tile])
        )

    def output_piece(i):
        here = aligned(i * 64, 64)
        total[here] = total[here] + resid1_ref[here]

    def round_piece(i):
        here = aligned(i * 64, 64)
        output_ref[here] = shuffled[here].astype(output_ref.dtype)

    def norm1_piece(i):
        here = aligned(i * 64, 64)
        resid1_grad[here] = resid1_grad[here] + norm_back(
            resid_ref[here].astype(jnp.float32), total[here], norm1_ref[...], norm1_grad
        )

    def small_piece():
        base = at_small
        data[base : at_end] = jnp.zeros((at_end - base, width), jnp.float32)
        data[base : base + 4] = taps_grad[...]
        data[base + 4 : base + 5] = norm1_grad[...]
        data[base + 5 : base + 6] = norm2_grad[...]
        data[base + 6 : base + 7, 0:values] = gain_grad[...]
        data[base + 6 : base + 7, values : values + rate_grad.shape[1]] = rate_grad[...]
        data[base + 8 : base + 16] = dot_tn(small_low[...], hidden1_ref[...])[0:8]

    def start_ffn():
        load_ffn.start()
        load_ffn.wait()
        sums[1].start()

    pieces = []

    def plan(first, count, each, run):
        assert count % each == 0
        pieces.append((first, count, each, run))
        return first + -(-count // each)

    plan(0, 1, 1, lambda i: wait_loads())
    plan(0, 3 * tiles - 1, 1, lambda i: units_piece(i + 1))
    for i in range(1, 3 * tiles):
        assert i <= (at_down + i // tiles * count_units + i % tiles * 128) // SLOT
    at = plan(0, BLOCKS, 2, sums[0].cross)
    at = plan(at, BLOCKS, 2, sums[0].share)
    at = plan(at, 1, 1, lambda i: sums[0].finish())
    at = plan(at, length // 64, 2, norm2_piece)
    at = plan(at, values // 256, 1, mixed_piece)
    side = at
    at = plan(at, values // 256, 1, out_piece)
    at_ready_out = at
    at = plan(at, length // SPAN, 1, lambda i: backward_chunk(heads, key_dim, value_dim, length // SPAN - 1 - i, refs))
    side = plan(side, 1, 1, lambda i: start_ffn())
    side = plan(side, BLOCKS, 2, sums[1].cross)
    side = plan(side, BLOCKS, 2, sums[1].share)
    side = plan(side, 1, 1, lambda i: sums[1].finish())
    part_free = side
    side = plan(side, length // 64, 4, output_piece)
    side = plan(side, 1, 1, lambda i: swaps[0].start())
    side = plan(side, n, 2, swaps[0].gather)
    side = plan(side, 1, 1, lambda i: swaps[0].sent())
    total_free = side
    side = plan(side, n, 2, swaps[0].forward)
    side = plan(side, 1, 1, lambda i: swaps[0].finish())
    side = plan(side, length // 64, 4, round_piece)
    at = plan(at, width // 512, 1, gate_piece)
    at_ready_gate = at
    at = plan(at, width // 256, 1, mix_piece)
    at_ready_mix = at
    at = plan(max(at, part_free), width // 256, 1, hidden_piece)
    at = plan(max(at, total_free), 1, 1, lambda i: sums[2].start())
    at = plan(at, BLOCKS, 2, sums[2].cross)
    at = plan(at, BLOCKS, 2, sums[2].share)
    at = plan(at, 1, 1, lambda i: sums[2].finish())
    at = plan(at, length // 64, 2, norm1_piece)
    at = plan(at, 1, 1, lambda i: small_piece())
    at_ready_small = at
    at = plan(at, 1, 1, lambda i: swaps[1].start())
    at = plan(at, n, 2, swaps[1].gather)
    plan(at, 1, 1, lambda i: swaps[1].sent())
    at = plan(at, n, 2, swaps[1].forward)
    at = plan(at, 1, 1, lambda i: swaps[1].finish())
    assert at_ready_out <= at_out // SLOT and at_ready_gate <= at_gate // SLOT
    assert at_ready_mix <= at_mix // SLOT and at_ready_small <= at_small // SLOT
    last = max(chunks + settle(lines), at, side)

    def step(slot, carry):
        reduce_slot(
            slot, chunks, data, (split_x, split_z, split_out, split_aside), (whole_x, whole_z, whole_s, whole_out), sems
        )
        for first, count, each, run in pieces:
            steps = -(-count // each)

            @pl.when((slot >= first) & (slot < first + steps))
            def _(first=first, each=each, run=run):
                if each == 1:
                    run(slot - first)
                else:
                    def inner(i, carry):
                        run((slot - first) * each + i)
                        return carry

                    lax.fori_loop(0, each, inner, 0)

        return carry

    lax.fori_loop(0, last, step, 0)


def tail(
    part2, ffn, pre, core, update, states, resid1, upstream, resid, mixed, hidden1, hidden2, units,
    w_out, w_query, w_key, w_value, w_gate, w_small, gate, small, inverses, norm1, norm2, taps, rate, gain,
    heads, key_dim, value_dim, count_units, places, collective_id,
):
    length, width = resid1.shape
    values = heads * value_dim
    qk = heads * key_dim
    lanes = small.shape[1]
    heights = [count_units, 2 * count_units, values, values, width, 64]
    ranges = [0]
    for height in heights:
        ranges.append(ranges[-1] + height)
    rows_all = -(-ranges[-1] // SLOT) * SLOT
    chunks = rows_all // SLOT
    f32, bf = jnp.float32, jnp.bfloat16
    shape = jax.ShapeDtypeStruct
    out_shape = [
        pltpu.VMEM((rows_all, width), f32),
        pltpu.VMEM((length, width), bf),
        pltpu.VMEM((length, width), f32),
    ]
    vmem, any_ = VM, pl.BlockSpec(memory_space=pl.ANY)
    dma = pltpu.SemaphoreType.DMA
    scratch = (
        [
            pltpu.VMEM(a.shape, a.dtype)
            for a in (
                resid1, upstream, resid, mixed, hidden1, hidden2, units, w_out, shape((width, width), bf), w_gate, w_small,
                gate, small, inverses,
            )
        ]
        + reduce_scratch(width)
        + [
            pltpu.VMEM((length, width), f32),
            pltpu.VMEM((length, width), f32),
            pltpu.VMEM((length // 2, width), f32),
            pltpu.VMEM((length // 2, width), f32),
            pltpu.VMEM((2, length // 2, width), f32),
            dma((3, 3, BLOCKS)),
            dma((3, 3, BLOCKS)),
            pltpu.VMEM((length, width), f32),
            pltpu.VMEM((length, width), bf),
            pltpu.VMEM((length, values), f32),
            pltpu.VMEM((length, width), bf),
            pltpu.VMEM((length, values), bf),
            pltpu.VMEM((length, lanes), bf),
            pltpu.VMEM(taps.shape, f32),
            pltpu.VMEM((1, values), f32),
            pltpu.VMEM((1, lanes), f32),
            pltpu.VMEM((1, width), f32),
            pltpu.VMEM((1, width), f32),
            pltpu.VMEM((HALO + SPAN, width), f32),
            pltpu.VMEM((HALO + SPAN, width), f32),
            pltpu.VMEM((heads, key_dim, value_dim), f32),
            pltpu.VMEM((length, width), f32),
            dma((2, places)),
            dma((2, places)),
            dma((2, 3, places)),
            dma((2, 3, places)),
            dma((24,)),
        ]
    )
    return pl.pallas_call(
        functools.partial(tail_kernel, heads, key_dim, value_dim, tuple(ranges) + (rows_all,), chunks),
        out_shape=out_shape,
        in_specs=[any_] * 22 + [vmem] * 5,
        out_specs=[vmem] * 3,
        scratch_shapes=scratch,
        compiler_params=pltpu.CompilerParams(
            collective_id=collective_id, has_side_effects=True,
            vmem_limit_bytes=67043328 - 4 * width * rows_all - 6 * width * length - (1 << 18),
        ),
        name="tail",
    )(
        part2, ffn, pre, core, update, states, resid1, upstream, resid, mixed, hidden1, hidden2, units,
        w_out, w_query, w_key, w_value, w_gate, w_small, gate, small, inverses, norm1, norm2, taps, rate, gain,
    ), tuple(ranges)


def finish_kernel(heads, qk, values, ranges, data, output, inputs_grad, *refs):
    big, smalls, sems = refs[:10], refs[10:19], refs[19]
    at_down, at_units, at_out, at_gate, at_mix, at_small, _ = ranges
    width = data.shape[1]
    units = big[2].shape[0]

    def rows(start, height, left=0, wide=None):
        return data.at[pl.ds(start, height), pl.ds(left, width if wide is None else wide)]

    half = width // 2
    moves = [
        (output, big[0]),
        (inputs_grad, big[1]),
        (rows(at_units, units), big[2]),
        (rows(at_units + units, units), big[3]),
        (rows(at_down, units), big[4]),
        (rows(at_out, values), big[5]),
        (rows(at_gate, half, 0, values), big[6].at[pl.ds(0, half)]),
        (rows(at_gate, half, values, values), big[6].at[pl.ds(half, half)]),
        (rows(at_mix, width, 0, qk), big[7]),
        (rows(at_mix, width, qk, qk), big[8]),
        (rows(at_mix, width, 2 * qk, values), big[9]),
    ]
    moves = [pltpu.make_async_copy(src, dst, sems.at[i]) for i, (src, dst) in enumerate(moves)]
    for move in moves:
        move.start()
    norm1, norm2, head, rate, beta, decay, query, key, value = smalls
    small = data[at_small : at_small + 16]
    norm1[...] = small[4:5]
    norm2[...] = small[5:6]
    head[...] = small[6:7, 0:values]
    rate[...] = small[6:7, values : values + 2 * heads][:, heads:]
    beta[...] = small[8 : 8 + heads]
    decay[...] = small[8 + heads : 8 + 2 * heads]
    query[...] = small[0:4, 0:qk]
    key[...] = small[0:4, qk : 2 * qk]
    value[...] = small[0:4, 2 * qk :]
    for move in moves:
        move.wait()


def finish(data, output, inputs_grad, ranges, units, heads, qk, values):
    width = data.shape[1]
    length = output.shape[0]
    any_ = pl.BlockSpec(memory_space=pl.ANY)
    f32 = jnp.float32
    bigs = [
        (units, width), (units, width), (units, width), (values, width), (width, values), (width, qk), (width, qk), (width, values)
    ]
    smalls = [(1, width), (1, width), (1, values), (1, heads), (heads, width), (heads, width), (4, qk), (4, qk), (4, values)]
    held = [pltpu.with_memory_space_constraint(a, pltpu.VMEM) for a in (data, output, inputs_grad)]
    return pl.pallas_call(
        functools.partial(finish_kernel, heads, qk, values, ranges),
        out_shape=[jax.ShapeDtypeStruct((length, width), output.dtype), jax.ShapeDtypeStruct((length, width), f32)]
        + [jax.ShapeDtypeStruct(shape, f32) for shape in bigs + smalls],
        in_specs=[VM] * 3,
        out_specs=[any_] * 10 + [VM] * len(smalls),
        scratch_shapes=[pltpu.SemaphoreType.DMA((11,))],
        compiler_params=pltpu.CompilerParams(vmem_limit_bytes=8 << 20),
        name="finish",
    )(*held)


PAIR = 2


def unit_inverses(lowers, rows, cols):
    count = lowers[0].shape[0]
    near = (rows // 2 == cols // 2) & (rows > cols)
    inverses = [jnp.where(rows == cols, 1.0, jnp.where(near, -lower, 0.0)) for lower in lowers]
    block = 2
    while block < count:
        cross = (rows // (2 * block) == cols // (2 * block)) & (rows // block > cols // block)
        steps = [mm(inverse, jnp.where(cross, lower, 0.0)) for inverse, lower in zip(inverses, lowers)]
        inverses = [inverse - mm(step, inverse) for inverse, step in zip(inverses, steps)]
        block *= 2
    return inverses


def head_body(
    heads, key_dim, value_dim, begin, early, halfway,
    pre_ref, gate_ref, small_ref, taps_ref, rate_ref, gain_ref, w_out_ref, resid_ref, norm2_ref,
    w_gate_hbm, w_up_hbm, w_down_hbm,
    mixed_ref, core_ref, update_ref, state_ref, inverse_ref, resid1_ref, upstream_ref, hidden_ref, units_ref, part2_ref, ffn_ref,
    pad, now, solved_key, rise_query, key_tail, attend_all, ends,
    part, land_mate, land_across, half, sum_send, sum_recv,
    arrived, w_gate, w_up, w_down, gate_pre, up_pre, inner_grad, load_sem,
):
    length, width = pre_ref.shape
    span = SPAN
    chunks = length // span
    rows, cols = grids(span)
    qk = heads * key_dim
    n, _, me, t, _, _ = grid_place()
    _, mate, across = tensor_peers()
    loads = [(w_gate_hbm, w_gate), (w_up_hbm, w_up), (w_down_hbm, w_down)]
    loads = [pltpu.make_async_copy(src, dst, load_sem.at[i]) for i, (src, dst) in enumerate(loads)]
    for load in loads:
        load.start()
    total = TensorSum(part, resid1_ref, land_mate, land_across, half, sum_send, sum_recv)
    swap = begin
    pad[0:HALO] = jnp.zeros((HALO, width), jnp.float32)
    now[...] = jnp.zeros_like(now)

    def prepare_pair(turn):
        items = []
        for k in range(PAIR):
            index = turn * PAIR + k
            here = aligned(index * span, span)
            pad[HALO : HALO + span] = pre_ref[here, :]
            total_pre = conv_window(pad[...], taps_ref[...], span)
            pad[0:HALO] = pad[span : span + HALO]
            active = total_pre * sigmoid(total_pre)
            beta, _, _, cumul = gates_of(small_ref[here, :], rate_ref[...], heads, rows, cols)
            beta_t = jnp.transpose(beta)
            cumul_t = jnp.transpose(cumul)
            for head in range(heads):
                query = active[:, head * key_dim : (head + 1) * key_dim]
                query = query * (lax.rsqrt(jnp.sum(query * query, -1, keepdims=True) + EPS) * key_dim ** (-0.5))
                key = active[:, qk + head * key_dim : qk + (head + 1) * key_dim]
                key = key * lax.rsqrt(jnp.sum(key * key, -1, keepdims=True) + EPS)
                value = active[:, 2 * qk + head * value_dim : 2 * qk + (head + 1) * value_dim]
                beta_col = beta[:, head : head + 1]
                cum_col = cumul[:, heads + head : heads + head + 1]
                cum_row = cumul_t[heads + head : heads + head + 1]
                within = cols <= rows
                decays = jnp.where(within, jnp.exp(jnp.where(within, cum_col - cum_row, 0.0)), 0.0)
                scaled = decays * beta_t[head : head + 1]
                products = mm_nt(jnp.concatenate([query, key], 0), key)
                lower = jnp.where(cols < rows, scaled * products[span:], 0.0)
                attend = scaled * products[:span]
                last = cum_col[span - 1 : span]
                rise = jnp.exp(cum_col)
                narrow = slice(head * key_dim, (head + 1) * key_dim)
                attend_all[index, head] = attend
                rise_query[here, narrow] = rise * query
                key_tail[here, narrow] = key * (jnp.exp(last - cum_col) * beta_col)
                ends[index, head] = jnp.broadcast_to(jnp.exp(last), (8, 128))
                items.append((index, head, here, lower, jnp.concatenate([value, rise * key], 1)))
        inverses = unit_inverses([item[3] for item in items], rows, cols)
        solved = [mm(inverse, item[4]) for inverse, item in zip(inverses, items)]
        for (index, head, here, _, _), inverse, solution_ in zip(items, inverses, solved):
            inverse_ref[index, head] = inverse
            update_ref[here, head * value_dim : (head + 1) * value_dim] = solution_[:, :value_dim]
            solved_key[here, head * key_dim : (head + 1) * key_dim] = solution_[:, value_dim:]

    def chain(index):
        here = aligned(index * span, span)
        gate = gate_ref[here, :]
        gated = gate * sigmoid(gate) * gain_ref[...]
        for head in range(heads):
            narrow = slice(head * key_dim, (head + 1) * key_dim)
            wide = slice(head * value_dim, (head + 1) * value_dim)
            state = now[head]
            state_ref[state_place(index, head, heads, key_dim, value_dim, width)] = state
            both = mm(jnp.concatenate([solved_key[here, narrow], rise_query[here, narrow]], 0), state)
            update = update_ref[here, wide] - both[:span]
            now[head] = ends[index, head][0:1, 0:1] * state + mm_tn(key_tail[here, narrow], update)
            core = both[span:] + mm(attend_all[index, head], update)
            update_ref[here, wide] = update
            core_ref[here, wide] = core
            normed = core * lax.rsqrt(jnp.mean(core * core, -1, keepdims=True) + EPS)
            mixed_ref[here, wide] = (normed * gated[:, wide]).astype(mixed_ref.dtype)

    def chain_pair(turn):
        for k in range(PAIR):
            chain(turn * PAIR + k)

    def send_pair(turn):
        here = aligned(turn * PAIR * span, PAIR * span)
        part[here] = dot_plain(mixed_ref[here], w_out_ref[...])
        for k in range(PAIR):
            total.first(turn * PAIR + k).start()

    def cross_pair(turn):
        for k in range(PAIR):
            total.cross(turn * PAIR + k)

    def share_pair(turn):
        for k in range(PAIR):
            total.share(turn * PAIR + k, resid_ref)

    pairs = chunks // PAIR
    prepare_pair(0)

    def step(turn, carry):
        chain_pair(turn - 1)
        prepare_pair(turn)
        send_pair(turn - 1)

        cross_pair(turn - 1)

        @pl.when(turn > 1)
        def _():
            share_pair(turn - 2)

        return carry

    lax.fori_loop(1, pairs, step, 0)
    chain_pair(pairs - 1)
    send_pair(pairs - 1)
    cross_pair(pairs - 1)
    share_pair(pairs - 2)

    def gather(k, carry):
        swap.gather(k)
        return carry

    lax.fori_loop(0, n, gather, 0)

    swap.sent()
    swap.finish()

    def turn_low(i, carry):
        here = aligned(i * 64, 64)
        upstream_ref[here] = arrived[here].astype(upstream_ref.dtype)
        return carry

    lax.fori_loop(0, length // 64, turn_low, 0)
    for load in loads:
        load.wait()
    units = w_gate.shape[0]
    whole = units // 128 * 128
    low = units_ref.dtype
    units_ref[:, :, whole:] = jnp.zeros((3, length, units_ref.shape[2] - whole), low)
    some = length // 2

    def feed(first):
        def norm(i, carry):
            here = aligned(first + i * 64, 64)
            value = resid1_ref[here]
            scale = lax.rsqrt(jnp.mean(value * value, -1, keepdims=True) + EPS)
            hidden_ref[here] = (value * scale * norm2_ref[...]).astype(low)
            return carry

        lax.fori_loop(0, some // 64, norm, 0)
        block = pl.ds(first, some)
        gate_pre[...] = dot_nt(hidden_ref[block], w_gate[...])
        up_pre[...] = dot_nt(hidden_ref[block], w_up[...])
        inner_grad[...] = dot_nt(upstream_ref[block], w_down[...])

        def bend(i, carry):
            at = aligned(i * 64, 64)
            here = aligned(first + i * 64, 64)
            gate = gate_pre[at]
            upper = up_pre[at]
            grad = inner_grad[at]
            sig = sigmoid(gate)
            silu = gate * sig
            units_ref[0, here, 0:units] = (silu * upper).astype(low)
            units_ref[1, here, 0:units] = (grad * upper * (sig * (1.0 + gate * (1.0 - sig)))).astype(low)
            units_ref[2, here, 0:units] = (grad * silu).astype(low)
            return carry

        lax.fori_loop(0, some // 64, bend, 0)
        part2_ref[block] = dot_plain(units_ref[1, block, 0:units], w_gate[...]) + dot_plain(
            units_ref[2, block, 0:units], w_up[...]
        )
        ffn_ref[block] = dot_plain(units_ref[0, block, 0:units], w_down[...])

    early()
    for block in range(BLOCKS // 2):
        total.third(block).wait_recv()
    feed(0)
    halfway()
    share_pair(pairs - 1)
    total.finish(BLOCKS // 2)
    feed(some)


def front_kernel(
    heads, key_dim, value_dim,
    x_ref, norm1_ref, beta_ref, decay_ref, rate_ref, taps_q, taps_k, taps_v, gain_ref, cotangent_ref, norm2_ref,
    query_hbm, key_hbm, value_hbm, gate_hbm, w_out_hbm, w_gate_hbm, w_up_hbm, w_down_hbm,
    low_out, hidden1_out, pre_out, gate_out, small_out, w_small_out,
    mixed_out, core_out, update_out, state_out, inverse_out, upstream_out, resid1_out,
    hidden2_out, units_out, part2_out, ffn_out, taps_ref, rate_row_ref,
    low, hidden1, pre, gate_pre, small, w_small, mixed, core, update, state, inverse, upstream, resid1,
    hidden2, units, part2, ffn, w_out,
    w_mix, w_gate_mix, rows16, staged, arrived, send, recv, close_send, close_recv, load_sem,
    pad, now, solved_key, rise_query, key_tail, attend_all, ends,
    part, land_mate, land_across, half, sum_send, sum_recv,
    staged2, arrived2, send2, recv2, close_send2, close_recv2,
    w_gate, w_up, w_down, gate_in, up_in, inner_grad, load_sem2, out_sem,
):
    load_w_out = pltpu.make_async_copy(w_out_hbm, w_out, out_sem.at[0])
    load_w_out.start()
    cotangents = PlaneSwap(staged2, arrived2, send2, recv2, close_send2, close_recv2)

    def between():
        for place in range(cotangents.n):
            mine = cotangents.at(place, cotangents.core)
            staged2[mine] = cotangent_ref[mine].astype(jnp.float32)
        cotangents.start()

    prep_part(
        heads, between, x_ref, norm1_ref, query_hbm, key_hbm, value_hbm, gate_hbm, beta_ref, decay_ref, rate_ref,
        taps_q, taps_k, taps_v, low, hidden1, pre, gate_pre, small, w_small, taps_ref, rate_row_ref,
        w_mix, w_gate_mix, rows16, staged, arrived, send, recv, close_send, close_recv, load_sem,
    )
    pairs = [
        (low, low_out), (hidden1, hidden1_out), (pre, pre_out), (gate_pre, gate_out), (small, small_out),
        (w_small, w_small_out),
    ]
    later = [
        (mixed, mixed_out), (core, core_out), (update, update_out), (state, state_out), (inverse, inverse_out),
        (upstream, upstream_out),
    ]
    rows = hidden2.shape[0]
    halves = [pl.ds(0, rows // 2), pl.ds(rows // 2, rows // 2)]
    last = [
        [
            (hidden2.at[span], hidden2_out.at[span]), (part2.at[span], part2_out.at[span]), (ffn.at[span], ffn_out.at[span]),
            (resid1.at[span], resid1_out.at[span]),
        ]
        + [(units.at[k, span], units_out.at[k, span]) for k in range(3)]
        for span in halves
    ]
    every = pairs + later + last[0] + last[1]
    copies = [pltpu.make_async_copy(src, dst, out_sem.at[1 + i]) for i, (src, dst) in enumerate(every)]
    one, two, three = len(pairs), len(pairs) + len(later), len(pairs) + len(later) + len(last[0])

    def begin_copies(start, stop):
        for copy in copies[start:stop]:
            copy.start()

    begin_copies(0, one)
    load_w_out.wait()
    head_body(
        heads, key_dim, value_dim, cotangents, lambda: begin_copies(one, two), lambda: begin_copies(two, three),
        pre, gate_pre, small, taps_ref, rate_row_ref, gain_ref, w_out, low, norm2_ref, w_gate_hbm, w_up_hbm, w_down_hbm,
        mixed, core, update, state, inverse, resid1, upstream, hidden2, units, part2, ffn,
        pad, now, solved_key, rise_query, key_tail, attend_all, ends,
        part, land_mate, land_across, half, sum_send, sum_recv,
        arrived2, w_gate, w_up, w_down, gate_in, up_in, inner_grad, load_sem2,
    )
    begin_copies(three, len(copies))
    for copy in copies:
        copy.wait()


def front(
    x, cotangent, norm1, norm2, w_query, w_key, w_value, w_gate, w_beta_t, w_decay_t, rate, taps_q, taps_k, taps_v, gain,
    w_out, w_gate_t, w_up_t, w_down, heads, key_dim, value_dim, places, collective_id,
):
    length, width = x.shape
    values = heads * value_dim
    qk = heads * key_dim
    lanes = 128
    chunks = length // SPAN
    units = w_down.shape[0]
    padded = -(-units // 128) * 128
    f32, bf = jnp.float32, jnp.bfloat16
    dma = pltpu.SemaphoreType.DMA
    any_ = pl.BlockSpec(memory_space=pl.ANY)
    shapes = [
        ((length, width), bf),
        ((length, width), bf),
        ((length, width), f32),
        ((length, values), f32),
        ((length, lanes), f32),
        ((lanes, width), bf),
        ((length, values), bf),
        ((length, values), f32),
        ((length, values), f32),
        ((chunks * heads * key_dim * value_dim // width, width), f32),
        ((chunks, heads, SPAN, SPAN), f32),
        ((length, width), bf),
        ((length, width), f32),
        ((length, width), bf),
        ((3, length, padded), bf),
        ((length, width), f32),
        ((length, width), f32),
    ]
    smalls = [((taps_q.shape[0], width), f32), ((1, lanes), f32)]
    vmem = [
        (w_out.shape, bf),
        ((width, width), bf),
        ((width, values), bf),
        ((16, width), f32),
        ((length, width), f32),
        ((length, width), f32),
    ]
    swap_sems = [dma((places,)), dma((places,)), dma((3, places)), dma((3, places))]
    more = [
        ((HALO + SPAN, width), f32),
        ((heads, key_dim, value_dim), f32),
        ((length, qk), f32),
        ((length, qk), f32),
        ((length, qk), f32),
        ((chunks, heads, SPAN, SPAN), f32),
        ((chunks, heads, 8, 128), f32),
        ((length, width), f32),
        ((length // 2, width), f32),
        ((length // 2, width), f32),
        ((length // 2, width), f32),
    ]
    last = [((units, width), bf)] * 3 + [((length // 2, units), f32)] * 3

    def scratch(items):
        return [pltpu.VMEM(shape, kind) for shape, kind in items]

    return pl.pallas_call(
        functools.partial(front_kernel, heads, key_dim, value_dim),
        out_shape=[jax.ShapeDtypeStruct(shape, kind) for shape, kind in shapes + smalls],
        in_specs=[VM] * 11 + [any_] * 8,
        out_specs=[any_] * len(shapes) + [VM] * len(smalls),
        scratch_shapes=scratch(shapes) + scratch(vmem) + swap_sems + [dma((4,))] + scratch(more)
        + [dma((3, BLOCKS)), dma((3, BLOCKS))] + scratch([((length, width), f32)] * 2) + swap_sems + scratch(last)
        + [dma((3,)), dma((32,))],
        compiler_params=pltpu.CompilerParams(
            collective_id=collective_id, has_side_effects=True, vmem_limit_bytes=67043328
        ),
        name="front",
    )(
        x, norm1, w_beta_t, w_decay_t, rate, taps_q, taps_k, taps_v, gain, cotangent, norm2,
        w_query, w_key, w_value, w_gate, w_out, w_gate_t, w_up_t, w_down,
    )


def prep_part(
    heads, between,
    x_ref, norm1_ref, query_hbm, key_hbm, value_hbm, gate_hbm, beta_ref, decay_ref, rate_ref, taps_q, taps_k, taps_v,
    low_ref, hidden_ref, pre_ref, gate_pre_ref, small_ref, w_small_ref, taps_ref, rate_row_ref,
    w_mix, w_gate, rows16, staged, arrived, send, recv, close_send, close_recv, load_sem,
):
    length, width = x_ref.shape
    qk = query_hbm.shape[1]
    values = value_hbm.shape[1]
    n, _, me, t, _, _ = grid_place()
    _, mate, across = tensor_peers()
    peers = [(lax.rem(me + k, n), t) for k in range(1, n)] + [mate, across]
    call_out(peers)
    loads = [
        (query_hbm, w_mix.at[:, pl.ds(0, qk)]),
        (key_hbm, w_mix.at[:, pl.ds(qk, qk)]),
        (value_hbm, w_mix.at[:, pl.ds(2 * qk, values)]),
        (gate_hbm, w_gate),
    ]
    loads = [pltpu.make_async_copy(src, dst, load_sem.at[i]) for i, (src, dst) in enumerate(loads)]
    for load in loads:
        load.start()
    swap = Swap(staged, arrived, send, recv, close_send, close_recv)
    for place in range(n):
        mine = swap.at(place, t)
        staged[mine] = x_ref[mine].astype(jnp.float32)
    hear_all(peers)
    swap.start()
    taps_ref[:, 0:qk] = taps_q[...]
    taps_ref[:, qk : 2 * qk] = taps_k[...]
    taps_ref[:, 2 * qk :] = taps_v[...]
    lanes = rate_row_ref.shape[1]
    lane = lax.broadcasted_iota(jnp.int32, (1, lanes), 1)
    row = jnp.zeros((1, lanes), jnp.float32)
    for head in range(heads):
        row = jnp.where(lane == heads + head, rate_ref[:, head : head + 1], row)
    rate_row_ref[...] = row
    rows16[...] = jnp.zeros_like(rows16)
    rows16[0:heads] = beta_ref[...].astype(jnp.float32)
    rows16[heads : 2 * heads] = decay_ref[...].astype(jnp.float32)
    w_small_ref[...] = jnp.zeros_like(w_small_ref)
    w_small_ref[0:16] = rows16[...].astype(w_small_ref.dtype)

    def gather(k, carry):
        swap.gather(k)
        return carry

    def forward(k, carry):
        swap.forward(k)
        return carry

    lax.fori_loop(0, n, gather, 0)
    lax.fori_loop(0, n, forward, 0)
    between()
    for load in loads:
        load.wait()
    swap.sent()
    swap.finish()

    def norm(i, carry):
        here = aligned(i * 64, 64)
        value = arrived[here]
        low_ref[here] = value.astype(low_ref.dtype)
        scale = lax.rsqrt(jnp.mean(value * value, -1, keepdims=True) + EPS)
        hidden_ref[here] = (value * scale * norm1_ref[...]).astype(hidden_ref.dtype)
        return carry

    lax.fori_loop(0, length // 64, norm, 0)

    def mix_tile(i, carry):
        tile = aligned(i * 256, 256)
        pre_ref[:, tile] = dot_plain(hidden_ref[...], w_mix[:, tile])
        return carry

    def gate_tile(i, carry):
        tile = aligned(i * 256, 256)
        gate_pre_ref[:, tile] = dot_plain(hidden_ref[...], w_gate[:, tile])
        return carry

    lax.fori_loop(0, width // 256, mix_tile, 0)
    lax.fori_loop(0, values // 256, gate_tile, 0)
    small_ref[...] = dot_nt(hidden_ref[...], w_small_ref[...])


def whole_sequences(
    inputs,
    norm1_gain,
    w_query,
    w_key,
    w_value,
    w_gate,
    w_beta,
    w_decay,
    decay_rate,
    conv_query,
    conv_key,
    conv_value,
    head_gain,
    w_out,
    norm2_gain,
    w_ffn_gate,
    w_ffn_up,
    w_ffn_down,
    cotangent,
):
    batch, seg, width = inputs.shape
    count = batch * seg
    heads = decay_rate.shape[0]
    key_dim = w_query.shape[1] // heads
    value_dim = w_value.shape[1] // heads
    qk_width = heads * key_dim
    places = lax.axis_size("dp")
    gain = head_gain[None]
    (
        resid, hidden1, pre, gate_pre, small, w_small, mixed, core, update, states, inverses, upstream, resid1,
        hidden2, units, part2, ffn, taps, rate,
    ) = front(
        inputs.reshape(count, width), cotangent.reshape(count, width), norm1_gain[None], norm2_gain[None],
        w_query, w_key, w_value, w_gate, w_beta.T, w_decay.T, decay_rate[None], conv_query, conv_key, conv_value, gain,
        w_out, w_ffn_gate.T, w_ffn_up.T, w_ffn_down, heads, key_dim, value_dim, places, 2,
    )
    held, ranges = tail(
        part2, ffn, pre, core, update, states, resid1, upstream, resid, mixed, hidden1, hidden2, units,
        w_out, w_query, w_key, w_value, w_gate, w_small, gate_pre, small, inverses,
        norm1_gain[None], norm2_gain[None], taps, rate, gain,
        heads, key_dim, value_dim, w_ffn_down.shape[0], places, 7,
    )
    (
        output, grad_inputs, fgate, fup, grad_down, grad_out_w, grad_gate_w, grad_query_w, grad_key_w, grad_value_w,
        grad_norm1_gain, grad_norm2_gain, grad_head, grad_rate, grad_beta_w, grad_decay_w,
        grad_convq, grad_convk, grad_convv,
    ) = finish(*held, ranges, w_ffn_down.shape[0], heads, qk_width, heads * value_dim)
    return (
        output.reshape(batch, seg, width),
        grad_inputs.reshape(batch, seg, width),
        grad_norm1_gain[0],
        grad_query_w,
        grad_key_w,
        grad_value_w,
        grad_gate_w,
        grad_beta_w.T,
        grad_decay_w.T,
        grad_rate[0],
        grad_convq,
        grad_convk,
        grad_convv,
        grad_head[0],
        grad_out_w,
        grad_norm2_gain[0],
        fgate.T,
        fup.T,
        grad_down,
    )


def fits_whole(mesh, args):
    batch, length, width = args[0].shape
    places, ranks = mesh.shape["dp"], mesh.shape["tensor"]
    heads = args[8].shape[0] // ranks
    qk = args[2].shape[1] // ranks
    values = args[4].shape[1] // ranks
    units = args[15].shape[1] // ranks
    return (
        batch == places and places == 8 and ranks == 4 and length == places * SPAN and BLOCKS == places and heads <= 4
        and width == 2 * qk + values and width == 2 * values and width % 512 == 0 and length % 256 == 0
        and units % 64 == 0 and values % 256 == 0
        and length // SPAN * args[2].shape[1] // ranks * (values // heads) <= values * width
    )


def solution(mesh):
    placed = (
        P(None, "dp", None),
        P(),
        P(None, "tensor"),
        P(None, "tensor"),
        P(None, "tensor"),
        P(None, "tensor"),
        P(None, "tensor"),
        P(None, "tensor"),
        P("tensor"),
        P(None, "tensor"),
        P(None, "tensor"),
        P(None, "tensor"),
        P("tensor"),
        P("tensor", None),
        P(),
        P(None, "tensor"),
        P(None, "tensor"),
        P("tensor", None),
        P(None, "dp", None),
    )
    def step(*args):
        body = whole_sequences if fits_whole(mesh, args) else shards
        return placed_step(body)(*args)

    def placed_step(body):
      return jax.shard_map(
        body,
        mesh=mesh,
        in_specs=placed,
        out_specs=(
            P(None, "dp", None),
            P(None, "dp", None),
            P(),
            P(None, "tensor"),
            P(None, "tensor"),
            P(None, "tensor"),
            P(None, "tensor"),
            P(None, "tensor"),
            P(None, "tensor"),
            P("tensor"),
            P(None, "tensor"),
            P(None, "tensor"),
            P(None, "tensor"),
            P("tensor"),
            P("tensor", None),
            P(),
            P(None, "tensor"),
            P(None, "tensor"),
            P("tensor", None),
        ),
        check_vma=False,
    )

    return step
```
